32 devices in a mesh: seq: 4 (over y, x), wshard: 8 (over z, core).
Axes of the slice: x: 2, y: 2, z: 4, core: 2. Of those that a mesh axis runs over, the one named last changes fastest.
Arguments:
- layer_input: bfloat16 [8, 1024, 1536], P('wshard', 'seq'), may hold values from -6 to 6
- lengths: int32 [8], P('wshard'), may hold values from 256 to 1024, as said below
- norm_attn: float32 [1536], replicated, may hold values from 0.1 to 1.9
- w_query: bfloat16 [1536, 1536], P('wshard'), may hold values from -0.15625 to 0.15625
- w_key: bfloat16 [1536, 1536], P('wshard'), may hold values from -0.15625 to 0.15625
- w_value: bfloat16 [1536, 1536], P('wshard'), may hold values from -0.15625 to 0.15625
- w_ogate: bfloat16 [1536, 1536], P('wshard'), may hold values from -0.15625 to 0.15625
- w_forget: bfloat16 [1536, 24], P('wshard'), may hold values from -0.15625 to 0.15625
- forget_bias: float32 [24], replicated, may hold values from 3.5 to 8
- w_out: bfloat16 [1536, 1536], P('wshard'), may hold values from -1 to 1
- norm_ffn: float32 [1536], replicated, may hold values from 0.1 to 1.9
- w_gate: bfloat16 [1536, 4096], P('wshard'), may hold values from -0.15625 to 0.15625
- w_up: bfloat16 [1536, 4096], P('wshard'), may hold values from -0.15625 to 0.15625
- w_down: bfloat16 [4096, 1536], P('wshard'), may hold values from -0.09375 to 0.09375
- output_grad: bfloat16 [8, 1024, 1536], P('wshard', 'seq'), may hold values from -6 to 6
Outputs:
- layer_output: bfloat16 [8, 1024, 1536], P('wshard', 'seq')
- grad_input: float32 [8, 1024, 1536], P('wshard', 'seq')
- grad_norm_attn: float32 [1536], replicated
- grad_w_query: float32 [1536, 1536], P('wshard')
- grad_w_key: float32 [1536, 1536], P('wshard')
- grad_w_value: float32 [1536, 1536], P('wshard')
- grad_w_ogate: float32 [1536, 1536], P('wshard')
- grad_w_forget: float32 [1536, 24], P('wshard')
- grad_forget_bias: float32 [24], replicated
- grad_w_out: float32 [1536, 1536], P('wshard')
- grad_norm_ffn: float32 [1536], replicated
- grad_w_gate: float32 [1536, 4096], P('wshard')
- grad_w_up: float32 [1536, 4096], P('wshard')
- grad_w_down: float32 [4096, 1536], P('wshard')
The draws below stay inside these ranges and needn't reach their ends.
Inputs may be any that keep to these rules, and one draw needn't show every extreme that they name: Each sequence has 1024 slots of which the first lengths[s] are valid; in every draw one sequence is full and one has exactly 256 valid slots.
All inputs are finite; a program needn't handle non-finite values.
Results may differ from the reference program's by a relative error of at most 0.014.
Values may be sent and summed in bfloat16 or wider, within the bound.
A program may use at most 320 MiB of HBM per device.

```python
import jax
import jax.numpy as jnp
from jax import lax

D = 1536
H = 24
FF = 4096
SEQS = 8
SLOTS = 1024


def draw_lengths(key, part):
    lowest = SLOTS // 4
    drawn = jax.random.randint(jax.random.fold_in(key, 11), (SEQS,), lowest, SLOTS + 1, dtype=jnp.int32)
    order = jax.random.permutation(jax.random.fold_in(key, 12), SEQS)
    drawn = drawn.at[order[0]].set(SLOTS)
    drawn = drawn.at[order[1]].set(lowest)
    return drawn.astype(jnp.int32)


def levels(rng, shape, shards, low, high):
    def one(dim, parts):
        steps = jax.random.uniform(jax.random.fold_in(jax.random.fold_in(rng, 6), dim), (parts,), jnp.float32, low / len(shards), high / len(shards))
        return jnp.repeat(jnp.exp(steps), shape[dim] // parts).reshape((-1,) + (1,) * (len(shape) - dim - 1))

    loudness = one(*shards[0])
    for cut in shards[1:]:
        loudness = loudness * one(*cut)
    return loudness


def centred(own_key, extent, scale, most, cuts=(), kind=jnp.bfloat16):
    array = scale * jax.random.normal(own_key, extent, jnp.float32)
    if cuts:
        array = array * levels(own_key, extent, cuts, -0.22, 0.18)
    return jnp.clip(array, -most, most).astype(kind)


def setup_inputs(seed: int = 0) -> dict:
    key_list = jax.random.split(jax.random.key(seed), 16)
    layer_input = centred(key_list[0], (SEQS, SLOTS, D), 1.0, 6.0, ((0, 8), (1, 4)))
    lengths = draw_lengths(jax.random.fold_in(key_list[15], 71), 0)
    norm_attn = jnp.clip(1.0 + 0.18 * jax.random.normal(key_list[2], (D,), jnp.float32), 0.1, 1.9)
    w_query = centred(key_list[3], (D, D), D ** -0.5, 0.15625, ((0, 8),))
    w_key = centred(key_list[4], (D, D), D ** -0.5, 0.15625, ((0, 8),))
    w_value = centred(key_list[5], (D, D), D ** -0.5, 0.15625, ((0, 8),))
    w_ogate = centred(key_list[6], (D, D), D ** -0.5, 0.15625, ((0, 8),))
    w_forget = centred(key_list[7], (D, H), D ** -0.5, 0.15625, ((0, 8),))
    forget_bias = jnp.clip(jax.random.uniform(key_list[8], (H,), jnp.float32, 3.5, 8.0), 3.5, 8.0)
    w_out = centred(key_list[9], (D, D), 32 ** -0.5, 1.0, ((0, 8),))
    norm_ffn = jnp.clip(1.0 + 0.18 * jax.random.normal(key_list[10], (D,), jnp.float32), 0.1, 1.9)
    w_gate = centred(key_list[11], (D, FF), D ** -0.5, 0.15625, ((0, 8),))
    w_up = centred(key_list[12], (D, FF), D ** -0.5, 0.15625, ((0, 8),))
    w_down = centred(key_list[13], (FF, D), FF ** -0.5, 0.09375, ((0, 8),))
    output_grad = centred(key_list[14], (SEQS, SLOTS, D), 1.0, 6.0, ((0, 8), (1, 4)))
    return dict(layer_input=layer_input, lengths=lengths, norm_attn=norm_attn, w_query=w_query, w_key=w_key, w_value=w_value, w_ogate=w_ogate, w_forget=w_forget, forget_bias=forget_bias, w_out=w_out, norm_ffn=norm_ffn, w_gate=w_gate, w_up=w_up, w_down=w_down, output_grad=output_grad)


@jax.custom_vjp
def low(v):
    return lax.optimization_barrier(v.astype(jnp.bfloat16)).astype(jnp.float32)

@jax.custom_vjp
def low_back(v):
    return v

def low_keep(v):
    return (low(v), None)

def low_pass(kept, grad):
    return (grad,)

def back_keep(v):
    return (v, None)

def back_low(kept, grad):
    return (low(grad),)
low.defvjp(low_keep, low_pass)
low_back.defvjp(back_keep, back_low)
EPS = 1e-06
NEG_FILL = -1e+30

def highest(left, right):
    return jnp.dot(left, right, precision=lax.Precision.HIGHEST)

def rms_norm(values, gain):
    return values * lax.rsqrt(lax.optimization_barrier(jnp.mean(values * values, axis=-1, keepdims=True)) + EPS) * gain

def attend(queries, keys_all, values_all, cumulative, length):
    slots, heads, head_size = queries.shape
    block = min(512, slots)
    scale = head_size ** (-0.5)
    columns = jnp.arange(slots, dtype=jnp.int32)

    def one_block(first):
        query_block = lax.dynamic_slice_in_dim(queries, first, block, 0)
        cum_rows = lax.dynamic_slice_in_dim(cumulative, first, block, 0)
        plain = jnp.einsum('qhd,khd->hqk', query_block, keys_all, precision=lax.Precision.HIGHEST) * scale
        plain = low_back(plain)
        plain = plain + cum_rows.T[:, :, None] - cumulative.T[:, None, :]
        rows = first + jnp.arange(block, dtype=jnp.int32)
        allowed = (columns[None, :] <= rows[:, None]) & (columns[None, :] < length)
        masked = jnp.where(allowed[None], plain, NEG_FILL)
        log_total = jax.nn.logsumexp(masked, axis=-1, keepdims=True)
        weights = low(jnp.exp(masked - log_total))
        return jnp.einsum('hqk,khd->qhd', weights, values_all, precision=lax.Precision.HIGHEST)
    firsts = jnp.arange(slots // block, dtype=jnp.int32) * block
    blocks = lax.map(jax.checkpoint(one_block), firsts)
    return blocks.reshape(slots, heads * head_size)

def forward(inputs, length, norm_attn, w_query, w_key, w_value, w_ogate, w_forget, forget_bias, w_out, norm_ffn, w_gate, w_up, w_down):
    slots = inputs.shape[0]
    heads = forget_bias.shape[0]
    head_size = w_query.shape[1] // heads
    normed_attn = low(rms_norm(inputs, norm_attn))
    queries = low_back(low(highest(normed_attn, w_query)))
    keys_all = low_back(low(highest(normed_attn, w_key)))
    values_all = low_back(low(highest(normed_attn, w_value)))
    gate_pre = low_back(highest(normed_attn, w_ogate))
    forget_pre = low_back(low(highest(normed_attn, w_forget)))
    cumulative = jnp.cumsum(jax.nn.log_sigmoid(forget_pre + forget_bias), axis=0)
    attended = attend(queries.reshape(slots, heads, head_size), keys_all.reshape(slots, heads, head_size), values_all.reshape(slots, heads, head_size), cumulative, length)
    attended = low_back(low(attended))
    gated = low(attended * jax.nn.sigmoid(gate_pre))
    middle = inputs + low_back(highest(gated, w_out))
    normed_ffn = low(rms_norm(middle, norm_ffn))
    gate = low_back(highest(normed_ffn, w_gate))
    upward = low_back(highest(normed_ffn, w_up))
    hidden = low(jax.nn.silu(gate) * upward)
    return middle + low_back(highest(hidden, w_down))

def reference(layer_input, lengths, norm_attn, w_query, w_key, w_value, w_ogate, w_forget, forget_bias, w_out, norm_ffn, w_gate, w_up, w_down, output_grad):
    params = tuple((p.astype(jnp.float32) for p in (norm_attn, w_query, w_key, w_value, w_ogate, w_forget, forget_bias, w_out, norm_ffn, w_gate, w_up, w_down)))

    def per_sequence(totals, item):
        inputs, length, cotangent = item
        valid_slots = (jnp.arange(inputs.shape[0], dtype=jnp.int32) < length).astype(jnp.float32)

        def run(values, *weights):
            return forward(values, length, *weights)
        result, pull = jax.vjp(run, inputs.astype(jnp.float32), *params)
        grads = pull(cotangent.astype(jnp.float32) * valid_slots[:, None])
        totals = tuple((total + grad for total, grad in zip(totals, grads[1:])))
        return (totals, (result.astype(jnp.bfloat16), grads[0]))
    start = tuple((jnp.zeros_like(p) for p in params))
    totals, (outputs, grad_inputs) = lax.scan(per_sequence, start, (layer_input, lengths, output_grad))
    return (outputs, grad_inputs, totals[0], totals[1], totals[2], totals[3], totals[4], totals[5], totals[6], totals[7], totals[8], totals[9], totals[10], totals[11])
```

```python
import jax
import jax.numpy as jnp
from jax import lax
from jax.experimental import pallas as pl
from jax.experimental.pallas import tpu as pltpu
from jax.sharding import PartitionSpec as P

EPS = 1e-06
NEG_FILL = -1e30
PAIR = 128


def product(left, right):
    return jnp.dot(left, right, preferred_element_type=jnp.float32)


def product_tn(left, right):
    return lax.dot_general(
        left, right, (((0,), (0,)), ((), ())), preferred_element_type=jnp.float32
    )


def product_nt(left, right):
    return lax.dot_general(
        left, right, (((1,), (1,)), ((), ())), preferred_element_type=jnp.float32
    )


def rms_norm(values, gain):
    return values * lax.rsqrt(jnp.mean(values * values, axis=-1, keepdims=True) + EPS) * gain


def gate_product(attended, gate_pre):
    return attended * jax.nn.sigmoid(gate_pre)


def swiglu(gate, upward):
    return jax.nn.silu(gate) * upward


def attention_fwd(q, k, v, cum_row, key_col, heads_half):
    slots, width = q.shape
    pairs = width // PAIR
    tile = min(256, slots)
    half = heads_half

    def body(q_ref, k_ref, v_ref, row_ref, col_ref, o_ref, lse_ref):
        key_all = k_ref[...]
        value_t = v_ref[...].T
        query_t = q_ref[...].T
        sub = lax.broadcasted_iota(jnp.int32, (PAIR, tile), 0)
        diag = lax.broadcasted_iota(jnp.int32, (tile, tile), 0) <= lax.broadcasted_iota(
            jnp.int32, (tile, tile), 1
        )
        for number in range(slots // tile):
            first, last = number * tile, (number + 1) * tile
            outs = []
            for a in range(2):
                mine = (sub >= a * half) & (sub < (a + 1) * half)
                query = jnp.where(mine, query_t[:, first:last], jnp.zeros((), query_t.dtype))
                scores = product(key_all[:last], query)
                scores = scores + (row_ref[0, a : a + 1, first:last] - col_ref[0, :last, a : a + 1])
                tail = jnp.where(diag, scores[first:], NEG_FILL)
                scores = tail if number == 0 else jnp.concatenate([scores[:first], tail], axis=0)
                top = jnp.max(scores, axis=0, keepdims=True)
                weights = jnp.exp(scores - top)
                total = jnp.sum(weights, axis=0, keepdims=True)
                mixed = product(value_t[a * half : (a + 1) * half, :last], weights.astype(jnp.bfloat16))
                outs.append(mixed / total)
                lse_ref[0, a : a + 1, first:last] = top + jnp.log(total)
            o_ref[first:last, :] = jnp.concatenate(outs, axis=0).T.astype(o_ref.dtype)

    lane = pl.BlockSpec((slots, PAIR), lambda p: (0, p))
    row = pl.BlockSpec((1, 2, slots), lambda p: (p, 0, 0))
    col = pl.BlockSpec((1, slots, 2), lambda p: (p, 0, 0))
    return pl.pallas_call(
        body,
        grid=(pairs,),
        in_specs=[lane, lane, lane, row, col],
        out_specs=[lane, row],
        out_shape=[
            jax.ShapeDtypeStruct((slots, width), jnp.bfloat16),
            jax.ShapeDtypeStruct((pairs, 2, slots), jnp.float32),
        ],
        compiler_params=pltpu.CompilerParams(vmem_limit_bytes=56 << 20),
        cost_estimate=pl.CostEstimate(
            flops=4 * slots * slots * width, bytes_accessed=8 * slots * width, transcendentals=0
        ),
        name="attention_fwd",
    )(q, k, v, cum_row, key_col)


def attention_bwd(q, k, v, d_out, cum_row, key_col, lse, heads_half, scale):
    slots, width = q.shape
    pairs = width // PAIR
    tile = min(256, slots)
    half = heads_half

    def body(q_ref, k_ref, v_ref, do_ref, row_ref, col_ref, lse_ref,
             dq_ref, dk_ref, dv_ref, drow_ref, dcol_ref, dk_acc, dv_acc, dcol_acc):
        key_all = k_ref[...]
        value_all = v_ref[...]
        query_t = q_ref[...].T
        key_t = k_ref[...].T
        dout_t = do_ref[...].T
        sub = lax.broadcasted_iota(jnp.int32, (PAIR, tile), 0)
        lanes = lax.broadcasted_iota(jnp.int32, (tile, PAIR), 1)
        diag = lax.broadcasted_iota(jnp.int32, (tile, tile), 0) <= lax.broadcasted_iota(
            jnp.int32, (tile, tile), 1
        )
        zero = jnp.zeros((), jnp.bfloat16)
        dk_acc[...] = jnp.zeros_like(dk_acc)
        dv_acc[...] = jnp.zeros_like(dv_acc)
        dcol_acc[...] = jnp.zeros_like(dcol_acc)
        for number in range(slots // tile):
            first, last = number * tile, (number + 1) * tile
            outs = []
            for a in range(2):
                mine = (sub >= a * half) & (sub < (a + 1) * half)
                own = (lanes >= a * half) & (lanes < (a + 1) * half)
                scores = product(key_all[:last], jnp.where(mine, query_t[:, first:last], zero))
                offset = row_ref[0, a : a + 1, first:last] - lse_ref[0, a : a + 1, first:last]
                scores = scores + (offset - col_ref[0, :last, a : a + 1])
                tail = jnp.where(diag, scores[first:], NEG_FILL)
                scores = tail if number == 0 else jnp.concatenate([scores[:first], tail], axis=0)
                probs = jnp.exp(scores)
                d_probs = product(value_all[:last], jnp.where(mine, dout_t[:, first:last], zero))
                dot = jnp.sum(d_probs * probs, axis=0, keepdims=True)
                d_full = probs * (d_probs - dot)
                d_scores = d_full.astype(jnp.bfloat16)
                drow_ref[0, a : a + 1, first:last] = jnp.sum(d_full, axis=0, keepdims=True)
                dcol_acc[:last, a : a + 1] += jnp.sum(d_full, axis=1, keepdims=True)
                outs.append(product(key_t[a * half : (a + 1) * half, :last], d_scores) * scale)
                dk_acc[:last, :] += product(d_scores, jnp.where(own, q_ref[first:last, :], zero))
                dv_acc[:last, :] += product(
                    probs.astype(jnp.bfloat16), jnp.where(own, do_ref[first:last, :], zero)
                )
            dq_ref[first:last, :] = jnp.concatenate(outs, axis=0).T.astype(dq_ref.dtype)
        dk_ref[...] = dk_acc[...].astype(dk_ref.dtype)
        dv_ref[...] = dv_acc[...].astype(dv_ref.dtype)
        dcol_ref[0] = dcol_acc[...]

    lane = pl.BlockSpec((slots, PAIR), lambda p: (0, p))
    row = pl.BlockSpec((1, 2, slots), lambda p: (p, 0, 0))
    col = pl.BlockSpec((1, slots, 2), lambda p: (p, 0, 0))
    return pl.pallas_call(
        body,
        grid=(pairs,),
        in_specs=[lane, lane, lane, lane, row, col, row],
        out_specs=[lane, lane, lane, row, col],
        out_shape=[jax.ShapeDtypeStruct((slots, width), jnp.bfloat16)] * 3
        + [
            jax.ShapeDtypeStruct((pairs, 2, slots), jnp.float32),
            jax.ShapeDtypeStruct((pairs, slots, 2), jnp.float32),
        ],
        scratch_shapes=[
            pltpu.VMEM((slots, PAIR), jnp.float32),
            pltpu.VMEM((slots, PAIR), jnp.float32),
            pltpu.VMEM((slots, 2), jnp.float32),
        ],
        compiler_params=pltpu.CompilerParams(vmem_limit_bytes=56 << 20),
        cost_estimate=pl.CostEstimate(
            flops=10 * slots * slots * width, bytes_accessed=14 * slots * width, transcendentals=0
        ),
        name="attention_bwd",
    )(q, k, v, d_out, cum_row, key_col, lse)


def gather(value, axis_name):
    return lax.all_gather(value, axis_name, axis=0, tiled=True)


def scatter(value, axis_name):
    return lax.psum_scatter(value, axis_name, scatter_dimension=0, tiled=True)


def on_device(
    layer_input,
    lengths,
    norm_attn,
    w_query,
    w_key,
    w_value,
    w_ogate,
    w_forget,
    forget_bias,
    w_out,
    norm_ffn,
    w_gate,
    w_up,
    w_down,
    output_grad,
):
    low = jnp.bfloat16
    tokens, width = layer_input.shape[1:]
    heads = forget_bias.shape[0]
    groups = lax.axis_size("seq")
    shards = lax.axis_size("wshard")
    local_heads = heads // groups
    head_size = width // heads
    columns = width // groups
    slots = tokens * groups
    hidden_size = w_gate.shape[1]
    part = hidden_size // (groups * shards)
    scale = head_size ** (-0.5)
    length = lengths[0]
    seq_rank = lax.axis_index("seq")
    shard_rank = lax.axis_index("wshard")
    per_block = shards // groups
    positions = seq_rank * tokens + jnp.arange(tokens, dtype=jnp.int32)
    valid_slots = (positions < length)[:, None]
    inputs = layer_input[0].astype(jnp.float32)
    cotangent_low = jnp.where(valid_slots, output_grad[0], jnp.zeros((), low))
    cotangent = cotangent_low.astype(jnp.float32)
    pad_heads = PAIR

    def own_columns(weight):
        return lax.dynamic_slice_in_dim(weight, seq_rank * columns, columns, 1)

    def own_units(weight):
        split = weight.reshape(weight.shape[0], shards, groups, part)
        mine = lax.dynamic_index_in_dim(split, seq_rank, 2, keepdims=False)
        return mine.reshape(weight.shape[0], shards * part)

    own_forget = lax.dynamic_slice_in_dim(w_forget, seq_rank * local_heads, local_heads, 1)
    own_forget = jnp.pad(own_forget, ((0, 0), (0, pad_heads - local_heads)))
    mine_attn = jnp.concatenate(
        [own_columns(w_query), own_columns(w_key), own_columns(w_value), own_columns(w_ogate), own_forget],
        axis=1,
    )
    mine_ffn = jnp.concatenate([own_units(w_gate), own_units(w_up)], axis=1)
    mine_down = lax.dynamic_slice_in_dim(w_down, seq_rank * part, part, 0)
    full_attn = gather(mine_attn, "wshard")
    full_out = lax.dynamic_slice_in_dim(gather(w_out, "wshard"), seq_rank * columns, columns, 0)
    full_ffn = gather(mine_ffn, "wshard")
    full_down = gather(mine_down, "wshard")

    normed_attn = gather(rms_norm(inputs, norm_attn).astype(low), "seq")
    projected = product(normed_attn, full_attn)
    queries = projected[:, :columns].astype(low)
    keys = projected[:, columns : 2 * columns].astype(low)
    values = projected[:, 2 * columns : 3 * columns].astype(low)
    gate_pre = projected[:, 3 * columns : 4 * columns]
    forget_pre = projected[:, 4 * columns : 4 * columns + local_heads].astype(low)
    bias_local = lax.dynamic_slice_in_dim(forget_bias, seq_rank * local_heads, local_heads)
    forget_total = forget_pre.astype(jnp.float32) + bias_local
    log_forget, pull_forget = jax.vjp(jax.nn.log_sigmoid, forget_total)
    cumulative = jnp.cumsum(log_forget, axis=0)
    even = -local_heads % 2

    def pad_lanes(value):
        return jnp.pad(value, ((0, 0), (0, even * head_size))) if even else value

    pairs = (local_heads + even) // 2
    cum = jnp.pad(cumulative, ((0, 0), (0, even))) if even else cumulative
    usable = (jnp.arange(slots, dtype=jnp.int32) < length)[:, None]
    cum_row = cum.T.reshape(pairs, 2, slots)
    key_col = jnp.where(usable, cum, -NEG_FILL).reshape(slots, pairs, 2).transpose(1, 0, 2)
    q_in = pad_lanes((queries.astype(jnp.float32) * scale).astype(low))
    k_in = pad_lanes(keys)
    v_in = pad_lanes(values)
    attended_low, log_total = attention_fwd(q_in, k_in, v_in, cum_row, key_col, head_size)
    attended = attended_low[:, :columns].astype(jnp.float32)
    gated_full, pull_gate = jax.vjp(gate_product, attended, gate_pre)
    gated = gated_full.astype(low)
    branch = scatter(product(gated, full_out).astype(low), "seq")
    middle = inputs + branch.astype(jnp.float32)
    normed_ffn_own, pull_ffn_norm = jax.vjp(rms_norm, middle, norm_ffn)
    normed_ffn = gather(normed_ffn_own.astype(low), "seq")
    gate_up = product(normed_ffn, full_ffn)
    units = shards * part
    hidden_full, pull_swiglu = jax.vjp(swiglu, gate_up[:, :units], gate_up[:, units:])
    hidden = hidden_full.astype(low)
    lowered = scatter(product(hidden, full_down).astype(low), "seq")
    layer_output = (middle + lowered.astype(jnp.float32)).astype(low)[None]

    cotangent_all = gather(cotangent_low, "seq")
    grad_w_down = product_tn(hidden, cotangent_all).astype(low)
    grad_hidden = product_nt(cotangent_all, full_down)
    grad_gate_full, grad_up_full = pull_swiglu(grad_hidden)
    grad_gate_up = jnp.concatenate([grad_gate_full.astype(low), grad_up_full.astype(low)], axis=1)
    grad_w_ffn = product_tn(normed_ffn, grad_gate_up).astype(low)
    grad_normed_ffn = scatter(product_nt(grad_gate_up, full_ffn).astype(low), "seq")
    share_down = scatter(grad_w_down, "wshard")
    share_ffn = scatter(grad_w_ffn, "wshard")
    grad_middle_part, grad_norm_ffn = pull_ffn_norm(grad_normed_ffn.astype(jnp.float32))
    grad_middle = cotangent + grad_middle_part
    grad_branch = gather(grad_middle.astype(low), "seq")
    grad_w_out = product_tn(gated, grad_branch).astype(low)
    grad_gated = product_nt(grad_branch, full_out)
    grad_attended_full, grad_gate_pre_full = pull_gate(grad_gated)
    grad_attended = pad_lanes(grad_attended_full.astype(low))
    grad_gate_pre = grad_gate_pre_full.astype(low)
    dq, dk, dv, drow, dcol = attention_bwd(
        q_in, k_in, v_in, grad_attended, cum_row, key_col, log_total, head_size, scale
    )
    grad_cum = drow.reshape(2 * pairs, slots).T - dcol.transpose(1, 0, 2).reshape(slots, 2 * pairs)
    grad_cum = grad_cum[:, :local_heads]
    grad_log_forget = jnp.flip(jnp.cumsum(jnp.flip(grad_cum, 0), axis=0), 0)
    grad_forget_total = pull_forget(grad_log_forget)[0]
    grad_bias_local = jnp.sum(grad_forget_total, axis=0)
    grad_forget = jnp.pad(grad_forget_total.astype(low), ((0, 0), (0, pad_heads - local_heads)))
    grad_bias = lax.dynamic_update_slice_in_dim(
        jnp.zeros((heads,), jnp.float32), grad_bias_local, seq_rank * local_heads, 0
    )
    grad_projected = jnp.concatenate(
        [dq[:, :columns], dk[:, :columns], dv[:, :columns], grad_gate_pre, grad_forget], axis=1
    )
    grad_w_attn = product_tn(normed_attn, grad_projected).astype(low)
    share_attn = scatter(grad_w_attn, "wshard")
    grad_normed_attn = scatter(product_nt(grad_projected, full_attn).astype(low), "seq")
    unused_normed, pull_attn_norm = jax.vjp(rms_norm, inputs, norm_attn)
    grad_input_part, grad_norm_attn = pull_attn_norm(grad_normed_attn.astype(jnp.float32))
    grad_input = (grad_middle + grad_input_part)[None]

    share_out = scatter(grad_w_out, "wshard")
    rows_out = columns // shards
    pieces_out = lax.all_gather(share_out, "seq", axis=0, tiled=False)
    lane_of = shard_rank // (shards // per_block)
    slots_out = jnp.where(
        (jnp.arange(per_block) == lane_of)[None, :, None, None], pieces_out[:, None], jnp.zeros((), low)
    ).reshape(shards, rows_out, width)
    moved = lax.all_to_all(slots_out, "wshard", split_axis=0, concat_axis=0, tiled=True)
    moved = moved.reshape(per_block, shards // per_block, rows_out, width)
    mine_out = lax.dynamic_index_in_dim(moved, shard_rank % per_block, 0, keepdims=False)
    grad_out = mine_out.reshape(columns // per_block, width).astype(jnp.float32)

    every_attn = lax.all_gather(share_attn, "seq", axis=0, tiled=False)
    every_ffn = lax.all_gather(share_ffn, "seq", axis=0, tiled=False)
    grad_down = gather(share_down, "seq").astype(jnp.float32)
    rows = share_attn.shape[0]

    def join(first):
        taken = every_attn[:, :, first * columns : (first + 1) * columns]
        return taken.transpose(1, 0, 2).reshape(rows, width).astype(jnp.float32)

    def join_units(first):
        taken = every_ffn[:, :, first * units : (first + 1) * units]
        taken = taken.reshape(groups, rows, shards, part).transpose(1, 2, 0, 3)
        return taken.reshape(rows, hidden_size).astype(jnp.float32)

    grad_forget_w = every_attn[:, :, 4 * columns : 4 * columns + local_heads]
    grad_forget_w = grad_forget_w.transpose(1, 0, 2).reshape(rows, heads).astype(jnp.float32)
    small = lax.psum((grad_norm_attn, grad_norm_ffn, grad_bias), ("seq", "wshard"))
    return (
        layer_output,
        grad_input,
        small[0],
        join(0),
        join(1),
        join(2),
        join(3),
        grad_forget_w,
        small[2],
        grad_out,
        small[1],
        join_units(0),
        join_units(1),
        grad_down,
    )


def solution(mesh):
    return jax.shard_map(
        on_device,
        mesh=mesh,
        in_specs=(
            P("wshard", "seq", None),
            P("wshard"),
            P(),
            P("wshard", None),
            P("wshard", None),
            P("wshard", None),
            P("wshard", None),
            P("wshard", None),
            P(),
            P("wshard", None),
            P(),
            P("wshard", None),
            P("wshard", None),
            P("wshard", None),
            P("wshard", "seq", None),
        ),
        out_specs=(
            P("wshard", "seq", None),
            P("wshard", "seq", None),
            P(),
            P("wshard", None),
            P("wshard", None),
            P("wshard", None),
            P("wshard", None),
            P("wshard", None),
            P(),
            P("wshard", None),
            P(),
            P("wshard", None),
            P("wshard", None),
            P("wshard", None),
        ),
        check_vma=False,
    )
```

```python
import jax
import jax.numpy as jnp
from jax import lax
from jax.experimental import pallas as pl
from jax.experimental.pallas import tpu as pltpu
from jax.sharding import PartitionSpec as P

EPS = 1e-06
NEG_FILL = -1e30
PAIR = 128


def product(left, right):
    return jnp.dot(left, right, preferred_element_type=jnp.float32)


def product_tn(left, right):
    return lax.dot_general(
        left, right, (((0,), (0,)), ((), ())), preferred_element_type=jnp.float32
    )


def product_nt(left, right):
    return lax.dot_general(
        left, right, (((1,), (1,)), ((), ())), preferred_element_type=jnp.float32
    )


def rms_norm(values, gain):
    return values * lax.rsqrt(jnp.mean(values * values, axis=-1, keepdims=True) + EPS) * gain


def gate_product(attended, gate_pre):
    return attended * jax.nn.sigmoid(gate_pre)


def swiglu(gate, upward):
    return jax.nn.silu(gate) * upward


def attention_fwd(q, k, v, cum_row, key_col, heads_half):
    slots, width = q.shape
    pairs = width // PAIR
    tile = min(256, slots)
    half = heads_half

    def body(q_ref, k_ref, v_ref, row_ref, col_ref, o_ref, lse_ref):
        key_all = k_ref[...]
        value_t = v_ref[...].T
        query_t = q_ref[...].T
        sub = lax.broadcasted_iota(jnp.int32, (PAIR, tile), 0)
        diag = lax.broadcasted_iota(jnp.int32, (tile, tile), 0) <= lax.broadcasted_iota(
            jnp.int32, (tile, tile), 1
        )
        for number in range(slots // tile):
            first, last = number * tile, (number + 1) * tile
            outs = []
            for a in range(2):
                mine = (sub >= a * half) & (sub < (a + 1) * half)
                query = jnp.where(mine, query_t[:, first:last], jnp.zeros((), query_t.dtype))
                scores = product(key_all[:last], query)
                scores = scores + (row_ref[0, a : a + 1, first:last] - col_ref[0, :last, a : a + 1])
                tail = jnp.where(diag, scores[first:], NEG_FILL)
                scores = tail if number == 0 else jnp.concatenate([scores[:first], tail], axis=0)
                top = jnp.max(scores, axis=0, keepdims=True)
                weights = jnp.exp(scores - top)
                total = jnp.sum(weights, axis=0, keepdims=True)
                mixed = product(value_t[a * half : (a + 1) * half, :last], weights.astype(jnp.bfloat16))
                outs.append(mixed / total)
                lse_ref[0, a : a + 1, first:last] = top + jnp.log(total)
            o_ref[first:last, :] = jnp.concatenate(outs, axis=0).T.astype(o_ref.dtype)

    lane = pl.BlockSpec((slots, PAIR), lambda p: (0, p))
    row = pl.BlockSpec((1, 2, slots), lambda p: (p, 0, 0))
    col = pl.BlockSpec((1, slots, 2), lambda p: (p, 0, 0))
    return pl.pallas_call(
        body,
        grid=(pairs,),
        in_specs=[lane, lane, lane, row, col],
        out_specs=[lane, row],
        out_shape=[
            jax.ShapeDtypeStruct((slots, width), jnp.bfloat16),
            jax.ShapeDtypeStruct((pairs, 2, slots), jnp.float32),
        ],
        compiler_params=pltpu.CompilerParams(vmem_limit_bytes=56 << 20),
        cost_estimate=pl.CostEstimate(
            flops=4 * slots * slots * width, bytes_accessed=8 * slots * width, transcendentals=0
        ),
        name="attention_fwd",
    )(q, k, v, cum_row, key_col)


def attention_bwd(q, k, v, d_out, cum_row, key_col, lse, heads_half, scale):
    slots, width = q.shape
    pairs = width // PAIR
    tile = min(256, slots)
    half = heads_half

    def body(q_ref, k_ref, v_ref, do_ref, row_ref, col_ref, lse_ref,
             dq_ref, dk_ref, dv_ref, drow_ref, dcol_ref, dk_acc, dv_acc, dcol_acc):
        key_all = k_ref[...]
        value_all = v_ref[...]
        query_t = q_ref[...].T
        key_t = k_ref[...].T
        dout_t = do_ref[...].T
        sub = lax.broadcasted_iota(jnp.int32, (PAIR, tile), 0)
        lanes = lax.broadcasted_iota(jnp.int32, (tile, PAIR), 1)
        diag = lax.broadcasted_iota(jnp.int32, (tile, tile), 0) <= lax.broadcasted_iota(
            jnp.int32, (tile, tile), 1
        )
        zero = jnp.zeros((), jnp.bfloat16)
        dk_acc[...] = jnp.zeros_like(dk_acc)
        dv_acc[...] = jnp.zeros_like(dv_acc)
        dcol_acc[...] = jnp.zeros_like(dcol_acc)
        for number in range(slots // tile):
            first, last = number * tile, (number + 1) * tile
            outs = []
            for a in range(2):
                mine = (sub >= a * half) & (sub < (a + 1) * half)
                own = (lanes >= a * half) & (lanes < (a + 1) * half)
                scores = product(key_all[:last], jnp.where(mine, query_t[:, first:last], zero))
                offset = row_ref[0, a : a + 1, first:last] - lse_ref[0, a : a + 1, first:last]
                scores = scores + (offset - col_ref[0, :last, a : a + 1])
                tail = jnp.where(diag, scores[first:], NEG_FILL)
                scores = tail if number == 0 else jnp.concatenate([scores[:first], tail], axis=0)
                probs = jnp.exp(scores)
                d_probs = product(value_all[:last], jnp.where(mine, dout_t[:, first:last], zero))
                dot = jnp.sum(d_probs * probs, axis=0, keepdims=True)
                d_full = probs * (d_probs - dot)
                d_scores = d_full.astype(jnp.bfloat16)
                drow_ref[0, a : a + 1, first:last] = jnp.sum(d_full, axis=0, keepdims=True)
                dcol_acc[:last, a : a + 1] += jnp.sum(d_full, axis=1, keepdims=True)
                outs.append(product(key_t[a * half : (a + 1) * half, :last], d_scores) * scale)
                dk_acc[:last, :] += product(d_scores, jnp.where(own, q_ref[first:last, :], zero))
                dv_acc[:last, :] += product(
                    probs.astype(jnp.bfloat16), jnp.where(own, do_ref[first:last, :], zero)
                )
            dq_ref[first:last, :] = jnp.concatenate(outs, axis=0).T.astype(dq_ref.dtype)
        dk_ref[...] = dk_acc[...].astype(dk_ref.dtype)
        dv_ref[...] = dv_acc[...].astype(dv_ref.dtype)
        dcol_ref[0] = dcol_acc[...]

    lane = pl.BlockSpec((slots, PAIR), lambda p: (0, p))
    row = pl.BlockSpec((1, 2, slots), lambda p: (p, 0, 0))
    col = pl.BlockSpec((1, slots, 2), lambda p: (p, 0, 0))
    return pl.pallas_call(
        body,
        grid=(pairs,),
        in_specs=[lane, lane, lane, lane, row, col, row],
        out_specs=[lane, lane, lane, row, col],
        out_shape=[jax.ShapeDtypeStruct((slots, width), jnp.bfloat16)] * 3
        + [
            jax.ShapeDtypeStruct((pairs, 2, slots), jnp.float32),
            jax.ShapeDtypeStruct((pairs, slots, 2), jnp.float32),
        ],
        scratch_shapes=[
            pltpu.VMEM((slots, PAIR), jnp.float32),
            pltpu.VMEM((slots, PAIR), jnp.float32),
            pltpu.VMEM((slots, 2), jnp.float32),
        ],
        compiler_params=pltpu.CompilerParams(vmem_limit_bytes=56 << 20),
        cost_estimate=pl.CostEstimate(
            flops=10 * slots * slots * width, bytes_accessed=14 * slots * width, transcendentals=0
        ),
        name="attention_bwd",
    )(q, k, v, d_out, cum_row, key_col, lse)


MESH = pl.DeviceIdType.MESH
VMEM_LIMIT = 62 << 20


def square(groups):
    return groups == 4


def sides():
    rank = lax.axis_index("seq")
    return rank, rank + 1 - 2 * lax.rem(rank, 2), lax.rem(rank + 2, 4), 3 - rank


def meet(*others):
    barrier = pltpu.get_barrier_semaphore()
    for other in others:
        pl.semaphore_signal(barrier, inc=1, device_id=other, device_id_type=MESH)
    pl.semaphore_wait(barrier, len(others))


def push(source, target, send, recv, device):
    copy = pltpu.make_async_remote_copy(
        src_ref=source,
        dst_ref=target,
        send_sem=send,
        recv_sem=recv,
        device_id=device,
        device_id_type=MESH,
    )
    copy.start()
    return copy


class SquareGather:
    def __init__(self, own, full, send, recv):
        self.own, self.full, self.send, self.recv = own, full, send, recv
        self.rows = own.shape[0]
        self.half = self.rows // 2

    def place(self, rank, part):
        return self.full.at[pl.ds(pl.multiple_of(rank * self.rows + part * self.half, self.half), self.half)]

    def start(self):
        me, side, down, across = sides()
        mine = [self.own.at[pl.ds(part * self.half, self.half)] for part in (0, 1)]
        to_side, to_down = {"seq": side}, {"seq": down}
        self.first = push(mine[0], self.place(me, 0), self.send.at[0], self.recv.at[0], to_side)
        self.second = push(mine[1], self.place(me, 1), self.send.at[1], self.recv.at[1], to_down)
        self.third = push(mine[1], self.place(me, 1), self.send.at[2], self.recv.at[2], to_side)
        self.fourth = push(mine[0], self.place(me, 0), self.send.at[3], self.recv.at[3], to_down)

    def relay(self):
        me, side, down, across = sides()
        self.first.wait_recv()
        self.fifth = push(
            self.place(side, 0), self.place(side, 0), self.send.at[4], self.recv.at[4], {"seq": down}
        )
        self.second.wait_recv()
        self.sixth = push(
            self.place(down, 1), self.place(down, 1), self.send.at[5], self.recv.at[5], {"seq": side}
        )

    def near(self):
        self.third.wait_recv()
        self.fourth.wait_recv()

    def far(self):
        self.fifth.wait_recv()
        self.sixth.wait_recv()

    def finish(self):
        for copy in (self.first, self.second, self.third, self.fourth, self.fifth, self.sixth):
            copy.wait_send()


def gather_square(values, collective_id):
    count = len(values)

    def body(*refs):
        own, full = refs[:count], refs[count : 2 * count]
        send, recv, local = refs[2 * count :]
        me, side, down, across = sides()
        meet({"seq": side}, {"seq": down})
        jobs = [SquareGather(own[i], full[i], send.at[i], recv.at[i]) for i in range(count)]
        keeps = []
        for i, job in enumerate(jobs):
            job.start()
            rows = own[i].shape[0]
            keep = pltpu.make_async_copy(
                own[i], full[i].at[pl.ds(pl.multiple_of(me * rows, rows), rows)], local.at[i]
            )
            keep.start()
            keeps.append(keep)
        for job in jobs:
            job.relay()
        for job, keep in zip(jobs, keeps):
            job.near()
            job.far()
            job.finish()
            keep.wait()

    return pl.pallas_call(
        body,
        in_specs=[pl.BlockSpec(memory_space=pltpu.VMEM)] * count,
        out_specs=[pl.BlockSpec(memory_space=pl.ANY)] * count,
        out_shape=[jax.ShapeDtypeStruct((4 * v.shape[0],) + v.shape[1:], v.dtype) for v in values],
        scratch_shapes=[
            pltpu.SemaphoreType.DMA((count, 6)),
            pltpu.SemaphoreType.DMA((count, 6)),
            pltpu.SemaphoreType.DMA((count,)),
        ],
        compiler_params=pltpu.CompilerParams(
            collective_id=collective_id, has_side_effects=True, vmem_limit_bytes=VMEM_LIMIT
        ),
        name="gather_square",
    )(*values)


def block_product(left, right, transposed, tile, store):
    total = right.shape[0] if transposed else right.shape[1]

    def step(number, carry):
        columns = pl.ds(pl.multiple_of(number * tile, tile), tile)
        if transposed:
            store(columns, product_nt(left, right[columns, :]))
        else:
            store(columns, product(left, right[:, columns]))
        return carry

    lax.fori_loop(0, total // tile, step, 0)


def gather_product(own, weight, transposed, collective_id):
    rows, depth = own.shape
    width = weight.shape[0] if transposed else weight.shape[1]
    tile = 512 if width % 512 == 0 else 128 * (width // 128 // 3) if width % 384 == 0 else 128

    def body(own_ref, weight_ref, full, out, send, recv):
        me, side, down, across = sides()
        meet({"seq": side}, {"seq": down})
        job = SquareGather(own_ref, full, send, recv)
        job.start()

        def multiply(rank, block):
            at = pl.ds(pl.multiple_of(rank * rows, rows), rows)

            def store(columns, value):
                out[at, columns] = value.astype(out.dtype)

            block_product(block, weight_ref, transposed, tile, store)

        def arrived(rank):
            return full[pl.ds(pl.multiple_of(rank * rows, rows), rows), :]

        full[pl.ds(pl.multiple_of(me * rows, rows), rows), :] = own_ref[...]
        multiply(me, own_ref[...])
        job.relay()
        job.near()
        multiply(side, arrived(side))
        multiply(down, arrived(down))
        job.far()
        multiply(across, arrived(across))
        job.finish()

    vmem = pl.BlockSpec(memory_space=pltpu.VMEM)
    return pl.pallas_call(
        body,
        in_specs=[vmem, vmem],
        out_specs=[vmem, vmem],
        out_shape=[
            jax.ShapeDtypeStruct((4 * rows, depth), own.dtype),
            jax.ShapeDtypeStruct((4 * rows, width), jnp.float32),
        ],
        scratch_shapes=[pltpu.SemaphoreType.DMA((6,)), pltpu.SemaphoreType.DMA((6,))],
        compiler_params=pltpu.CompilerParams(
            collective_id=collective_id, has_side_effects=True, vmem_limit_bytes=VMEM_LIMIT
        ),
        name="gather_product",
    )(own, weight)


def product_scatter(lefts, rights, transposed, collective_id):
    count = len(lefts)
    rows = lefts[0].shape[0] // 4
    half = rows // 2
    width = rights[0].shape[0] if transposed else rights[0].shape[1]
    tile = width // 3 if width % 384 == 0 else width

    def body(*refs):
        left, right = refs[:count], refs[count : 2 * count]
        out, far, near, kept, land, carry, send, recv = refs[2 * count :]
        me, side, down, across = sides()
        meet({"seq": side}, {"seq": down})
        to_side, to_down = {"seq": side}, {"seq": down}

        def partial(rank, store):
            at = pl.ds(pl.multiple_of(rank * rows, rows), rows)

            def step(number, carried):
                columns = pl.ds(pl.multiple_of(number * tile, tile), tile)
                value = None
                for a, b in zip(left, right):
                    term = product_nt(a[at, :], b[columns, :]) if transposed else product(a[at, :], b[:, columns])
                    value = term if value is None else value + term
                store(columns, value)
                return carried

            lax.fori_loop(0, width // tile, step, 0)

        def store_far(columns, value):
            far[:, columns] = value.astype(far.dtype)

        def store_side(columns, value):
            kept[0, :, columns] = value[:half]
            near[0, :, columns] = value[half:].astype(near.dtype)

        def store_down(columns, value):
            near[1, :, columns] = value[:half].astype(near.dtype)
            kept[1, :, columns] = value[half:]

        def store_own(columns, value):
            out[:, columns] = value

        partial(across, store_far)
        first = push(far.at[pl.ds(0, half)], land.at[0], send.at[0], recv.at[0], to_down)
        second = push(far.at[pl.ds(half, half)], land.at[1], send.at[1], recv.at[1], to_side)
        partial(side, store_side)
        third = push(near.at[0], land.at[2], send.at[2], recv.at[2], to_side)
        partial(down, store_down)
        fourth = push(near.at[1], land.at[3], send.at[3], recv.at[3], to_down)
        first.wait_recv()
        carry[0] = (kept[0] + land[0].astype(jnp.float32)).astype(carry.dtype)
        fifth = push(carry.at[0], land.at[4], send.at[4], recv.at[4], to_side)
        second.wait_recv()
        carry[1] = (kept[1] + land[1].astype(jnp.float32)).astype(carry.dtype)
        sixth = push(carry.at[1], land.at[5], send.at[5], recv.at[5], to_down)
        partial(me, store_own)
        third.wait_recv()
        fourth.wait_recv()
        fifth.wait_recv()
        out[:half, :] += land[3].astype(jnp.float32) + land[4].astype(jnp.float32)
        sixth.wait_recv()
        out[half:, :] += land[2].astype(jnp.float32) + land[5].astype(jnp.float32)
        for copy in (first, second, third, fourth, fifth, sixth):
            copy.wait_send()

    vmem = pl.BlockSpec(memory_space=pltpu.VMEM)
    low = jnp.bfloat16
    return pl.pallas_call(
        body,
        in_specs=[vmem] * (2 * count),
        out_specs=vmem,
        out_shape=jax.ShapeDtypeStruct((rows, width), jnp.float32),
        scratch_shapes=[
            pltpu.VMEM((rows, width), low),
            pltpu.VMEM((2, half, width), low),
            pltpu.VMEM((2, half, width), jnp.float32),
            pltpu.VMEM((6, half, width), low),
            pltpu.VMEM((2, half, width), low),
            pltpu.SemaphoreType.DMA((6,)),
            pltpu.SemaphoreType.DMA((6,)),
        ],
        compiler_params=pltpu.CompilerParams(
            collective_id=collective_id, has_side_effects=True, vmem_limit_bytes=VMEM_LIMIT
        ),
        name="product_scatter",
    )(*lefts, *rights)


def gather_and_spread(values, block, collective_id):
    count = len(values)
    rows, width = block.shape

    def body(*refs):
        own, mine = refs[:count], refs[count]
        full, whole = refs[count + 1 : 2 * count + 1], refs[2 * count + 1]
        send, recv, local, line_send, line_recv = refs[2 * count + 2 :]
        me, side, down, across = sides()
        shards = lax.axis_size("wshard")
        place = lax.axis_index("wshard")
        chips = shards // 2
        chip, core = place // 2, lax.rem(place, 2)
        nexts = {"wshard": lax.rem(place + 2, shards)}
        before = {"wshard": lax.rem(place + shards - 2, shards)}
        twin = {"wshard": place + 1 - 2 * core}
        meet({"seq": side}, {"seq": down}, nexts, before, twin)
        jobs = [SquareGather(own[i], full[i], send.at[i], recv.at[i]) for i in range(count)]
        mine_at = whole.at[core]

        def along(index, device):
            return pltpu.make_async_remote_copy(
                src_ref=mine_at,
                dst_ref=mine_at,
                send_sem=line_send.at[index],
                recv_sem=line_recv.at[0],
                device_id=device,
                device_id_type=MESH,
            )

        forth, back = along(0, nexts), along(1, before)
        to_twin = pltpu.make_async_remote_copy(
            src_ref=mine_at,
            dst_ref=mine_at,
            send_sem=line_send.at[2],
            recv_sem=line_recv.at[1],
            device_id=twin,
            device_id_type=MESH,
        )
        goes_forth = (chip >= me) & (chip < chips - 1)
        goes_back = (chip <= me) & (chip > 0)
        jobs[0].start()

        @pl.when(chip == me)
        def _():
            whole[core] = mine[...]

        @pl.when(chip != me)
        def _():
            forth.wait_recv()

        @pl.when(goes_forth)
        def _():
            forth.start()

        @pl.when(goes_back)
        def _():
            back.start()

        to_twin.start()
        keeps = []
        for i, job in enumerate(jobs):
            if i:
                job.start()
            size = own[i].shape[0]
            keep = pltpu.make_async_copy(
                own[i], full[i].at[pl.ds(pl.multiple_of(me * size, size), size)], local.at[i]
            )
            keep.start()
            keeps.append(keep)
        for job in jobs:
            job.relay()
        for job, keep in zip(jobs, keeps):
            job.near()
            job.far()
            job.finish()
            keep.wait()
        to_twin.wait_recv()
        to_twin.wait_send()

        @pl.when(goes_forth)
        def _():
            forth.wait_send()

        @pl.when(goes_back)
        def _():
            back.wait_send()

    vmem = pl.BlockSpec(memory_space=pltpu.VMEM)
    anywhere = pl.BlockSpec(memory_space=pl.ANY)
    return pl.pallas_call(
        body,
        in_specs=[vmem] * (count + 1),
        out_specs=[anywhere] * count + [vmem],
        out_shape=[jax.ShapeDtypeStruct((4 * v.shape[0],) + v.shape[1:], v.dtype) for v in values]
        + [jax.ShapeDtypeStruct((2, rows, width), block.dtype)],
        scratch_shapes=[
            pltpu.SemaphoreType.DMA((count, 6)),
            pltpu.SemaphoreType.DMA((count, 6)),
            pltpu.SemaphoreType.DMA((count,)),
            pltpu.SemaphoreType.DMA((3,)),
            pltpu.SemaphoreType.DMA((2,)),
        ],
        compiler_params=pltpu.CompilerParams(
            collective_id=collective_id, has_side_effects=True, vmem_limit_bytes=VMEM_LIMIT
        ),
        name="gather_and_spread",
    )(*values, block)


def gather(value, axis_name):
    return lax.all_gather(value, axis_name, axis=0, tiled=True)


def scatter(value, axis_name):
    return lax.psum_scatter(value, axis_name, scatter_dimension=0, tiled=True)


def gather_multiply(own, weight, transposed, collective_id):
    if square(lax.axis_size("seq")):
        return gather_product(own, weight, transposed, collective_id)
    whole = gather(own, "seq")
    return whole, product_nt(whole, weight) if transposed else product(whole, weight)


def multiply_scatter(lefts, rights, transposed, collective_id):
    if square(lax.axis_size("seq")):
        return product_scatter(lefts, rights, transposed, collective_id)
    total = sum(product_nt(a, b) if transposed else product(a, b) for a, b in zip(lefts, rights))
    return scatter(total.astype(jnp.bfloat16), "seq").astype(jnp.float32)


def on_device(
    layer_input,
    lengths,
    norm_attn,
    w_query,
    w_key,
    w_value,
    w_ogate,
    w_forget,
    forget_bias,
    w_out,
    norm_ffn,
    w_gate,
    w_up,
    w_down,
    output_grad,
):
    low = jnp.bfloat16
    tokens, width = layer_input.shape[1:]
    heads = forget_bias.shape[0]
    groups = lax.axis_size("seq")
    shards = lax.axis_size("wshard")
    local_heads = heads // groups
    head_size = width // heads
    columns = width // groups
    slots = tokens * groups
    hidden_size = w_gate.shape[1]
    part = hidden_size // (groups * shards)
    scale = head_size ** (-0.5)
    length = lengths[0]
    seq_rank = lax.axis_index("seq")
    shard_rank = lax.axis_index("wshard")
    per_block = shards // groups
    positions = seq_rank * tokens + jnp.arange(tokens, dtype=jnp.int32)
    valid_slots = (positions < length)[:, None]
    inputs = layer_input[0].astype(jnp.float32)
    cotangent_low = jnp.where(valid_slots, output_grad[0], jnp.zeros((), low))
    cotangent = cotangent_low.astype(jnp.float32)
    pad_heads = PAIR

    def own_columns(weight):
        return lax.dynamic_slice_in_dim(weight, seq_rank * columns, columns, 1)

    def own_units(weight):
        split = weight.reshape(weight.shape[0], shards, groups, part)
        mine = lax.dynamic_index_in_dim(split, seq_rank, 2, keepdims=False)
        return mine.reshape(weight.shape[0], shards * part)

    own_forget = lax.dynamic_slice_in_dim(w_forget, seq_rank * local_heads, local_heads, 1)
    own_forget = jnp.pad(own_forget, ((0, 0), (0, pad_heads - local_heads)))
    mine_attn = jnp.concatenate(
        [own_columns(w_query), own_columns(w_key), own_columns(w_value), own_forget],
        axis=1,
    )
    mine_ffn = jnp.concatenate([own_units(w_gate), own_units(w_up)], axis=1)
    mine_down = lax.dynamic_slice_in_dim(w_down, seq_rank * part, part, 0)
    fast = square(groups) and shards == 2 * groups
    full_attn = gather(mine_attn, "wshard")
    full_ogate = gather(own_columns(w_ogate), "wshard")
    normed_attn_own = rms_norm(inputs, norm_attn).astype(low)
    if fast:
        normed_attn, cotangent_all, full_out = gather_and_spread([normed_attn_own, cotangent_low], w_out, 0)
        full_out = full_out.reshape(columns, width)
    else:
        normed_attn = gather(normed_attn_own, "seq")
        cotangent_all = gather(cotangent_low, "seq")
        full_out = lax.dynamic_slice_in_dim(gather(w_out, "wshard"), seq_rank * columns, columns, 0)
    full_ffn = gather(mine_ffn, "wshard")
    full_down = gather(mine_down, "wshard")

    projected = product(normed_attn, full_attn)
    queries = projected[:, :columns].astype(low)
    keys = projected[:, columns : 2 * columns].astype(low)
    values = projected[:, 2 * columns : 3 * columns].astype(low)
    gate_pre = product(normed_attn, full_ogate)
    forget_pre = projected[:, 3 * columns : 3 * columns + local_heads].astype(low)
    bias_local = lax.dynamic_slice_in_dim(forget_bias, seq_rank * local_heads, local_heads)
    forget_total = forget_pre.astype(jnp.float32) + bias_local
    log_forget, pull_forget = jax.vjp(jax.nn.log_sigmoid, forget_total)
    cumulative = jnp.cumsum(log_forget, axis=0)
    even = -local_heads % 2

    def pad_lanes(value):
        return jnp.pad(value, ((0, 0), (0, even * head_size))) if even else value

    pairs = (local_heads + even) // 2
    cum = jnp.pad(cumulative, ((0, 0), (0, even))) if even else cumulative
    usable = (jnp.arange(slots, dtype=jnp.int32) < length)[:, None]
    cum_row = cum.T.reshape(pairs, 2, slots)
    key_col = jnp.where(usable, cum, -NEG_FILL).reshape(slots, pairs, 2).transpose(1, 0, 2)
    q_in = pad_lanes((queries.astype(jnp.float32) * scale).astype(low))
    k_in = pad_lanes(keys)
    v_in = pad_lanes(values)
    attended_low, log_total = attention_fwd(q_in, k_in, v_in, cum_row, key_col, head_size)
    attended = attended_low[:, :columns].astype(jnp.float32)
    gated_full, pull_gate = jax.vjp(gate_product, attended, gate_pre)
    gated = gated_full.astype(low)
    branch = multiply_scatter([gated], [full_out], False, 1)
    middle = inputs + branch
    normed_ffn_own, pull_ffn_norm = jax.vjp(rms_norm, middle, norm_ffn)
    normed_ffn, gate_up = gather_multiply(normed_ffn_own.astype(low), full_ffn, False, 2)
    units = shards * part
    hidden_full, pull_swiglu = jax.vjp(swiglu, gate_up[:, :units], gate_up[:, units:])
    hidden = hidden_full.astype(low)

    grad_w_down = product_tn(hidden, cotangent_all).astype(low)
    grad_hidden = product_nt(cotangent_all, full_down)
    grad_gate_full, grad_up_full = pull_swiglu(grad_hidden)
    grad_gate_up = jnp.concatenate([grad_gate_full.astype(low), grad_up_full.astype(low)], axis=1)
    grad_w_ffn = product_tn(normed_ffn, grad_gate_up).astype(low)
    grad_normed_ffn = multiply_scatter([grad_gate_up], [full_ffn], True, 3)
    share_down = scatter(grad_w_down, "wshard")
    share_ffn = scatter(grad_w_ffn, "wshard")
    grad_middle_part, grad_norm_ffn = pull_ffn_norm(grad_normed_ffn)
    grad_middle = cotangent + grad_middle_part
    grad_branch, grad_gated = gather_multiply(grad_middle.astype(low), full_out, True, 4)
    grad_w_out = product_tn(gated, grad_branch).astype(low)
    grad_attended_full, grad_gate_pre_full = pull_gate(grad_gated)
    grad_attended = pad_lanes(grad_attended_full.astype(low))
    grad_gate_pre = grad_gate_pre_full.astype(low)
    dq, dk, dv, drow, dcol = attention_bwd(
        q_in, k_in, v_in, grad_attended, cum_row, key_col, log_total, head_size, scale
    )
    grad_cum = drow.reshape(2 * pairs, slots).T - dcol.transpose(1, 0, 2).reshape(slots, 2 * pairs)
    grad_cum = grad_cum[:, :local_heads]
    grad_log_forget = jnp.flip(jnp.cumsum(jnp.flip(grad_cum, 0), axis=0), 0)
    grad_forget_total = pull_forget(grad_log_forget)[0]
    grad_bias_local = jnp.sum(grad_forget_total, axis=0)
    grad_forget = jnp.pad(grad_forget_total.astype(low), ((0, 0), (0, pad_heads - local_heads)))
    grad_bias = lax.dynamic_update_slice_in_dim(
        jnp.zeros((heads,), jnp.float32), grad_bias_local, seq_rank * local_heads, 0
    )
    grad_projected = jnp.concatenate(
        [dq[:, :columns], dk[:, :columns], dv[:, :columns], grad_forget, grad_gate_pre], axis=1
    )
    grad_w_attn = product_tn(normed_attn, grad_projected).astype(low)
    share_attn = scatter(grad_w_attn, "wshard")
    front = full_attn.shape[1]
    grad_normed_attn = multiply_scatter(
        [grad_projected[:, :front], grad_gate_pre], [full_attn, full_ogate], True, 5
    )
    unused_normed, pull_attn_norm = jax.vjp(rms_norm, inputs, norm_attn)
    grad_input_part, grad_norm_attn = pull_attn_norm(grad_normed_attn)
    grad_input = (grad_middle + grad_input_part)[None]
    lowered = multiply_scatter([hidden], [full_down], False, 6)
    layer_output = (middle + lowered).astype(low)[None]

    share_out = scatter(grad_w_out, "wshard")
    rows_out = columns // shards
    pieces_out = lax.all_gather(share_out, "seq", axis=0, tiled=False)
    lane_of = shard_rank // (shards // per_block)
    slots_out = jnp.where(
        (jnp.arange(per_block) == lane_of)[None, :, None, None], pieces_out[:, None], jnp.zeros((), low)
    ).reshape(shards, rows_out, width)
    moved = lax.all_to_all(slots_out, "wshard", split_axis=0, concat_axis=0, tiled=True)
    moved = moved.reshape(per_block, shards // per_block, rows_out, width)
    mine_out = lax.dynamic_index_in_dim(moved, shard_rank % per_block, 0, keepdims=False)
    grad_out = mine_out.reshape(columns // per_block, width).astype(jnp.float32)

    rows = share_attn.shape[0]
    if fast:
        every_ffn, grad_down = gather_square([share_ffn, share_down], 7)
        every_attn = gather_square([share_attn], 8)[0]
    else:
        every_ffn, grad_down, every_attn = [gather(v, "seq") for v in (share_ffn, share_down, share_attn)]
    every_ffn = every_ffn.reshape((groups,) + share_ffn.shape)
    every_attn = every_attn.reshape((groups,) + share_attn.shape)
    grad_down = grad_down.astype(jnp.float32)

    def join(first):
        taken = every_attn[:, :, first : first + columns]
        return taken.transpose(1, 0, 2).reshape(rows, width).astype(jnp.float32)

    def join_units(first):
        taken = every_ffn[:, :, first * units : (first + 1) * units]
        taken = taken.reshape(groups, rows, shards, part).transpose(1, 2, 0, 3)
        return taken.reshape(rows, hidden_size).astype(jnp.float32)

    grad_forget_w = every_attn[:, :, 3 * columns : 3 * columns + local_heads]
    grad_forget_w = grad_forget_w.transpose(1, 0, 2).reshape(rows, heads).astype(jnp.float32)
    small = lax.psum((grad_norm_attn, grad_norm_ffn, grad_bias), ("seq", "wshard"))
    return (
        layer_output,
        grad_input,
        small[0],
        join(0),
        join(columns),
        join(2 * columns),
        join(front),
        grad_forget_w,
        small[2],
        grad_out,
        small[1],
        join_units(0),
        join_units(1),
        grad_down,
    )


def solution(mesh):
    return jax.shard_map(
        on_device,
        mesh=mesh,
        in_specs=(
            P("wshard", "seq", None),
            P("wshard"),
            P(),
            P("wshard", None),
            P("wshard", None),
            P("wshard", None),
            P("wshard", None),
            P("wshard", None),
            P(),
            P("wshard", None),
            P(),
            P("wshard", None),
            P("wshard", None),
            P("wshard", None),
            P("wshard", "seq", None),
        ),
        out_specs=(
            P("wshard", "seq", None),
            P("wshard", "seq", None),
            P(),
            P("wshard", None),
            P("wshard", None),
            P("wshard", None),
            P("wshard", None),
            P("wshard", None),
            P(),
            P("wshard", None),
            P(),
            P("wshard", None),
            P("wshard", None),
            P("wshard", None),
        ),
        check_vma=False,
    )
```

```python
import jax
import jax.numpy as jnp
from jax import lax
from jax.experimental import pallas as pl
from jax.experimental.pallas import tpu as pltpu
from jax.sharding import PartitionSpec as P

EPS = 1e-06
NEG_FILL = -1e30
PAIR = 128


def product(left, right):
    return jnp.dot(left, right, preferred_element_type=jnp.float32)


def product_tn(left, right):
    return lax.dot_general(
        left, right, (((0,), (0,)), ((), ())), preferred_element_type=jnp.float32
    )


def product_nt(left, right):
    return lax.dot_general(
        left, right, (((1,), (1,)), ((), ())), preferred_element_type=jnp.float32
    )


def rms_norm(values, gain):
    return values * lax.rsqrt(jnp.mean(values * values, axis=-1, keepdims=True) + EPS) * gain


def gate_product(attended, gate_pre):
    return attended * jax.nn.sigmoid(gate_pre)


def swiglu(gate, upward):
    return jax.nn.silu(gate) * upward


def attention_fwd(q, k, v, cum_row, key_col, heads_half):
    slots, width = q.shape
    pairs = width // PAIR
    tile = min(256, slots)
    half = heads_half

    def body(q_ref, k_ref, v_ref, row_ref, col_ref, o_ref, lse_ref):
        key_all = k_ref[...]
        value_t = v_ref[...].T
        query_t = q_ref[...].T
        sub = lax.broadcasted_iota(jnp.int32, (PAIR, tile), 0)
        diag = lax.broadcasted_iota(jnp.int32, (tile, tile), 0) <= lax.broadcasted_iota(
            jnp.int32, (tile, tile), 1
        )
        for number in range(slots // tile):
            first, last = number * tile, (number + 1) * tile
            outs = []
            for a in range(2):
                mine = (sub >= a * half) & (sub < (a + 1) * half)
                query = jnp.where(mine, query_t[:, first:last], jnp.zeros((), query_t.dtype))
                scores = product(key_all[:last], query)
                scores = scores + (row_ref[0, a : a + 1, first:last] - col_ref[0, :last, a : a + 1])
                tail = jnp.where(diag, scores[first:], NEG_FILL)
                scores = tail if number == 0 else jnp.concatenate([scores[:first], tail], axis=0)
                top = jnp.max(scores, axis=0, keepdims=True)
                weights = jnp.exp(scores - top)
                total = jnp.sum(weights, axis=0, keepdims=True)
                mixed = product(value_t[a * half : (a + 1) * half, :last], weights.astype(jnp.bfloat16))
                outs.append(mixed / total)
                lse_ref[0, a : a + 1, first:last] = top + jnp.log(total)
            o_ref[first:last, :] = jnp.concatenate(outs, axis=0).T.astype(o_ref.dtype)

    lane = pl.BlockSpec((slots, PAIR), lambda p: (0, p))
    row = pl.BlockSpec((1, 2, slots), lambda p: (p, 0, 0))
    col = pl.BlockSpec((1, slots, 2), lambda p: (p, 0, 0))
    return pl.pallas_call(
        body,
        grid=(pairs,),
        in_specs=[lane, lane, lane, row, col],
        out_specs=[lane, row],
        out_shape=[
            jax.ShapeDtypeStruct((slots, width), jnp.bfloat16),
            jax.ShapeDtypeStruct((pairs, 2, slots), jnp.float32),
        ],
        compiler_params=pltpu.CompilerParams(vmem_limit_bytes=56 << 20),
        cost_estimate=pl.CostEstimate(
            flops=4 * slots * slots * width, bytes_accessed=8 * slots * width, transcendentals=0
        ),
        name="attention_fwd",
    )(q, k, v, cum_row, key_col)


def attention_bwd(q, k, v, d_out, cum_row, key_col, lse, heads_half, scale):
    slots, width = q.shape
    pairs = width // PAIR
    tile = min(256, slots)
    half = heads_half

    def body(q_ref, k_ref, v_ref, do_ref, row_ref, col_ref, lse_ref,
             dq_ref, dk_ref, dv_ref, drow_ref, dcol_ref, dk_acc, dv_acc, dcol_acc):
        key_all = k_ref[...]
        value_all = v_ref[...]
        query_t = q_ref[...].T
        key_t = k_ref[...].T
        dout_t = do_ref[...].T
        sub = lax.broadcasted_iota(jnp.int32, (PAIR, tile), 0)
        lanes = lax.broadcasted_iota(jnp.int32, (tile, PAIR), 1)
        diag = lax.broadcasted_iota(jnp.int32, (tile, tile), 0) <= lax.broadcasted_iota(
            jnp.int32, (tile, tile), 1
        )
        zero = jnp.zeros((), jnp.bfloat16)
        dk_acc[...] = jnp.zeros_like(dk_acc)
        dv_acc[...] = jnp.zeros_like(dv_acc)
        dcol_acc[...] = jnp.zeros_like(dcol_acc)
        for number in range(slots // tile):
            first, last = number * tile, (number + 1) * tile
            outs = []
            for a in range(2):
                mine = (sub >= a * half) & (sub < (a + 1) * half)
                own = (lanes >= a * half) & (lanes < (a + 1) * half)
                scores = product(key_all[:last], jnp.where(mine, query_t[:, first:last], zero))
                offset = row_ref[0, a : a + 1, first:last] - lse_ref[0, a : a + 1, first:last]
                scores = scores + (offset - col_ref[0, :last, a : a + 1])
                tail = jnp.where(diag, scores[first:], NEG_FILL)
                scores = tail if number == 0 else jnp.concatenate([scores[:first], tail], axis=0)
                probs = jnp.exp(scores)
                d_probs = product(value_all[:last], jnp.where(mine, dout_t[:, first:last], zero))
                dot = jnp.sum(d_probs * probs, axis=0, keepdims=True)
                d_full = probs * (d_probs - dot)
                d_scores = d_full.astype(jnp.bfloat16)
                drow_ref[0, a : a + 1, first:last] = jnp.sum(d_full, axis=0, keepdims=True)
                dcol_acc[:last, a : a + 1] += jnp.sum(d_full, axis=1, keepdims=True)
                outs.append(product(key_t[a * half : (a + 1) * half, :last], d_scores) * scale)
                dk_acc[:last, :] += product(d_scores, jnp.where(own, q_ref[first:last, :], zero))
                dv_acc[:last, :] += product(
                    probs.astype(jnp.bfloat16), jnp.where(own, do_ref[first:last, :], zero)
                )
            dq_ref[first:last, :] = jnp.concatenate(outs, axis=0).T.astype(dq_ref.dtype)
        dk_ref[...] = dk_acc[...].astype(dk_ref.dtype)
        dv_ref[...] = dv_acc[...].astype(dv_ref.dtype)
        dcol_ref[0] = dcol_acc[...]

    lane = pl.BlockSpec((slots, PAIR), lambda p: (0, p))
    row = pl.BlockSpec((1, 2, slots), lambda p: (p, 0, 0))
    col = pl.BlockSpec((1, slots, 2), lambda p: (p, 0, 0))
    return pl.pallas_call(
        body,
        grid=(pairs,),
        in_specs=[lane, lane, lane, lane, row, col, row],
        out_specs=[lane, lane, lane, row, col],
        out_shape=[jax.ShapeDtypeStruct((slots, width), jnp.bfloat16)] * 3
        + [
            jax.ShapeDtypeStruct((pairs, 2, slots), jnp.float32),
            jax.ShapeDtypeStruct((pairs, slots, 2), jnp.float32),
        ],
        scratch_shapes=[
            pltpu.VMEM((slots, PAIR), jnp.float32),
            pltpu.VMEM((slots, PAIR), jnp.float32),
            pltpu.VMEM((slots, 2), jnp.float32),
        ],
        compiler_params=pltpu.CompilerParams(vmem_limit_bytes=56 << 20),
        cost_estimate=pl.CostEstimate(
            flops=10 * slots * slots * width, bytes_accessed=14 * slots * width, transcendentals=0
        ),
        name="attention_bwd",
    )(q, k, v, d_out, cum_row, key_col, lse)


MESH = pl.DeviceIdType.MESH
VMEM_LIMIT = 62 << 20


def square(groups):
    return groups == 4


def sides():
    rank = lax.axis_index("seq")
    return rank, rank + 1 - 2 * lax.rem(rank, 2), lax.rem(rank + 2, 4), 3 - rank


def meet(*others):
    barrier = pltpu.get_barrier_semaphore()
    for other in others:
        pl.semaphore_signal(barrier, inc=1, device_id=other, device_id_type=MESH)
    pl.semaphore_wait(barrier, len(others))


def push(source, target, send, recv, device):
    copy = pltpu.make_async_remote_copy(
        src_ref=source,
        dst_ref=target,
        send_sem=send,
        recv_sem=recv,
        device_id=device,
        device_id_type=MESH,
    )
    copy.start()
    return copy


class SquareGather:
    def __init__(self, own, full, send, recv):
        self.own, self.full, self.send, self.recv = own, full, send, recv
        self.rows = own.shape[0]
        self.half = self.rows // 2

    def place(self, rank, part):
        return self.full.at[pl.ds(pl.multiple_of(rank * self.rows + part * self.half, self.half), self.half)]

    def start(self):
        me, side, down, across = sides()
        mine = [self.own.at[pl.ds(part * self.half, self.half)] for part in (0, 1)]
        to_side, to_down = {"seq": side}, {"seq": down}
        self.first = push(mine[0], self.place(me, 0), self.send.at[0], self.recv.at[0], to_side)
        self.second = push(mine[1], self.place(me, 1), self.send.at[1], self.recv.at[1], to_down)
        self.third = push(mine[1], self.place(me, 1), self.send.at[2], self.recv.at[2], to_side)
        self.fourth = push(mine[0], self.place(me, 0), self.send.at[3], self.recv.at[3], to_down)

    def relay(self):
        me, side, down, across = sides()
        self.first.wait_recv()
        self.fifth = push(
            self.place(side, 0), self.place(side, 0), self.send.at[4], self.recv.at[4], {"seq": down}
        )
        self.second.wait_recv()
        self.sixth = push(
            self.place(down, 1), self.place(down, 1), self.send.at[5], self.recv.at[5], {"seq": side}
        )

    def near(self):
        self.third.wait_recv()
        self.fourth.wait_recv()

    def far(self):
        self.fifth.wait_recv()
        self.sixth.wait_recv()

    def finish(self):
        for copy in (self.first, self.second, self.third, self.fourth, self.fifth, self.sixth):
            copy.wait_send()


def gather_square(values, collective_id):
    count = len(values)

    def body(*refs):
        own, full = refs[:count], refs[count : 2 * count]
        send, recv, local = refs[2 * count :]
        me, side, down, across = sides()
        meet({"seq": side}, {"seq": down})
        jobs = [SquareGather(own[i], full[i], send.at[i], recv.at[i]) for i in range(count)]
        keeps = []
        for i, job in enumerate(jobs):
            job.start()
            rows = own[i].shape[0]
            keep = pltpu.make_async_copy(
                own[i], full[i].at[pl.ds(pl.multiple_of(me * rows, rows), rows)], local.at[i]
            )
            keep.start()
            keeps.append(keep)
        for job in jobs:
            job.relay()
        for job, keep in zip(jobs, keeps):
            job.near()
            job.far()
            job.finish()
            keep.wait()

    return pl.pallas_call(
        body,
        in_specs=[pl.BlockSpec(memory_space=pltpu.VMEM)] * count,
        out_specs=[pl.BlockSpec(memory_space=pl.ANY)] * count,
        out_shape=[jax.ShapeDtypeStruct((4 * v.shape[0],) + v.shape[1:], v.dtype) for v in values],
        scratch_shapes=[
            pltpu.SemaphoreType.DMA((count, 6)),
            pltpu.SemaphoreType.DMA((count, 6)),
            pltpu.SemaphoreType.DMA((count,)),
        ],
        compiler_params=pltpu.CompilerParams(
            collective_id=collective_id, has_side_effects=True, vmem_limit_bytes=VMEM_LIMIT
        ),
        name="gather_square",
    )(*values)


def block_product(left, right, transposed, tile, store):
    total = right.shape[0] if transposed else right.shape[1]

    def step(number, carry):
        columns = pl.ds(pl.multiple_of(number * tile, tile), tile)
        if transposed:
            store(columns, product_nt(left, right[columns, :]))
        else:
            store(columns, product(left, right[:, columns]))
        return carry

    lax.fori_loop(0, total // tile, step, 0)


def gather_product(own, weight, transposed, collective_id):
    rows, depth = own.shape
    width = weight.shape[0] if transposed else weight.shape[1]
    tile = 512 if width % 512 == 0 else 128 * (width // 128 // 3) if width % 384 == 0 else 128

    def body(own_ref, weight_ref, full, out, send, recv):
        me, side, down, across = sides()
        meet({"seq": side}, {"seq": down})
        job = SquareGather(own_ref, full, send, recv)
        job.start()

        def multiply(rank, block):
            at = pl.ds(pl.multiple_of(rank * rows, rows), rows)

            def store(columns, value):
                out[at, columns] = value.astype(out.dtype)

            block_product(block, weight_ref, transposed, tile, store)

        def arrived(rank):
            return full[pl.ds(pl.multiple_of(rank * rows, rows), rows), :]

        full[pl.ds(pl.multiple_of(me * rows, rows), rows), :] = own_ref[...]
        multiply(me, own_ref[...])
        job.relay()
        job.near()
        multiply(side, arrived(side))
        multiply(down, arrived(down))
        job.far()
        multiply(across, arrived(across))
        job.finish()

    vmem = pl.BlockSpec(memory_space=pltpu.VMEM)
    return pl.pallas_call(
        body,
        in_specs=[vmem, vmem],
        out_specs=[vmem, vmem],
        out_shape=[
            jax.ShapeDtypeStruct((4 * rows, depth), own.dtype),
            jax.ShapeDtypeStruct((4 * rows, width), jnp.float32),
        ],
        scratch_shapes=[pltpu.SemaphoreType.DMA((6,)), pltpu.SemaphoreType.DMA((6,))],
        compiler_params=pltpu.CompilerParams(
            collective_id=collective_id, has_side_effects=True, vmem_limit_bytes=VMEM_LIMIT
        ),
        name="gather_product",
    )(own, weight)


def transposed_product(left, right, out):
    tall = 512 if out.shape[0] % 512 == 0 else 384
    wide = 512 if out.shape[1] % 512 == 0 else 384
    across = out.shape[1] // wide

    def step(number, carry):
        rows = pl.ds(pl.multiple_of((number // across) * tall, tall), tall)
        columns = pl.ds(pl.multiple_of(lax.rem(number, across) * wide, wide), wide)
        out[rows, columns] = product_tn(left[:, rows], right[:, columns]).astype(out.dtype)
        return carry

    lax.fori_loop(0, (out.shape[0] // tall) * across, step, 0)


def product_scatter(lefts, rights, transposed, collective_id, extras=()):
    count = len(lefts)
    more = len(extras)
    rows = lefts[0].shape[0] // 4
    half = rows // 2
    width = rights[0].shape[0] if transposed else rights[0].shape[1]
    tile = width // 3 if width % 384 == 0 else width

    def body(*refs):
        left, right = refs[:count], refs[count : 2 * count]
        sides_in = refs[2 * count : 2 * count + 2 * more]
        out = refs[2 * count + 2 * more]
        sides_out = refs[2 * count + 2 * more + 1 : 2 * count + 3 * more + 1]
        far, near, kept, land, carry, send, recv = refs[2 * count + 3 * more + 1 :]
        me, side, down, across = sides()
        meet({"seq": side}, {"seq": down})
        to_side, to_down = {"seq": side}, {"seq": down}

        def partial(rank, store):
            at = pl.ds(pl.multiple_of(rank * rows, rows), rows)

            def step(number, carried):
                columns = pl.ds(pl.multiple_of(number * tile, tile), tile)
                value = None
                for a, b in zip(left, right):
                    term = product_nt(a[at, :], b[columns, :]) if transposed else product(a[at, :], b[:, columns])
                    value = term if value is None else value + term
                store(columns, value)
                return carried

            lax.fori_loop(0, width // tile, step, 0)

        def store_far(columns, value):
            far[:, columns] = value.astype(far.dtype)

        def store_side(columns, value):
            kept[0, :, columns] = value[:half]
            near[0, :, columns] = value[half:].astype(near.dtype)

        def store_down(columns, value):
            near[1, :, columns] = value[:half].astype(near.dtype)
            kept[1, :, columns] = value[half:]

        def store_own(columns, value):
            out[:, columns] = value

        partial(across, store_far)
        first = push(far.at[pl.ds(0, half)], land.at[0], send.at[0], recv.at[0], to_down)
        second = push(far.at[pl.ds(half, half)], land.at[1], send.at[1], recv.at[1], to_side)
        partial(side, store_side)
        third = push(near.at[0], land.at[2], send.at[2], recv.at[2], to_side)
        partial(down, store_down)
        fourth = push(near.at[1], land.at[3], send.at[3], recv.at[3], to_down)
        first.wait_recv()
        carry[0] = (kept[0] + land[0].astype(jnp.float32)).astype(carry.dtype)
        fifth = push(carry.at[0], land.at[4], send.at[4], recv.at[4], to_side)
        second.wait_recv()
        carry[1] = (kept[1] + land[1].astype(jnp.float32)).astype(carry.dtype)
        sixth = push(carry.at[1], land.at[5], send.at[5], recv.at[5], to_down)
        partial(me, store_own)
        for index in range(more):
            transposed_product(sides_in[2 * index], sides_in[2 * index + 1], sides_out[index])
        third.wait_recv()
        fourth.wait_recv()
        fifth.wait_recv()
        out[:half, :] += land[3].astype(jnp.float32) + land[4].astype(jnp.float32)
        sixth.wait_recv()
        out[half:, :] += land[2].astype(jnp.float32) + land[5].astype(jnp.float32)
        for copy in (first, second, third, fourth, fifth, sixth):
            copy.wait_send()

    vmem = pl.BlockSpec(memory_space=pltpu.VMEM)
    low = jnp.bfloat16
    return pl.pallas_call(
        body,
        in_specs=[vmem] * (2 * count + 2 * more),
        out_specs=[vmem] * (1 + more),
        out_shape=[jax.ShapeDtypeStruct((rows, width), jnp.float32)]
        + [jax.ShapeDtypeStruct((a.shape[1], b.shape[1]), low) for a, b in extras],
        scratch_shapes=[
            pltpu.VMEM((rows, width), low),
            pltpu.VMEM((2, half, width), low),
            pltpu.VMEM((2, half, width), jnp.float32),
            pltpu.VMEM((6, half, width), low),
            pltpu.VMEM((2, half, width), low),
            pltpu.SemaphoreType.DMA((6,)),
            pltpu.SemaphoreType.DMA((6,)),
        ],
        compiler_params=pltpu.CompilerParams(
            collective_id=collective_id, has_side_effects=True, vmem_limit_bytes=VMEM_LIMIT
        ),
        name="product_scatter",
    )(*lefts, *rights, *(value for pair in extras for value in pair))


def line():
    shards, place = lax.axis_size("wshard"), lax.axis_index("wshard")
    chips = shards // 2
    chip, core = place // 2, lax.rem(place, 2)
    forth = {"wshard": lax.rem(place + 2, shards)}
    back = {"wshard": lax.rem(place + shards - 2, shards)}
    twin = {"wshard": place + 1 - 2 * core}
    return chips, chip, core, forth, back, twin


class LineGather:
    def __init__(self, own, full, forth_send, back_send, twin_send, recv, local):
        self.own, self.full, self.local = own, full, local
        self.sends = (forth_send, back_send, twin_send)
        self.recv = recv
        self.rows = own.shape[0]
        self.chips, self.chip, self.core, *self.devices = line()

    def place(self, chip, core):
        return self.full.at[pl.ds(pl.multiple_of((2 * chip + core) * self.rows, self.rows), self.rows)]

    def copy(self, way, chip, source=None):
        target = self.place(chip, self.core)
        return pltpu.make_async_remote_copy(
            src_ref=target if source is None else source,
            dst_ref=target,
            send_sem=self.sends[way].at[chip],
            recv_sem=self.recv.at[2 * chip + self.core],
            device_id=self.devices[way],
            device_id_type=MESH,
        )

    def wait_for(self, chip, core):
        target = self.place(chip, core)
        pltpu.make_async_remote_copy(
            src_ref=target,
            dst_ref=target,
            send_sem=self.sends[2].at[0],
            recv_sem=self.recv.at[2 * chip + core],
            device_id=self.devices[2],
            device_id_type=MESH,
        ).wait_recv()

    def start(self):
        @pl.when(self.chip < self.chips - 1)
        def _():
            self.copy(0, self.chip, self.own).start()

        @pl.when(self.chip > 0)
        def _():
            self.copy(1, self.chip, self.own).start()

        self.copy(2, self.chip, self.own).start()
        self.keep = pltpu.make_async_copy(self.own, self.place(self.chip, self.core), self.local)
        self.keep.start()

    def step(self, number):
        left, right = self.chip - number, self.chip + number

        @pl.when(left >= 0)
        def _():
            self.wait_for(left, self.core)

            @pl.when(self.chip < self.chips - 1)
            def _():
                self.copy(0, left).start()

            self.copy(2, left).start()

        @pl.when(right < self.chips)
        def _():
            self.wait_for(right, self.core)

            @pl.when(self.chip > 0)
            def _():
                self.copy(1, right).start()

            self.copy(2, right).start()

    def finish(self):
        for chip in range(self.chips):
            self.wait_for(chip, 1 - self.core)
            self.copy(2, chip).wait_send()

            @pl.when((chip <= self.chip) & (self.chip < self.chips - 1))
            def _():
                self.copy(0, chip).wait_send()

            @pl.when((chip >= self.chip) & (self.chip > 0))
            def _():
                self.copy(1, chip).wait_send()

        self.keep.wait()


class LineSpread:
    pieces = 4

    def __init__(self, own, whole, send, recv):
        self.own, self.whole, self.send, self.recv = own, whole, send, recv
        self.rows = own.shape[0] // self.pieces
        self.source = lax.axis_index("seq")
        self.chips, self.chip, self.core, *self.devices = line()
        self.goes = (
            (self.chip >= self.source) & (self.chip < self.chips - 1),
            (self.chip <= self.source) & (self.chip > 0),
        )

    def copy(self, way, piece):
        target = self.whole.at[self.core, pl.ds(piece * self.rows, self.rows)]
        return pltpu.make_async_remote_copy(
            src_ref=target,
            dst_ref=target,
            send_sem=self.send.at[way, piece],
            recv_sem=self.recv.at[way // 2, piece],
            device_id=self.devices[way],
            device_id_type=MESH,
        )

    def start(self):
        @pl.when(self.chip == self.source)
        def _():
            self.whole[self.core] = self.own[...]

    def step(self, piece):
        @pl.when(self.chip != self.source)
        def _():
            self.copy(0, piece).wait_recv()

        for way in (0, 1):

            @pl.when(self.goes[way])
            def _():
                self.copy(way, piece).start()

        self.copy(2, piece).start()

    def finish(self):
        for piece in range(self.pieces):
            other = self.whole.at[1 - self.core, pl.ds(piece * self.rows, self.rows)]
            pltpu.make_async_remote_copy(
                src_ref=other,
                dst_ref=other,
                send_sem=self.send.at[2, piece],
                recv_sem=self.recv.at[1, piece],
                device_id=self.devices[2],
                device_id_type=MESH,
            ).wait_recv()
            self.copy(2, piece).wait_send()
            for way in (0, 1):

                @pl.when(self.goes[way])
                def _():
                    self.copy(way, piece).wait_send()


def first_gather(first, second, weights, block, collective_id):
    rows, width = block.shape
    shards = 2 * lax.axis_size("seq")
    chips = shards // 2

    def body(first_ref, second_ref, weights_ref, block_ref, first_full, second_full, weights_full, whole,
             send, recv, local, line_send, line_recv, spread_send, spread_recv):
        me, side, down, across = sides()
        line_chips, chip, core, forth, back, twin = line()
        meet({"seq": side}, {"seq": down}, forth, back, twin)
        one = SquareGather(first_ref, first_full, send.at[0], recv.at[0])
        two = SquareGather(second_ref, second_full, send.at[1], recv.at[1])
        run = LineGather(
            weights_ref, weights_full, line_send.at[0], line_send.at[1], line_send.at[2], line_recv, local.at[2]
        )
        spread = LineSpread(block_ref, whole, spread_send, spread_recv)
        spread.start()
        one.start()
        run.start()
        keeps = []
        for index, (own, full) in enumerate(((first_ref, first_full), (second_ref, second_full))):
            size = own.shape[0]
            keep = pltpu.make_async_copy(
                own, full.at[pl.ds(pl.multiple_of(me * size, size), size)], local.at[index]
            )
            keep.start()
            keeps.append(keep)
        two.start()
        spread.step(0)
        run.step(1)
        one.relay()
        spread.step(1)
        run.step(2)
        two.relay()
        spread.step(2)
        run.step(3)
        spread.step(3)
        for job, keep in zip((one, two), keeps):
            job.near()
            job.far()
            job.finish()
            keep.wait()
        run.finish()
        spread.finish()

    vmem = pl.BlockSpec(memory_space=pltpu.VMEM)
    anywhere = pl.BlockSpec(memory_space=pl.ANY)
    dma = pltpu.SemaphoreType.DMA
    return pl.pallas_call(
        body,
        in_specs=[vmem] * 4,
        out_specs=[anywhere] * 3 + [vmem],
        out_shape=[
            jax.ShapeDtypeStruct((4 * first.shape[0],) + first.shape[1:], first.dtype),
            jax.ShapeDtypeStruct((4 * second.shape[0],) + second.shape[1:], second.dtype),
            jax.ShapeDtypeStruct((shards * weights.shape[0],) + weights.shape[1:], weights.dtype),
            jax.ShapeDtypeStruct((2, rows, width), block.dtype),
        ],
        scratch_shapes=[
            dma((2, 6)),
            dma((2, 6)),
            dma((3,)),
            dma((3, chips)),
            dma((shards,)),
            dma((3, LineSpread.pieces)),
            dma((2, LineSpread.pieces)),
        ],
        compiler_params=pltpu.CompilerParams(
            collective_id=collective_id, has_side_effects=True, vmem_limit_bytes=VMEM_LIMIT
        ),
        name="first_gather",
    )(first, second, weights, block)


def add_everywhere(values, collective_id):
    shape = values.shape
    groups, shards = 4, 8

    def body(values_ref, out, ranks, total, places, send, recv):
        rank, place = lax.axis_index("seq"), lax.axis_index("wshard")
        others = [{"seq": lax.rem(rank + k, groups)} for k in range(1, groups)]
        along = [{"wshard": lax.rem(place + k, shards)} for k in range(1, shards)]
        meet(*others, *along)
        copies = [
            push(values_ref, ranks.at[rank], send.at[k], recv.at[k], other) for k, other in enumerate(others)
        ]
        ranks[rank] = values_ref[...]
        for copy in copies:
            copy.wait()
        total[...] = (ranks[0] + ranks[1]) + (ranks[2] + ranks[3])
        copies = [
            push(total, places.at[place], send.at[groups + k], recv.at[groups + k], other)
            for k, other in enumerate(along)
        ]
        places[place] = total[...]
        for copy in copies:
            copy.wait()
        sums = [places[k] + places[k + 1] for k in range(0, shards, 2)]
        out[...] = (sums[0] + sums[1]) + (sums[2] + sums[3])

    vmem = pl.BlockSpec(memory_space=pltpu.VMEM)
    return pl.pallas_call(
        body,
        in_specs=[vmem],
        out_specs=vmem,
        out_shape=jax.ShapeDtypeStruct(shape, jnp.float32),
        scratch_shapes=[
            pltpu.VMEM((groups,) + shape, jnp.float32),
            pltpu.VMEM(shape, jnp.float32),
            pltpu.VMEM((shards,) + shape, jnp.float32),
            pltpu.SemaphoreType.DMA((groups + shards,)),
            pltpu.SemaphoreType.DMA((groups + shards,)),
        ],
        compiler_params=pltpu.CompilerParams(collective_id=collective_id, has_side_effects=True),
        name="add_everywhere",
    )(values)


def join_units(every, down, part):
    groups, rows, both = every.shape
    units = both // 2
    blocks = units // part
    steps = 4
    tall = rows // steps

    def body(every_ref, down_ref, gate_ref, up_ref, down_out):
        for half, out in enumerate((gate_ref, up_ref)):
            for group in range(groups):
                for block in range(blocks):
                    at = half * units + block * part
                    to = (block * groups + group) * part
                    out[:, to : to + part] = every_ref[group, :, at : at + part].astype(jnp.float32)
        down_out[...] = down_ref[...].astype(jnp.float32)

    wide = jax.ShapeDtypeStruct((rows, groups * units), jnp.float32)
    return pl.pallas_call(
        body,
        grid=(steps,),
        in_specs=[
            pl.BlockSpec((groups, tall, both), lambda i: (0, i, 0)),
            pl.BlockSpec((down.shape[0] // steps, down.shape[1]), lambda i: (i, 0)),
        ],
        out_specs=[pl.BlockSpec((tall, groups * units), lambda i: (i, 0))] * 2
        + [pl.BlockSpec((down.shape[0] // steps, down.shape[1]), lambda i: (i, 0))],
        out_shape=[wide, wide, jax.ShapeDtypeStruct(down.shape, jnp.float32)],
        name="join_units",
    )(every, down)


def join_columns(every, columns, starts):
    groups, rows, lanes = every.shape
    steps = 4
    tall = rows // steps

    def body(every_ref, *outs):
        for start, out in zip(starts, outs):
            for group in range(groups):
                out[:, group * columns : (group + 1) * columns] = every_ref[
                    group, :, start : start + columns
                ].astype(jnp.float32)

    wide = jax.ShapeDtypeStruct((rows, groups * columns), jnp.float32)
    return pl.pallas_call(
        body,
        grid=(steps,),
        in_specs=[pl.BlockSpec((groups, tall, lanes), lambda i: (0, i, 0))],
        out_specs=[pl.BlockSpec((tall, groups * columns), lambda i: (i, 0))] * len(starts),
        out_shape=[wide] * len(starts),
        name="join_columns",
    )(every)


def gather(value, axis_name):
    return lax.all_gather(value, axis_name, axis=0, tiled=True)


def scatter(value, axis_name):
    return lax.psum_scatter(value, axis_name, scatter_dimension=0, tiled=True)


def gather_multiply(own, weight, transposed, collective_id):
    if square(lax.axis_size("seq")):
        return gather_product(own, weight, transposed, collective_id)
    whole = gather(own, "seq")
    return whole, product_nt(whole, weight) if transposed else product(whole, weight)


def multiply_scatter(lefts, rights, transposed, collective_id, extras=()):
    if square(lax.axis_size("seq")):
        summed, *products = product_scatter(lefts, rights, transposed, collective_id, extras)
        return (summed, *products) if extras else summed
    products = [product_tn(a, b).astype(jnp.bfloat16) for a, b in extras]
    total = sum(product_nt(a, b) if transposed else product(a, b) for a, b in zip(lefts, rights))
    summed = scatter(total.astype(jnp.bfloat16), "seq").astype(jnp.float32)
    return (summed, *products) if extras else summed


def on_device(
    layer_input,
    lengths,
    norm_attn,
    w_query,
    w_key,
    w_value,
    w_ogate,
    w_forget,
    forget_bias,
    w_out,
    norm_ffn,
    w_gate,
    w_up,
    w_down,
    output_grad,
):
    low = jnp.bfloat16
    tokens, width = layer_input.shape[1:]
    heads = forget_bias.shape[0]
    groups = lax.axis_size("seq")
    shards = lax.axis_size("wshard")
    local_heads = heads // groups
    head_size = width // heads
    columns = width // groups
    slots = tokens * groups
    hidden_size = w_gate.shape[1]
    part = hidden_size // (groups * shards)
    scale = head_size ** (-0.5)
    length = lengths[0]
    seq_rank = lax.axis_index("seq")
    shard_rank = lax.axis_index("wshard")
    per_block = shards // groups
    positions = seq_rank * tokens + jnp.arange(tokens, dtype=jnp.int32)
    valid_slots = (positions < length)[:, None]
    inputs = layer_input[0].astype(jnp.float32)
    cotangent_low = jnp.where(valid_slots, output_grad[0], jnp.zeros((), low))
    cotangent = cotangent_low.astype(jnp.float32)
    pad_heads = PAIR

    def own_columns(weight):
        return lax.dynamic_slice_in_dim(weight, seq_rank * columns, columns, 1)

    def own_units(weight):
        split = weight.reshape(weight.shape[0], shards, groups, part)
        mine = lax.dynamic_index_in_dim(split, seq_rank, 2, keepdims=False)
        return mine.reshape(weight.shape[0], shards * part)

    own_forget = lax.dynamic_slice_in_dim(w_forget, seq_rank * local_heads, local_heads, 1)
    own_forget = jnp.pad(own_forget, ((0, 0), (0, pad_heads - local_heads)))
    mine_attn = jnp.concatenate(
        [own_columns(w_query), own_columns(w_key), own_columns(w_value), own_forget],
        axis=1,
    )
    fast = square(groups) and shards == 2 * groups
    normed_attn_own = rms_norm(inputs, norm_attn).astype(low)
    if fast:
        normed_attn, cotangent_all, full_attn, full_out = first_gather(
            normed_attn_own, cotangent_low, mine_attn, w_out, 0
        )
        full_out = full_out.reshape(columns, width)
        later = lax.optimization_barrier((full_out, w_ogate, w_gate, w_up, w_down))
        full_out, w_ogate, w_gate, w_up, w_down = later
    else:
        full_attn = gather(mine_attn, "wshard")
        normed_attn = gather(normed_attn_own, "seq")
        cotangent_all = gather(cotangent_low, "seq")
        full_out = lax.dynamic_slice_in_dim(gather(w_out, "wshard"), seq_rank * columns, columns, 0)
    full_ogate = gather(own_columns(w_ogate), "wshard")
    mine_ffn = jnp.concatenate([own_units(w_gate), own_units(w_up)], axis=1)
    mine_down = lax.dynamic_slice_in_dim(w_down, seq_rank * part, part, 0)
    full_ffn = gather(mine_ffn, "wshard")
    full_down = gather(mine_down, "wshard")

    projected = product(normed_attn, full_attn)
    queries = projected[:, :columns].astype(low)
    keys = projected[:, columns : 2 * columns].astype(low)
    values = projected[:, 2 * columns : 3 * columns].astype(low)
    gate_pre = product(normed_attn, full_ogate)
    forget_pre = projected[:, 3 * columns : 3 * columns + local_heads].astype(low)
    bias_local = lax.dynamic_slice_in_dim(forget_bias, seq_rank * local_heads, local_heads)
    forget_total = forget_pre.astype(jnp.float32) + bias_local
    log_forget, pull_forget = jax.vjp(jax.nn.log_sigmoid, forget_total)
    cumulative = jnp.cumsum(log_forget, axis=0)
    even = -local_heads % 2

    def pad_lanes(value):
        return jnp.pad(value, ((0, 0), (0, even * head_size))) if even else value

    pairs = (local_heads + even) // 2
    cum = jnp.pad(cumulative, ((0, 0), (0, even))) if even else cumulative
    usable = (jnp.arange(slots, dtype=jnp.int32) < length)[:, None]
    cum_row = cum.T.reshape(pairs, 2, slots)
    key_col = jnp.where(usable, cum, -NEG_FILL).reshape(slots, pairs, 2).transpose(1, 0, 2)
    q_in = pad_lanes((queries.astype(jnp.float32) * scale).astype(low))
    k_in = pad_lanes(keys)
    v_in = pad_lanes(values)
    attended_low, log_total = attention_fwd(q_in, k_in, v_in, cum_row, key_col, head_size)
    attended = attended_low[:, :columns].astype(jnp.float32)
    gated_full, pull_gate = jax.vjp(gate_product, attended, gate_pre)
    gated = gated_full.astype(low)
    branch = multiply_scatter([gated], [full_out], False, 1)
    middle = inputs + branch
    normed_ffn_own, pull_ffn_norm = jax.vjp(rms_norm, middle, norm_ffn)
    normed_ffn, gate_up = gather_multiply(normed_ffn_own.astype(low), full_ffn, False, 2)
    units = shards * part
    hidden_full, pull_swiglu = jax.vjp(swiglu, gate_up[:, :units], gate_up[:, units:])
    hidden = hidden_full.astype(low)

    grad_hidden = product_nt(cotangent_all, full_down)
    grad_gate_full, grad_up_full = pull_swiglu(grad_hidden)
    grad_gate_up = jnp.concatenate([grad_gate_full.astype(low), grad_up_full.astype(low)], axis=1)
    grad_normed_ffn, grad_w_down, grad_w_ffn = multiply_scatter(
        [grad_gate_up], [full_ffn], True, 3, [(hidden, cotangent_all), (normed_ffn, grad_gate_up)]
    )
    share_down = scatter(grad_w_down, "wshard")
    share_ffn = scatter(grad_w_ffn, "wshard")
    grad_middle_part, grad_norm_ffn = pull_ffn_norm(grad_normed_ffn)
    grad_middle = cotangent + grad_middle_part
    grad_branch, grad_gated = gather_multiply(grad_middle.astype(low), full_out, True, 4)
    grad_w_out = product_tn(gated, grad_branch).astype(low)
    grad_attended_full, grad_gate_pre_full = pull_gate(grad_gated)
    grad_attended = pad_lanes(grad_attended_full.astype(low))
    grad_gate_pre = grad_gate_pre_full.astype(low)
    dq, dk, dv, drow, dcol = attention_bwd(
        q_in, k_in, v_in, grad_attended, cum_row, key_col, log_total, head_size, scale
    )
    grad_cum = drow.reshape(2 * pairs, slots).T - dcol.transpose(1, 0, 2).reshape(slots, 2 * pairs)
    grad_cum = grad_cum[:, :local_heads]
    grad_log_forget = jnp.flip(jnp.cumsum(jnp.flip(grad_cum, 0), axis=0), 0)
    grad_forget_total = pull_forget(grad_log_forget)[0]
    grad_bias_local = jnp.sum(grad_forget_total, axis=0)
    grad_forget = jnp.pad(grad_forget_total.astype(low), ((0, 0), (0, pad_heads - local_heads)))
    grad_bias = lax.dynamic_update_slice_in_dim(
        jnp.zeros((heads,), jnp.float32), grad_bias_local, seq_rank * local_heads, 0
    )
    grad_projected = jnp.concatenate(
        [dq[:, :columns], dk[:, :columns], dv[:, :columns], grad_forget, grad_gate_pre], axis=1
    )
    grad_w_attn = product_tn(normed_attn, grad_projected).astype(low)
    share_attn = scatter(grad_w_attn, "wshard")
    front = full_attn.shape[1]
    grad_normed_attn = multiply_scatter(
        [grad_projected[:, :front], grad_gate_pre], [full_attn, full_ogate], True, 5
    )
    unused_normed, pull_attn_norm = jax.vjp(rms_norm, inputs, norm_attn)
    grad_input_part, grad_norm_attn = pull_attn_norm(grad_normed_attn)
    grad_input = (grad_middle + grad_input_part)[None]
    lowered = multiply_scatter([hidden], [full_down], False, 6)
    layer_output = (middle + lowered).astype(low)[None]

    share_out = scatter(grad_w_out, "wshard")
    rows_out = columns // shards
    pieces_out = lax.all_gather(share_out, "seq", axis=0, tiled=False)
    lane_of = shard_rank // (shards // per_block)
    slots_out = jnp.where(
        (jnp.arange(per_block) == lane_of)[None, :, None, None], pieces_out[:, None], jnp.zeros((), low)
    ).reshape(shards, rows_out, width)
    moved = lax.all_to_all(slots_out, "wshard", split_axis=0, concat_axis=0, tiled=True)
    moved = moved.reshape(per_block, shards // per_block, rows_out, width)
    mine_out = lax.dynamic_index_in_dim(moved, shard_rank % per_block, 0, keepdims=False)
    grad_out = mine_out.reshape(columns // per_block, width).astype(jnp.float32)

    rows = share_attn.shape[0]
    if fast:
        every_ffn, grad_down = gather_square([share_ffn, share_down], 7)
        every_attn = gather_square([share_attn], 8)[0]
    else:
        every_ffn, grad_down, every_attn = [gather(v, "seq") for v in (share_ffn, share_down, share_attn)]
    every_ffn = every_ffn.reshape((groups,) + share_ffn.shape)
    every_attn = every_attn.reshape((groups,) + share_attn.shape)
    if fast:
        grad_w_gate, grad_w_up, grad_down = join_units(every_ffn, grad_down, part)
        grads = join_columns(every_attn, columns, (0, columns, 2 * columns, front))
        vector = jnp.concatenate([grad_norm_attn, grad_norm_ffn, grad_bias])
        vector = jnp.pad(vector, (0, -vector.shape[0] % 1024)).reshape(-1, 128)
        vector = add_everywhere(vector, 9).reshape(-1)
        small = vector[:width], vector[width : 2 * width], vector[2 * width : 2 * width + heads]
    else:

        def join(first):
            taken = every_attn[:, :, first : first + columns]
            return taken.transpose(1, 0, 2).reshape(rows, width).astype(jnp.float32)

        def join_own_units(first):
            taken = every_ffn[:, :, first * units : (first + 1) * units]
            taken = taken.reshape(groups, rows, shards, part).transpose(1, 2, 0, 3)
            return taken.reshape(rows, hidden_size).astype(jnp.float32)

        grads = [join(first) for first in (0, columns, 2 * columns, front)]
        grad_w_gate, grad_w_up = join_own_units(0), join_own_units(1)
        grad_down = grad_down.astype(jnp.float32)
        small = lax.psum((grad_norm_attn, grad_norm_ffn, grad_bias), ("seq", "wshard"))

    grad_forget_w = every_attn[:, :, 3 * columns : 3 * columns + local_heads]
    grad_forget_w = grad_forget_w.transpose(1, 0, 2).reshape(rows, heads).astype(jnp.float32)
    return (
        layer_output,
        grad_input,
        small[0],
        *grads,
        grad_forget_w,
        small[2],
        grad_out,
        small[1],
        grad_w_gate,
        grad_w_up,
        grad_down,
    )


def solution(mesh):
    return jax.shard_map(
        on_device,
        mesh=mesh,
        in_specs=(
            P("wshard", "seq", None),
            P("wshard"),
            P(),
            P("wshard", None),
            P("wshard", None),
            P("wshard", None),
            P("wshard", None),
            P("wshard", None),
            P(),
            P("wshard", None),
            P(),
            P("wshard", None),
            P("wshard", None),
            P("wshard", None),
            P("wshard", "seq", None),
        ),
        out_specs=(
            P("wshard", "seq", None),
            P("wshard", "seq", None),
            P(),
            P("wshard", None),
            P("wshard", None),
            P("wshard", None),
            P("wshard", None),
            P("wshard", None),
            P(),
            P("wshard", None),
            P(),
            P("wshard", None),
            P("wshard", None),
            P("wshard", None),
        ),
        check_vma=False,
    )
```

```python
import jax
import jax.numpy as jnp
from jax import lax
from jax.experimental import pallas as pl
from jax.experimental.pallas import tpu as pltpu
from jax.sharding import PartitionSpec as P

EPS = 1e-06
NEG_FILL = -1e30
PAIR = 128


def product(left, right):
    return jnp.dot(left, right, preferred_element_type=jnp.float32)


def product_tn(left, right):
    return lax.dot_general(
        left, right, (((0,), (0,)), ((), ())), preferred_element_type=jnp.float32
    )


def product_nt(left, right):
    return lax.dot_general(
        left, right, (((1,), (1,)), ((), ())), preferred_element_type=jnp.float32
    )


def rms_norm(values, gain):
    return values * lax.rsqrt(jnp.mean(values * values, axis=-1, keepdims=True) + EPS) * gain


def gate_product(attended, gate_pre):
    return attended * jax.nn.sigmoid(gate_pre)


def swiglu(gate, upward):
    return jax.nn.silu(gate) * upward


def low_triangle(size):
    rows = lax.broadcasted_iota(jnp.int32, (size, size), 0)
    return rows <= lax.broadcasted_iota(jnp.int32, (size, size), 1)


def exact(left, right):
    return jnp.dot(left, right, precision=lax.Precision.HIGHEST, preferred_element_type=jnp.float32)


def attention_fwd(joined, bias, length, head_size, scale):
    slots = joined.shape[0]
    pairs = (joined.shape[1] // PAIR - 1) // 3
    tile = min(256, slots)
    some = 8

    def body(length_ref, q_ref, k_ref, v_ref, f_ref, bias_ref, o_ref, offset_ref, col_ref, logit_ref, row):
        pair = pl.program_id(0)

        @pl.when(pair == 0)
        def _():
            logits = f_ref[...].astype(jnp.float32) + bias_ref[...]
            logit_rows = logits.T[:some]
            logit_ref[...] = logit_rows
            logs = jnp.minimum(logit_rows, 0.0) - jnp.log1p(jnp.exp(-jnp.abs(logit_rows)))
            ones = low_triangle(tile).astype(jnp.float32)
            carry = jnp.zeros((some, 1), jnp.float32)
            for first in range(0, slots, tile):
                sums = exact(logs[:, first : first + tile], ones) + carry
                row[:, first : first + tile] = sums
                carry = sums[:, tile - 1 : tile]
            wide = jnp.concatenate([row[...], jnp.zeros((PAIR - some, slots), jnp.float32)], axis=0).T
            usable = lax.broadcasted_iota(jnp.int32, (slots, PAIR), 0) < length_ref[0]
            col_ref[...] = jnp.where(usable, wide, -NEG_FILL)

        key_all = k_ref[...]
        value_t = v_ref[...].T
        query_t = (q_ref[...].astype(jnp.float32) * scale).astype(jnp.bfloat16).T
        sub = lax.broadcasted_iota(jnp.int32, (PAIR, tile), 0)
        lanes = lax.broadcasted_iota(jnp.int32, (slots, PAIR), 1)
        diag = low_triangle(tile)
        columns = [
            jnp.sum(jnp.where(lanes == 2 * pair + a, col_ref[...], 0.0), axis=1, keepdims=True) for a in range(2)
        ]
        for number in range(slots // tile):
            first, last = number * tile, (number + 1) * tile
            outs = []
            for a in range(2):
                mine = (sub >= a * head_size) & (sub < (a + 1) * head_size)
                query = jnp.where(mine, query_t[:, first:last], jnp.zeros((), query_t.dtype))
                scores = product(key_all[:last], query)
                own_row = row[pl.ds(2 * pair + a, 1), first:last]
                scores = scores + (own_row - columns[a][:last])
                tail = jnp.where(diag, scores[first:], NEG_FILL)
                scores = tail if number == 0 else jnp.concatenate([scores[:first], tail], axis=0)
                top = jnp.max(scores, axis=0, keepdims=True)
                weights = jnp.exp(scores - top)
                total = jnp.sum(weights, axis=0, keepdims=True)
                mixed = product(
                    value_t[a * head_size : (a + 1) * head_size, :last], weights.astype(jnp.bfloat16)
                )
                outs.append(mixed / total)
                offset_ref[pl.ds(2 * pair + a, 1), first:last] = own_row - (top + jnp.log(total))
            o_ref[first:last, :] = jnp.concatenate(outs, axis=0).T.astype(o_ref.dtype)

    def lane(start):
        return pl.BlockSpec((slots, PAIR), lambda p, start=start: (0, start + p))

    def fixed(shape):
        return pl.BlockSpec(shape, lambda p: (0, 0))

    rows = jax.ShapeDtypeStruct((some, slots), jnp.float32)
    return pl.pallas_call(
        body,
        grid=(pairs,),
        in_specs=[
            pl.BlockSpec(memory_space=pltpu.SMEM),
            lane(0),
            lane(pairs),
            lane(2 * pairs),
            pl.BlockSpec((slots, PAIR), lambda p: (0, 3 * pairs)),
            fixed((1, PAIR)),
        ],
        out_specs=[lane(0), fixed((some, slots)), fixed((slots, PAIR)), fixed((some, slots))],
        out_shape=[
            jax.ShapeDtypeStruct((slots, pairs * PAIR), jnp.bfloat16),
            rows,
            jax.ShapeDtypeStruct((slots, PAIR), jnp.float32),
            rows,
        ],
        scratch_shapes=[pltpu.VMEM((some, slots), jnp.float32)],
        compiler_params=pltpu.CompilerParams(vmem_limit_bytes=56 << 20),
        cost_estimate=pl.CostEstimate(
            flops=4 * slots * slots * pairs * PAIR, bytes_accessed=8 * slots * pairs * PAIR, transcendentals=0
        ),
        name="attention_fwd",
    )(length, joined, joined, joined, joined, bias)


def backward_scratch(slots):
    return [
        pltpu.VMEM((slots, PAIR), jnp.float32),
        pltpu.VMEM((slots, PAIR), jnp.float32),
        pltpu.VMEM((slots, PAIR), jnp.float32),
        pltpu.VMEM((8, slots), jnp.float32),
    ]


class Backward:
    def __init__(self, joined, d_out, offset, col, logit, grads, dk_acc, dv_acc, dcol, drow, head_size, scale):
        self.joined, self.d_out, self.offset, self.col = joined, d_out, offset, col
        self.logit, self.grads, self.dk_acc, self.dv_acc = logit, grads, dk_acc, dv_acc
        self.dcol, self.drow, self.head_size, self.scale = dcol, drow, head_size, scale
        self.slots = joined.shape[0]
        self.pairs = (joined.shape[1] // PAIR - 1) // 3
        self.tile = min(256, self.slots)

    def start(self):
        self.dcol[...] = jnp.zeros_like(self.dcol)
        self.drow[...] = jnp.zeros_like(self.drow)

    def lanes(self, pair, part=0):
        return pl.ds(pl.multiple_of((part * self.pairs + pair) * PAIR, PAIR), PAIR)

    def pair(self, pair):
        slots, tile, half = self.slots, self.tile, self.head_size
        dk_acc, dv_acc, dcol, drow = self.dk_acc, self.dv_acc, self.dcol, self.drow
        queries = (self.joined[:, self.lanes(pair)].astype(jnp.float32) * self.scale).astype(jnp.bfloat16)
        key_all = self.joined[:, self.lanes(pair, 1)]
        value_all = self.joined[:, self.lanes(pair, 2)]
        d_out = self.d_out[:, self.lanes(pair)]
        query_t, key_t, dout_t = queries.T, key_all.T, d_out.T
        sub = lax.broadcasted_iota(jnp.int32, (PAIR, tile), 0)
        lanes = lax.broadcasted_iota(jnp.int32, (tile, PAIR), 1)
        wide = lax.broadcasted_iota(jnp.int32, (slots, PAIR), 1)
        diag = low_triangle(tile)
        zero = jnp.zeros((), jnp.bfloat16)
        columns = [
            jnp.sum(jnp.where(wide == 2 * pair + a, self.col[...], 0.0), axis=1, keepdims=True) for a in range(2)
        ]
        dk_acc[...] = jnp.zeros_like(dk_acc)
        dv_acc[...] = jnp.zeros_like(dv_acc)
        for number in range(slots // tile):
            first, last = number * tile, (number + 1) * tile
            outs = []
            for a in range(2):
                mine = (sub >= a * half) & (sub < (a + 1) * half)
                own = (lanes >= a * half) & (lanes < (a + 1) * half)
                at = pl.ds(2 * pair + a, 1)
                scores = product(key_all[:last], jnp.where(mine, query_t[:, first:last], zero))
                scores = scores + (self.offset[at, first:last] - columns[a][:last])
                tail = jnp.where(diag, scores[first:], NEG_FILL)
                scores = tail if number == 0 else jnp.concatenate([scores[:first], tail], axis=0)
                probs = jnp.exp(scores)
                d_probs = product(value_all[:last], jnp.where(mine, dout_t[:, first:last], zero))
                dot = jnp.sum(d_probs * probs, axis=0, keepdims=True)
                d_full = probs * (d_probs - dot)
                d_scores = d_full.astype(jnp.bfloat16)
                drow[at, first:last] = jnp.sum(d_full, axis=0, keepdims=True)
                sums = jnp.sum(d_full, axis=1, keepdims=True)
                dcol[:last, :] += jnp.where(wide[:last] == 2 * pair + a, sums, 0.0)
                outs.append(product(key_t[a * half : (a + 1) * half, :last], d_scores) * self.scale)
                dk_acc[:last, :] += product(d_scores, jnp.where(own, queries[first:last, :], zero))
                dv_acc[:last, :] += product(
                    probs.astype(jnp.bfloat16), jnp.where(own, d_out[first:last, :], zero)
                )
            self.grads[first:last, self.lanes(pair)] = jnp.concatenate(outs, axis=0).T.astype(self.grads.dtype)
        self.grads[:, self.lanes(pair, 1)] = dk_acc[...].astype(self.grads.dtype)
        self.grads[:, self.lanes(pair, 2)] = dv_acc[...].astype(self.grads.dtype)

    def end(self, bias_grad):
        slots, tile, some = self.slots, self.tile, 8
        change = self.drow[...] - self.dcol[...].T[:some]
        rows = lax.broadcasted_iota(jnp.int32, (tile, tile), 0)
        ones = (rows >= lax.broadcasted_iota(jnp.int32, (tile, tile), 1)).astype(jnp.float32)
        carry = jnp.zeros((some, 1), jnp.float32)
        pieces = []
        for first in reversed(range(0, slots, tile)):
            sums = exact(change[:, first : first + tile], ones) + carry
            carry = sums[:, :1]
            pieces.insert(0, sums)
        grad = jnp.concatenate(pieces, axis=1) * jax.nn.sigmoid(-self.logit[...])
        heads = lax.broadcasted_iota(jnp.int32, (some, slots), 0)
        grad = jnp.where(heads < 2 * self.pairs, grad, 0.0)
        bias_grad[...] = jnp.broadcast_to(jnp.sum(grad, axis=1, keepdims=True), bias_grad.shape)
        wide = jnp.concatenate([grad, jnp.zeros((PAIR - some, slots), jnp.float32)], axis=0).T
        self.grads[:, 3 * self.pairs * PAIR : (3 * self.pairs + 1) * PAIR] = wide.astype(self.grads.dtype)


def attention_bwd(joined, d_out, offset, col, logit, head_size, scale):
    slots, width = joined.shape
    pairs = (width // PAIR - 1) // 3

    def body(joined_ref, d_out_ref, offset_ref, col_ref, logit_ref, grads, bias_grad, *scratch):
        work = Backward(
            joined_ref, d_out_ref, offset_ref, col_ref, logit_ref, grads, *scratch, head_size, scale
        )
        work.start()

        def step(pair, carry):
            work.pair(pair)
            return carry

        lax.fori_loop(0, pairs, step, 0)
        work.end(bias_grad)

    vmem = pl.BlockSpec(memory_space=pltpu.VMEM)
    return pl.pallas_call(
        body,
        in_specs=[vmem] * 5,
        out_specs=[vmem] * 2,
        out_shape=[
            jax.ShapeDtypeStruct((slots, width), jnp.bfloat16),
            jax.ShapeDtypeStruct((8, PAIR), jnp.float32),
        ],
        scratch_shapes=backward_scratch(slots),
        compiler_params=pltpu.CompilerParams(vmem_limit_bytes=56 << 20),
        cost_estimate=pl.CostEstimate(
            flops=10 * slots * slots * pairs * PAIR, bytes_accessed=14 * slots * pairs * PAIR, transcendentals=0
        ),
        name="attention_bwd",
    )(joined, d_out, offset, col, logit)


MESH = pl.DeviceIdType.MESH
VMEM_LIMIT = 62 << 20


def square(groups):
    return groups == 4


def sides():
    rank = lax.axis_index("seq")
    return rank, rank + 1 - 2 * lax.rem(rank, 2), lax.rem(rank + 2, 4), 3 - rank


def meet(*others):
    barrier = pltpu.get_barrier_semaphore()
    for other in others:
        pl.semaphore_signal(barrier, inc=1, device_id=other, device_id_type=MESH)
    pl.semaphore_wait(barrier, len(others))


def push(source, target, send, recv, device):
    copy = pltpu.make_async_remote_copy(
        src_ref=source,
        dst_ref=target,
        send_sem=send,
        recv_sem=recv,
        device_id=device,
        device_id_type=MESH,
    )
    copy.start()
    return copy


class SquareGather:
    def __init__(self, own, full, send, recv):
        self.own, self.full, self.send, self.recv = own, full, send, recv
        self.rows = own.shape[0]
        self.half = self.rows // 2

    def place(self, rank, part):
        return self.full.at[pl.ds(pl.multiple_of(rank * self.rows + part * self.half, self.half), self.half)]

    def start(self):
        me, side, down, across = sides()
        mine = [self.own.at[pl.ds(part * self.half, self.half)] for part in (0, 1)]
        to_side, to_down = {"seq": side}, {"seq": down}
        self.first = push(mine[0], self.place(me, 0), self.send.at[0], self.recv.at[0], to_side)
        self.second = push(mine[1], self.place(me, 1), self.send.at[1], self.recv.at[1], to_down)
        self.third = push(mine[1], self.place(me, 1), self.send.at[2], self.recv.at[2], to_side)
        self.fourth = push(mine[0], self.place(me, 0), self.send.at[3], self.recv.at[3], to_down)

    def relay(self):
        me, side, down, across = sides()
        self.first.wait_recv()
        self.fifth = push(
            self.place(side, 0), self.place(side, 0), self.send.at[4], self.recv.at[4], {"seq": down}
        )
        self.second.wait_recv()
        self.sixth = push(
            self.place(down, 1), self.place(down, 1), self.send.at[5], self.recv.at[5], {"seq": side}
        )

    def near(self):
        self.third.wait_recv()
        self.fourth.wait_recv()

    def far(self):
        self.fifth.wait_recv()
        self.sixth.wait_recv()

    def finish(self):
        for copy in (self.first, self.second, self.third, self.fourth, self.fifth, self.sixth):
            copy.wait_send()


def gather_square(values, collective_id):
    count = len(values)

    def body(*refs):
        own, full = refs[:count], refs[count : 2 * count]
        send, recv, local = refs[2 * count :]
        me, side, down, across = sides()
        meet({"seq": side}, {"seq": down})
        jobs = [SquareGather(own[i], full[i], send.at[i], recv.at[i]) for i in range(count)]
        keeps = []
        for i, job in enumerate(jobs):
            job.start()
            rows = own[i].shape[0]
            keep = pltpu.make_async_copy(
                own[i], full[i].at[pl.ds(pl.multiple_of(me * rows, rows), rows)], local.at[i]
            )
            keep.start()
            keeps.append(keep)
        for job in jobs:
            job.relay()
        for job, keep in zip(jobs, keeps):
            job.near()
            job.far()
            job.finish()
            keep.wait()

    return pl.pallas_call(
        body,
        in_specs=[pl.BlockSpec(memory_space=pltpu.VMEM)] * count,
        out_specs=[pl.BlockSpec(memory_space=pl.ANY)] * count,
        out_shape=[jax.ShapeDtypeStruct((4 * v.shape[0],) + v.shape[1:], v.dtype) for v in values],
        scratch_shapes=[
            pltpu.SemaphoreType.DMA((count, 6)),
            pltpu.SemaphoreType.DMA((count, 6)),
            pltpu.SemaphoreType.DMA((count,)),
        ],
        compiler_params=pltpu.CompilerParams(
            collective_id=collective_id, has_side_effects=True, vmem_limit_bytes=VMEM_LIMIT
        ),
        name="gather_square",
    )(*values)


def block_product(left, right, transposed, tile, store):
    total = right.shape[0] if transposed else right.shape[1]

    def step(number, carry):
        columns = pl.ds(pl.multiple_of(number * tile, tile), tile)
        if transposed:
            store(columns, product_nt(left, right[columns, :]))
        else:
            store(columns, product(left, right[:, columns]))
        return carry

    lax.fori_loop(0, total // tile, step, 0)


def gather_product(own, weight, transposed, collective_id):
    rows, depth = own.shape
    width = weight.shape[0] if transposed else weight.shape[1]
    tile = 512 if width % 512 == 0 else 128 * (width // 128 // 3) if width % 384 == 0 else 128

    def body(own_ref, weight_ref, full, out, send, recv):
        me, side, down, across = sides()
        meet({"seq": side}, {"seq": down})
        job = SquareGather(own_ref, full, send, recv)
        job.start()

        def multiply(rank, block):
            at = pl.ds(pl.multiple_of(rank * rows, rows), rows)

            def store(columns, value):
                out[at, columns] = value.astype(out.dtype)

            block_product(block, weight_ref, transposed, tile, store)

        def arrived(rank):
            return full[pl.ds(pl.multiple_of(rank * rows, rows), rows), :]

        full[pl.ds(pl.multiple_of(me * rows, rows), rows), :] = own_ref[...]
        multiply(me, own_ref[...])
        job.relay()
        job.near()
        multiply(side, arrived(side))
        multiply(down, arrived(down))
        job.far()
        multiply(across, arrived(across))
        job.finish()

    vmem = pl.BlockSpec(memory_space=pltpu.VMEM)
    return pl.pallas_call(
        body,
        in_specs=[vmem, vmem],
        out_specs=[vmem, vmem],
        out_shape=[
            jax.ShapeDtypeStruct((4 * rows, depth), own.dtype),
            jax.ShapeDtypeStruct((4 * rows, width), jnp.float32),
        ],
        scratch_shapes=[pltpu.SemaphoreType.DMA((6,)), pltpu.SemaphoreType.DMA((6,))],
        compiler_params=pltpu.CompilerParams(
            collective_id=collective_id, has_side_effects=True, vmem_limit_bytes=VMEM_LIMIT
        ),
        name="gather_product",
    )(own, weight)


def transposed_product(left, right, out):
    tall = 512 if out.shape[0] % 512 == 0 else 384
    wide = next(size for size in (512, 384, 640, 128) if out.shape[1] % size == 0)
    across = out.shape[1] // wide

    def step(number, carry):
        rows = pl.ds(pl.multiple_of((number // across) * tall, tall), tall)
        columns = pl.ds(pl.multiple_of(lax.rem(number, across) * wide, wide), wide)
        out[rows, columns] = product_tn(left[:, rows], right[:, columns]).astype(out.dtype)
        return carry

    lax.fori_loop(0, (out.shape[0] // tall) * across, step, 0)


def line():
    shards, place = lax.axis_size("wshard"), lax.axis_index("wshard")
    chips = shards // 2
    chip, core = place // 2, lax.rem(place, 2)
    forth = {"wshard": lax.rem(place + 2, shards)}
    back = {"wshard": lax.rem(place + shards - 2, shards)}
    twin = {"wshard": place + 1 - 2 * core}
    return chips, chip, core, forth, back, twin


class LineGather:
    def __init__(self, own, full, forth_send, back_send, twin_send, recv, local):
        self.own, self.full, self.local = own, full, local
        self.sends = (forth_send, back_send, twin_send)
        self.recv = recv
        self.rows = own.shape[0]
        self.chips, self.chip, self.core, *self.devices = line()

    def place(self, chip, core):
        return self.full.at[pl.ds(pl.multiple_of((2 * chip + core) * self.rows, self.rows), self.rows)]

    def copy(self, way, chip, source=None):
        target = self.place(chip, self.core)
        return pltpu.make_async_remote_copy(
            src_ref=target if source is None else source,
            dst_ref=target,
            send_sem=self.sends[way].at[chip],
            recv_sem=self.recv.at[2 * chip + self.core],
            device_id=self.devices[way],
            device_id_type=MESH,
        )

    def wait_for(self, chip, core):
        target = self.place(chip, core)
        pltpu.make_async_remote_copy(
            src_ref=target,
            dst_ref=target,
            send_sem=self.sends[2].at[0],
            recv_sem=self.recv.at[2 * chip + core],
            device_id=self.devices[2],
            device_id_type=MESH,
        ).wait_recv()

    def start(self):
        @pl.when(self.chip < self.chips - 1)
        def _():
            self.copy(0, self.chip, self.own).start()

        @pl.when(self.chip > 0)
        def _():
            self.copy(1, self.chip, self.own).start()

        self.copy(2, self.chip, self.own).start()
        self.keep = pltpu.make_async_copy(self.own, self.place(self.chip, self.core), self.local)
        self.keep.start()

    def step(self, number):
        left, right = self.chip - number, self.chip + number

        @pl.when(left >= 0)
        def _():
            self.wait_for(left, self.core)

            @pl.when(self.chip < self.chips - 1)
            def _():
                self.copy(0, left).start()

            self.copy(2, left).start()

        @pl.when(right < self.chips)
        def _():
            self.wait_for(right, self.core)

            @pl.when(self.chip > 0)
            def _():
                self.copy(1, right).start()

            self.copy(2, right).start()

    def finish(self):
        for chip in range(self.chips):
            self.wait_for(chip, 1 - self.core)
            self.copy(2, chip).wait_send()

            @pl.when((chip <= self.chip) & (self.chip < self.chips - 1))
            def _():
                self.copy(0, chip).wait_send()

            @pl.when((chip >= self.chip) & (self.chip > 0))
            def _():
                self.copy(1, chip).wait_send()

        self.keep.wait()


class LineSpread:
    pieces = 4

    def __init__(self, own, whole, send, recv):
        self.own, self.whole, self.send, self.recv = own, whole, send, recv
        self.rows = own.shape[0] // self.pieces
        self.source = lax.axis_index("seq")
        self.chips, self.chip, self.core, *self.devices = line()
        self.goes = (
            (self.chip >= self.source) & (self.chip < self.chips - 1),
            (self.chip <= self.source) & (self.chip > 0),
        )

    def copy(self, way, piece):
        target = self.whole.at[self.core, pl.ds(piece * self.rows, self.rows)]
        return pltpu.make_async_remote_copy(
            src_ref=target,
            dst_ref=target,
            send_sem=self.send.at[way, piece],
            recv_sem=self.recv.at[way // 2, piece],
            device_id=self.devices[way],
            device_id_type=MESH,
        )

    def start(self):
        @pl.when(self.chip == self.source)
        def _():
            self.whole[self.core] = self.own[...]

    def step(self, piece):
        @pl.when(self.chip != self.source)
        def _():
            self.copy(0, piece).wait_recv()

        for way in (0, 1):

            @pl.when(self.goes[way])
            def _():
                self.copy(way, piece).start()

        self.copy(2, piece).start()

    def finish(self):
        for piece in range(self.pieces):
            other = self.whole.at[1 - self.core, pl.ds(piece * self.rows, self.rows)]
            pltpu.make_async_remote_copy(
                src_ref=other,
                dst_ref=other,
                send_sem=self.send.at[2, piece],
                recv_sem=self.recv.at[1, piece],
                device_id=self.devices[2],
                device_id_type=MESH,
            ).wait_recv()
            self.copy(2, piece).wait_send()
            for way in (0, 1):

                @pl.when(self.goes[way])
                def _():
                    self.copy(way, piece).wait_send()


def first_gather(first, second, weights, block, w_gate, w_up, part, collective_id):
    rows, width = block.shape
    shards = 2 * lax.axis_size("seq")
    chips = shards // 2
    units = w_gate.shape[1] // 4
    blocks = units // part

    def body(first_ref, second_ref, weights_ref, block_ref, gate_ref, up_ref,
             first_full, second_full, weights_full, whole, picked,
             send, recv, local, line_send, line_recv, spread_send, spread_recv, pick):
        me, side, down, across = sides()
        line_chips, chip, core, forth, back, twin = line()
        meet({"seq": side}, {"seq": down}, forth, back, twin)
        one = SquareGather(first_ref, first_full, send.at[0], recv.at[0])
        two = SquareGather(second_ref, second_full, send.at[1], recv.at[1])
        run = LineGather(
            weights_ref, weights_full, line_send.at[0], line_send.at[1], line_send.at[2], line_recv, local.at[2]
        )
        spread = LineSpread(block_ref, whole, spread_send, spread_recv)
        spread.start()
        one.start()
        run.start()
        keeps = []
        for index, (own, full) in enumerate(((first_ref, first_full), (second_ref, second_full))):
            size = own.shape[0]
            keep = pltpu.make_async_copy(
                own, full.at[pl.ds(pl.multiple_of(me * size, size), size)], local.at[index]
            )
            keep.start()
            keeps.append(keep)
        two.start()
        spread.step(0)
        for index, source in enumerate((gate_ref, up_ref)):
            for number in range(blocks):
                column = pl.multiple_of((number * 4 + me) * part, part)
                taken = pltpu.make_async_copy(
                    source.at[:, pl.ds(column, part)],
                    picked.at[:, pl.ds(index * units + number * part, part)],
                    pick.at[index, number],
                )
                taken.start()
                keeps.append(taken)
        run.step(1)
        one.relay()
        spread.step(1)
        run.step(2)
        two.relay()
        spread.step(2)
        run.step(3)
        spread.step(3)
        for job in (one, two):
            job.near()
            job.far()
            job.finish()
        for keep in keeps:
            keep.wait()
        run.finish()
        spread.finish()

    vmem = pl.BlockSpec(memory_space=pltpu.VMEM)
    anywhere = pl.BlockSpec(memory_space=pl.ANY)
    dma = pltpu.SemaphoreType.DMA
    return pl.pallas_call(
        body,
        in_specs=[vmem] * 4 + [anywhere] * 2,
        out_specs=[anywhere] * 3 + [vmem] * 2,
        out_shape=[
            jax.ShapeDtypeStruct((4 * first.shape[0],) + first.shape[1:], first.dtype),
            jax.ShapeDtypeStruct((4 * second.shape[0],) + second.shape[1:], second.dtype),
            jax.ShapeDtypeStruct((shards * weights.shape[0],) + weights.shape[1:], weights.dtype),
            jax.ShapeDtypeStruct((2, rows, width), block.dtype),
            jax.ShapeDtypeStruct((w_gate.shape[0], 2 * units), w_gate.dtype),
        ],
        scratch_shapes=[
            dma((2, 6)),
            dma((2, 6)),
            dma((3,)),
            dma((3, chips)),
            dma((shards,)),
            dma((3, LineSpread.pieces)),
            dma((2, LineSpread.pieces)),
            dma((2, blocks)),
        ],
        compiler_params=pltpu.CompilerParams(
            collective_id=collective_id, has_side_effects=True, vmem_limit_bytes=VMEM_LIMIT
        ),
        name="first_gather",
    )(first, second, weights, block, w_gate, w_up)


class Everywhere:
    def __init__(self, values, out, ranks, total, places, send, recv):
        self.values, self.out, self.ranks, self.total, self.places = values, out, ranks, total, places
        self.send, self.recv = send, recv
        self.groups, self.shards = ranks.shape[0], places.shape[0]
        self.rank, self.place = lax.axis_index("seq"), lax.axis_index("wshard")

    def others(self):
        return [{"seq": lax.rem(self.rank + k, self.groups)} for k in range(1, self.groups)]

    def along(self):
        return [{"wshard": lax.rem(self.place + k, self.shards)} for k in range(1, self.shards)]

    def start(self):
        self.first = [
            push(self.values, self.ranks.at[self.rank], self.send.at[k], self.recv.at[k], other)
            for k, other in enumerate(self.others())
        ]
        self.ranks[self.rank] = self.values[...]

    def relay(self):
        for copy in self.first:
            copy.wait()
        ranks, groups = self.ranks, self.groups
        self.total[...] = (ranks[0] + ranks[1]) + (ranks[2] + ranks[3])
        self.second = [
            push(self.total, self.places.at[self.place], self.send.at[groups + k], self.recv.at[groups + k], other)
            for k, other in enumerate(self.along())
        ]
        self.places[self.place] = self.total[...]

    def end(self):
        for copy in self.second:
            copy.wait()
        sums = [self.places[k] + self.places[k + 1] for k in range(0, self.shards, 2)]
        self.out[...] = (sums[0] + sums[1]) + (sums[2] + sums[3])


def last_gather(values, small, collective_id):
    count = len(values)
    groups = lax.axis_size("seq")
    shards = 2 * groups

    def body(*refs):
        own, small_ref = refs[:count], refs[count]
        full, small_out = refs[count + 1 : 2 * count + 1], refs[2 * count + 1]
        send, recv, local = refs[2 * count + 2 : 2 * count + 5]
        me, side, down, across = sides()
        total = Everywhere(small_ref, small_out, *refs[2 * count + 5 :])
        meet(*total.others(), *total.along())
        jobs = [SquareGather(own[i], full[i], send.at[i], recv.at[i]) for i in range(count)]
        total.start()
        keeps = []
        for i, job in enumerate(jobs):
            job.start()
            rows = own[i].shape[0]
            keep = pltpu.make_async_copy(
                own[i], full[i].at[pl.ds(pl.multiple_of(me * rows, rows), rows)], local.at[i]
            )
            keep.start()
            keeps.append(keep)
        total.relay()
        for job in jobs:
            job.relay()
        total.end()
        for job, keep in zip(jobs, keeps):
            job.near()
            job.far()
            job.finish()
            keep.wait()

    vmem = pl.BlockSpec(memory_space=pltpu.VMEM)
    dma = pltpu.SemaphoreType.DMA
    return pl.pallas_call(
        body,
        in_specs=[vmem] * (count + 1),
        out_specs=[pl.BlockSpec(memory_space=pl.ANY)] * count + [vmem],
        out_shape=[jax.ShapeDtypeStruct((4 * v.shape[0],) + v.shape[1:], v.dtype) for v in values]
        + [jax.ShapeDtypeStruct(small.shape, jnp.float32)],
        scratch_shapes=[
            dma((count, 6)),
            dma((count, 6)),
            dma((count,)),
            pltpu.VMEM((groups,) + small.shape, jnp.float32),
            pltpu.VMEM(small.shape, jnp.float32),
            pltpu.VMEM((shards,) + small.shape, jnp.float32),
            dma((groups + shards,)),
            dma((groups + shards,)),
        ],
        compiler_params=pltpu.CompilerParams(
            collective_id=collective_id, has_side_effects=True, vmem_limit_bytes=VMEM_LIMIT
        ),
        name="last_gather",
    )(*values, small)


def join_units(every, down, part):
    groups, rows, both = every.shape
    units = both // 2
    blocks = units // part
    steps = 4
    tall = rows // steps

    def body(every_ref, down_ref, gate_ref, up_ref, down_out):
        for half, out in enumerate((gate_ref, up_ref)):
            for group in range(groups):
                for block in range(blocks):
                    at = half * units + block * part
                    to = (block * groups + group) * part
                    out[:, to : to + part] = every_ref[group, :, at : at + part].astype(jnp.float32)
        down_out[...] = down_ref[...].astype(jnp.float32)

    wide = jax.ShapeDtypeStruct((rows, groups * units), jnp.float32)
    return pl.pallas_call(
        body,
        grid=(steps,),
        in_specs=[
            pl.BlockSpec((groups, tall, both), lambda i: (0, i, 0)),
            pl.BlockSpec((down.shape[0] // steps, down.shape[1]), lambda i: (i, 0)),
        ],
        out_specs=[pl.BlockSpec((tall, groups * units), lambda i: (i, 0))] * 2
        + [pl.BlockSpec((down.shape[0] // steps, down.shape[1]), lambda i: (i, 0))],
        out_shape=[wide, wide, jax.ShapeDtypeStruct(down.shape, jnp.float32)],
        name="join_units",
    )(every, down)


def join_columns(every, columns, starts):
    groups, rows, lanes = every.shape
    steps = 4
    tall = rows // steps

    def body(every_ref, *outs):
        for start, out in zip(starts, outs):
            for group in range(groups):
                out[:, group * columns : (group + 1) * columns] = every_ref[
                    group, :, start : start + columns
                ].astype(jnp.float32)

    wide = jax.ShapeDtypeStruct((rows, groups * columns), jnp.float32)
    return pl.pallas_call(
        body,
        grid=(steps,),
        in_specs=[pl.BlockSpec((groups, tall, lanes), lambda i: (0, i, 0))],
        out_specs=[pl.BlockSpec((tall, groups * columns), lambda i: (i, 0))] * len(starts),
        out_shape=[wide] * len(starts),
        name="join_columns",
    )(every)


class SquareScatter:
    @staticmethod
    def scratch(rows, width):
        half = rows // 2
        low = jnp.bfloat16
        return [
            pltpu.VMEM((rows, width), low),
            pltpu.VMEM((2, half, width), low),
            pltpu.VMEM((2, half, width), jnp.float32),
            pltpu.VMEM((6, half, width), low),
            pltpu.VMEM((2, half, width), low),
            pltpu.SemaphoreType.DMA((6,)),
            pltpu.SemaphoreType.DMA((6,)),
        ]

    def __init__(self, lefts, rights, transposed, out, far, near, kept, land, carry, send, recv):
        self.lefts, self.rights, self.transposed, self.out = lefts, rights, transposed, out
        self.far, self.near, self.kept, self.land, self.carry = far, near, kept, land, carry
        self.send, self.recv = send, recv
        self.rows, self.width = out.shape
        self.half = self.rows // 2
        self.tile = self.width // 3 if self.width % 384 == 0 else self.width

    def copy(self, index):
        me, side, down, across = sides()
        source = (
            self.far.at[pl.ds(0, self.half)],
            self.far.at[pl.ds(self.half, self.half)],
            self.near.at[0],
            self.near.at[1],
            self.carry.at[0],
            self.carry.at[1],
        )[index]
        return pltpu.make_async_remote_copy(
            src_ref=source,
            dst_ref=self.land.at[index],
            send_sem=self.send.at[index],
            recv_sem=self.recv.at[index],
            device_id={"seq": down if index in (0, 3, 5) else side},
            device_id_type=MESH,
        )

    def partial(self, rank, store):
        at = pl.ds(pl.multiple_of(rank * self.rows, self.rows), self.rows)

        def step(number, carried):
            columns = pl.ds(pl.multiple_of(number * self.tile, self.tile), self.tile)
            value = None
            for a, b in zip(self.lefts, self.rights):
                if self.transposed:
                    term = product_nt(a[at, :], b[columns, :])
                else:
                    term = product(a[at, :], b[:, columns])
                value = term if value is None else value + term
            store(columns, value)
            return carried

        lax.fori_loop(0, self.width // self.tile, step, 0)

    def begin(self):
        me, side, down, across = sides()
        half, far, near, kept = self.half, self.far, self.near, self.kept

        def store_far(columns, value):
            far[:, columns] = value.astype(far.dtype)

        def store_side(columns, value):
            kept[0, :, columns] = value[:half]
            near[0, :, columns] = value[half:].astype(near.dtype)

        def store_down(columns, value):
            near[1, :, columns] = value[:half].astype(near.dtype)
            kept[1, :, columns] = value[half:]

        self.partial(across, store_far)
        self.copy(0).start()
        self.copy(1).start()
        self.partial(side, store_side)
        self.copy(2).start()
        self.partial(down, store_down)
        self.copy(3).start()

    def relay(self):
        for index in (0, 1):
            self.copy(index).wait_recv()
            total = self.kept[index] + self.land[index].astype(jnp.float32)
            self.carry[index] = total.astype(self.carry.dtype)
            self.copy(4 + index).start()

    def own(self):
        out = self.out

        def store_own(columns, value):
            out[:, columns] = value

        self.partial(lax.axis_index("seq"), store_own)

    def end(self):
        for index in (2, 3, 4, 5):
            self.copy(index).wait_recv()
        land, half = self.land, self.half
        self.out[:half, :] += land[3].astype(jnp.float32) + land[4].astype(jnp.float32)
        self.out[half:, :] += land[2].astype(jnp.float32) + land[5].astype(jnp.float32)
        for index in range(6):
            self.copy(index).wait_send()


class LineScatter:
    @staticmethod
    def scratch(chips, rows, width):
        low = jnp.bfloat16
        dma = pltpu.SemaphoreType.DMA
        return [pltpu.VMEM((chips, rows, width), low)] * 3 + [dma((2, chips)), dma((3, chips))]

    def __init__(self, terms, out, twin_in, forth_in, back_in, send, recv):
        self.terms, self.out, self.twin_in = terms, out, twin_in
        self.forth_in, self.back_in, self.send, self.recv = forth_in, back_in, send, recv
        self.chips, self.chip, self.core, *self.devices = line()
        self.rows = twin_in.shape[1]

    def term(self, chip, core):
        return self.terms.at[pl.ds(pl.multiple_of((2 * chip + core) * self.rows, self.rows), self.rows)]

    def swap(self, chip):
        return pltpu.make_async_remote_copy(
            src_ref=self.term(chip, 1 - self.core),
            dst_ref=self.twin_in.at[chip],
            send_sem=self.send.at[0, chip],
            recv_sem=self.recv.at[0, chip],
            device_id=self.devices[2],
            device_id_type=MESH,
        )

    def hop(self, way, chip):
        return pltpu.make_async_remote_copy(
            src_ref=self.twin_in.at[chip],
            dst_ref=(self.forth_in, self.back_in)[way].at[chip],
            send_sem=self.send.at[1, chip],
            recv_sem=self.recv.at[1 + way, chip],
            device_id=self.devices[way],
            device_id_type=MESH,
        )

    def start(self):
        for chip in (self.chips - 1, 0, *range(1, self.chips - 1)):
            self.swap(chip).start()

    def pair(self, chip):
        return self.term(chip, self.core)[...].astype(jnp.float32) + self.twin_in[chip].astype(jnp.float32)

    def pass_on(self, way, chip, first):
        self.swap(chip).wait_recv()
        source = (self.forth_in, self.back_in)[way]

        @pl.when(first)
        def _():
            self.twin_in[chip] = self.pair(chip).astype(self.twin_in.dtype)

        @pl.when(jnp.logical_not(first))
        def _():
            self.hop(way, chip).wait_recv()
            total = self.pair(chip) + source[chip].astype(jnp.float32)
            self.twin_in[chip] = total.astype(self.twin_in.dtype)

        self.hop(way, chip).start()

    def step(self, number):
        forth, back = self.chips - number, number - 1
        low_end = self.chip < self.chips // 2

        @pl.when(low_end & (forth > self.chip))
        def _():
            self.pass_on(0, forth, self.chip == 0)

        @pl.when(back < self.chip)
        def _():
            self.pass_on(1, back, self.chip == self.chips - 1)

        @pl.when(jnp.logical_not(low_end) & (forth > self.chip))
        def _():
            self.pass_on(0, forth, self.chip == 0)

    def end(self):
        for chip in range(self.chips):

            @pl.when(self.chip == chip)
            def _():
                self.swap(chip).wait_recv()
                total = self.pair(chip)
                if chip > 0:
                    self.hop(0, chip).wait_recv()
                    total = total + self.forth_in[chip].astype(jnp.float32)
                if chip < self.chips - 1:
                    self.hop(1, chip).wait_recv()
                    total = total + self.back_in[chip].astype(jnp.float32)
                self.out[...] = total.astype(self.out.dtype)

            self.swap(chip).wait_send()

            @pl.when(self.chip != chip)
            def _():
                self.hop(0, chip).wait_send()


class LineCollect:
    pieces = 2

    @staticmethod
    def scratch(rows, width):
        low = jnp.bfloat16
        dma = pltpu.SemaphoreType.DMA
        pieces = LineCollect.pieces
        return [pltpu.VMEM((rows, width), low)] * 3 + [dma((2, pieces)), dma((3, pieces))]

    def __init__(self, terms, out, twin_in, forth_in, back_in, send, recv):
        self.terms, self.out, self.twin_in = terms, out, twin_in
        self.forth_in, self.back_in, self.send, self.recv = forth_in, back_in, send, recv
        self.target = lax.axis_index("seq")
        self.chips, self.chip, self.core, *self.devices = line()
        self.rows = twin_in.shape[0]
        self.tall = self.rows // self.pieces

    def at(self, piece):
        return pl.ds(piece * self.tall, self.tall)

    def term(self, piece, core):
        start = pl.multiple_of(core * self.rows + piece * self.tall, self.tall)
        return self.terms.at[pl.ds(start, self.tall)]

    def swap(self, piece):
        return pltpu.make_async_remote_copy(
            src_ref=self.term(piece, 1 - self.core),
            dst_ref=self.twin_in.at[self.at(piece)],
            send_sem=self.send.at[0, piece],
            recv_sem=self.recv.at[0, piece],
            device_id=self.devices[2],
            device_id_type=MESH,
        )

    def hop(self, way, piece):
        return pltpu.make_async_remote_copy(
            src_ref=self.out.at[self.at(piece)],
            dst_ref=(self.forth_in, self.back_in)[way].at[self.at(piece)],
            send_sem=self.send.at[1, piece],
            recv_sem=self.recv.at[1 + way, piece],
            device_id=self.devices[way],
            device_id_type=MESH,
        )

    def start(self):
        for piece in range(self.pieces):
            self.swap(piece).start()

    def add(self, piece):
        low = self.out.dtype
        self.swap(piece).wait_recv()
        total = self.term(piece, self.core)[...].astype(jnp.float32)
        total = total + self.twin_in[self.at(piece), :].astype(jnp.float32)
        self.out[self.at(piece), :] = total.astype(low)
        for way, there in enumerate(
            (
                (self.chip <= self.target) & (self.chip > 0),
                (self.chip >= self.target) & (self.chip < self.chips - 1),
            )
        ):

            @pl.when(there)
            def _():
                self.hop(way, piece).wait_recv()
                more = (self.forth_in, self.back_in)[way][self.at(piece), :].astype(jnp.float32)
                self.out[self.at(piece), :] = (self.out[self.at(piece), :].astype(jnp.float32) + more).astype(low)

    def level(self, number):
        for way, goes in enumerate(
            (
                (self.chip < self.target) & (self.chip == number),
                (self.chip > self.target) & (self.chips - 1 - self.chip == number),
            )
        ):

            @pl.when(goes)
            def _():
                for piece in range(self.pieces):
                    self.add(piece)
                    self.hop(way, piece).start()

    def end(self):
        @pl.when(self.chip == self.target)
        def _():
            for piece in range(self.pieces):
                self.add(piece)

        for piece in range(self.pieces):
            self.swap(piece).wait_send()

            @pl.when(self.chip != self.target)
            def _():
                self.hop(0, piece).wait_send()


class SquareSpread:
    def __init__(self, own, out, send, recv):
        self.own, self.out, self.send, self.recv = own, out, send, recv
        self.chip = line()[1]
        self.half = own.shape[0] // 2

    def copy(self, index):
        me, side, down, across = sides()
        if index < 2:
            source, target = self.own, self.out
        else:
            source = target = self.out.at[pl.ds((index - 2) * self.half, self.half)]
        return pltpu.make_async_remote_copy(
            src_ref=source,
            dst_ref=target,
            send_sem=self.send.at[index],
            recv_sem=self.recv.at[index],
            device_id={"seq": (side, down, down, side)[index]},
            device_id_type=MESH,
        )

    def roles(self):
        me, side, down, across = sides()
        return [self.chip == rank for rank in (me, side, down, across)]

    def start(self):
        @pl.when(self.roles()[0])
        def _():
            self.copy(0).start()
            self.copy(1).start()
            self.out[...] = self.own[...]

    def relay(self):
        for index in (0, 1):

            @pl.when(self.roles()[1 + index])
            def _():
                self.copy(index).wait_recv()
                self.copy(2 + index).start()

    def end(self):
        mine, by_side, by_down, far = self.roles()

        @pl.when(mine)
        def _():
            self.copy(0).wait_send()
            self.copy(1).wait_send()

        @pl.when(by_side)
        def _():
            self.copy(2).wait_send()

        @pl.when(by_down)
        def _():
            self.copy(3).wait_send()

        @pl.when(far)
        def _():
            self.copy(2).wait_recv()
            self.copy(3).wait_recv()


def product_scatter(lefts, rights, transposed, collective_id, extras=()):
    count = len(lefts)
    more = len(extras)
    rows = lefts[0].shape[0] // 4
    width = rights[0].shape[0] if transposed else rights[0].shape[1]

    def body(*refs):
        left, right = refs[:count], refs[count : 2 * count]
        sides_in = refs[2 * count : 2 * count + 2 * more]
        out = refs[2 * count + 2 * more]
        sides_out = refs[2 * count + 2 * more + 1 : 2 * count + 3 * more + 1]
        me, side, down, across = sides()
        meet({"seq": side}, {"seq": down})
        job = SquareScatter(left, right, transposed, out, *refs[2 * count + 3 * more + 1 :])
        job.begin()
        job.relay()
        job.own()
        for index in range(more):
            transposed_product(sides_in[2 * index], sides_in[2 * index + 1], sides_out[index])
        job.end()

    vmem = pl.BlockSpec(memory_space=pltpu.VMEM)
    return pl.pallas_call(
        body,
        in_specs=[vmem] * (2 * count + 2 * more),
        out_specs=[vmem] * (1 + more),
        out_shape=[jax.ShapeDtypeStruct((rows, width), jnp.float32)]
        + [jax.ShapeDtypeStruct((a.shape[1], b.shape[1]), jnp.bfloat16) for a, b in extras],
        scratch_shapes=SquareScatter.scratch(rows, width),
        compiler_params=pltpu.CompilerParams(
            collective_id=collective_id, has_side_effects=True, vmem_limit_bytes=VMEM_LIMIT
        ),
        name="product_scatter",
    )(*lefts, *rights, *(value for pair in extras for value in pair))


def middle_backward(joined, d_out, offset, col, logit, hidden, w_down, gated, grad_branch,
                    head_size, scale, collective_id):
    slots, lanes = joined.shape
    width = w_down.shape[1]
    tokens = slots // 4
    columns = gated.shape[1]

    def body(joined_ref, d_out_ref, offset_ref, col_ref, logit_ref, hidden_ref, down_ref, gated_ref, branch_ref,
             grads, bias_grad, lowered, collected, terms, *scratch):
        me, side, down, across = sides()
        chips, chip, core, forth, back, twin = line()
        meet({"seq": side}, {"seq": down}, forth, back, twin)
        work = Backward(
            joined_ref, d_out_ref, offset_ref, col_ref, logit_ref, grads, *scratch[:4], head_size, scale
        )
        job = SquareScatter([hidden_ref], [down_ref], False, lowered, *scratch[4:11])
        collect = LineCollect(terms, collected, *scratch[11:])
        transposed_product(gated_ref, branch_ref, terms)
        collect.start()
        job.begin()
        work.start()
        collect.level(0)

        def step(pair, carry):
            work.pair(pair)

            @pl.when(pair == 0)
            def _():
                job.relay()

            @pl.when(pair == 1)
            def _():
                collect.level(1)

            return carry

        lax.fori_loop(0, work.pairs, step, 0)
        collect.level(2)
        job.own()
        work.end(bias_grad)
        job.end()
        collect.end()

    vmem = pl.BlockSpec(memory_space=pltpu.VMEM)
    low = jnp.bfloat16
    return pl.pallas_call(
        body,
        in_specs=[vmem] * 9,
        out_specs=[vmem] * 4,
        out_shape=[
            jax.ShapeDtypeStruct((slots, lanes), low),
            jax.ShapeDtypeStruct((8, PAIR), jnp.float32),
            jax.ShapeDtypeStruct((tokens, width), jnp.float32),
            jax.ShapeDtypeStruct((columns // 2, width), low),
        ],
        scratch_shapes=[pltpu.VMEM((columns, width), low)]
        + backward_scratch(slots)
        + SquareScatter.scratch(tokens, width)
        + LineCollect.scratch(columns // 2, width),
        compiler_params=pltpu.CompilerParams(
            collective_id=collective_id, has_side_effects=True, vmem_limit_bytes=VMEM_LIMIT
        ),
        name="middle_backward",
    )(joined, d_out, offset, col, logit, hidden, w_down, gated, grad_branch)


def last_backward(grads, grad_gate_pre, normed, weights, collected, collective_id):
    slots, depth = normed.shape
    front = grads.shape[1]
    lanes = weights.shape[1]
    tokens = slots // 4
    shards = 2 * lax.axis_size("seq")
    rows = depth // shards

    def body(grads_ref, gate_ref, normed_ref, weights_ref, collected_ref, summed, share, spread_out, terms,
             spread_send, spread_recv, *scratch):
        me, side, down, across = sides()
        chips, chip, core, forth, back, twin = line()
        meet({"seq": side}, {"seq": down}, forth, back, twin)
        job = SquareScatter(
            [grads_ref, gate_ref],
            [weights_ref.at[:, pl.ds(0, front)], weights_ref.at[:, pl.ds(front, lanes - front)]],
            True,
            summed,
            *scratch[:7],
        )
        run = LineScatter(terms, share, *scratch[7:])
        spread = SquareSpread(collected_ref, spread_out, spread_send, spread_recv)
        transposed_product(normed_ref, grads_ref, terms.at[:, pl.ds(0, front)])
        transposed_product(normed_ref, gate_ref, terms.at[:, pl.ds(front, lanes - front)])
        run.start()
        spread.start()
        job.begin()
        run.step(1)
        job.relay()
        spread.relay()
        run.step(2)
        run.step(3)
        job.own()
        job.end()
        spread.end()
        run.end()

    vmem = pl.BlockSpec(memory_space=pltpu.VMEM)
    low = jnp.bfloat16
    return pl.pallas_call(
        body,
        in_specs=[vmem] * 5,
        out_specs=[vmem] * 3,
        out_shape=[
            jax.ShapeDtypeStruct((tokens, depth), jnp.float32),
            jax.ShapeDtypeStruct((rows, lanes), low),
            jax.ShapeDtypeStruct(collected.shape, low),
        ],
        scratch_shapes=[
            pltpu.VMEM((depth, lanes), low),
            pltpu.SemaphoreType.DMA((4,)),
            pltpu.SemaphoreType.DMA((4,)),
        ]
        + SquareScatter.scratch(tokens, depth)
        + LineScatter.scratch(shards // 2, rows, lanes),
        compiler_params=pltpu.CompilerParams(
            collective_id=collective_id, has_side_effects=True, vmem_limit_bytes=VMEM_LIMIT
        ),
        name="last_backward",
    )(grads, grad_gate_pre, normed, weights, collected)


def gather(value, axis_name):
    return lax.all_gather(value, axis_name, axis=0, tiled=True)


def scatter(value, axis_name):
    return lax.psum_scatter(value, axis_name, scatter_dimension=0, tiled=True)


def gather_multiply(own, weight, transposed, collective_id):
    if square(lax.axis_size("seq")):
        return gather_product(own, weight, transposed, collective_id)
    whole = gather(own, "seq")
    return whole, product_nt(whole, weight) if transposed else product(whole, weight)


def multiply_scatter(lefts, rights, transposed, collective_id, extras=()):
    if square(lax.axis_size("seq")):
        return product_scatter(lefts, rights, transposed, collective_id, extras)
    products = [product_tn(a, b).astype(jnp.bfloat16) for a, b in extras]
    total = sum(product_nt(a, b) if transposed else product(a, b) for a, b in zip(lefts, rights))
    return [scatter(total.astype(jnp.bfloat16), "seq").astype(jnp.float32), *products]


def on_device(
    layer_input,
    lengths,
    norm_attn,
    w_query,
    w_key,
    w_value,
    w_ogate,
    w_forget,
    forget_bias,
    w_out,
    norm_ffn,
    w_gate,
    w_up,
    w_down,
    output_grad,
):
    low = jnp.bfloat16
    tokens, width = layer_input.shape[1:]
    heads = forget_bias.shape[0]
    groups = lax.axis_size("seq")
    shards = lax.axis_size("wshard")
    fast = square(groups) and shards == 2 * groups
    local_heads = heads // groups
    head_size = width // heads
    columns = width // groups
    lanes = columns + -columns % PAIR
    front = 3 * lanes + PAIR
    slots = tokens * groups
    hidden_size = w_gate.shape[1]
    part = hidden_size // (groups * shards)
    units = shards * part
    scale = head_size ** (-0.5)
    length = lengths[0]
    seq_rank = lax.axis_index("seq")
    shard_rank = lax.axis_index("wshard")
    per_block = shards // groups
    positions = seq_rank * tokens + jnp.arange(tokens, dtype=jnp.int32)
    valid_slots = (positions < length)[:, None]
    inputs = layer_input[0].astype(jnp.float32)
    cotangent_low = jnp.where(valid_slots, output_grad[0], jnp.zeros((), low))
    cotangent = cotangent_low.astype(jnp.float32)

    def own_columns(weight, size):
        taken = lax.dynamic_slice_in_dim(weight, seq_rank * columns, columns, 1)
        return jnp.pad(taken, ((0, 0), (0, size - columns))) if size > columns else taken

    def own_units(weight):
        split = weight.reshape(weight.shape[0], shards, groups, part)
        mine = lax.dynamic_index_in_dim(split, seq_rank, 2, keepdims=False)
        return mine.reshape(weight.shape[0], units)

    own_forget = lax.dynamic_slice_in_dim(w_forget, seq_rank * local_heads, local_heads, 1)
    own_forget = jnp.pad(own_forget, ((0, 0), (0, PAIR - local_heads)))
    own_bias = lax.dynamic_slice_in_dim(forget_bias, seq_rank * local_heads, local_heads)
    own_bias = jnp.pad(own_bias, (0, PAIR - local_heads))[None]
    mine_attn = jnp.concatenate(
        [*(own_columns(w, lanes) for w in (w_query, w_key, w_value)), own_forget, own_columns(w_ogate, columns)],
        axis=1,
    )
    mine_down = lax.dynamic_slice_in_dim(w_down, seq_rank * part, part, 0)
    normed_attn_own = rms_norm(inputs, norm_attn).astype(low)
    if fast:
        normed_attn, cotangent_all, full_attn, full_out, mine_ffn = first_gather(
            normed_attn_own, cotangent_low, mine_attn, w_out, w_gate, w_up, part, 0
        )
        full_out = full_out.reshape(columns, width)
        mine_ffn, mine_down = lax.optimization_barrier((mine_ffn, mine_down))
    else:
        full_attn = gather(mine_attn, "wshard")
        normed_attn = gather(normed_attn_own, "seq")
        cotangent_all = gather(cotangent_low, "seq")
        full_out = lax.dynamic_slice_in_dim(gather(w_out, "wshard"), seq_rank * columns, columns, 0)
        mine_ffn = jnp.concatenate([own_units(w_gate), own_units(w_up)], axis=1)
    full_ffn = gather(mine_ffn, "wshard")
    full_down = gather(mine_down, "wshard")

    joined = product(normed_attn, full_attn[:, :front]).astype(low)
    gate_pre = product(normed_attn, full_attn[:, front:])
    attended_low, offset, col, logit = attention_fwd(joined, own_bias, lengths, head_size, scale)
    attended = attended_low[:, :columns].astype(jnp.float32)
    gated_full, pull_gate = jax.vjp(gate_product, attended, gate_pre)
    gated = gated_full.astype(low)
    (branch,) = multiply_scatter([gated], [full_out], False, 1)
    middle = inputs + branch
    normed_ffn_own, pull_ffn_norm = jax.vjp(rms_norm, middle, norm_ffn)
    normed_ffn, gate_up = gather_multiply(normed_ffn_own.astype(low), full_ffn, False, 2)
    hidden_full, pull_swiglu = jax.vjp(swiglu, gate_up[:, :units], gate_up[:, units:])
    hidden = hidden_full.astype(low)

    grad_w_down = product_tn(hidden, cotangent_all).astype(low)
    share_down = scatter(grad_w_down, "wshard")
    grad_hidden = product_nt(cotangent_all, full_down)
    grad_gate_full, grad_up_full = pull_swiglu(grad_hidden)
    grad_gate_up = jnp.concatenate([grad_gate_full.astype(low), grad_up_full.astype(low)], axis=1)
    grad_gate_up, grad_w_down = lax.optimization_barrier((grad_gate_up, grad_w_down))
    grad_normed_ffn, grad_w_ffn = multiply_scatter(
        [grad_gate_up], [full_ffn], True, 3, [(normed_ffn, grad_gate_up)]
    )
    share_ffn = scatter(grad_w_ffn, "wshard")
    grad_middle_part, grad_norm_ffn = pull_ffn_norm(grad_normed_ffn)
    grad_middle = cotangent + grad_middle_part
    grad_branch, grad_gated = gather_multiply(grad_middle.astype(low), full_out, True, 4)
    grad_attended_full, grad_gate_pre_full = pull_gate(grad_gated)
    grad_attended = grad_attended_full.astype(low)
    grad_gate_pre = grad_gate_pre_full.astype(low)
    if lanes > columns:
        grad_attended = jnp.pad(grad_attended, ((0, 0), (0, lanes - columns)))
    if fast:
        grads, bias_rows, lowered, collected = middle_backward(
            joined, grad_attended, offset, col, logit, hidden, full_down, gated, grad_branch, head_size, scale, 5
        )
        grad_normed_attn, share_attn, grad_out = last_backward(
            grads, grad_gate_pre, normed_attn, full_attn, collected, 6
        )
        grad_out = grad_out.astype(jnp.float32)
    else:
        grads, bias_rows = attention_bwd(joined, grad_attended, offset, col, logit, head_size, scale)
        grad_projected = jnp.concatenate([grads, grad_gate_pre], axis=1)
        share_attn = scatter(product_tn(normed_attn, grad_projected).astype(low), "wshard")
        grad_normed_attn = scatter(product_nt(grad_projected, full_attn).astype(low), "seq").astype(jnp.float32)
        lowered = scatter(product(hidden, full_down).astype(low), "seq").astype(jnp.float32)
        share_out = scatter(product_tn(gated, grad_branch).astype(low), "wshard")
        rows_out = columns // shards
        pieces_out = lax.all_gather(share_out, "seq", axis=0, tiled=False)
        takes = shards // per_block
        slots_out = jnp.where(
            (jnp.arange(per_block) == shard_rank // takes)[None, :, None, None],
            pieces_out[:, None],
            jnp.zeros((), low),
        ).reshape(shards, rows_out, width)
        moved = lax.all_to_all(slots_out, "wshard", split_axis=0, concat_axis=0, tiled=True)
        moved = moved.reshape(per_block, takes, rows_out, width)
        mine_out = lax.dynamic_index_in_dim(moved, shard_rank % per_block, 0, keepdims=False)
        grad_out = mine_out.reshape(columns // per_block, width).astype(jnp.float32)
    layer_output = (middle + lowered).astype(low)[None]
    grad_bias = lax.dynamic_update_slice_in_dim(
        jnp.zeros((heads,), jnp.float32), bias_rows[:local_heads, 0], seq_rank * local_heads, 0
    )
    unused_normed, pull_attn_norm = jax.vjp(rms_norm, inputs, norm_attn)
    grad_input_part, grad_norm_attn = pull_attn_norm(grad_normed_attn)
    grad_input = (grad_middle + grad_input_part)[None]

    rows = share_attn.shape[0]
    if fast:
        vector = jnp.concatenate([grad_norm_attn, grad_norm_ffn, grad_bias])
        vector = jnp.pad(vector, (0, -vector.shape[0] % 1024)).reshape(-1, 128)
        every_attn, every_ffn, grad_down, vector = last_gather([share_attn, share_ffn, share_down], vector, 7)
        vector = vector.reshape(-1)
        small = vector[:width], vector[width : 2 * width], vector[2 * width : 2 * width + heads]
    else:
        every_attn, every_ffn, grad_down = [gather(v, "seq") for v in (share_attn, share_ffn, share_down)]
        small = lax.psum((grad_norm_attn, grad_norm_ffn, grad_bias), ("seq", "wshard"))
    every_ffn = every_ffn.reshape((groups,) + share_ffn.shape)
    every_attn = every_attn.reshape((groups,) + share_attn.shape)
    starts = (0, lanes, 2 * lanes, front)
    if fast:
        grad_w_gate, grad_w_up, grad_down = join_units(every_ffn, grad_down, part)
        weight_grads = join_columns(every_attn, columns, starts)
    else:

        def join(first):
            taken = every_attn[:, :, first : first + columns]
            return taken.transpose(1, 0, 2).reshape(rows, width).astype(jnp.float32)

        def join_own_units(first):
            taken = every_ffn[:, :, first * units : (first + 1) * units]
            taken = taken.reshape(groups, rows, shards, part).transpose(1, 2, 0, 3)
            return taken.reshape(rows, hidden_size).astype(jnp.float32)

        weight_grads = [join(first) for first in starts]
        grad_w_gate, grad_w_up = join_own_units(0), join_own_units(1)
        grad_down = grad_down.astype(jnp.float32)

    grad_forget_w = every_attn[:, :, 3 * lanes : 3 * lanes + local_heads]
    grad_forget_w = grad_forget_w.transpose(1, 0, 2).reshape(rows, heads).astype(jnp.float32)
    return (
        layer_output,
        grad_input,
        small[0],
        *weight_grads,
        grad_forget_w,
        small[2],
        grad_out,
        small[1],
        grad_w_gate,
        grad_w_up,
        grad_down,
    )


def solution(mesh):
    return jax.shard_map(
        on_device,
        mesh=mesh,
        in_specs=(
            P("wshard", "seq", None),
            P("wshard"),
            P(),
            P("wshard", None),
            P("wshard", None),
            P("wshard", None),
            P("wshard", None),
            P("wshard", None),
            P(),
            P("wshard", None),
            P(),
            P("wshard", None),
            P("wshard", None),
            P("wshard", None),
            P("wshard", "seq", None),
        ),
        out_specs=(
            P("wshard", "seq", None),
            P("wshard", "seq", None),
            P(),
            P("wshard", None),
            P("wshard", None),
            P("wshard", None),
            P("wshard", None),
            P("wshard", None),
            P(),
            P("wshard", None),
            P(),
            P("wshard", None),
            P("wshard", None),
            P("wshard", None),
        ),
        check_vma=False,
    )
```

```python
import jax
import jax.numpy as jnp
from jax import lax
from jax.experimental import pallas as pl
from jax.experimental.pallas import tpu as pltpu
from jax.sharding import PartitionSpec as P

EPS = 1e-06
NEG_FILL = -1e30
PAIR = 128


def product(left, right):
    return jnp.dot(left, right, preferred_element_type=jnp.float32)


def product_tn(left, right):
    return lax.dot_general(
        left, right, (((0,), (0,)), ((), ())), preferred_element_type=jnp.float32
    )


def product_nt(left, right):
    return lax.dot_general(
        left, right, (((1,), (1,)), ((), ())), preferred_element_type=jnp.float32
    )


def rms_norm(values, gain):
    return values * lax.rsqrt(jnp.mean(values * values, axis=-1, keepdims=True) + EPS) * gain


def gate_product(attended, gate_pre):
    return attended * jax.nn.sigmoid(gate_pre)


def swiglu(gate, upward):
    return jax.nn.silu(gate) * upward


def low_triangle(size):
    rows = lax.broadcasted_iota(jnp.int32, (size, size), 0)
    return rows <= lax.broadcasted_iota(jnp.int32, (size, size), 1)


def exact(left, right):
    return jnp.dot(left, right, precision=lax.Precision.HIGHEST, preferred_element_type=jnp.float32)


class Forward:
    some = 8

    def __init__(self, joined, bias, length, attended, offset, col, logit, row, head_size, scale):
        self.joined, self.bias, self.length = joined, bias, length
        self.attended, self.offset, self.col, self.logit, self.row = attended, offset, col, logit, row
        self.head_size, self.scale = head_size, scale
        self.slots = joined.shape[0]
        self.pairs = (joined.shape[1] // PAIR - 1) // 3
        self.tile = min(256, self.slots)

    @staticmethod
    def results(slots, pairs):
        rows = jax.ShapeDtypeStruct((Forward.some, slots), jnp.float32)
        return [
            jax.ShapeDtypeStruct((slots, pairs * PAIR), jnp.bfloat16),
            rows,
            jax.ShapeDtypeStruct((slots, PAIR), jnp.float32),
            rows,
        ]

    def lanes(self, pair, part=0):
        return pl.ds(pl.multiple_of((part * self.pairs + pair) * PAIR, PAIR), PAIR)

    def start(self):
        slots, tile, some = self.slots, self.tile, self.some
        logits = self.joined[:, 3 * self.pairs * PAIR :].astype(jnp.float32) + self.bias[...]
        logit_rows = logits.T[:some]
        self.logit[...] = logit_rows
        logs = jnp.minimum(logit_rows, 0.0) - jnp.log1p(jnp.exp(-jnp.abs(logit_rows)))
        ones = low_triangle(tile).astype(jnp.float32)
        carry = jnp.zeros((some, 1), jnp.float32)
        for first in range(0, slots, tile):
            sums = exact(logs[:, first : first + tile], ones) + carry
            self.row[:, first : first + tile] = sums
            carry = sums[:, tile - 1 : tile]
        wide = jnp.concatenate([self.row[...], jnp.zeros((PAIR - some, slots), jnp.float32)], axis=0).T
        usable = lax.broadcasted_iota(jnp.int32, (slots, PAIR), 0) < self.length[...]
        self.col[...] = jnp.where(usable, wide, -NEG_FILL)

    def pair(self, pair):
        slots, tile, half = self.slots, self.tile, self.head_size
        key_all = self.joined[:, self.lanes(pair, 1)]
        value_t = self.joined[:, self.lanes(pair, 2)].T
        query_t = (self.joined[:, self.lanes(pair)].astype(jnp.float32) * self.scale).astype(jnp.bfloat16).T
        sub = lax.broadcasted_iota(jnp.int32, (PAIR, tile), 0)
        wide = lax.broadcasted_iota(jnp.int32, (slots, PAIR), 1)
        diag = low_triangle(tile)
        columns = [
            jnp.sum(jnp.where(wide == 2 * pair + a, self.col[...], 0.0), axis=1, keepdims=True) for a in range(2)
        ]
        for number in range(slots // tile):
            first, last = number * tile, (number + 1) * tile
            outs = []
            for a in range(2):
                mine = (sub >= a * half) & (sub < (a + 1) * half)
                at = pl.ds(2 * pair + a, 1)
                query = jnp.where(mine, query_t[:, first:last], jnp.zeros((), query_t.dtype))
                scores = product(key_all[:last], query)
                own_row = self.row[at, first:last]
                scores = scores + (own_row - columns[a][:last])
                tail = jnp.where(diag, scores[first:], NEG_FILL)
                scores = tail if number == 0 else jnp.concatenate([scores[:first], tail], axis=0)
                top = jnp.max(scores, axis=0, keepdims=True)
                weights = jnp.exp(scores - top)
                total = jnp.sum(weights, axis=0, keepdims=True)
                mixed = product(value_t[a * half : (a + 1) * half, :last], weights.astype(jnp.bfloat16))
                outs.append(mixed / total)
                self.offset[at, first:last] = own_row - (top + jnp.log(total))
            self.attended[first:last, self.lanes(pair)] = jnp.concatenate(outs, axis=0).T.astype(jnp.bfloat16)


def attention_fwd(joined, bias, length, head_size, scale):
    slots = joined.shape[0]
    pairs = (joined.shape[1] // PAIR - 1) // 3

    def body(joined_ref, bias_ref, length_ref, attended, offset, col, logit, row):
        work = Forward(joined_ref, bias_ref, length_ref, attended, offset, col, logit, row, head_size, scale)
        work.start()
        offset[...] = jnp.zeros_like(offset)

        def step(pair, carry):
            work.pair(pair)
            return carry

        lax.fori_loop(0, pairs, step, 0)

    vmem = pl.BlockSpec(memory_space=pltpu.VMEM)
    return pl.pallas_call(
        body,
        in_specs=[vmem] * 3,
        out_specs=[vmem] * 4,
        out_shape=Forward.results(slots, pairs),
        scratch_shapes=[pltpu.VMEM((Forward.some, slots), jnp.float32)],
        compiler_params=pltpu.CompilerParams(vmem_limit_bytes=56 << 20),
        cost_estimate=pl.CostEstimate(
            flops=4 * slots * slots * pairs * PAIR, bytes_accessed=8 * slots * pairs * PAIR, transcendentals=0
        ),
        name="attention_fwd",
    )(joined, bias, length)


def backward_scratch(slots):
    return [
        pltpu.VMEM((slots, PAIR), jnp.float32),
        pltpu.VMEM((slots, PAIR), jnp.float32),
        pltpu.VMEM((slots, PAIR), jnp.float32),
        pltpu.VMEM((8, slots), jnp.float32),
    ]


class Backward:
    def __init__(self, joined, d_out, offset, col, logit, grads, dk_acc, dv_acc, dcol, drow, head_size, scale):
        self.joined, self.d_out, self.offset, self.col = joined, d_out, offset, col
        self.logit, self.grads, self.dk_acc, self.dv_acc = logit, grads, dk_acc, dv_acc
        self.dcol, self.drow, self.head_size, self.scale = dcol, drow, head_size, scale
        self.slots = joined.shape[0]
        self.pairs = (joined.shape[1] // PAIR - 1) // 3
        self.tile = min(256, self.slots)

    def start(self):
        self.dcol[...] = jnp.zeros_like(self.dcol)
        self.drow[...] = jnp.zeros_like(self.drow)

    def lanes(self, pair, part=0):
        return pl.ds(pl.multiple_of((part * self.pairs + pair) * PAIR, PAIR), PAIR)

    def pair(self, pair):
        slots, tile, half = self.slots, self.tile, self.head_size
        dk_acc, dv_acc, dcol, drow = self.dk_acc, self.dv_acc, self.dcol, self.drow
        queries = (self.joined[:, self.lanes(pair)].astype(jnp.float32) * self.scale).astype(jnp.bfloat16)
        key_all = self.joined[:, self.lanes(pair, 1)]
        value_all = self.joined[:, self.lanes(pair, 2)]
        d_out = self.d_out[:, self.lanes(pair)]
        query_t, key_t, dout_t = queries.T, key_all.T, d_out.T
        sub = lax.broadcasted_iota(jnp.int32, (PAIR, tile), 0)
        lanes = lax.broadcasted_iota(jnp.int32, (tile, PAIR), 1)
        wide = lax.broadcasted_iota(jnp.int32, (slots, PAIR), 1)
        diag = low_triangle(tile)
        zero = jnp.zeros((), jnp.bfloat16)
        columns = [
            jnp.sum(jnp.where(wide == 2 * pair + a, self.col[...], 0.0), axis=1, keepdims=True) for a in range(2)
        ]
        dk_acc[...] = jnp.zeros_like(dk_acc)
        dv_acc[...] = jnp.zeros_like(dv_acc)
        for number in range(slots // tile):
            first, last = number * tile, (number + 1) * tile
            outs = []
            for a in range(2):
                mine = (sub >= a * half) & (sub < (a + 1) * half)
                own = (lanes >= a * half) & (lanes < (a + 1) * half)
                at = pl.ds(2 * pair + a, 1)
                scores = product(key_all[:last], jnp.where(mine, query_t[:, first:last], zero))
                scores = scores + (self.offset[at, first:last] - columns[a][:last])
                tail = jnp.where(diag, scores[first:], NEG_FILL)
                scores = tail if number == 0 else jnp.concatenate([scores[:first], tail], axis=0)
                probs = jnp.exp(scores)
                d_probs = product(value_all[:last], jnp.where(mine, dout_t[:, first:last], zero))
                dot = jnp.sum(d_probs * probs, axis=0, keepdims=True)
                d_full = probs * (d_probs - dot)
                d_scores = d_full.astype(jnp.bfloat16)
                drow[at, first:last] = jnp.sum(d_full, axis=0, keepdims=True)
                sums = jnp.sum(d_full, axis=1, keepdims=True)
                dcol[:last, :] += jnp.where(wide[:last] == 2 * pair + a, sums, 0.0)
                outs.append(product(key_t[a * half : (a + 1) * half, :last], d_scores) * self.scale)
                dk_acc[:last, :] += product(d_scores, jnp.where(own, queries[first:last, :], zero))
                dv_acc[:last, :] += product(
                    probs.astype(jnp.bfloat16), jnp.where(own, d_out[first:last, :], zero)
                )
            self.grads[first:last, self.lanes(pair)] = jnp.concatenate(outs, axis=0).T.astype(self.grads.dtype)
        self.grads[:, self.lanes(pair, 1)] = dk_acc[...].astype(self.grads.dtype)
        self.grads[:, self.lanes(pair, 2)] = dv_acc[...].astype(self.grads.dtype)

    def end(self, bias_grad):
        slots, tile, some = self.slots, self.tile, 8
        change = self.drow[...] - self.dcol[...].T[:some]
        rows = lax.broadcasted_iota(jnp.int32, (tile, tile), 0)
        ones = (rows >= lax.broadcasted_iota(jnp.int32, (tile, tile), 1)).astype(jnp.float32)
        carry = jnp.zeros((some, 1), jnp.float32)
        pieces = []
        for first in reversed(range(0, slots, tile)):
            sums = exact(change[:, first : first + tile], ones) + carry
            carry = sums[:, :1]
            pieces.insert(0, sums)
        grad = jnp.concatenate(pieces, axis=1) * jax.nn.sigmoid(-self.logit[...])
        heads = lax.broadcasted_iota(jnp.int32, (some, slots), 0)
        grad = jnp.where(heads < 2 * self.pairs, grad, 0.0)
        bias_grad[...] = jnp.broadcast_to(jnp.sum(grad, axis=1, keepdims=True), bias_grad.shape)
        wide = jnp.concatenate([grad, jnp.zeros((PAIR - some, slots), jnp.float32)], axis=0).T
        self.grads[:, 3 * self.pairs * PAIR : (3 * self.pairs + 1) * PAIR] = wide.astype(self.grads.dtype)


def attention_bwd(joined, d_out, offset, col, logit, head_size, scale):
    slots, width = joined.shape
    pairs = (width // PAIR - 1) // 3

    def body(joined_ref, d_out_ref, offset_ref, col_ref, logit_ref, grads, bias_grad, *scratch):
        work = Backward(
            joined_ref, d_out_ref, offset_ref, col_ref, logit_ref, grads, *scratch, head_size, scale
        )
        work.start()

        def step(pair, carry):
            work.pair(pair)
            return carry

        lax.fori_loop(0, pairs, step, 0)
        work.end(bias_grad)

    vmem = pl.BlockSpec(memory_space=pltpu.VMEM)
    return pl.pallas_call(
        body,
        in_specs=[vmem] * 5,
        out_specs=[vmem] * 2,
        out_shape=[
            jax.ShapeDtypeStruct((slots, width), jnp.bfloat16),
            jax.ShapeDtypeStruct((8, PAIR), jnp.float32),
        ],
        scratch_shapes=backward_scratch(slots),
        compiler_params=pltpu.CompilerParams(vmem_limit_bytes=56 << 20),
        cost_estimate=pl.CostEstimate(
            flops=10 * slots * slots * pairs * PAIR, bytes_accessed=14 * slots * pairs * PAIR, transcendentals=0
        ),
        name="attention_bwd",
    )(joined, d_out, offset, col, logit)


MESH = pl.DeviceIdType.MESH
VMEM_LIMIT = 62 << 20


def square(groups):
    return groups == 4


def sides():
    rank = lax.axis_index("seq")
    return rank, rank + 1 - 2 * lax.rem(rank, 2), lax.rem(rank + 2, 4), 3 - rank


def meet(*others):
    barrier = pltpu.get_barrier_semaphore()
    for other in others:
        pl.semaphore_signal(barrier, inc=1, device_id=other, device_id_type=MESH)
    pl.semaphore_wait(barrier, len(others))


def push(source, target, send, recv, device):
    copy = pltpu.make_async_remote_copy(
        src_ref=source,
        dst_ref=target,
        send_sem=send,
        recv_sem=recv,
        device_id=device,
        device_id_type=MESH,
    )
    copy.start()
    return copy


class SquareGather:
    def __init__(self, own, full, send, recv):
        self.own, self.full, self.send, self.recv = own, full, send, recv
        self.rows = own.shape[0]
        self.half = self.rows // 2

    def place(self, rank, part):
        return self.full.at[pl.ds(pl.multiple_of(rank * self.rows + part * self.half, self.half), self.half)]

    def copy(self, index):
        me, side, down, across = sides()
        mine = [self.own.at[pl.ds(part * self.half, self.half)] for part in (0, 1)]
        source, target, peer = (
            (mine[0], self.place(me, 0), side),
            (mine[1], self.place(me, 1), down),
            (mine[1], self.place(me, 1), side),
            (mine[0], self.place(me, 0), down),
            (self.place(side, 0), self.place(side, 0), down),
            (self.place(down, 1), self.place(down, 1), side),
        )[index]
        return pltpu.make_async_remote_copy(
            src_ref=source,
            dst_ref=target,
            send_sem=self.send.at[index],
            recv_sem=self.recv.at[index],
            device_id={"seq": peer},
            device_id_type=MESH,
        )

    def start(self):
        for index in range(4):
            self.copy(index).start()

    def relay(self):
        for index in (0, 1):
            self.copy(index).wait_recv()
            self.copy(4 + index).start()

    def near(self):
        self.copy(2).wait_recv()
        self.copy(3).wait_recv()

    def far(self):
        self.copy(4).wait_recv()
        self.copy(5).wait_recv()

    def finish(self):
        for index in range(6):
            self.copy(index).wait_send()


def block_product(left, right, transposed, tile, store):
    total = right.shape[0] if transposed else right.shape[1]

    def step(number, carry):
        columns = pl.ds(pl.multiple_of(number * tile, tile), tile)
        if transposed:
            store(columns, product_nt(left[...], right[columns, :]))
        else:
            store(columns, product(left[...], right[:, columns]))
        return carry

    lax.fori_loop(0, total // tile, step, 0)


def gather_product(own, weight, transposed, collective_id):
    rows, depth = own.shape
    width = weight.shape[0] if transposed else weight.shape[1]
    tile = 512 if width % 512 == 0 else 128 * (width // 128 // 3) if width % 384 == 0 else 128

    def body(own_ref, weight_ref, full, out, send, recv):
        me, side, down, across = sides()
        meet({"seq": side}, {"seq": down})
        job = SquareGather(own_ref, full, send, recv)
        job.start()

        def multiply(rank, block):
            at = pl.ds(pl.multiple_of(rank * rows, rows), rows)

            def store(columns, value):
                out[at, columns] = value.astype(out.dtype)

            block_product(block, weight_ref, transposed, tile, store)

        def arrived(rank):
            return full[pl.ds(pl.multiple_of(rank * rows, rows), rows), :]

        full[pl.ds(pl.multiple_of(me * rows, rows), rows), :] = own_ref[...]
        multiply(me, own_ref[...])
        job.relay()
        job.near()
        multiply(side, arrived(side))
        multiply(down, arrived(down))
        job.far()
        multiply(across, arrived(across))
        job.finish()

    vmem = pl.BlockSpec(memory_space=pltpu.VMEM)
    return pl.pallas_call(
        body,
        in_specs=[vmem, vmem],
        out_specs=[vmem, vmem],
        out_shape=[
            jax.ShapeDtypeStruct((4 * rows, depth), own.dtype),
            jax.ShapeDtypeStruct((4 * rows, width), jnp.float32),
        ],
        scratch_shapes=[pltpu.SemaphoreType.DMA((6,)), pltpu.SemaphoreType.DMA((6,))],
        compiler_params=pltpu.CompilerParams(
            collective_id=collective_id, has_side_effects=True, vmem_limit_bytes=VMEM_LIMIT
        ),
        name="gather_product",
    )(own, weight)


def transposed_product(left, right, out):
    tall = 512 if out.shape[0] % 512 == 0 else 384
    wide = next(size for size in (512, 384, 640, 128) if out.shape[1] % size == 0)
    across = out.shape[1] // wide

    def step(number, carry):
        rows = pl.ds(pl.multiple_of((number // across) * tall, tall), tall)
        columns = pl.ds(pl.multiple_of(lax.rem(number, across) * wide, wide), wide)
        out[rows, columns] = product_tn(left[:, rows], right[:, columns]).astype(out.dtype)
        return carry

    lax.fori_loop(0, (out.shape[0] // tall) * across, step, 0)


def line():
    shards, place = lax.axis_size("wshard"), lax.axis_index("wshard")
    chips = shards // 2
    chip, core = place // 2, lax.rem(place, 2)
    forth = {"wshard": lax.rem(place + 2, shards)}
    back = {"wshard": lax.rem(place + shards - 2, shards)}
    twin = {"wshard": place + 1 - 2 * core}
    return chips, chip, core, forth, back, twin


class LineGather:
    @staticmethod
    def scratch(chips):
        dma = pltpu.SemaphoreType.DMA
        return [dma((3, chips)), dma((2 * chips,)), dma((1,))]

    def __init__(self, own, full, send, recv, local):
        self.own, self.full, self.local = own, full, local.at[0]
        self.sends = (send.at[0], send.at[1], send.at[2])
        self.recv = recv
        self.rows = own.shape[0]
        self.chips, self.chip, self.core, *self.devices = line()

    def place(self, chip, core):
        return self.full.at[pl.ds(pl.multiple_of((2 * chip + core) * self.rows, self.rows), self.rows)]

    def copy(self, way, chip, source=None):
        target = self.place(chip, self.core)
        return pltpu.make_async_remote_copy(
            src_ref=target if source is None else source,
            dst_ref=target,
            send_sem=self.sends[way].at[chip],
            recv_sem=self.recv.at[2 * chip + self.core],
            device_id=self.devices[way],
            device_id_type=MESH,
        )

    def wait_for(self, chip, core):
        target = self.place(chip, core)
        pltpu.make_async_remote_copy(
            src_ref=target,
            dst_ref=target,
            send_sem=self.sends[2].at[0],
            recv_sem=self.recv.at[2 * chip + core],
            device_id=self.devices[2],
            device_id_type=MESH,
        ).wait_recv()

    def start(self):
        @pl.when(self.chip < self.chips - 1)
        def _():
            self.copy(0, self.chip, self.own).start()

        @pl.when(self.chip > 0)
        def _():
            self.copy(1, self.chip, self.own).start()

        self.copy(2, self.chip, self.own).start()
        self.keep = pltpu.make_async_copy(self.own, self.place(self.chip, self.core), self.local)
        self.keep.start()

    def step(self, number):
        left, right = self.chip - number, self.chip + number

        @pl.when(left >= 0)
        def _():
            self.wait_for(left, self.core)

            @pl.when(self.chip < self.chips - 1)
            def _():
                self.copy(0, left).start()

            self.copy(2, left).start()

        @pl.when(right < self.chips)
        def _():
            self.wait_for(right, self.core)

            @pl.when(self.chip > 0)
            def _():
                self.copy(1, right).start()

            self.copy(2, right).start()

    def finish(self):
        for chip in range(self.chips):
            self.wait_for(chip, 1 - self.core)
            self.copy(2, chip).wait_send()

            @pl.when((chip <= self.chip) & (self.chip < self.chips - 1))
            def _():
                self.copy(0, chip).wait_send()

            @pl.when((chip >= self.chip) & (self.chip > 0))
            def _():
                self.copy(1, chip).wait_send()

        self.keep.wait()


class LineSpread:
    pieces = 4

    @staticmethod
    def scratch():
        dma = pltpu.SemaphoreType.DMA
        return [dma((3, LineSpread.pieces)), dma((2, LineSpread.pieces))]

    def __init__(self, own, whole, send, recv):
        self.own, self.whole, self.send, self.recv = own, whole, send, recv
        self.rows = own.shape[0] // self.pieces
        self.source = lax.axis_index("seq")
        self.chips, self.chip, self.core, *self.devices = line()
        self.goes = (
            (self.chip >= self.source) & (self.chip < self.chips - 1),
            (self.chip <= self.source) & (self.chip > 0),
        )

    def copy(self, way, piece):
        target = self.whole.at[self.core, pl.ds(piece * self.rows, self.rows)]
        return pltpu.make_async_remote_copy(
            src_ref=target,
            dst_ref=target,
            send_sem=self.send.at[way, piece],
            recv_sem=self.recv.at[way // 2, piece],
            device_id=self.devices[way],
            device_id_type=MESH,
        )

    def level(self, number, pieces):
        @pl.when((self.chip == self.source + number) | (self.chip == self.source - number))
        def _():
            if number == 0:
                self.whole[self.core] = self.own[...]
            for piece in pieces:
                if number:
                    self.copy(0, piece).wait_recv()
                for way in (0, 1):

                    @pl.when(self.goes[way])
                    def _():
                        self.copy(way, piece).start()

                self.copy(2, piece).start()

    def end(self):
        for piece in range(self.pieces):
            other = self.whole.at[1 - self.core, pl.ds(piece * self.rows, self.rows)]
            pltpu.make_async_remote_copy(
                src_ref=other,
                dst_ref=other,
                send_sem=self.send.at[2, piece],
                recv_sem=self.recv.at[1, piece],
                device_id=self.devices[2],
                device_id_type=MESH,
            ).wait_recv()
            self.copy(2, piece).wait_send()
            for way in (0, 1):

                @pl.when(self.goes[way])
                def _():
                    self.copy(way, piece).wait_send()


class Everywhere:
    def __init__(self, values, out, ranks, total, places, send, recv):
        self.values, self.out, self.ranks, self.total, self.places = values, out, ranks, total, places
        self.send, self.recv = send, recv
        self.groups, self.shards = ranks.shape[0], places.shape[0]
        self.rank, self.place = lax.axis_index("seq"), lax.axis_index("wshard")

    def others(self):
        return [{"seq": lax.rem(self.rank + k, self.groups)} for k in range(1, self.groups)]

    def along(self):
        return [{"wshard": lax.rem(self.place + k, self.shards)} for k in range(1, self.shards)]

    def start(self):
        self.first = [
            push(self.values, self.ranks.at[self.rank], self.send.at[k], self.recv.at[k], other)
            for k, other in enumerate(self.others())
        ]
        self.ranks[self.rank] = self.values[...]

    def relay(self):
        for copy in self.first:
            copy.wait()
        ranks, groups = self.ranks, self.groups
        self.total[...] = (ranks[0] + ranks[1]) + (ranks[2] + ranks[3])
        self.second = [
            push(self.total, self.places.at[self.place], self.send.at[groups + k], self.recv.at[groups + k], other)
            for k, other in enumerate(self.along())
        ]
        self.places[self.place] = self.total[...]

    def end(self):
        for copy in self.second:
            copy.wait()
        sums = [self.places[k] + self.places[k + 1] for k in range(0, self.shards, 2)]
        self.out[...] = (sums[0] + sums[1]) + (sums[2] + sums[3])


def last_gather(values, small, collective_id):
    count = len(values)
    groups = lax.axis_size("seq")
    shards = 2 * groups

    def body(*refs):
        own, small_ref = refs[:count], refs[count]
        full, small_out = refs[count + 1 : 2 * count + 1], refs[2 * count + 1]
        send, recv, local = refs[2 * count + 2 : 2 * count + 5]
        me, side, down, across = sides()
        total = Everywhere(small_ref, small_out, *refs[2 * count + 5 :])
        meet(*total.others(), *total.along())
        jobs = [SquareGather(own[i], full[i], send.at[i], recv.at[i]) for i in range(count)]
        total.start()
        keeps = []
        for i, job in enumerate(jobs):
            job.start()
            rows = own[i].shape[0]
            keep = pltpu.make_async_copy(
                own[i], full[i].at[pl.ds(pl.multiple_of(me * rows, rows), rows)], local.at[i]
            )
            keep.start()
            keeps.append(keep)
        total.relay()
        for job in jobs:
            job.relay()
        total.end()
        for job, keep in zip(jobs, keeps):
            job.near()
            job.far()
            job.finish()
            keep.wait()

    vmem = pl.BlockSpec(memory_space=pltpu.VMEM)
    dma = pltpu.SemaphoreType.DMA
    return pl.pallas_call(
        body,
        in_specs=[vmem] * (count + 1),
        out_specs=[pl.BlockSpec(memory_space=pl.ANY)] * count + [vmem],
        out_shape=[jax.ShapeDtypeStruct((4 * v.shape[0],) + v.shape[1:], v.dtype) for v in values]
        + [jax.ShapeDtypeStruct(small.shape, jnp.float32)],
        scratch_shapes=[
            dma((count, 6)),
            dma((count, 6)),
            dma((count,)),
            pltpu.VMEM((groups,) + small.shape, jnp.float32),
            pltpu.VMEM(small.shape, jnp.float32),
            pltpu.VMEM((shards,) + small.shape, jnp.float32),
            dma((groups + shards,)),
            dma((groups + shards,)),
        ],
        compiler_params=pltpu.CompilerParams(
            collective_id=collective_id, has_side_effects=True, vmem_limit_bytes=VMEM_LIMIT
        ),
        name="last_gather",
    )(*values, small)


def join_units(every, down, part):
    groups, rows, both = every.shape
    units = both // 2
    blocks = units // part
    steps = 4
    tall = rows // steps

    def body(every_ref, down_ref, gate_ref, up_ref, down_out):
        for half, out in enumerate((gate_ref, up_ref)):
            for group in range(groups):
                for block in range(blocks):
                    at = half * units + block * part
                    to = (block * groups + group) * part
                    out[:, to : to + part] = every_ref[group, :, at : at + part].astype(jnp.float32)
        down_out[...] = down_ref[...].astype(jnp.float32)

    wide = jax.ShapeDtypeStruct((rows, groups * units), jnp.float32)
    return pl.pallas_call(
        body,
        grid=(steps,),
        in_specs=[
            pl.BlockSpec((groups, tall, both), lambda i: (0, i, 0)),
            pl.BlockSpec((down.shape[0] // steps, down.shape[1]), lambda i: (i, 0)),
        ],
        out_specs=[pl.BlockSpec((tall, groups * units), lambda i: (i, 0))] * 2
        + [pl.BlockSpec((down.shape[0] // steps, down.shape[1]), lambda i: (i, 0))],
        out_shape=[wide, wide, jax.ShapeDtypeStruct(down.shape, jnp.float32)],
        name="join_units",
    )(every, down)


def join_columns(every, columns, starts):
    groups, rows, lanes = every.shape
    steps = 4
    tall = rows // steps

    def body(every_ref, *outs):
        for start, out in zip(starts, outs):
            for group in range(groups):
                out[:, group * columns : (group + 1) * columns] = every_ref[
                    group, :, start : start + columns
                ].astype(jnp.float32)

    wide = jax.ShapeDtypeStruct((rows, groups * columns), jnp.float32)
    return pl.pallas_call(
        body,
        grid=(steps,),
        in_specs=[pl.BlockSpec((groups, tall, lanes), lambda i: (0, i, 0))],
        out_specs=[pl.BlockSpec((tall, groups * columns), lambda i: (i, 0))] * len(starts),
        out_shape=[wide] * len(starts),
        name="join_columns",
    )(every)


class SquareScatter:
    @staticmethod
    def scratch(rows, width):
        half = rows // 2
        low = jnp.bfloat16
        return [
            pltpu.VMEM((rows, width), low),
            pltpu.VMEM((2, half, width), low),
            pltpu.VMEM((2, half, width), jnp.float32),
            pltpu.VMEM((6, half, width), low),
            pltpu.VMEM((2, half, width), low),
            pltpu.SemaphoreType.DMA((6,)),
            pltpu.SemaphoreType.DMA((6,)),
        ]

    def __init__(self, lefts, rights, transposed, out, far, near, kept, land, carry, send, recv):
        self.lefts, self.rights, self.transposed, self.out = lefts, rights, transposed, out
        self.far, self.near, self.kept, self.land, self.carry = far, near, kept, land, carry
        self.send, self.recv = send, recv
        self.rows, self.width = out.shape
        self.half = self.rows // 2
        self.tile = self.width // 3 if self.width % 384 == 0 else self.width

    def copy(self, index):
        me, side, down, across = sides()
        source = (
            self.far.at[pl.ds(0, self.half)],
            self.far.at[pl.ds(self.half, self.half)],
            self.near.at[0],
            self.near.at[1],
            self.carry.at[0],
            self.carry.at[1],
        )[index]
        return pltpu.make_async_remote_copy(
            src_ref=source,
            dst_ref=self.land.at[index],
            send_sem=self.send.at[index],
            recv_sem=self.recv.at[index],
            device_id={"seq": down if index in (0, 3, 5) else side},
            device_id_type=MESH,
        )

    def partial(self, rank, store):
        at = pl.ds(pl.multiple_of(rank * self.rows, self.rows), self.rows)

        def step(number, carried):
            columns = pl.ds(pl.multiple_of(number * self.tile, self.tile), self.tile)
            value = None
            for a, b in zip(self.lefts, self.rights):
                if self.transposed:
                    term = product_nt(a[at, :], b[columns, :])
                else:
                    term = product(a[at, :], b[:, columns])
                value = term if value is None else value + term
            store(columns, value)
            return carried

        lax.fori_loop(0, self.width // self.tile, step, 0)

    def begin(self):
        me, side, down, across = sides()
        half, far, near, kept = self.half, self.far, self.near, self.kept

        def store_far(columns, value):
            far[:, columns] = value.astype(far.dtype)

        def store_side(columns, value):
            kept[0, :, columns] = value[:half]
            near[0, :, columns] = value[half:].astype(near.dtype)

        def store_down(columns, value):
            near[1, :, columns] = value[:half].astype(near.dtype)
            kept[1, :, columns] = value[half:]

        self.partial(across, store_far)
        self.copy(0).start()
        self.copy(1).start()
        self.partial(side, store_side)
        self.copy(2).start()
        self.partial(down, store_down)
        self.copy(3).start()

    def relay(self):
        for index in (0, 1):
            self.copy(index).wait_recv()
            total = self.kept[index] + self.land[index].astype(jnp.float32)
            self.carry[index] = total.astype(self.carry.dtype)
            self.copy(4 + index).start()

    def own(self):
        out = self.out

        def store_own(columns, value):
            out[:, columns] = value

        self.partial(lax.axis_index("seq"), store_own)

    def end(self):
        for index in (2, 3, 4, 5):
            self.copy(index).wait_recv()
        land, half = self.land, self.half
        self.out[:half, :] += land[3].astype(jnp.float32) + land[4].astype(jnp.float32)
        self.out[half:, :] += land[2].astype(jnp.float32) + land[5].astype(jnp.float32)
        for index in range(6):
            self.copy(index).wait_send()


class LineScatter:
    @staticmethod
    def scratch(chips, rows, width):
        low = jnp.bfloat16
        dma = pltpu.SemaphoreType.DMA
        return [pltpu.VMEM((chips, rows, width), low)] * 3 + [dma((2, chips)), dma((3, chips))]

    def __init__(self, terms, out, twin_in, forth_in, back_in, send, recv):
        self.terms, self.out, self.twin_in = terms, out, twin_in
        self.forth_in, self.back_in, self.send, self.recv = forth_in, back_in, send, recv
        self.chips, self.chip, self.core, *self.devices = line()
        self.rows = twin_in.shape[1]

    def term(self, chip, core):
        return self.terms.at[pl.ds(pl.multiple_of((2 * chip + core) * self.rows, self.rows), self.rows)]

    def swap(self, chip):
        return pltpu.make_async_remote_copy(
            src_ref=self.term(chip, 1 - self.core),
            dst_ref=self.twin_in.at[chip],
            send_sem=self.send.at[0, chip],
            recv_sem=self.recv.at[0, chip],
            device_id=self.devices[2],
            device_id_type=MESH,
        )

    def hop(self, way, chip):
        return pltpu.make_async_remote_copy(
            src_ref=self.twin_in.at[chip],
            dst_ref=(self.forth_in, self.back_in)[way].at[chip],
            send_sem=self.send.at[1, chip],
            recv_sem=self.recv.at[1 + way, chip],
            device_id=self.devices[way],
            device_id_type=MESH,
        )

    def start(self):
        for chip in (self.chips - 1, 0, *range(1, self.chips - 1)):
            self.swap(chip).start()

    def pair(self, chip):
        return self.term(chip, self.core)[...].astype(jnp.float32) + self.twin_in[chip].astype(jnp.float32)

    def pass_on(self, way, chip, first):
        self.swap(chip).wait_recv()
        source = (self.forth_in, self.back_in)[way]

        @pl.when(first)
        def _():
            self.twin_in[chip] = self.pair(chip).astype(self.twin_in.dtype)

        @pl.when(jnp.logical_not(first))
        def _():
            self.hop(way, chip).wait_recv()
            total = self.pair(chip) + source[chip].astype(jnp.float32)
            self.twin_in[chip] = total.astype(self.twin_in.dtype)

        self.hop(way, chip).start()

    def step(self, number):
        forth, back = self.chips - number, number - 1
        low_end = self.chip < self.chips // 2

        @pl.when(low_end & (forth > self.chip))
        def _():
            self.pass_on(0, forth, self.chip == 0)

        @pl.when(back < self.chip)
        def _():
            self.pass_on(1, back, self.chip == self.chips - 1)

        @pl.when(jnp.logical_not(low_end) & (forth > self.chip))
        def _():
            self.pass_on(0, forth, self.chip == 0)

    def end(self):
        for chip in range(self.chips):

            @pl.when(self.chip == chip)
            def _():
                self.swap(chip).wait_recv()
                total = self.pair(chip)
                if chip > 0:
                    self.hop(0, chip).wait_recv()
                    total = total + self.forth_in[chip].astype(jnp.float32)
                if chip < self.chips - 1:
                    self.hop(1, chip).wait_recv()
                    total = total + self.back_in[chip].astype(jnp.float32)
                self.out[...] = total.astype(self.out.dtype)

            self.swap(chip).wait_send()

            @pl.when(self.chip != chip)
            def _():
                self.hop(0, chip).wait_send()


class LineCollect:
    pieces = 2

    @staticmethod
    def scratch(rows, width):
        low = jnp.bfloat16
        dma = pltpu.SemaphoreType.DMA
        pieces = LineCollect.pieces
        return [pltpu.VMEM((rows, width), low)] * 3 + [dma((2, pieces)), dma((3, pieces))]

    def __init__(self, terms, out, twin_in, forth_in, back_in, send, recv):
        self.terms, self.out, self.twin_in = terms, out, twin_in
        self.forth_in, self.back_in, self.send, self.recv = forth_in, back_in, send, recv
        self.target = lax.axis_index("seq")
        self.chips, self.chip, self.core, *self.devices = line()
        self.rows = twin_in.shape[0]
        self.tall = self.rows // self.pieces

    def at(self, piece):
        return pl.ds(piece * self.tall, self.tall)

    def term(self, piece, core):
        start = pl.multiple_of(core * self.rows + piece * self.tall, self.tall)
        return self.terms.at[pl.ds(start, self.tall)]

    def swap(self, piece):
        return pltpu.make_async_remote_copy(
            src_ref=self.term(piece, 1 - self.core),
            dst_ref=self.twin_in.at[self.at(piece)],
            send_sem=self.send.at[0, piece],
            recv_sem=self.recv.at[0, piece],
            device_id=self.devices[2],
            device_id_type=MESH,
        )

    def hop(self, way, piece):
        return pltpu.make_async_remote_copy(
            src_ref=self.out.at[self.at(piece)],
            dst_ref=(self.forth_in, self.back_in)[way].at[self.at(piece)],
            send_sem=self.send.at[1, piece],
            recv_sem=self.recv.at[1 + way, piece],
            device_id=self.devices[way],
            device_id_type=MESH,
        )

    def start(self):
        for piece in range(self.pieces):
            self.swap(piece).start()

    def add(self, piece):
        low = self.out.dtype
        self.swap(piece).wait_recv()
        total = self.term(piece, self.core)[...].astype(jnp.float32)
        total = total + self.twin_in[self.at(piece), :].astype(jnp.float32)
        self.out[self.at(piece), :] = total.astype(low)
        for way, there in enumerate(
            (
                (self.chip <= self.target) & (self.chip > 0),
                (self.chip >= self.target) & (self.chip < self.chips - 1),
            )
        ):

            @pl.when(there)
            def _():
                self.hop(way, piece).wait_recv()
                more = (self.forth_in, self.back_in)[way][self.at(piece), :].astype(jnp.float32)
                self.out[self.at(piece), :] = (self.out[self.at(piece), :].astype(jnp.float32) + more).astype(low)

    def level(self, number):
        for way, goes in enumerate(
            (
                (self.chip < self.target) & (self.chip == number),
                (self.chip > self.target) & (self.chips - 1 - self.chip == number),
            )
        ):

            @pl.when(goes)
            def _():
                for piece in range(self.pieces):
                    self.add(piece)
                    self.hop(way, piece).start()

    def end(self):
        @pl.when(self.chip == self.target)
        def _():
            for piece in range(self.pieces):
                self.add(piece)

        for piece in range(self.pieces):
            self.swap(piece).wait_send()

            @pl.when(self.chip != self.target)
            def _():
                self.hop(0, piece).wait_send()


class SquareSpread:
    def __init__(self, own, out, send, recv):
        self.own, self.out, self.send, self.recv = own, out, send, recv
        self.chip = line()[1]
        self.half = own.shape[0] // 2

    def copy(self, index):
        me, side, down, across = sides()
        if index < 2:
            source, target = self.own, self.out
        else:
            source = target = self.out.at[pl.ds((index - 2) * self.half, self.half)]
        return pltpu.make_async_remote_copy(
            src_ref=source,
            dst_ref=target,
            send_sem=self.send.at[index],
            recv_sem=self.recv.at[index],
            device_id={"seq": (side, down, down, side)[index]},
            device_id_type=MESH,
        )

    def roles(self):
        me, side, down, across = sides()
        return [self.chip == rank for rank in (me, side, down, across)]

    def start(self):
        @pl.when(self.roles()[0])
        def _():
            self.copy(0).start()
            self.copy(1).start()
            self.out[...] = self.own[...]

    def relay(self):
        for index in (0, 1):

            @pl.when(self.roles()[1 + index])
            def _():
                self.copy(index).wait_recv()
                self.copy(2 + index).start()

    def end(self):
        mine, by_side, by_down, far = self.roles()

        @pl.when(mine)
        def _():
            self.copy(0).wait_send()
            self.copy(1).wait_send()

        @pl.when(by_side)
        def _():
            self.copy(2).wait_send()

        @pl.when(by_down)
        def _():
            self.copy(3).wait_send()

        @pl.when(far)
        def _():
            self.copy(2).wait_recv()
            self.copy(3).wait_recv()


def product_scatter(lefts, rights, transposed, collective_id, extras=()):
    count = len(lefts)
    more = len(extras)
    rows = lefts[0].shape[0] // 4
    width = rights[0].shape[0] if transposed else rights[0].shape[1]

    def body(*refs):
        left, right = refs[:count], refs[count : 2 * count]
        sides_in = refs[2 * count : 2 * count + 2 * more]
        out = refs[2 * count + 2 * more]
        sides_out = refs[2 * count + 2 * more + 1 : 2 * count + 3 * more + 1]
        me, side, down, across = sides()
        meet({"seq": side}, {"seq": down})
        job = SquareScatter(left, right, transposed, out, *refs[2 * count + 3 * more + 1 :])
        job.begin()
        job.relay()
        job.own()
        for index in range(more):
            transposed_product(sides_in[2 * index], sides_in[2 * index + 1], sides_out[index])
        job.end()

    vmem = pl.BlockSpec(memory_space=pltpu.VMEM)
    return pl.pallas_call(
        body,
        in_specs=[vmem] * (2 * count + 2 * more),
        out_specs=[vmem] * (1 + more),
        out_shape=[jax.ShapeDtypeStruct((rows, width), jnp.float32)]
        + [jax.ShapeDtypeStruct((a.shape[1], b.shape[1]), jnp.bfloat16) for a, b in extras],
        scratch_shapes=SquareScatter.scratch(rows, width),
        compiler_params=pltpu.CompilerParams(
            collective_id=collective_id, has_side_effects=True, vmem_limit_bytes=VMEM_LIMIT
        ),
        name="product_scatter",
    )(*lefts, *rights, *(value for pair in extras for value in pair))


def middle_backward(joined, d_out, offset, col, logit, hidden, w_down, gated, grad_branch,
                    head_size, scale, collective_id):
    slots, lanes = joined.shape
    width = w_down.shape[1]
    tokens = slots // 4
    columns = gated.shape[1]

    def body(joined_ref, d_out_ref, offset_ref, col_ref, logit_ref, hidden_ref, down_ref, gated_ref, branch_ref,
             grads, bias_grad, lowered, collected, terms, *scratch):
        me, side, down, across = sides()
        chips, chip, core, forth, back, twin = line()
        meet({"seq": side}, {"seq": down}, forth, back, twin)
        work = Backward(
            joined_ref, d_out_ref, offset_ref, col_ref, logit_ref, grads, *scratch[:4], head_size, scale
        )
        job = SquareScatter([hidden_ref], [down_ref], False, lowered, *scratch[4:11])
        collect = LineCollect(terms, collected, *scratch[11:])
        transposed_product(gated_ref, branch_ref, terms)
        collect.start()
        job.begin()
        work.start()
        collect.level(0)

        def step(pair, carry):
            work.pair(pair)

            @pl.when(pair == 0)
            def _():
                job.relay()

            @pl.when(pair == 1)
            def _():
                collect.level(1)

            return carry

        lax.fori_loop(0, work.pairs, step, 0)
        collect.level(2)
        job.own()
        work.end(bias_grad)
        job.end()
        collect.end()

    vmem = pl.BlockSpec(memory_space=pltpu.VMEM)
    low = jnp.bfloat16
    return pl.pallas_call(
        body,
        in_specs=[vmem] * 9,
        out_specs=[vmem] * 4,
        out_shape=[
            jax.ShapeDtypeStruct((slots, lanes), low),
            jax.ShapeDtypeStruct((8, PAIR), jnp.float32),
            jax.ShapeDtypeStruct((tokens, width), jnp.float32),
            jax.ShapeDtypeStruct((columns // 2, width), low),
        ],
        scratch_shapes=[pltpu.VMEM((columns, width), low)]
        + backward_scratch(slots)
        + SquareScatter.scratch(tokens, width)
        + LineCollect.scratch(columns // 2, width),
        compiler_params=pltpu.CompilerParams(
            collective_id=collective_id, has_side_effects=True, vmem_limit_bytes=VMEM_LIMIT
        ),
        name="middle_backward",
    )(joined, d_out, offset, col, logit, hidden, w_down, gated, grad_branch)


def last_backward(grads, grad_gate_pre, normed, weights, gate_weights, collected, collective_id):
    slots, depth = normed.shape
    front = grads.shape[1]
    lanes = front + gate_weights.shape[1]
    tokens = slots // 4
    shards = 2 * lax.axis_size("seq")
    rows = depth // shards

    def body(grads_ref, gate_ref, normed_ref, weights_ref, gate_weights_ref, collected_ref,
             summed, share, spread_out, terms,
             spread_send, spread_recv, *scratch):
        me, side, down, across = sides()
        chips, chip, core, forth, back, twin = line()
        meet({"seq": side}, {"seq": down}, forth, back, twin)
        job = SquareScatter(
            [grads_ref, gate_ref],
            [weights_ref, gate_weights_ref],
            True,
            summed,
            *scratch[:7],
        )
        run = LineScatter(terms, share, *scratch[7:])
        spread = SquareSpread(collected_ref, spread_out, spread_send, spread_recv)
        transposed_product(normed_ref, grads_ref, terms.at[:, pl.ds(0, front)])
        transposed_product(normed_ref, gate_ref, terms.at[:, pl.ds(front, lanes - front)])
        run.start()
        spread.start()
        job.begin()
        run.step(1)
        job.relay()
        spread.relay()
        run.step(2)
        run.step(3)
        job.own()
        job.end()
        spread.end()
        run.end()

    vmem = pl.BlockSpec(memory_space=pltpu.VMEM)
    low = jnp.bfloat16
    return pl.pallas_call(
        body,
        in_specs=[vmem] * 6,
        out_specs=[vmem] * 3,
        out_shape=[
            jax.ShapeDtypeStruct((tokens, depth), jnp.float32),
            jax.ShapeDtypeStruct((rows, lanes), low),
            jax.ShapeDtypeStruct(collected.shape, low),
        ],
        scratch_shapes=[
            pltpu.VMEM((depth, lanes), low),
            pltpu.SemaphoreType.DMA((4,)),
            pltpu.SemaphoreType.DMA((4,)),
        ]
        + SquareScatter.scratch(tokens, depth)
        + LineScatter.scratch(shards // 2, rows, lanes),
        compiler_params=pltpu.CompilerParams(
            collective_id=collective_id, has_side_effects=True, vmem_limit_bytes=VMEM_LIMIT
        ),
        name="last_backward",
    )(grads, grad_gate_pre, normed, weights, gate_weights, collected)


def norm_rows(values, gain):
    scale = lax.rsqrt(jnp.mean(values * values, axis=-1, keepdims=True) + EPS)
    return scale, values * scale * gain


def whole_forward(inputs, gain, cotangent, weights, forget, bias, length, block, w_gate, w_up,
                  head_size, scale, collective_id):
    rows, depth = inputs.shape
    groups = 4
    slots = groups * rows
    chips = groups
    shards = 2 * chips
    mine = weights[0].shape[0]
    columns = depth // groups
    front = 3 * columns + PAIR
    pairs = columns // PAIR
    part = w_gate.shape[1] // (groups * shards)
    units = shards * part
    low = jnp.bfloat16

    def body(inputs_ref, gain_ref, cot_ref, q_ref, k_ref, v_ref, og_ref, forget_ref, bias_ref, length_ref, block_ref,
             gate_ref, up_ref,
             normed, cot_full, full_front, full_gate, full_out, full_ffn, joined, attended, offset, col, logit,
             gate_pre, gated, middle,
             own_normed, own_front, own_gate, own_ffn, row, picks, cot_send, cot_recv, keep,
             x_send, x_recv, *scratch):
        me, side, down, across = sides()
        line_chips, chip, core, forth, back, twin = line()
        front_line = LineGather(own_front, full_front, *scratch[0:3])
        gate_line = LineGather(own_gate, full_gate, *scratch[3:6])
        ffn_line = LineGather(own_ffn, full_ffn, *scratch[6:9])
        spread = LineSpread(block_ref, full_out, *scratch[9:11])
        job = SquareScatter([gated], [full_out_rows(full_out)], False, middle, *scratch[11:18])
        taken = []
        my_columns = pl.ds(pl.multiple_of(me * columns, columns), columns)
        for index, source in enumerate((q_ref, k_ref, v_ref)):
            taken.append((source.at[:, my_columns], own_front.at[:, pl.ds(index * columns, columns)]))
        taken.append((og_ref.at[:, my_columns], own_gate))
        for index, source in enumerate((gate_ref, up_ref)):
            for number in range(shards):
                column = pl.ds(pl.multiple_of((number * groups + me) * part, part), part)
                taken.append((source.at[:, column], own_ffn.at[:, pl.ds(index * units + number * part, part)]))
        taken = [pltpu.make_async_copy(a, b, picks.at[i]) for i, (a, b) in enumerate(taken)]
        for copy in taken:
            copy.start()
        values = inputs_ref[...].astype(jnp.float32)
        own_normed[...] = norm_rows(values, gain_ref[...])[1].astype(low)
        own_front[:, 3 * columns :] = forget_ref[...]
        meet({"seq": side}, {"seq": down}, forth, back, twin)
        one = SquareGather(own_normed, normed, x_send, x_recv)
        two = SquareGather(cot_ref, cot_full, cot_send, cot_recv)
        one.start()
        for copy in taken:
            copy.wait()
        front_line.start()
        at_me = pl.ds(pl.multiple_of(me * rows, rows), rows)
        kept = pltpu.make_async_copy(cot_ref, cot_full.at[at_me], keep.at[0])
        kept.start()
        normed[at_me, :] = own_normed[...]
        one.relay()
        front_line.step(1)
        front_line.step(2)
        one.near()
        one.far()
        front_line.step(3)
        front_line.finish()
        one.finish()
        spread.level(0, range(4))
        gate_line.start()
        two.start()

        def store_joined(at_columns, value):
            joined[:, at_columns] = value.astype(low)

        block_product(normed, full_front, False, 256, store_joined)
        spread.level(1, (0,))
        work = Forward(joined, bias_ref, length_ref, attended, offset, col, logit, row, head_size, scale)
        offset[...] = jnp.zeros_like(offset)
        work.start()

        def step(pair, carry):
            work.pair(pair)

            @pl.when(pair == 0)
            def _():
                spread.level(1, (1, 2))
                spread.level(2, (0, 1))
                gate_line.step(1)
                two.relay()

            @pl.when(pair == 1)
            def _():
                spread.level(1, (3,))
                spread.level(2, (2, 3))
                gate_line.step(2)

            return carry

        lax.fori_loop(0, pairs, step, 0)
        ffn_line.start()
        gate_line.step(3)
        spread.level(3, range(4))
        gate_line.finish()

        def store_gate(at_columns, value):
            gate_pre[:, at_columns] = value

        block_product(normed, full_gate, False, PAIR, store_gate)
        gated[...] = (attended[...].astype(jnp.float32) * jax.nn.sigmoid(gate_pre[...])).astype(low)
        spread.end()
        job.begin()
        ffn_line.step(1)
        job.relay()
        job.own()
        ffn_line.step(2)
        two.near()
        two.far()
        two.finish()
        kept.wait()
        job.end()
        middle[...] += inputs_ref[...].astype(jnp.float32)
        ffn_line.step(3)
        ffn_line.finish()

    def shape(size, kind=low):
        return jax.ShapeDtypeStruct(size, kind)

    vmem = pl.BlockSpec(memory_space=pltpu.VMEM)
    anywhere = pl.BlockSpec(memory_space=pl.ANY)
    dma = pltpu.SemaphoreType.DMA
    return pl.pallas_call(
        body,
        in_specs=[vmem] * 3 + [anywhere] * 4 + [vmem] * 4 + [anywhere] * 2,
        out_specs=[vmem, anywhere, vmem, vmem, vmem, anywhere] + [vmem] * 8,
        out_shape=[
            shape((slots, depth)),
            shape((slots, depth)),
            shape((depth, front)),
            shape((depth, columns)),
            shape((2, block.shape[0], depth)),
            shape((depth, 2 * units)),
            shape((slots, front)),
            *Forward.results(slots, pairs),
            shape((slots, columns), jnp.float32),
            shape((slots, columns)),
            shape((rows, depth), jnp.float32),
        ],
        scratch_shapes=[
            pltpu.VMEM((rows, depth), low),
            pltpu.VMEM((mine, front), low),
            pltpu.VMEM((mine, columns), low),
            pltpu.VMEM((mine, 2 * units), low),
            pltpu.VMEM((Forward.some, slots), jnp.float32),
            dma((4 + 2 * shards,)),
            dma((6,)),
            dma((6,)),
            dma((1,)),
            dma((6,)),
            dma((6,)),
        ]
        + 3 * LineGather.scratch(chips)
        + LineSpread.scratch()
        + SquareScatter.scratch(rows, depth),
        compiler_params=pltpu.CompilerParams(
            collective_id=collective_id, has_side_effects=True, vmem_limit_bytes=VMEM_LIMIT
        ),
        name="whole_forward",
    )(inputs, gain, cotangent, *weights, forget, bias, length, block, w_gate, w_up)


class full_out_rows:
    def __init__(self, ref):
        self.ref = ref
        self.shape = (2 * ref.shape[1], ref.shape[2])

    def __getitem__(self, index):
        rows, columns = index
        return jnp.concatenate([self.ref[0, :, columns], self.ref[1, :, columns]], axis=0)


def feed_forward(middle, gain, weights, own_down, cotangent, collective_id):
    rows, depth = middle.shape
    slots = 4 * rows
    units = weights.shape[1] // 2
    chips = 4
    low = jnp.bfloat16

    def body(middle_ref, gain_ref, weights_ref, down_ref, cot_ref, normed, hidden, full_down, grads, terms,
             own_normed, both, send, recv, *scratch):
        me, side, down, across = sides()
        line_chips, chip, core, forth, back, twin = line()
        down_line = LineGather(down_ref, full_down, *scratch)
        own_normed[...] = norm_rows(middle_ref[...], gain_ref[...])[1].astype(low)
        meet({"seq": side}, {"seq": down}, forth, back, twin)
        job = SquareGather(own_normed, normed, send, recv)
        job.start()
        down_line.start()

        def ahead(rank):
            at = pl.ds(pl.multiple_of(rank * rows, rows), rows)

            def store(columns, value):
                both[at, columns] = value

            block_product(normed.at[at], weights_ref, False, 512, store)
            gate, upward = both[at, :units], both[at, units:]
            hidden[at, :] = (gate * jax.nn.sigmoid(gate) * upward).astype(low)

        normed[pl.ds(pl.multiple_of(me * rows, rows), rows), :] = own_normed[...]
        ahead(me)
        job.relay()
        down_line.step(1)
        down_line.step(2)
        job.near()
        ahead(side)
        ahead(down)
        down_line.step(3)
        job.far()
        ahead(across)
        down_line.finish()
        job.finish()

        def behind(number, carry):
            at = pl.ds(pl.multiple_of(number * rows, rows), rows)
            grad_hidden = product_nt(cot_ref[at, :], full_down[...])
            gate, upward = both[at, :units], both[at, units:]
            sigma = jax.nn.sigmoid(gate)
            grads[at, :units] = (grad_hidden * upward * sigma * (1.0 + gate * (1.0 - sigma))).astype(low)
            grads[at, units:] = (grad_hidden * gate * sigma).astype(low)
            return carry

        lax.fori_loop(0, 4, behind, 0)
        transposed_product(hidden, cot_ref, terms)

    def shape(size, kind=low):
        return jax.ShapeDtypeStruct(size, kind)

    vmem = pl.BlockSpec(memory_space=pltpu.VMEM)
    dma = pltpu.SemaphoreType.DMA
    return pl.pallas_call(
        body,
        in_specs=[vmem] * 5,
        out_specs=[vmem] * 5,
        out_shape=[
            shape((slots, depth)),
            shape((slots, units)),
            shape((units, depth)),
            shape((slots, 2 * units)),
            shape((units, depth)),
        ],
        scratch_shapes=[
            pltpu.VMEM((rows, depth), low),
            pltpu.VMEM((slots, 2 * units), jnp.float32),
            dma((6,)),
            dma((6,)),
        ]
        + LineGather.scratch(chips),
        compiler_params=pltpu.CompilerParams(
            collective_id=collective_id, has_side_effects=True, vmem_limit_bytes=VMEM_LIMIT
        ),
        name="feed_forward",
    )(middle, gain, weights, own_down, cotangent)


def gather(value, axis_name):
    return lax.all_gather(value, axis_name, axis=0, tiled=True)


def scatter(value, axis_name):
    return lax.psum_scatter(value, axis_name, scatter_dimension=0, tiled=True)


def gather_multiply(own, weight, transposed, collective_id):
    if square(lax.axis_size("seq")):
        return gather_product(own, weight, transposed, collective_id)
    whole = gather(own, "seq")
    return whole, product_nt(whole, weight) if transposed else product(whole, weight)


def multiply_scatter(lefts, rights, transposed, collective_id, extras=()):
    if square(lax.axis_size("seq")):
        return product_scatter(lefts, rights, transposed, collective_id, extras)
    products = [product_tn(a, b).astype(jnp.bfloat16) for a, b in extras]
    total = sum(product_nt(a, b) if transposed else product(a, b) for a, b in zip(lefts, rights))
    return [scatter(total.astype(jnp.bfloat16), "seq").astype(jnp.float32), *products]


def on_device(
    layer_input,
    lengths,
    norm_attn,
    w_query,
    w_key,
    w_value,
    w_ogate,
    w_forget,
    forget_bias,
    w_out,
    norm_ffn,
    w_gate,
    w_up,
    w_down,
    output_grad,
):
    low = jnp.bfloat16
    tokens, width = layer_input.shape[1:]
    heads = forget_bias.shape[0]
    groups = lax.axis_size("seq")
    shards = lax.axis_size("wshard")
    fast = square(groups) and shards == 2 * groups
    local_heads = heads // groups
    head_size = width // heads
    columns = width // groups
    lanes = columns + -columns % PAIR
    front = 3 * lanes + PAIR
    slots = tokens * groups
    hidden_size = w_gate.shape[1]
    part = hidden_size // (groups * shards)
    units = shards * part
    scale = head_size ** (-0.5)
    length = lengths[0]
    seq_rank = lax.axis_index("seq")
    shard_rank = lax.axis_index("wshard")
    per_block = shards // groups
    positions = seq_rank * tokens + jnp.arange(tokens, dtype=jnp.int32)
    valid_slots = (positions < length)[:, None]
    inputs = layer_input[0].astype(jnp.float32)
    cotangent_low = jnp.where(valid_slots, output_grad[0], jnp.zeros((), low))
    cotangent = cotangent_low.astype(jnp.float32)

    def own_columns(weight, size):
        taken = lax.dynamic_slice_in_dim(weight, seq_rank * columns, columns, 1)
        return jnp.pad(taken, ((0, 0), (0, size - columns))) if size > columns else taken

    def own_units(weight):
        split = weight.reshape(weight.shape[0], shards, groups, part)
        mine = lax.dynamic_index_in_dim(split, seq_rank, 2, keepdims=False)
        return mine.reshape(weight.shape[0], units)

    own_forget = lax.dynamic_slice_in_dim(w_forget, seq_rank * local_heads, local_heads, 1)
    own_forget = jnp.pad(own_forget, ((0, 0), (0, PAIR - local_heads)))
    own_bias = lax.dynamic_slice_in_dim(forget_bias, seq_rank * local_heads, local_heads)
    own_bias = jnp.pad(own_bias, (0, PAIR - local_heads))[None]
    length_row = jnp.broadcast_to(lengths[:, None], (1, PAIR))
    mine_down = lax.dynamic_slice_in_dim(w_down, seq_rank * part, part, 0)
    if fast:
        (
            normed_attn, cotangent_all, full_front, full_ogate, full_out, full_ffn,
            joined, attended_low, offset, col, logit, gate_pre, gated, middle,
        ) = whole_forward(
            layer_input[0], norm_attn[None], cotangent_low, (w_query, w_key, w_value, w_ogate), own_forget,
            own_bias, length_row, w_out, w_gate, w_up, head_size, scale, 0,
        )
        full_out = full_out.reshape(columns, width)
    else:
        mine_front = jnp.concatenate(
            [*(own_columns(w, lanes) for w in (w_query, w_key, w_value)), own_forget], axis=1
        )
        full_front = gather(mine_front, "wshard")
        full_ogate = gather(own_columns(w_ogate, columns), "wshard")
        normed_attn = gather(rms_norm(inputs, norm_attn).astype(low), "seq")
        cotangent_all = gather(cotangent_low, "seq")
        full_out = lax.dynamic_slice_in_dim(gather(w_out, "wshard"), seq_rank * columns, columns, 0)
        mine_ffn = jnp.concatenate([own_units(w_gate), own_units(w_up)], axis=1)
        full_ffn = gather(mine_ffn, "wshard")
        joined = product(normed_attn, full_front).astype(low)
        gate_pre = product(normed_attn, full_ogate)
        attended_low, offset, col, logit = attention_fwd(joined, own_bias, length_row, head_size, scale)
        gated = gate_product(attended_low[:, :columns].astype(jnp.float32), gate_pre).astype(low)
        middle = inputs + multiply_scatter([gated], [full_out], False, 1)[0]
    unused_gated, pull_gate = jax.vjp(gate_product, attended_low[:, :columns].astype(jnp.float32), gate_pre)
    normed_ffn_own, pull_ffn_norm = jax.vjp(rms_norm, middle, norm_ffn)
    if fast:
        normed_ffn, hidden, full_down, grad_gate_up, grad_w_down = feed_forward(
            middle, norm_ffn[None], full_ffn, mine_down, cotangent_all, 2
        )
    else:
        full_down = gather(mine_down, "wshard")
        normed_ffn, gate_up = gather_multiply(normed_ffn_own.astype(low), full_ffn, False, 2)
        hidden_full, pull_swiglu = jax.vjp(swiglu, gate_up[:, :units], gate_up[:, units:])
        hidden = hidden_full.astype(low)
        grad_w_down = product_tn(hidden, cotangent_all).astype(low)
        grad_hidden = product_nt(cotangent_all, full_down)
        grad_gate_full, grad_up_full = pull_swiglu(grad_hidden)
        grad_gate_up = jnp.concatenate([grad_gate_full.astype(low), grad_up_full.astype(low)], axis=1)
    share_down = scatter(grad_w_down, "wshard")
    grad_normed_ffn, grad_w_ffn = multiply_scatter(
        [grad_gate_up], [full_ffn], True, 3, [(normed_ffn, grad_gate_up)]
    )
    share_ffn = scatter(grad_w_ffn, "wshard")
    grad_middle_part, grad_norm_ffn = pull_ffn_norm(grad_normed_ffn)
    grad_middle = cotangent + grad_middle_part
    grad_branch, grad_gated = gather_multiply(grad_middle.astype(low), full_out, True, 4)
    grad_attended_full, grad_gate_pre_full = pull_gate(grad_gated)
    grad_attended = grad_attended_full.astype(low)
    grad_gate_pre = grad_gate_pre_full.astype(low)
    if lanes > columns:
        grad_attended = jnp.pad(grad_attended, ((0, 0), (0, lanes - columns)))
    if fast:
        grads, bias_rows, lowered, collected = middle_backward(
            joined, grad_attended, offset, col, logit, hidden, full_down, gated, grad_branch, head_size, scale, 5
        )
        grad_normed_attn, share_attn, grad_out = last_backward(
            grads, grad_gate_pre, normed_attn, full_front, full_ogate, collected, 6
        )
        grad_out = grad_out.astype(jnp.float32)
    else:
        grads, bias_rows = attention_bwd(joined, grad_attended, offset, col, logit, head_size, scale)
        grad_projected = jnp.concatenate([grads, grad_gate_pre], axis=1)
        share_attn = scatter(product_tn(normed_attn, grad_projected).astype(low), "wshard")
        full_attn = jnp.concatenate([full_front, full_ogate], axis=1)
        grad_normed_attn = scatter(product_nt(grad_projected, full_attn).astype(low), "seq").astype(jnp.float32)
        lowered = scatter(product(hidden, full_down).astype(low), "seq").astype(jnp.float32)
        share_out = scatter(product_tn(gated, grad_branch).astype(low), "wshard")
        rows_out = columns // shards
        pieces_out = lax.all_gather(share_out, "seq", axis=0, tiled=False)
        takes = shards // per_block
        slots_out = jnp.where(
            (jnp.arange(per_block) == shard_rank // takes)[None, :, None, None],
            pieces_out[:, None],
            jnp.zeros((), low),
        ).reshape(shards, rows_out, width)
        moved = lax.all_to_all(slots_out, "wshard", split_axis=0, concat_axis=0, tiled=True)
        moved = moved.reshape(per_block, takes, rows_out, width)
        mine_out = lax.dynamic_index_in_dim(moved, shard_rank % per_block, 0, keepdims=False)
        grad_out = mine_out.reshape(columns // per_block, width).astype(jnp.float32)
    layer_output = (middle + lowered).astype(low)[None]
    grad_bias = lax.dynamic_update_slice_in_dim(
        jnp.zeros((heads,), jnp.float32), bias_rows[:local_heads, 0], seq_rank * local_heads, 0
    )
    unused_normed, pull_attn_norm = jax.vjp(rms_norm, inputs, norm_attn)
    grad_input_part, grad_norm_attn = pull_attn_norm(grad_normed_attn)
    grad_input = (grad_middle + grad_input_part)[None]

    rows = share_attn.shape[0]
    if fast:
        vector = jnp.concatenate([grad_norm_attn, grad_norm_ffn, grad_bias])
        vector = jnp.pad(vector, (0, -vector.shape[0] % 1024)).reshape(-1, 128)
        every_attn, every_ffn, grad_down, vector = last_gather([share_attn, share_ffn, share_down], vector, 7)
        vector = vector.reshape(-1)
        small = vector[:width], vector[width : 2 * width], vector[2 * width : 2 * width + heads]
    else:
        every_attn, every_ffn, grad_down = [gather(v, "seq") for v in (share_attn, share_ffn, share_down)]
        small = lax.psum((grad_norm_attn, grad_norm_ffn, grad_bias), ("seq", "wshard"))
    every_ffn = every_ffn.reshape((groups,) + share_ffn.shape)
    every_attn = every_attn.reshape((groups,) + share_attn.shape)
    starts = (0, lanes, 2 * lanes, front)
    if fast:
        grad_w_gate, grad_w_up, grad_down = join_units(every_ffn, grad_down, part)
        weight_grads = join_columns(every_attn, columns, starts)
    else:

        def join(first):
            taken = every_attn[:, :, first : first + columns]
            return taken.transpose(1, 0, 2).reshape(rows, width).astype(jnp.float32)

        def join_own_units(first):
            taken = every_ffn[:, :, first * units : (first + 1) * units]
            taken = taken.reshape(groups, rows, shards, part).transpose(1, 2, 0, 3)
            return taken.reshape(rows, hidden_size).astype(jnp.float32)

        weight_grads = [join(first) for first in starts]
        grad_w_gate, grad_w_up = join_own_units(0), join_own_units(1)
        grad_down = grad_down.astype(jnp.float32)

    grad_forget_w = every_attn[:, :, 3 * lanes : 3 * lanes + local_heads]
    grad_forget_w = grad_forget_w.transpose(1, 0, 2).reshape(rows, heads).astype(jnp.float32)
    return (
        layer_output,
        grad_input,
        small[0],
        *weight_grads,
        grad_forget_w,
        small[2],
        grad_out,
        small[1],
        grad_w_gate,
        grad_w_up,
        grad_down,
    )


def solution(mesh):
    return jax.shard_map(
        on_device,
        mesh=mesh,
        in_specs=(
            P("wshard", "seq", None),
            P("wshard"),
            P(),
            P("wshard", None),
            P("wshard", None),
            P("wshard", None),
            P("wshard", None),
            P("wshard", None),
            P(),
            P("wshard", None),
            P(),
            P("wshard", None),
            P("wshard", None),
            P("wshard", None),
            P("wshard", "seq", None),
        ),
        out_specs=(
            P("wshard", "seq", None),
            P("wshard", "seq", None),
            P(),
            P("wshard", None),
            P("wshard", None),
            P("wshard", None),
            P("wshard", None),
            P("wshard", None),
            P(),
            P("wshard", None),
            P(),
            P("wshard", None),
            P("wshard", None),
            P("wshard", None),
        ),
        check_vma=False,
    )
```

```python
import jax
import jax.numpy as jnp
from jax import lax
from jax.experimental import pallas as pl
from jax.experimental.pallas import tpu as pltpu
from jax.sharding import PartitionSpec as P

EPS = 1e-06
NEG_FILL = -1e30
PAIR = 128


def product(left, right):
    return jnp.dot(left, right, preferred_element_type=jnp.float32)


def product_tn(left, right):
    return lax.dot_general(
        left, right, (((0,), (0,)), ((), ())), preferred_element_type=jnp.float32
    )


def product_nt(left, right):
    return lax.dot_general(
        left, right, (((1,), (1,)), ((), ())), preferred_element_type=jnp.float32
    )


def rms_norm(values, gain):
    return values * lax.rsqrt(jnp.mean(values * values, axis=-1, keepdims=True) + EPS) * gain


def gate_product(attended, gate_pre):
    return attended * jax.nn.sigmoid(gate_pre)


def swiglu(gate, upward):
    return jax.nn.silu(gate) * upward


def low_triangle(size):
    rows = lax.broadcasted_iota(jnp.int32, (size, size), 0)
    return rows <= lax.broadcasted_iota(jnp.int32, (size, size), 1)


def exact(left, right):
    return jnp.dot(left, right, precision=lax.Precision.HIGHEST, preferred_element_type=jnp.float32)


class Forward:
    some = 8

    def __init__(self, joined, bias, length, attended, offset, col, logit, row, head_size, scale):
        self.joined, self.bias, self.length = joined, bias, length
        self.attended, self.offset, self.col, self.logit, self.row = attended, offset, col, logit, row
        self.head_size, self.scale = head_size, scale
        self.slots = joined.shape[0]
        self.pairs = (joined.shape[1] // PAIR - 1) // 3
        self.tile = min(256, self.slots)

    @staticmethod
    def results(slots, pairs):
        rows = jax.ShapeDtypeStruct((Forward.some, slots), jnp.float32)
        return [
            jax.ShapeDtypeStruct((slots, pairs * PAIR), jnp.bfloat16),
            rows,
            jax.ShapeDtypeStruct((slots, PAIR), jnp.float32),
            rows,
        ]

    def lanes(self, pair, part=0):
        return pl.ds(pl.multiple_of((part * self.pairs + pair) * PAIR, PAIR), PAIR)

    def start(self):
        slots, tile, some = self.slots, self.tile, self.some
        logits = self.joined[:, 3 * self.pairs * PAIR :].astype(jnp.float32) + self.bias[...]
        logit_rows = logits.T[:some]
        self.logit[...] = logit_rows
        logs = jnp.minimum(logit_rows, 0.0) - jnp.log1p(jnp.exp(-jnp.abs(logit_rows)))
        ones = low_triangle(tile).astype(jnp.float32)
        carry = jnp.zeros((some, 1), jnp.float32)
        for first in range(0, slots, tile):
            sums = exact(logs[:, first : first + tile], ones) + carry
            self.row[:, first : first + tile] = sums
            carry = sums[:, tile - 1 : tile]
        wide = jnp.concatenate([self.row[...], jnp.zeros((PAIR - some, slots), jnp.float32)], axis=0).T
        usable = lax.broadcasted_iota(jnp.int32, (slots, PAIR), 0) < self.length[...]
        self.col[...] = jnp.where(usable, wide, -NEG_FILL)

    def pair(self, pair):
        slots, tile, half = self.slots, self.tile, self.head_size
        key_all = self.joined[:, self.lanes(pair, 1)]
        value_t = self.joined[:, self.lanes(pair, 2)].T
        query_t = (self.joined[:, self.lanes(pair)].astype(jnp.float32) * self.scale).astype(jnp.bfloat16).T
        sub = lax.broadcasted_iota(jnp.int32, (PAIR, tile), 0)
        wide = lax.broadcasted_iota(jnp.int32, (slots, PAIR), 1)
        diag = low_triangle(tile)
        columns = [
            jnp.sum(jnp.where(wide == 2 * pair + a, self.col[...], 0.0), axis=1, keepdims=True) for a in range(2)
        ]
        for number in range(slots // tile):
            first, last = number * tile, (number + 1) * tile
            outs = []
            for a in range(2):
                mine = (sub >= a * half) & (sub < (a + 1) * half)
                at = pl.ds(2 * pair + a, 1)
                query = jnp.where(mine, query_t[:, first:last], jnp.zeros((), query_t.dtype))
                scores = product(key_all[:last], query)
                own_row = self.row[at, first:last]
                scores = scores + (own_row - columns[a][:last])
                tail = jnp.where(diag, scores[first:], NEG_FILL)
                scores = tail if number == 0 else jnp.concatenate([scores[:first], tail], axis=0)
                top = jnp.max(scores, axis=0, keepdims=True)
                weights = jnp.exp(scores - top)
                total = jnp.sum(weights, axis=0, keepdims=True)
                mixed = product(value_t[a * half : (a + 1) * half, :last], weights.astype(jnp.bfloat16))
                outs.append(mixed / total)
                self.offset[at, first:last] = own_row - (top + jnp.log(total))
            self.attended[first:last, self.lanes(pair)] = jnp.concatenate(outs, axis=0).T.astype(jnp.bfloat16)


def attention_fwd(joined, bias, length, head_size, scale):
    slots = joined.shape[0]
    pairs = (joined.shape[1] // PAIR - 1) // 3

    def body(joined_ref, bias_ref, length_ref, attended, offset, col, logit, row):
        work = Forward(joined_ref, bias_ref, length_ref, attended, offset, col, logit, row, head_size, scale)
        work.start()
        offset[...] = jnp.zeros_like(offset)

        def step(pair, carry):
            work.pair(pair)
            return carry

        lax.fori_loop(0, pairs, step, 0)

    vmem = pl.BlockSpec(memory_space=pltpu.VMEM)
    return pl.pallas_call(
        body,
        in_specs=[vmem] * 3,
        out_specs=[vmem] * 4,
        out_shape=Forward.results(slots, pairs),
        scratch_shapes=[pltpu.VMEM((Forward.some, slots), jnp.float32)],
        compiler_params=pltpu.CompilerParams(vmem_limit_bytes=56 << 20),
        cost_estimate=pl.CostEstimate(
            flops=4 * slots * slots * pairs * PAIR, bytes_accessed=8 * slots * pairs * PAIR, transcendentals=0
        ),
        name="attention_fwd",
    )(joined, bias, length)


def backward_scratch(slots):
    return [
        pltpu.VMEM((slots, PAIR), jnp.float32),
        pltpu.VMEM((slots, PAIR), jnp.float32),
        pltpu.VMEM((slots, PAIR), jnp.float32),
        pltpu.VMEM((8, slots), jnp.float32),
    ]


class Backward:
    def __init__(self, joined, d_out, offset, col, logit, grads, dk_acc, dv_acc, dcol, drow, head_size, scale):
        self.joined, self.d_out, self.offset, self.col = joined, d_out, offset, col
        self.logit, self.grads, self.dk_acc, self.dv_acc = logit, grads, dk_acc, dv_acc
        self.dcol, self.drow, self.head_size, self.scale = dcol, drow, head_size, scale
        self.slots = joined.shape[0]
        self.pairs = (joined.shape[1] // PAIR - 1) // 3
        self.tile = min(256, self.slots)

    def start(self):
        self.dcol[...] = jnp.zeros_like(self.dcol)
        self.drow[...] = jnp.zeros_like(self.drow)

    def lanes(self, pair, part=0):
        return pl.ds(pl.multiple_of((part * self.pairs + pair) * PAIR, PAIR), PAIR)

    def pair(self, pair):
        slots, tile, half = self.slots, self.tile, self.head_size
        dk_acc, dv_acc, dcol, drow = self.dk_acc, self.dv_acc, self.dcol, self.drow
        queries = (self.joined[:, self.lanes(pair)].astype(jnp.float32) * self.scale).astype(jnp.bfloat16)
        key_all = self.joined[:, self.lanes(pair, 1)]
        value_all = self.joined[:, self.lanes(pair, 2)]
        d_out = self.d_out[:, self.lanes(pair)]
        query_t, key_t, dout_t = queries.T, key_all.T, d_out.T
        sub = lax.broadcasted_iota(jnp.int32, (PAIR, tile), 0)
        lanes = lax.broadcasted_iota(jnp.int32, (tile, PAIR), 1)
        wide = lax.broadcasted_iota(jnp.int32, (slots, PAIR), 1)
        diag = low_triangle(tile)
        zero = jnp.zeros((), jnp.bfloat16)
        columns = [
            jnp.sum(jnp.where(wide == 2 * pair + a, self.col[...], 0.0), axis=1, keepdims=True) for a in range(2)
        ]
        dk_acc[...] = jnp.zeros_like(dk_acc)
        dv_acc[...] = jnp.zeros_like(dv_acc)
        for number in range(slots // tile):
            first, last = number * tile, (number + 1) * tile
            outs = []
            for a in range(2):
                mine = (sub >= a * half) & (sub < (a + 1) * half)
                own = (lanes >= a * half) & (lanes < (a + 1) * half)
                at = pl.ds(2 * pair + a, 1)
                scores = product(key_all[:last], jnp.where(mine, query_t[:, first:last], zero))
                scores = scores + (self.offset[at, first:last] - columns[a][:last])
                tail = jnp.where(diag, scores[first:], NEG_FILL)
                scores = tail if number == 0 else jnp.concatenate([scores[:first], tail], axis=0)
                probs = jnp.exp(scores)
                d_probs = product(value_all[:last], jnp.where(mine, dout_t[:, first:last], zero))
                dot = jnp.sum(d_probs * probs, axis=0, keepdims=True)
                d_full = probs * (d_probs - dot)
                d_scores = d_full.astype(jnp.bfloat16)
                drow[at, first:last] = jnp.sum(d_full, axis=0, keepdims=True)
                sums = jnp.sum(d_full, axis=1, keepdims=True)
                dcol[:last, :] += jnp.where(wide[:last] == 2 * pair + a, sums, 0.0)
                outs.append(product(key_t[a * half : (a + 1) * half, :last], d_scores) * self.scale)
                dk_acc[:last, :] += product(d_scores, jnp.where(own, queries[first:last, :], zero))
                dv_acc[:last, :] += product(
                    probs.astype(jnp.bfloat16), jnp.where(own, d_out[first:last, :], zero)
                )
            self.grads[first:last, self.lanes(pair)] = jnp.concatenate(outs, axis=0).T.astype(self.grads.dtype)
        self.grads[:, self.lanes(pair, 1)] = dk_acc[...].astype(self.grads.dtype)
        self.grads[:, self.lanes(pair, 2)] = dv_acc[...].astype(self.grads.dtype)

    def end(self, bias_grad):
        slots, tile, some = self.slots, self.tile, 8
        change = self.drow[...] - self.dcol[...].T[:some]
        rows = lax.broadcasted_iota(jnp.int32, (tile, tile), 0)
        ones = (rows >= lax.broadcasted_iota(jnp.int32, (tile, tile), 1)).astype(jnp.float32)
        carry = jnp.zeros((some, 1), jnp.float32)
        pieces = []
        for first in reversed(range(0, slots, tile)):
            sums = exact(change[:, first : first + tile], ones) + carry
            carry = sums[:, :1]
            pieces.insert(0, sums)
        grad = jnp.concatenate(pieces, axis=1) * jax.nn.sigmoid(-self.logit[...])
        heads = lax.broadcasted_iota(jnp.int32, (some, slots), 0)
        grad = jnp.where(heads < 2 * self.pairs, grad, 0.0)
        bias_grad[...] = jnp.broadcast_to(jnp.sum(grad, axis=1, keepdims=True), bias_grad.shape)
        wide = jnp.concatenate([grad, jnp.zeros((PAIR - some, slots), jnp.float32)], axis=0).T
        self.grads[:, 3 * self.pairs * PAIR : (3 * self.pairs + 1) * PAIR] = wide.astype(self.grads.dtype)


def attention_bwd(joined, d_out, offset, col, logit, head_size, scale):
    slots, width = joined.shape
    pairs = (width // PAIR - 1) // 3

    def body(joined_ref, d_out_ref, offset_ref, col_ref, logit_ref, grads, bias_grad, *scratch):
        work = Backward(
            joined_ref, d_out_ref, offset_ref, col_ref, logit_ref, grads, *scratch, head_size, scale
        )
        work.start()

        def step(pair, carry):
            work.pair(pair)
            return carry

        lax.fori_loop(0, pairs, step, 0)
        work.end(bias_grad)

    vmem = pl.BlockSpec(memory_space=pltpu.VMEM)
    return pl.pallas_call(
        body,
        in_specs=[vmem] * 5,
        out_specs=[vmem] * 2,
        out_shape=[
            jax.ShapeDtypeStruct((slots, width), jnp.bfloat16),
            jax.ShapeDtypeStruct((8, PAIR), jnp.float32),
        ],
        scratch_shapes=backward_scratch(slots),
        compiler_params=pltpu.CompilerParams(vmem_limit_bytes=56 << 20),
        cost_estimate=pl.CostEstimate(
            flops=10 * slots * slots * pairs * PAIR, bytes_accessed=14 * slots * pairs * PAIR, transcendentals=0
        ),
        name="attention_bwd",
    )(joined, d_out, offset, col, logit)


MESH = pl.DeviceIdType.MESH
VMEM_LIMIT = 62 << 20


def square(groups):
    return groups == 4


def sides():
    rank = lax.axis_index("seq")
    return rank, rank + 1 - 2 * lax.rem(rank, 2), lax.rem(rank + 2, 4), 3 - rank


def meet(*others):
    barrier = pltpu.get_barrier_semaphore()
    for other in others:
        pl.semaphore_signal(barrier, inc=1, device_id=other, device_id_type=MESH)
    pl.semaphore_wait(barrier, len(others))


def push(source, target, send, recv, device):
    copy = pltpu.make_async_remote_copy(
        src_ref=source,
        dst_ref=target,
        send_sem=send,
        recv_sem=recv,
        device_id=device,
        device_id_type=MESH,
    )
    copy.start()
    return copy


class SquareGather:
    def __init__(self, own, full, send, recv):
        self.own, self.full, self.send, self.recv = own, full, send, recv
        self.rows = own.shape[0]
        self.half = self.rows // 2

    def place(self, rank, part):
        return self.full.at[pl.ds(pl.multiple_of(rank * self.rows + part * self.half, self.half), self.half)]

    def copy(self, index):
        me, side, down, across = sides()
        mine = [self.own.at[pl.ds(part * self.half, self.half)] for part in (0, 1)]
        source, target, peer = (
            (mine[0], self.place(me, 0), side),
            (mine[1], self.place(me, 1), down),
            (mine[1], self.place(me, 1), side),
            (mine[0], self.place(me, 0), down),
            (self.place(side, 0), self.place(side, 0), down),
            (self.place(down, 1), self.place(down, 1), side),
        )[index]
        return pltpu.make_async_remote_copy(
            src_ref=source,
            dst_ref=target,
            send_sem=self.send.at[index],
            recv_sem=self.recv.at[index],
            device_id={"seq": peer},
            device_id_type=MESH,
        )

    def start(self):
        for index in range(4):
            self.copy(index).start()

    def relay(self):
        for index in (0, 1):
            self.copy(index).wait_recv()
            self.copy(4 + index).start()

    def near(self):
        self.copy(2).wait_recv()
        self.copy(3).wait_recv()

    def far(self):
        self.copy(4).wait_recv()
        self.copy(5).wait_recv()

    def finish(self):
        for index in range(6):
            self.copy(index).wait_send()


def block_product(left, right, transposed, tile, store):
    total = right.shape[0] if transposed else right.shape[1]

    def step(number, carry):
        columns = pl.ds(pl.multiple_of(number * tile, tile), tile)
        if transposed:
            store(columns, product_nt(left[...], right[columns, :]))
        else:
            store(columns, product(left[...], right[:, columns]))
        return carry

    lax.fori_loop(0, total // tile, step, 0)


def transposed_product(left, right, out):
    tall = 512 if out.shape[0] % 512 == 0 else 384
    wide = next(size for size in (512, 384, 640, 128) if out.shape[1] % size == 0)
    across = out.shape[1] // wide

    def step(number, carry):
        rows = pl.ds(pl.multiple_of((number // across) * tall, tall), tall)
        columns = pl.ds(pl.multiple_of(lax.rem(number, across) * wide, wide), wide)
        out[rows, columns] = product_tn(left[:, rows], right[:, columns]).astype(out.dtype)
        return carry

    lax.fori_loop(0, (out.shape[0] // tall) * across, step, 0)


def line():
    shards, place = lax.axis_size("wshard"), lax.axis_index("wshard")
    chips = shards // 2
    chip, core = place // 2, lax.rem(place, 2)
    forth = {"wshard": lax.rem(place + 2, shards)}
    back = {"wshard": lax.rem(place + shards - 2, shards)}
    twin = {"wshard": place + 1 - 2 * core}
    return chips, chip, core, forth, back, twin


class LineGather:
    @staticmethod
    def scratch(chips):
        dma = pltpu.SemaphoreType.DMA
        return [dma((3, chips)), dma((2 * chips,)), dma((1,))]

    def __init__(self, own, full, send, recv, local):
        self.own, self.full, self.local = own, full, local.at[0]
        self.sends = (send.at[0], send.at[1], send.at[2])
        self.recv = recv
        self.rows = own.shape[0]
        self.chips, self.chip, self.core, *self.devices = line()

    def place(self, chip, core):
        return self.full.at[pl.ds(pl.multiple_of((2 * chip + core) * self.rows, self.rows), self.rows)]

    def copy(self, way, chip, source=None):
        target = self.place(chip, self.core)
        return pltpu.make_async_remote_copy(
            src_ref=target if source is None else source,
            dst_ref=target,
            send_sem=self.sends[way].at[chip],
            recv_sem=self.recv.at[2 * chip + self.core],
            device_id=self.devices[way],
            device_id_type=MESH,
        )

    def wait_for(self, chip, core):
        target = self.place(chip, core)
        pltpu.make_async_remote_copy(
            src_ref=target,
            dst_ref=target,
            send_sem=self.sends[2].at[0],
            recv_sem=self.recv.at[2 * chip + core],
            device_id=self.devices[2],
            device_id_type=MESH,
        ).wait_recv()

    def start(self):
        @pl.when(self.chip < self.chips - 1)
        def _():
            self.copy(0, self.chip, self.own).start()

        @pl.when(self.chip > 0)
        def _():
            self.copy(1, self.chip, self.own).start()

        self.copy(2, self.chip, self.own).start()
        self.keep().start()

    def keep(self):
        return pltpu.make_async_copy(self.own, self.place(self.chip, self.core), self.local)

    def step(self, number):
        left, right = self.chip - number, self.chip + number

        @pl.when(left >= 0)
        def _():
            self.wait_for(left, self.core)

            @pl.when(self.chip < self.chips - 1)
            def _():
                self.copy(0, left).start()

            self.copy(2, left).start()

        @pl.when(right < self.chips)
        def _():
            self.wait_for(right, self.core)

            @pl.when(self.chip > 0)
            def _():
                self.copy(1, right).start()

            self.copy(2, right).start()

    def finish(self):
        for chip in range(self.chips):
            self.wait_for(chip, 1 - self.core)
            self.copy(2, chip).wait_send()

            @pl.when((chip <= self.chip) & (self.chip < self.chips - 1))
            def _():
                self.copy(0, chip).wait_send()

            @pl.when((chip >= self.chip) & (self.chip > 0))
            def _():
                self.copy(1, chip).wait_send()

        self.keep().wait()


class LineSpread:
    @staticmethod
    def scratch(chips):
        dma = pltpu.SemaphoreType.DMA
        return [dma((chips,)), dma((2,))]

    def __init__(self, own, whole, send, recv):
        self.own, self.whole, self.send, self.recv = own, whole, send, recv
        self.chips, self.chip, self.core, forth, back, self.twin = line()
        shards, place = 2 * self.chips, lax.axis_index("wshard")
        self.devices = [{"wshard": lax.rem(place + 2 * k, shards)} for k in range(1, self.chips)]
        self.mine = self.chip == lax.axis_index("seq")

    def copy(self, index):
        target = self.whole.at[self.core]
        last = index == self.chips - 1
        return pltpu.make_async_remote_copy(
            src_ref=target if last else self.own,
            dst_ref=target,
            send_sem=self.send.at[index],
            recv_sem=self.recv.at[1 if last else 0],
            device_id=self.twin if last else self.devices[index],
            device_id_type=MESH,
        )

    def start(self):
        @pl.when(self.mine)
        def _():
            for index in range(self.chips - 1):
                self.copy(index).start()
            self.whole[self.core] = self.own[...]

    def relay(self):
        @pl.when(jnp.logical_not(self.mine))
        def _():
            self.copy(0).wait_recv()

        self.copy(self.chips - 1).start()

    def end(self):
        self.copy(self.chips - 1).wait()

        @pl.when(self.mine)
        def _():
            for index in range(self.chips - 1):
                self.copy(index).wait_send()


class Regroup:
    @staticmethod
    def scratch(rows, width):
        dma = pltpu.SemaphoreType.DMA
        return [pltpu.VMEM((4, rows, width), jnp.bfloat16), dma((7,)), dma((7,))]

    def __init__(self, piece, out, fours, send, recv):
        self.piece, self.out, self.fours, self.send, self.recv = piece, out, fours, send, recv
        self.rank, self.place = lax.axis_index("seq"), lax.axis_index("wshard")
        self.number = lax.rem(self.place, 4)
        self.others = [{"seq": lax.rem(self.rank + k, 4)} for k in range(1, 4)]
        self.along = [{"wshard": lax.rem(self.place + k, 8)} for k in range(1, 8)]

    def near(self, index):
        return pltpu.make_async_remote_copy(
            src_ref=self.piece,
            dst_ref=self.fours.at[self.rank],
            send_sem=self.send.at[index],
            recv_sem=self.recv.at[index],
            device_id=self.others[index],
            device_id_type=MESH,
        )

    def owner(self, rank):
        return 2 * rank + self.place // 4

    def far(self, rank, number):
        return pltpu.make_async_remote_copy(
            src_ref=self.fours.at[rank],
            dst_ref=self.out.at[number],
            send_sem=self.send.at[3 + rank],
            recv_sem=self.recv.at[3 + number],
            device_id={"wshard": self.owner(rank)},
            device_id_type=MESH,
        )

    def start(self):
        for index in range(3):
            self.near(index).start()
        self.fours[self.rank] = self.piece[...]

    def relay(self):
        for index in range(3):
            self.near(index).wait()
        for rank in range(4):

            @pl.when(self.owner(rank) != self.place)
            def _():
                self.far(rank, self.number).start()

            @pl.when(self.owner(rank) == self.place)
            def _():
                self.out[self.number] = self.fours[rank]

    def end(self):
        for rank in range(4):

            @pl.when(self.owner(rank) != self.place)
            def _():
                self.far(rank, self.number).wait_send()

        for number in range(4):

            @pl.when(4 * lax.rem(self.place, 2) + number != self.place)
            def _():
                self.far(0, number).wait_recv()


class Everywhere:
    def __init__(self, values, out, ranks, total, places, send, recv):
        self.values, self.out, self.ranks, self.total, self.places = values, out, ranks, total, places
        self.send, self.recv = send, recv
        self.groups, self.shards = ranks.shape[0], places.shape[0]
        self.rank, self.place = lax.axis_index("seq"), lax.axis_index("wshard")

    def others(self):
        return [{"seq": lax.rem(self.rank + k, self.groups)} for k in range(1, self.groups)]

    def along(self):
        return [{"wshard": lax.rem(self.place + k, self.shards)} for k in range(1, self.shards)]

    def start(self):
        self.first = [
            push(self.values, self.ranks.at[self.rank], self.send.at[k], self.recv.at[k], other)
            for k, other in enumerate(self.others())
        ]
        self.ranks[self.rank] = self.values[...]

    def relay(self):
        for copy in self.first:
            copy.wait()
        ranks, groups = self.ranks, self.groups
        self.total[...] = (ranks[0] + ranks[1]) + (ranks[2] + ranks[3])
        self.second = [
            push(self.total, self.places.at[self.place], self.send.at[groups + k], self.recv.at[groups + k], other)
            for k, other in enumerate(self.along())
        ]
        self.places[self.place] = self.total[...]

    def end(self):
        for copy in self.second:
            copy.wait()
        sums = [self.places[k] + self.places[k + 1] for k in range(0, self.shards, 2)]
        self.out[...] = (sums[0] + sums[1]) + (sums[2] + sums[3])


def last_gather(values, small, collective_id):
    count = len(values)
    groups = lax.axis_size("seq")
    shards = 2 * groups

    def body(*refs):
        own, small_ref = refs[:count], refs[count]
        full, small_out = refs[count + 1 : 2 * count + 1], refs[2 * count + 1]
        send, recv, local = refs[2 * count + 2 : 2 * count + 5]
        me, side, down, across = sides()
        total = Everywhere(small_ref, small_out, *refs[2 * count + 5 :])
        meet(*total.others(), *total.along())
        jobs = [SquareGather(own[i], full[i], send.at[i], recv.at[i]) for i in range(count)]
        total.start()
        keeps = []
        for i, job in enumerate(jobs):
            job.start()
            rows = own[i].shape[0]
            keep = pltpu.make_async_copy(
                own[i], full[i].at[pl.ds(pl.multiple_of(me * rows, rows), rows)], local.at[i]
            )
            keep.start()
            keeps.append(keep)
        total.relay()
        for job in jobs:
            job.relay()
        total.end()
        for job, keep in zip(jobs, keeps):
            job.near()
            job.far()
            job.finish()
            keep.wait()

    vmem = pl.BlockSpec(memory_space=pltpu.VMEM)
    dma = pltpu.SemaphoreType.DMA
    return pl.pallas_call(
        body,
        in_specs=[vmem] * (count + 1),
        out_specs=[pl.BlockSpec(memory_space=pl.ANY)] * count + [vmem],
        out_shape=[jax.ShapeDtypeStruct((4 * v.shape[0],) + v.shape[1:], v.dtype) for v in values]
        + [jax.ShapeDtypeStruct(small.shape, jnp.float32)],
        scratch_shapes=[
            dma((count, 6)),
            dma((count, 6)),
            dma((count,)),
            pltpu.VMEM((groups,) + small.shape, jnp.float32),
            pltpu.VMEM(small.shape, jnp.float32),
            pltpu.VMEM((shards,) + small.shape, jnp.float32),
            dma((groups + shards,)),
            dma((groups + shards,)),
        ],
        compiler_params=pltpu.CompilerParams(
            collective_id=collective_id, has_side_effects=True, vmem_limit_bytes=VMEM_LIMIT
        ),
        name="last_gather",
    )(*values, small)


def join_units(every_gate, every_up, down, out, part):
    groups, rows, units = every_gate.shape
    steps = 4
    tall = rows // steps

    def body(gate_in, up_in, down_in, out_in, gate_ref, up_ref, down_ref, out_ref):
        for every, to_ref in ((gate_in, gate_ref), (up_in, up_ref)):
            for group in range(groups):
                for block in range(units // part):
                    to = (block * groups + group) * part
                    to_ref[:, to : to + part] = every[group, :, block * part : (block + 1) * part].astype(
                        jnp.float32
                    )
        down_ref[...] = down_in[...].astype(jnp.float32)
        out_ref[...] = out_in[...].astype(jnp.float32)

    def flat(value):
        return pl.BlockSpec((value.shape[0] // steps, value.shape[1]), lambda i: (i, 0))

    wide = jax.ShapeDtypeStruct((rows, groups * units), jnp.float32)
    results = [wide, wide, *(jax.ShapeDtypeStruct(v.shape, jnp.float32) for v in (down, out))]
    return pl.pallas_call(
        body,
        grid=(steps,),
        in_specs=[pl.BlockSpec((groups, tall, units), lambda i: (0, i, 0))] * 2 + [flat(down), flat(out)],
        out_specs=[flat(value) for value in results],
        out_shape=results,
        name="join_units",
    )(every_gate, every_up, down, out)


def join_columns(every, gate, columns, starts, forget_at, heads):
    groups, rows, lanes = every.shape
    own = heads // groups
    steps = 4
    tall = rows // steps

    def body(every_ref, gate_ref, *outs):
        for group in range(groups):
            to = slice(group * columns, (group + 1) * columns)
            for start, out in zip(starts, outs):
                out[:, to] = every_ref[group, :, start : start + columns].astype(jnp.float32)
            outs[-2][:, to] = gate_ref[group].astype(jnp.float32)
            outs[-1][:, group * own : (group + 1) * own] = every_ref[
                group, :, forget_at : forget_at + own
            ].astype(jnp.float32)

    def flat(value):
        return pl.BlockSpec((tall, value.shape[1]), lambda i: (i, 0))

    wide = jax.ShapeDtypeStruct((rows, groups * columns), jnp.float32)
    results = [wide] * (len(starts) + 1) + [jax.ShapeDtypeStruct((rows, heads), jnp.float32)]
    return pl.pallas_call(
        body,
        grid=(steps,),
        in_specs=[pl.BlockSpec((groups, tall, v.shape[2]), lambda i: (0, i, 0)) for v in (every, gate)],
        out_specs=[flat(value) for value in results],
        out_shape=results,
        name="join_columns",
    )(every, gate)


class SquareScatter:
    @staticmethod
    def scratch(rows, width):
        half = rows // 2
        low = jnp.bfloat16
        return [
            pltpu.VMEM((rows, width), low),
            pltpu.VMEM((2, half, width), low),
            pltpu.VMEM((2, half, width), jnp.float32),
            pltpu.VMEM((6, half, width), low),
            pltpu.VMEM((2, half, width), low),
            pltpu.SemaphoreType.DMA((6,)),
            pltpu.SemaphoreType.DMA((6,)),
        ]

    def __init__(self, lefts, rights, transposed, out, far, near, kept, land, carry, send, recv):
        self.lefts, self.rights, self.transposed, self.out = lefts, rights, transposed, out
        self.far, self.near, self.kept, self.land, self.carry = far, near, kept, land, carry
        self.send, self.recv = send, recv
        self.rows, self.width = out.shape
        self.half = self.rows // 2
        self.tile = self.width // 3 if self.width % 384 == 0 else self.width

    def copy(self, index):
        me, side, down, across = sides()
        source = (
            self.far.at[pl.ds(0, self.half)],
            self.far.at[pl.ds(self.half, self.half)],
            self.near.at[0],
            self.near.at[1],
            self.carry.at[0],
            self.carry.at[1],
        )[index]
        return pltpu.make_async_remote_copy(
            src_ref=source,
            dst_ref=self.land.at[index],
            send_sem=self.send.at[index],
            recv_sem=self.recv.at[index],
            device_id={"seq": down if index in (0, 3, 5) else side},
            device_id_type=MESH,
        )

    def partial(self, rank, store):
        at = pl.ds(pl.multiple_of(rank * self.rows, self.rows), self.rows)

        def step(number, carried):
            columns = pl.ds(pl.multiple_of(number * self.tile, self.tile), self.tile)
            value = None
            for a, b in zip(self.lefts, self.rights):
                if self.transposed:
                    term = product_nt(a[at, :], b[columns, :])
                else:
                    term = product(a[at, :], b[:, columns])
                value = term if value is None else value + term
            store(columns, value)
            return carried

        lax.fori_loop(0, self.width // self.tile, step, 0)

    def begin(self):
        me, side, down, across = sides()
        half, far, near, kept = self.half, self.far, self.near, self.kept

        def store_far(columns, value):
            far[:, columns] = value.astype(far.dtype)

        def store_side(columns, value):
            kept[0, :, columns] = value[:half]
            near[0, :, columns] = value[half:].astype(near.dtype)

        def store_down(columns, value):
            near[1, :, columns] = value[:half].astype(near.dtype)
            kept[1, :, columns] = value[half:]

        self.partial(across, store_far)
        self.copy(0).start()
        self.copy(1).start()
        self.partial(side, store_side)
        self.copy(2).start()
        self.partial(down, store_down)
        self.copy(3).start()

    def relay(self):
        for index in (0, 1):
            self.copy(index).wait_recv()
            total = self.kept[index] + self.land[index].astype(jnp.float32)
            self.carry[index] = total.astype(self.carry.dtype)
            self.copy(4 + index).start()

    def own(self):
        out = self.out

        def store_own(columns, value):
            out[:, columns] = value

        self.partial(lax.axis_index("seq"), store_own)

    def end(self):
        for index in (2, 3, 4, 5):
            self.copy(index).wait_recv()
        land, half = self.land, self.half
        self.out[:half, :] += land[3].astype(jnp.float32) + land[4].astype(jnp.float32)
        self.out[half:, :] += land[2].astype(jnp.float32) + land[5].astype(jnp.float32)
        for index in range(6):
            self.copy(index).wait_send()


class LineScatter:
    @staticmethod
    def scratch(chips, rows, width):
        low = jnp.bfloat16
        dma = pltpu.SemaphoreType.DMA
        return [pltpu.VMEM((chips, rows, width), low)] * 3 + [dma((2, chips)), dma((3, chips))]

    def __init__(self, terms, out, twin_in, forth_in, back_in, send, recv):
        self.terms, self.out, self.twin_in = terms, out, twin_in
        self.forth_in, self.back_in, self.send, self.recv = forth_in, back_in, send, recv
        self.chips, self.chip, self.core, *self.devices = line()
        self.rows = twin_in.shape[1]

    def term(self, chip, core):
        return self.terms.at[pl.ds(pl.multiple_of((2 * chip + core) * self.rows, self.rows), self.rows)]

    def swap(self, chip):
        return pltpu.make_async_remote_copy(
            src_ref=self.term(chip, 1 - self.core),
            dst_ref=self.twin_in.at[chip],
            send_sem=self.send.at[0, chip],
            recv_sem=self.recv.at[0, chip],
            device_id=self.devices[2],
            device_id_type=MESH,
        )

    def hop(self, way, chip):
        return pltpu.make_async_remote_copy(
            src_ref=self.twin_in.at[chip],
            dst_ref=(self.forth_in, self.back_in)[way].at[chip],
            send_sem=self.send.at[1, chip],
            recv_sem=self.recv.at[1 + way, chip],
            device_id=self.devices[way],
            device_id_type=MESH,
        )

    def start(self):
        for chip in (self.chips - 1, 0, *range(1, self.chips - 1)):
            self.swap(chip).start()

    def pair(self, chip):
        return self.term(chip, self.core)[...].astype(jnp.float32) + self.twin_in[chip].astype(jnp.float32)

    def pass_on(self, way, chip, first):
        self.swap(chip).wait_recv()
        total = self.pair(chip)
        if not first:
            self.hop(way, chip).wait_recv()
            total = total + (self.forth_in, self.back_in)[way][chip].astype(jnp.float32)
        self.twin_in[chip] = total.astype(self.twin_in.dtype)
        self.hop(way, chip).start()

    def slot(self, number):
        last = self.chips - 1
        for chip in range(self.chips):
            forth, back = number - (last - chip), last - (number - chip)
            if 0 <= forth < chip:

                @pl.when(self.chip == forth)
                def _():
                    self.pass_on(0, chip, forth == 0)

            if chip < back <= last:

                @pl.when(self.chip == back)
                def _():
                    self.pass_on(1, chip, back == last)

    def end(self):
        for chip in range(self.chips):

            @pl.when(self.chip == chip)
            def _():
                self.swap(chip).wait_recv()
                total = self.pair(chip)
                if chip > 0:
                    self.hop(0, chip).wait_recv()
                    total = total + self.forth_in[chip].astype(jnp.float32)
                if chip < self.chips - 1:
                    self.hop(1, chip).wait_recv()
                    total = total + self.back_in[chip].astype(jnp.float32)
                self.out[...] = total.astype(self.out.dtype)

            self.swap(chip).wait_send()

            @pl.when(self.chip != chip)
            def _():
                self.hop(0, chip).wait_send()


def middle_backward(joined, d_out, offset, col, logit, hidden, w_down, gated, grad_branch, terms_up, share_down,
                    normed, d_pre, head_size, scale, collective_id):
    slots, lanes = joined.shape
    width = w_down.shape[1]
    tokens = slots // 4
    columns = gated.shape[1]
    shards = 2 * lax.axis_size("seq")
    chips = shards // 2
    rows_up = terms_up.shape[0] // shards

    def body(joined_ref, d_out_ref, offset_ref, col_ref, logit_ref, hidden_ref, down_ref, gated_ref, branch_ref,
             up_ref, share_ref, normed_ref, pre_ref,
             grads, bias_grad, lowered, collected, share_up, share_pre, every_down, terms, terms_pre, send, recv, keep, *scratch):
        me, side, down, across = sides()
        line_chips, chip, core, forth, back, twin = line()
        meet({"seq": side}, {"seq": down}, forth, back, twin)
        work = Backward(
            joined_ref, d_out_ref, offset_ref, col_ref, logit_ref, grads, *scratch[:4], head_size, scale
        )
        job = SquareScatter([hidden_ref], [down_ref], False, lowered, *scratch[4:11])
        collect = LineScatter(terms, collected, *scratch[11:16])
        run = LineScatter(up_ref, share_up, *scratch[16:21])
        run_pre = LineScatter(terms_pre, share_pre, *scratch[21:])
        every = SquareGather(share_ref, every_down, send, recv)
        size = share_ref.shape[0]
        kept = pltpu.make_async_copy(
            share_ref, every_down.at[pl.ds(pl.multiple_of(me * size, size), size)], keep.at[0]
        )
        kept.start()
        run.start()
        transposed_product(gated_ref, branch_ref, terms)
        collect.start()
        transposed_product(normed_ref, pre_ref, terms_pre)
        run_pre.start()
        collect.slot(0)
        run.slot(0)
        job.begin()
        run_pre.slot(0)
        work.start()

        def step(pair, carry):
            work.pair(pair)

            @pl.when(pair == 0)
            def _():
                job.relay()
                collect.slot(1)
                run.slot(1)
                run_pre.slot(1)
                every.start()

            @pl.when(pair == 1)
            def _():
                collect.slot(2)
                run.slot(2)
                run_pre.slot(2)

            return carry

        lax.fori_loop(0, work.pairs, step, 0)
        every.relay()
        job.own()
        work.end(bias_grad)
        job.end()
        run.end()
        run_pre.end()
        every.near()
        every.far()
        every.finish()
        kept.wait()
        collect.end()

    vmem = pl.BlockSpec(memory_space=pltpu.VMEM)
    low = jnp.bfloat16
    dma = pltpu.SemaphoreType.DMA
    return pl.pallas_call(
        body,
        in_specs=[vmem] * 13,
        out_specs=[vmem] * 6 + [pl.BlockSpec(memory_space=pl.ANY)],
        out_shape=[
            jax.ShapeDtypeStruct((slots, lanes), low),
            jax.ShapeDtypeStruct((8, PAIR), jnp.float32),
            jax.ShapeDtypeStruct((tokens, width), jnp.float32),
            jax.ShapeDtypeStruct((columns // shards, width), low),
            jax.ShapeDtypeStruct((rows_up, terms_up.shape[1]), low),
            jax.ShapeDtypeStruct((rows_up, columns), low),
            jax.ShapeDtypeStruct((4 * share_down.shape[0], width), low),
        ],
        scratch_shapes=[
            pltpu.VMEM((columns, width), low),
            pltpu.VMEM((width, columns), low),
            dma((6,)),
            dma((6,)),
            dma((1,)),
        ]
        + backward_scratch(slots)
        + SquareScatter.scratch(tokens, width)
        + LineScatter.scratch(chips, columns // shards, width)
        + LineScatter.scratch(chips, rows_up, terms_up.shape[1])
        + LineScatter.scratch(chips, rows_up, columns),
        compiler_params=pltpu.CompilerParams(
            collective_id=collective_id, has_side_effects=True, vmem_limit_bytes=VMEM_LIMIT
        ),
        name="middle_backward",
    )(joined, d_out, offset, col, logit, hidden, w_down, gated, grad_branch, terms_up, share_down, normed, d_pre)


def last_backward(grads, grad_gate_pre, normed, weights, gate_weights, collected, shares, collective_id):
    slots, depth = normed.shape
    front = grads.shape[1]
    count = len(shares)
    tokens = slots // 4
    shards = 2 * lax.axis_size("seq")
    rows = depth // shards

    def body(grads_ref, gate_ref, normed_ref, weights_ref, gate_weights_ref, collected_ref,
             *refs):
        share_refs, refs = refs[:count], refs[count:]
        summed, share, regrouped, *every_refs = refs[: 3 + count]
        terms, send, recv, keep, *scratch = refs[3 + count :]
        me, side, down, across = sides()
        chips, chip, core, forth, back, twin = line()
        regroup = Regroup(collected_ref, regrouped, *scratch[12:])
        meet(*regroup.others, *regroup.along)
        job = SquareScatter(
            [grads_ref, gate_ref],
            [weights_ref, gate_weights_ref],
            True,
            summed,
            *scratch[:7],
        )
        run = LineScatter(terms, share, *scratch[7:12])
        regroup.start()
        every = [
            SquareGather(share_refs[i], every_refs[i], send.at[i], recv.at[i]) for i in range(count)
        ]
        kept = []
        for i in range(count):
            size = share_refs[i].shape[0]
            kept.append(
                pltpu.make_async_copy(
                    share_refs[i],
                    every_refs[i].at[pl.ds(pl.multiple_of(me * size, size), size)],
                    keep.at[i],
                )
            )
            kept[i].start()
            every[i].start()
        transposed_product(normed_ref, grads_ref, terms)
        run.start()
        regroup.relay()
        job.begin()
        run.slot(0)
        for gathering in every:
            gathering.relay()
        job.relay()
        job.own()
        run.slot(1)
        run.slot(2)
        for gathering, copy in zip(every, kept):
            gathering.near()
            gathering.far()
            gathering.finish()
            copy.wait()
        job.end()
        regroup.end()
        run.end()

    vmem = pl.BlockSpec(memory_space=pltpu.VMEM)
    low = jnp.bfloat16
    dma = pltpu.SemaphoreType.DMA
    return pl.pallas_call(
        body,
        in_specs=[vmem] * (6 + count),
        out_specs=[vmem] * 3 + [pl.BlockSpec(memory_space=pl.ANY)] * count,
        out_shape=[
            jax.ShapeDtypeStruct((tokens, depth), jnp.float32),
            jax.ShapeDtypeStruct((rows, front), low),
            jax.ShapeDtypeStruct((4,) + collected.shape, low),
            *(jax.ShapeDtypeStruct((4 * v.shape[0], v.shape[1]), low) for v in shares),
        ],
        scratch_shapes=[
            pltpu.VMEM((depth, front), low),
            dma((count, 6)),
            dma((count, 6)),
            dma((count,)),
        ]
        + SquareScatter.scratch(tokens, depth)
        + LineScatter.scratch(shards // 2, rows, front)
        + Regroup.scratch(*collected.shape),
        compiler_params=pltpu.CompilerParams(
            collective_id=collective_id, has_side_effects=True, vmem_limit_bytes=VMEM_LIMIT
        ),
        name="last_backward",
    )(grads, grad_gate_pre, normed, weights, gate_weights, collected, *shares)


def norm_rows(values, gain):
    scale = lax.rsqrt(jnp.mean(values * values, axis=-1, keepdims=True) + EPS)
    return scale, values * scale * gain


def whole_forward(inputs, gain, cotangent, weights, forget, bias, length, block, w_gate, w_up,
                  head_size, scale, collective_id):
    rows, depth = inputs.shape
    groups = 4
    slots = groups * rows
    chips = groups
    shards = 2 * chips
    mine = weights[0].shape[0]
    columns = depth // groups
    front = 3 * columns + PAIR
    pairs = columns // PAIR
    part = w_gate.shape[1] // (groups * shards)
    units = shards * part
    early = units + units // 2
    low = jnp.bfloat16

    def body(inputs_ref, gain_ref, cot_ref, q_ref, k_ref, v_ref, og_ref, forget_ref, bias_ref, length_ref, block_ref,
             gate_ref, up_ref,
             normed, cot_full, full_front, full_gate, full_out, full_ffn, joined, attended, offset, col, logit,
             gate_pre, gated, middle, own_up,
             own_normed, own_front, own_gate, own_ffn, row, picks, cot_send, cot_recv, keep,
             x_send, x_recv, *scratch):
        me, side, down, across = sides()
        line_chips, chip, core, forth, back, twin = line()
        front_line = LineGather(own_front, full_front, *scratch[0:3])
        gate_line = LineGather(own_gate, full_gate, *scratch[3:6])
        ffn_line = LineGather(own_ffn, full_ffn, *scratch[6:9])
        spread = LineSpread(block_ref, full_out, *scratch[9:11])
        job = SquareScatter([gated], [full_out_rows(full_out)], False, middle, *scratch[11:18])
        taken = []
        my_columns = pl.ds(pl.multiple_of(me * columns, columns), columns)
        for index, source in enumerate((q_ref, k_ref, v_ref)):
            taken.append((source.at[:, my_columns], own_front.at[:, pl.ds(index * columns, columns)]))
        taken.append((og_ref.at[:, my_columns], own_gate))
        for index, source in enumerate((gate_ref, up_ref)):
            for number in range(shards):
                column = pl.ds(pl.multiple_of((number * groups + me) * part, part), part)
                to = index * units + number * part
                target = own_ffn.at[:, pl.ds(to, part)] if to < early else own_up.at[:, pl.ds(to - early, part)]
                taken.append((source.at[:, column], target))
        taken = [pltpu.make_async_copy(a, b, picks.at[i]) for i, (a, b) in enumerate(taken)]
        for copy in taken:
            copy.start()
        values = inputs_ref[...].astype(jnp.float32)
        own_normed[...] = norm_rows(values, gain_ref[...])[1].astype(low)
        own_front[:, 3 * columns :] = forget_ref[...]
        meet({"seq": side}, {"seq": down}, *spread.devices, twin)
        one = SquareGather(own_normed, normed, x_send, x_recv)
        two = SquareGather(cot_ref, cot_full, cot_send, cot_recv)
        one.start()
        for copy in taken:
            copy.wait()
        front_line.start()
        at_me = pl.ds(pl.multiple_of(me * rows, rows), rows)
        kept = pltpu.make_async_copy(cot_ref, cot_full.at[at_me], keep.at[0])
        kept.start()
        normed[at_me, :] = own_normed[...]
        one.relay()
        front_line.step(1)
        spread.start()
        front_line.step(2)
        one.near()
        one.far()
        front_line.step(3)
        front_line.finish()
        one.finish()
        gate_line.start()
        two.start()

        def store_joined(at_columns, value):
            joined[:, at_columns] = value.astype(low)

        block_product(normed, full_front, False, 256, store_joined)
        work = Forward(joined, bias_ref, length_ref, attended, offset, col, logit, row, head_size, scale)
        offset[...] = jnp.zeros_like(offset)
        work.start()

        def step(pair, carry):
            work.pair(pair)

            @pl.when(pair == 0)
            def _():
                gate_line.step(1)
                two.relay()

            @pl.when(pair == 1)
            def _():
                gate_line.step(2)
                ffn_line.start()

            return carry

        lax.fori_loop(0, pairs, step, 0)
        gate_line.step(3)
        spread.relay()
        gate_line.finish()

        def store_gate(at_columns, value):
            gate_pre[:, at_columns] = value

        block_product(normed, full_gate, False, PAIR, store_gate)
        gated[...] = (attended[...].astype(jnp.float32) * jax.nn.sigmoid(gate_pre[...])).astype(low)
        spread.end()
        job.begin()
        job.relay()
        ffn_line.step(1)
        job.own()
        two.near()
        two.far()
        two.finish()
        kept.wait()
        ffn_line.step(2)
        job.end()
        middle[...] += inputs_ref[...].astype(jnp.float32)
        ffn_line.step(3)
        ffn_line.finish()

    def shape(size, kind=low):
        return jax.ShapeDtypeStruct(size, kind)

    vmem = pl.BlockSpec(memory_space=pltpu.VMEM)
    anywhere = pl.BlockSpec(memory_space=pl.ANY)
    dma = pltpu.SemaphoreType.DMA
    return pl.pallas_call(
        body,
        in_specs=[vmem] * 3 + [anywhere] * 4 + [vmem] * 4 + [anywhere] * 2,
        out_specs=[vmem, anywhere, vmem, vmem, vmem, anywhere] + [vmem] * 9,
        out_shape=[
            shape((slots, depth)),
            shape((slots, depth)),
            shape((depth, front)),
            shape((depth, columns)),
            shape((2, block.shape[0], depth)),
            shape((depth, early)),
            shape((slots, front)),
            *Forward.results(slots, pairs),
            shape((slots, columns), jnp.float32),
            shape((slots, columns)),
            shape((rows, depth), jnp.float32),
            shape((mine, 2 * units - early)),
        ],
        scratch_shapes=[
            pltpu.VMEM((rows, depth), low),
            pltpu.VMEM((mine, front), low),
            pltpu.VMEM((mine, columns), low),
            pltpu.VMEM((mine, early), low),
            pltpu.VMEM((Forward.some, slots), jnp.float32),
            dma((4 + 2 * shards,)),
            dma((6,)),
            dma((6,)),
            dma((1,)),
            dma((6,)),
            dma((6,)),
        ]
        + 3 * LineGather.scratch(chips)
        + LineSpread.scratch(chips)
        + SquareScatter.scratch(rows, depth),
        compiler_params=pltpu.CompilerParams(
            collective_id=collective_id, has_side_effects=True, vmem_limit_bytes=VMEM_LIMIT
        ),
        name="whole_forward",
    )(inputs, gain, cotangent, *weights, forget, bias, length, block, w_gate, w_up)


class full_out_rows:
    def __init__(self, ref):
        self.ref = ref
        self.shape = (2 * ref.shape[1], ref.shape[2])

    def __getitem__(self, index):
        rows, columns = index
        return jnp.concatenate([self.ref[0, :, columns], self.ref[1, :, columns]], axis=0)


def feed_forward(middle, gain, weights, own_up, own_down, cotangent, collective_id):
    rows, depth = middle.shape
    slots = 4 * rows
    units = 4 * own_down.shape[0] * 2
    early = weights.shape[1]
    chips = 4
    low = jnp.bfloat16

    def body(middle_ref, gain_ref, weights_ref, up_ref, down_ref, cot_ref,
             normed, hidden, full_up, full_down, grads, terms, own_normed, both, send, recv, *scratch):
        me, side, down, across = sides()
        line_chips, chip, core, forth, back, twin = line()
        up_line = LineGather(up_ref, full_up, *scratch[:3])
        down_line = LineGather(down_ref, full_down, *scratch[3:])
        own_normed[...] = norm_rows(middle_ref[...], gain_ref[...])[1].astype(low)
        meet({"seq": side}, {"seq": down}, forth, back, twin)
        job = SquareGather(own_normed, normed, send, recv)
        up_line.start()
        job.start()

        def rows_of(rank):
            return pl.ds(pl.multiple_of(rank * rows, rows), rows)

        def multiply(rank):
            at = rows_of(rank)

            def store(columns, value):
                both[at, columns] = value

            block_product(normed.at[at], weights_ref, False, 512, store)

        normed[rows_of(me), :] = own_normed[...]
        multiply(me)
        up_line.step(1)
        job.relay()
        down_line.start()
        up_line.step(2)
        up_line.step(3)
        job.near()
        multiply(side)
        multiply(down)
        down_line.step(1)
        job.far()
        multiply(across)
        job.finish()
        up_line.finish()

        def ahead(number, carry):
            at = rows_of(number)
            both[at, early:] = product(normed[at, :], full_up[...])
            gate, upward = both[at, :units], both[at, units:]
            hidden[at, :] = (gate * jax.nn.sigmoid(gate) * upward).astype(low)
            return carry

        lax.fori_loop(0, 4, ahead, 0)
        down_line.step(2)
        transposed_product(hidden, cot_ref, terms)
        down_line.step(3)
        down_line.finish()

        def behind(number, carry):
            at = rows_of(number)
            grad_hidden = product_nt(cot_ref[at, :], full_down[...])
            gate, upward = both[at, :units], both[at, units:]
            sigma = jax.nn.sigmoid(gate)
            grads[at, :units] = (grad_hidden * upward * sigma * (1.0 + gate * (1.0 - sigma))).astype(low)
            grads[at, units:] = (grad_hidden * gate * sigma).astype(low)
            return carry

        lax.fori_loop(0, 4, behind, 0)

    def shape(size, kind=low):
        return jax.ShapeDtypeStruct(size, kind)

    vmem = pl.BlockSpec(memory_space=pltpu.VMEM)
    dma = pltpu.SemaphoreType.DMA
    return pl.pallas_call(
        body,
        in_specs=[vmem] * 6,
        out_specs=[vmem] * 6,
        out_shape=[
            shape((slots, depth)),
            shape((slots, units)),
            shape((depth, own_up.shape[1])),
            shape((units, depth)),
            shape((slots, 2 * units)),
            shape((units, depth)),
        ],
        scratch_shapes=[
            pltpu.VMEM((rows, depth), low),
            pltpu.VMEM((slots, 2 * units), jnp.float32),
            dma((6,)),
            dma((6,)),
        ]
        + 2 * LineGather.scratch(chips),
        compiler_params=pltpu.CompilerParams(
            collective_id=collective_id, has_side_effects=True, vmem_limit_bytes=VMEM_LIMIT
        ),
        name="feed_forward",
    )(middle, gain, weights, own_up, own_down, cotangent)


def feed_backward(grads, weights, up_weights, normed, terms_down, w_out, middle, gain, cotangent, attended, gate_pre,
                  collective_id):
    rows, depth = middle.shape
    slots = 4 * rows
    units = grads.shape[1] // 2
    early = weights.shape[1]
    columns = attended.shape[1]
    shards = 2 * lax.axis_size("seq")
    chips = shards // 2
    low = jnp.bfloat16

    def body(grads_ref, weights_ref, up_weights_ref, normed_ref, down_ref, out_ref, middle_ref, gain_ref, cot_ref, attended_ref,
             pre_ref,
             grad_middle, grad_gain, branch, d_attended, d_pre, terms_up, share_down, share_gate,
             own_branch, summed, terms_gate, send, recv, *scratch):
        me, side, down, across = sides()
        line_chips, chip, core, forth, back, twin = line()
        meet({"seq": side}, {"seq": down}, forth, back, twin)
        first, second = grads_ref.at[:, pl.ds(0, units)], grads_ref.at[:, pl.ds(units, units)]
        job = SquareScatter(
            [grads_ref.at[:, pl.ds(0, early)], grads_ref.at[:, pl.ds(early, 2 * units - early)]],
            [weights_ref, up_weights_ref],
            True,
            summed,
            *scratch[:7],
        )
        run_down = LineScatter(down_ref, share_down, *scratch[7:12])
        run_gate = LineScatter(terms_gate, share_gate, *scratch[12:])
        every = SquareGather(own_branch, branch, send, recv)
        run_down.start()
        job.begin()
        run_down.slot(0)
        transposed_product(normed_ref, first, terms_gate)
        run_gate.start()
        job.relay()
        run_down.slot(1)
        job.own()
        transposed_product(normed_ref, second, terms_up)
        run_down.slot(2)
        run_gate.slot(0)
        job.end()
        values, change = middle_ref[...], summed[...]
        scale = norm_rows(values, gain_ref[...])[0]
        grad_gain[...] = jnp.sum(change * values * scale, axis=0, keepdims=True)
        change = change * gain_ref[...]
        mean = jnp.mean(change * values, axis=-1, keepdims=True)
        total = cot_ref[...].astype(jnp.float32) + scale * change - values * (scale * scale * scale * mean)
        grad_middle[...] = total
        own_branch[...] = total.astype(low)
        every.start()

        def rows_of(rank):
            return pl.ds(pl.multiple_of(rank * rows, rows), rows)

        def multiply(rank):
            at = rows_of(rank)
            grad_gated = product_nt(branch[at, :], out_ref[...])
            sigma = jax.nn.sigmoid(pre_ref[at, :])
            d_attended[at, :] = (grad_gated * sigma).astype(low)
            d_pre[at, :] = (
                grad_gated * attended_ref[at, :].astype(jnp.float32) * sigma * (1.0 - sigma)
            ).astype(low)

        branch[rows_of(me), :] = own_branch[...]
        multiply(me)
        run_gate.slot(1)
        every.relay()
        run_gate.slot(2)
        every.near()
        multiply(side)
        multiply(down)
        run_down.end()
        every.far()
        multiply(across)
        every.finish()
        run_gate.end()

    def shape(size, kind=low):
        return jax.ShapeDtypeStruct(size, kind)

    vmem = pl.BlockSpec(memory_space=pltpu.VMEM)
    dma = pltpu.SemaphoreType.DMA
    return pl.pallas_call(
        body,
        in_specs=[vmem] * 11,
        out_specs=[vmem] * 8,
        out_shape=[
            shape((rows, depth), jnp.float32),
            shape((1, depth), jnp.float32),
            shape((slots, depth)),
            shape((slots, columns)),
            shape((slots, columns)),
            shape((depth, units)),
            shape((terms_down.shape[0] // shards, depth)),
            shape((depth // shards, units)),
        ],
        scratch_shapes=[
            pltpu.VMEM((rows, depth), low),
            pltpu.VMEM((rows, depth), jnp.float32),
            pltpu.VMEM((depth, units), low),
            dma((6,)),
            dma((6,)),
        ]
        + SquareScatter.scratch(rows, depth)
        + LineScatter.scratch(chips, terms_down.shape[0] // shards, depth)
        + LineScatter.scratch(chips, depth // shards, units),
        compiler_params=pltpu.CompilerParams(
            collective_id=collective_id, has_side_effects=True, vmem_limit_bytes=VMEM_LIMIT
        ),
        name="feed_backward",
    )(grads, weights, up_weights, normed, terms_down, w_out, middle, gain, cotangent, attended, gate_pre)


def gather(value, axis_name):
    return lax.all_gather(value, axis_name, axis=0, tiled=True)


def scatter(value, axis_name):
    return lax.psum_scatter(value, axis_name, scatter_dimension=0, tiled=True)


def on_device(
    layer_input,
    lengths,
    norm_attn,
    w_query,
    w_key,
    w_value,
    w_ogate,
    w_forget,
    forget_bias,
    w_out,
    norm_ffn,
    w_gate,
    w_up,
    w_down,
    output_grad,
):
    low = jnp.bfloat16
    tokens, width = layer_input.shape[1:]
    heads = forget_bias.shape[0]
    groups = lax.axis_size("seq")
    shards = lax.axis_size("wshard")
    fast = square(groups) and shards == 2 * groups
    local_heads = heads // groups
    head_size = width // heads
    columns = width // groups
    lanes = columns + -columns % PAIR
    front = 3 * lanes + PAIR
    slots = tokens * groups
    hidden_size = w_gate.shape[1]
    part = hidden_size // (groups * shards)
    units = shards * part
    scale = head_size ** (-0.5)
    length = lengths[0]
    seq_rank = lax.axis_index("seq")
    shard_rank = lax.axis_index("wshard")
    per_block = shards // groups
    positions = seq_rank * tokens + jnp.arange(tokens, dtype=jnp.int32)
    valid_slots = (positions < length)[:, None]
    inputs = layer_input[0].astype(jnp.float32)
    cotangent_low = jnp.where(valid_slots, output_grad[0], jnp.zeros((), low))
    cotangent = cotangent_low.astype(jnp.float32)

    def own_columns(weight, size):
        taken = lax.dynamic_slice_in_dim(weight, seq_rank * columns, columns, 1)
        return jnp.pad(taken, ((0, 0), (0, size - columns))) if size > columns else taken

    def own_units(weight):
        split = weight.reshape(weight.shape[0], shards, groups, part)
        mine = lax.dynamic_index_in_dim(split, seq_rank, 2, keepdims=False)
        return mine.reshape(weight.shape[0], units)

    own_forget = lax.dynamic_slice_in_dim(w_forget, seq_rank * local_heads, local_heads, 1)
    own_forget = jnp.pad(own_forget, ((0, 0), (0, PAIR - local_heads)))
    own_bias = lax.dynamic_slice_in_dim(forget_bias, seq_rank * local_heads, local_heads)
    own_bias = jnp.pad(own_bias, (0, PAIR - local_heads))[None]
    length_row = jnp.broadcast_to(lengths[:, None], (1, PAIR))
    mine_down = lax.dynamic_slice_in_dim(w_down, seq_rank * part, part, 0)
    if fast:
        (
            normed_attn, cotangent_all, full_front, full_ogate, full_out, full_ffn,
            joined, attended_low, offset, col, logit, gate_pre, gated, middle, mine_up,
        ) = whole_forward(
            layer_input[0], norm_attn[None], cotangent_low, (w_query, w_key, w_value, w_ogate), own_forget,
            own_bias, length_row, w_out, w_gate, w_up, head_size, scale, 0,
        )
        full_out = full_out.reshape(columns, width)
        normed_ffn, hidden, full_up, full_down, grad_gate_up, terms_down = feed_forward(
            middle, norm_ffn[None], full_ffn, mine_up, mine_down, cotangent_all, 1
        )
        (
            grad_middle, grad_norm_ffn, grad_branch, grad_attended, grad_gate_pre, terms_up, share_down, share_gate,
        ) = feed_backward(
            grad_gate_up, full_ffn, full_up, normed_ffn, terms_down, full_out, middle, norm_ffn[None],
            cotangent_low, attended_low, gate_pre, 2,
        )
        grad_norm_ffn = grad_norm_ffn[0]
        grads, bias_rows, lowered, collected, share_up, share_ogate, grad_down = middle_backward(
            joined, grad_attended, offset, col, logit, hidden, full_down, gated, grad_branch, terms_up, share_down,
            normed_attn, grad_gate_pre, head_size, scale, 3,
        )
        grad_normed_attn, share_attn, grad_out, every_gate, every_ogate = last_backward(
            grads, grad_gate_pre, normed_attn, full_front, full_ogate, collected, (share_gate, share_ogate), 4
        )
        grad_out = grad_out.reshape(columns // per_block, width)
    else:
        mine_front = jnp.concatenate(
            [*(own_columns(w, lanes) for w in (w_query, w_key, w_value)), own_forget], axis=1
        )
        full_front = gather(mine_front, "wshard")
        full_ogate = gather(own_columns(w_ogate, columns), "wshard")
        normed_attn = gather(rms_norm(inputs, norm_attn).astype(low), "seq")
        cotangent_all = gather(cotangent_low, "seq")
        full_out = lax.dynamic_slice_in_dim(gather(w_out, "wshard"), seq_rank * columns, columns, 0)
        full_ffn = gather(jnp.concatenate([own_units(w_gate), own_units(w_up)], axis=1), "wshard")
        joined = product(normed_attn, full_front).astype(low)
        gate_pre = product(normed_attn, full_ogate)
        attended_low, offset, col, logit = attention_fwd(joined, own_bias, length_row, head_size, scale)
        attended = attended_low[:, :columns].astype(jnp.float32)
        gated_full, pull_gate = jax.vjp(gate_product, attended, gate_pre)
        gated = gated_full.astype(low)
        middle = inputs + scatter(product(gated, full_out).astype(low), "seq").astype(jnp.float32)
        normed_ffn_own, pull_ffn_norm = jax.vjp(rms_norm, middle, norm_ffn)
        full_down = gather(mine_down, "wshard")
        normed_ffn = gather(normed_ffn_own.astype(low), "seq")
        gate_up = product(normed_ffn, full_ffn)
        hidden_full, pull_swiglu = jax.vjp(swiglu, gate_up[:, :units], gate_up[:, units:])
        hidden = hidden_full.astype(low)
        grad_hidden = product_nt(cotangent_all, full_down)
        grad_gate_full, grad_up_full = pull_swiglu(grad_hidden)
        grad_gate_up = jnp.concatenate([grad_gate_full.astype(low), grad_up_full.astype(low)], axis=1)
        share_down = scatter(product_tn(hidden, cotangent_all).astype(low), "wshard")
        share_ffn = scatter(product_tn(normed_ffn, grad_gate_up).astype(low), "wshard")
        grad_normed_ffn = scatter(product_nt(grad_gate_up, full_ffn).astype(low), "seq").astype(jnp.float32)
        grad_middle_part, grad_norm_ffn = pull_ffn_norm(grad_normed_ffn)
        grad_middle = cotangent + grad_middle_part
        grad_branch = gather(grad_middle.astype(low), "seq")
        grad_attended_full, grad_gate_pre_full = pull_gate(product_nt(grad_branch, full_out))
        grad_attended = grad_attended_full.astype(low)
        grad_gate_pre = grad_gate_pre_full.astype(low)
        if lanes > columns:
            grad_attended = jnp.pad(grad_attended, ((0, 0), (0, lanes - columns)))
        grads, bias_rows = attention_bwd(joined, grad_attended, offset, col, logit, head_size, scale)
        grad_projected = jnp.concatenate([grads, grad_gate_pre], axis=1)
        share_attn = scatter(product_tn(normed_attn, grad_projected).astype(low), "wshard")
        full_attn = jnp.concatenate([full_front, full_ogate], axis=1)
        grad_normed_attn = scatter(product_nt(grad_projected, full_attn).astype(low), "seq").astype(jnp.float32)
        lowered = scatter(product(hidden, full_down).astype(low), "seq").astype(jnp.float32)
        share_out = scatter(product_tn(gated, grad_branch).astype(low), "wshard")
        rows_out = columns // shards
        pieces_out = lax.all_gather(share_out, "seq", axis=0, tiled=False)
        takes = shards // per_block
        slots_out = jnp.where(
            (jnp.arange(per_block) == shard_rank // takes)[None, :, None, None],
            pieces_out[:, None],
            jnp.zeros((), low),
        ).reshape(shards, rows_out, width)
        moved = lax.all_to_all(slots_out, "wshard", split_axis=0, concat_axis=0, tiled=True)
        moved = moved.reshape(per_block, takes, rows_out, width)
        mine_out = lax.dynamic_index_in_dim(moved, shard_rank % per_block, 0, keepdims=False)
        grad_out = mine_out.reshape(columns // per_block, width).astype(jnp.float32)
    layer_output = (middle + lowered).astype(low)[None]
    grad_bias = lax.dynamic_update_slice_in_dim(
        jnp.zeros((heads,), jnp.float32), bias_rows[:local_heads, 0], seq_rank * local_heads, 0
    )
    unused_normed, pull_attn_norm = jax.vjp(rms_norm, inputs, norm_attn)
    grad_input_part, grad_norm_attn = pull_attn_norm(grad_normed_attn)
    grad_input = (grad_middle + grad_input_part)[None]

    rows = share_attn.shape[0]
    if fast:
        vector = jnp.concatenate([grad_norm_attn, grad_norm_ffn, grad_bias])
        vector = jnp.pad(vector, (0, -vector.shape[0] % 1024)).reshape(-1, 128)
        every_attn, every_up, vector = last_gather([share_attn, share_up], vector, 5)
        vector = vector.reshape(-1)
        small = vector[:width], vector[width : 2 * width], vector[2 * width : 2 * width + heads]
    else:
        every_attn, every_ffn, grad_down = [gather(v, "seq") for v in (share_attn, share_ffn, share_down)]
        small = lax.psum((grad_norm_attn, grad_norm_ffn, grad_bias), ("seq", "wshard"))
    every_attn = every_attn.reshape((groups,) + share_attn.shape)
    if fast:
        grad_w_gate, grad_w_up, grad_down, grad_out = join_units(
            every_gate.reshape((groups,) + share_gate.shape), every_up.reshape((groups,) + share_up.shape),
            grad_down, grad_out, part,
        )
        every_ogate = every_ogate.reshape((groups,) + share_ogate.shape)
        *weight_grads, grad_forget_w = join_columns(
            every_attn, every_ogate, columns, (0, lanes, 2 * lanes), 3 * lanes, heads
        )
    else:

        def join(first):
            taken = every_attn[:, :, first : first + columns]
            return taken.transpose(1, 0, 2).reshape(rows, width).astype(jnp.float32)

        def join_own_units(first):
            taken = every_ffn.reshape((groups,) + share_ffn.shape)[:, :, first * units : (first + 1) * units]
            taken = taken.reshape(groups, rows, shards, part).transpose(1, 2, 0, 3)
            return taken.reshape(rows, hidden_size).astype(jnp.float32)

        weight_grads = [join(first) for first in (0, lanes, 2 * lanes, front)]
        grad_w_gate, grad_w_up = join_own_units(0), join_own_units(1)
        grad_down = grad_down.astype(jnp.float32)
        grad_forget_w = every_attn[:, :, 3 * lanes : 3 * lanes + local_heads]
        grad_forget_w = grad_forget_w.transpose(1, 0, 2).reshape(rows, heads).astype(jnp.float32)
    return (
        layer_output,
        grad_input,
        small[0],
        *weight_grads,
        grad_forget_w,
        small[2],
        grad_out,
        small[1],
        grad_w_gate,
        grad_w_up,
        grad_down,
    )


def solution(mesh):
    return jax.shard_map(
        on_device,
        mesh=mesh,
        in_specs=(
            P("wshard", "seq", None),
            P("wshard"),
            P(),
            P("wshard", None),
            P("wshard", None),
            P("wshard", None),
            P("wshard", None),
            P("wshard", None),
            P(),
            P("wshard", None),
            P(),
            P("wshard", None),
            P("wshard", None),
            P("wshard", None),
            P("wshard", "seq", None),
        ),
        out_specs=(
            P("wshard", "seq", None),
            P("wshard", "seq", None),
            P(),
            P("wshard", None),
            P("wshard", None),
            P("wshard", None),
            P("wshard", None),
            P("wshard", None),
            P(),
            P("wshard", None),
            P(),
            P("wshard", None),
            P("wshard", None),
            P("wshard", None),
        ),
        check_vma=False,
    )
```

```python
import jax
import jax.numpy as jnp
from jax import lax
from jax.experimental import pallas as pl
from jax.experimental.pallas import tpu as pltpu
from jax.sharding import PartitionSpec as P

EPS = 1e-06
NEG_FILL = -1e30
PAIR = 128


def product(left, right):
    return jnp.dot(left, right, preferred_element_type=jnp.float32)


def product_tn(left, right):
    return lax.dot_general(
        left, right, (((0,), (0,)), ((), ())), preferred_element_type=jnp.float32
    )


def product_nt(left, right):
    return lax.dot_general(
        left, right, (((1,), (1,)), ((), ())), preferred_element_type=jnp.float32
    )


def rms_norm(values, gain):
    return values * lax.rsqrt(jnp.mean(values * values, axis=-1, keepdims=True) + EPS) * gain


def gate_product(attended, gate_pre):
    return attended * jax.nn.sigmoid(gate_pre)


def swiglu(gate, upward):
    return jax.nn.silu(gate) * upward


def low_triangle(size):
    rows = lax.broadcasted_iota(jnp.int32, (size, size), 0)
    return rows <= lax.broadcasted_iota(jnp.int32, (size, size), 1)


def exact(left, right):
    return jnp.dot(left, right, precision=lax.Precision.HIGHEST, preferred_element_type=jnp.float32)


class Forward:
    some = 8

    def __init__(self, joined, bias, length, attended, offset, col, logit, row, head_size, scale):
        self.joined, self.bias, self.length = joined, bias, length
        self.attended, self.offset, self.col, self.logit, self.row = attended, offset, col, logit, row
        self.head_size, self.scale = head_size, scale
        self.slots = joined.shape[0]
        self.pairs = (joined.shape[1] // PAIR - 1) // 3
        self.tile = min(256, self.slots)

    @staticmethod
    def results(slots, pairs):
        rows = jax.ShapeDtypeStruct((Forward.some, slots), jnp.float32)
        return [
            jax.ShapeDtypeStruct((slots, pairs * PAIR), jnp.bfloat16),
            rows,
            jax.ShapeDtypeStruct((slots, PAIR), jnp.float32),
            rows,
        ]

    def lanes(self, pair, part=0):
        return pl.ds(pl.multiple_of((part * self.pairs + pair) * PAIR, PAIR), PAIR)

    def start(self):
        slots, tile, some = self.slots, self.tile, self.some
        logits = self.joined[:, 3 * self.pairs * PAIR :].astype(jnp.float32) + self.bias[...]
        logit_rows = logits.T[:some]
        self.logit[...] = logit_rows
        logs = jnp.minimum(logit_rows, 0.0) - jnp.log1p(jnp.exp(-jnp.abs(logit_rows)))
        ones = low_triangle(tile).astype(jnp.float32)
        carry = jnp.zeros((some, 1), jnp.float32)
        for first in range(0, slots, tile):
            sums = exact(logs[:, first : first + tile], ones) + carry
            self.row[:, first : first + tile] = sums
            carry = sums[:, tile - 1 : tile]
        wide = jnp.concatenate([self.row[...], jnp.zeros((PAIR - some, slots), jnp.float32)], axis=0).T
        usable = lax.broadcasted_iota(jnp.int32, (slots, PAIR), 0) < self.length[...]
        self.col[...] = jnp.where(usable, wide, -NEG_FILL)

    def pair(self, pair):
        slots, tile, half = self.slots, self.tile, self.head_size
        key_all = self.joined[:, self.lanes(pair, 1)]
        value_t = self.joined[:, self.lanes(pair, 2)].T
        query_t = (self.joined[:, self.lanes(pair)].astype(jnp.float32) * self.scale).astype(jnp.bfloat16).T
        sub = lax.broadcasted_iota(jnp.int32, (PAIR, tile), 0)
        wide = lax.broadcasted_iota(jnp.int32, (slots, PAIR), 1)
        diag = low_triangle(tile)
        columns = [
            jnp.sum(jnp.where(wide == 2 * pair + a, self.col[...], 0.0), axis=1, keepdims=True) for a in range(2)
        ]
        for number in range(slots // tile):
            first, last = number * tile, (number + 1) * tile
            outs = []
            for a in range(2):
                mine = (sub >= a * half) & (sub < (a + 1) * half)
                at = pl.ds(2 * pair + a, 1)
                query = jnp.where(mine, query_t[:, first:last], jnp.zeros((), query_t.dtype))
                scores = product(key_all[:last], query)
                own_row = self.row[at, first:last]
                scores = scores + (own_row - columns[a][:last])
                tail = jnp.where(diag, scores[first:], NEG_FILL)
                scores = tail if number == 0 else jnp.concatenate([scores[:first], tail], axis=0)
                top = jnp.max(scores, axis=0, keepdims=True)
                weights = jnp.exp(scores - top)
                total = jnp.sum(weights, axis=0, keepdims=True)
                mixed = product(value_t[a * half : (a + 1) * half, :last], weights.astype(jnp.bfloat16))
                outs.append(mixed / total)
                self.offset[at, first:last] = own_row - (top + jnp.log(total))
            self.attended[first:last, self.lanes(pair)] = jnp.concatenate(outs, axis=0).T.astype(jnp.bfloat16)


def attention_fwd(joined, bias, length, head_size, scale):
    slots = joined.shape[0]
    pairs = (joined.shape[1] // PAIR - 1) // 3

    def body(joined_ref, bias_ref, length_ref, attended, offset, col, logit, row):
        work = Forward(joined_ref, bias_ref, length_ref, attended, offset, col, logit, row, head_size, scale)
        work.start()
        offset[...] = jnp.zeros_like(offset)

        def step(pair, carry):
            work.pair(pair)
            return carry

        lax.fori_loop(0, pairs, step, 0)

    vmem = pl.BlockSpec(memory_space=pltpu.VMEM)
    return pl.pallas_call(
        body,
        in_specs=[vmem] * 3,
        out_specs=[vmem] * 4,
        out_shape=Forward.results(slots, pairs),
        scratch_shapes=[pltpu.VMEM((Forward.some, slots), jnp.float32)],
        compiler_params=pltpu.CompilerParams(vmem_limit_bytes=56 << 20),
        cost_estimate=pl.CostEstimate(
            flops=4 * slots * slots * pairs * PAIR, bytes_accessed=8 * slots * pairs * PAIR, transcendentals=0
        ),
        name="attention_fwd",
    )(joined, bias, length)


def backward_scratch(slots):
    return [
        pltpu.VMEM((slots, PAIR), jnp.float32),
        pltpu.VMEM((slots, PAIR), jnp.float32),
        pltpu.VMEM((slots, PAIR), jnp.float32),
        pltpu.VMEM((8, slots), jnp.float32),
    ]


class Backward:
    def __init__(self, joined, d_out, offset, col, logit, grads, dk_acc, dv_acc, dcol, drow, head_size, scale):
        self.joined, self.d_out, self.offset, self.col = joined, d_out, offset, col
        self.logit, self.grads, self.dk_acc, self.dv_acc = logit, grads, dk_acc, dv_acc
        self.dcol, self.drow, self.head_size, self.scale = dcol, drow, head_size, scale
        self.slots = joined.shape[0]
        self.pairs = (joined.shape[1] // PAIR - 1) // 3
        self.tile = min(256, self.slots)

    def start(self):
        self.dcol[...] = jnp.zeros_like(self.dcol)
        self.drow[...] = jnp.zeros_like(self.drow)

    def lanes(self, pair, part=0):
        return pl.ds(pl.multiple_of((part * self.pairs + pair) * PAIR, PAIR), PAIR)

    def pair(self, pair):
        slots, tile, half = self.slots, self.tile, self.head_size
        dk_acc, dv_acc, dcol, drow = self.dk_acc, self.dv_acc, self.dcol, self.drow
        queries = (self.joined[:, self.lanes(pair)].astype(jnp.float32) * self.scale).astype(jnp.bfloat16)
        key_all = self.joined[:, self.lanes(pair, 1)]
        value_all = self.joined[:, self.lanes(pair, 2)]
        d_out = self.d_out[:, self.lanes(pair)]
        query_t, key_t, dout_t = queries.T, key_all.T, d_out.T
        sub = lax.broadcasted_iota(jnp.int32, (PAIR, tile), 0)
        lanes = lax.broadcasted_iota(jnp.int32, (tile, PAIR), 1)
        wide = lax.broadcasted_iota(jnp.int32, (slots, PAIR), 1)
        diag = low_triangle(tile)
        zero = jnp.zeros((), jnp.bfloat16)
        columns = [
            jnp.sum(jnp.where(wide == 2 * pair + a, self.col[...], 0.0), axis=1, keepdims=True) for a in range(2)
        ]
        dk_acc[...] = jnp.zeros_like(dk_acc)
        dv_acc[...] = jnp.zeros_like(dv_acc)
        for number in range(slots // tile):
            first, last = number * tile, (number + 1) * tile
            outs = []
            for a in range(2):
                mine = (sub >= a * half) & (sub < (a + 1) * half)
                own = (lanes >= a * half) & (lanes < (a + 1) * half)
                at = pl.ds(2 * pair + a, 1)
                scores = product(key_all[:last], jnp.where(mine, query_t[:, first:last], zero))
                scores = scores + (self.offset[at, first:last] - columns[a][:last])
                tail = jnp.where(diag, scores[first:], NEG_FILL)
                scores = tail if number == 0 else jnp.concatenate([scores[:first], tail], axis=0)
                probs = jnp.exp(scores)
                d_probs = product(value_all[:last], jnp.where(mine, dout_t[:, first:last], zero))
                dot = jnp.sum(d_probs * probs, axis=0, keepdims=True)
                d_full = probs * (d_probs - dot)
                d_scores = d_full.astype(jnp.bfloat16)
                drow[at, first:last] = jnp.sum(d_full, axis=0, keepdims=True)
                sums = jnp.sum(d_full, axis=1, keepdims=True)
                dcol[:last, :] += jnp.where(wide[:last] == 2 * pair + a, sums, 0.0)
                outs.append(product(key_t[a * half : (a + 1) * half, :last], d_scores) * self.scale)
                dk_acc[:last, :] += product(d_scores, jnp.where(own, queries[first:last, :], zero))
                dv_acc[:last, :] += product(
                    probs.astype(jnp.bfloat16), jnp.where(own, d_out[first:last, :], zero)
                )
            self.grads[first:last, self.lanes(pair)] = jnp.concatenate(outs, axis=0).T.astype(self.grads.dtype)
        self.grads[:, self.lanes(pair, 1)] = dk_acc[...].astype(self.grads.dtype)
        self.grads[:, self.lanes(pair, 2)] = dv_acc[...].astype(self.grads.dtype)

    def end(self, bias_grad):
        slots, tile, some = self.slots, self.tile, 8
        change = self.drow[...] - self.dcol[...].T[:some]
        rows = lax.broadcasted_iota(jnp.int32, (tile, tile), 0)
        ones = (rows >= lax.broadcasted_iota(jnp.int32, (tile, tile), 1)).astype(jnp.float32)
        carry = jnp.zeros((some, 1), jnp.float32)
        pieces = []
        for first in reversed(range(0, slots, tile)):
            sums = exact(change[:, first : first + tile], ones) + carry
            carry = sums[:, :1]
            pieces.insert(0, sums)
        grad = jnp.concatenate(pieces, axis=1) * jax.nn.sigmoid(-self.logit[...])
        heads = lax.broadcasted_iota(jnp.int32, (some, slots), 0)
        grad = jnp.where(heads < 2 * self.pairs, grad, 0.0)
        bias_grad[...] = jnp.broadcast_to(jnp.sum(grad, axis=1, keepdims=True), bias_grad.shape)
        wide = jnp.concatenate([grad, jnp.zeros((PAIR - some, slots), jnp.float32)], axis=0).T
        self.grads[:, 3 * self.pairs * PAIR : (3 * self.pairs + 1) * PAIR] = wide.astype(self.grads.dtype)


def attention_bwd(joined, d_out, offset, col, logit, head_size, scale):
    slots, width = joined.shape
    pairs = (width // PAIR - 1) // 3

    def body(joined_ref, d_out_ref, offset_ref, col_ref, logit_ref, grads, bias_grad, *scratch):
        work = Backward(
            joined_ref, d_out_ref, offset_ref, col_ref, logit_ref, grads, *scratch, head_size, scale
        )
        work.start()

        def step(pair, carry):
            work.pair(pair)
            return carry

        lax.fori_loop(0, pairs, step, 0)
        work.end(bias_grad)

    vmem = pl.BlockSpec(memory_space=pltpu.VMEM)
    return pl.pallas_call(
        body,
        in_specs=[vmem] * 5,
        out_specs=[vmem] * 2,
        out_shape=[
            jax.ShapeDtypeStruct((slots, width), jnp.bfloat16),
            jax.ShapeDtypeStruct((8, PAIR), jnp.float32),
        ],
        scratch_shapes=backward_scratch(slots),
        compiler_params=pltpu.CompilerParams(vmem_limit_bytes=56 << 20),
        cost_estimate=pl.CostEstimate(
            flops=10 * slots * slots * pairs * PAIR, bytes_accessed=14 * slots * pairs * PAIR, transcendentals=0
        ),
        name="attention_bwd",
    )(joined, d_out, offset, col, logit)


MESH = pl.DeviceIdType.MESH
VMEM_LIMIT = 62 << 20


def square(groups):
    return groups == 4


def sides():
    rank = lax.axis_index("seq")
    return rank, rank + 1 - 2 * lax.rem(rank, 2), lax.rem(rank + 2, 4), 3 - rank


def meet(*others):
    barrier = pltpu.get_barrier_semaphore()
    for other in others:
        pl.semaphore_signal(barrier, inc=1, device_id=other, device_id_type=MESH)
    pl.semaphore_wait(barrier, len(others))


def push(source, target, send, recv, device):
    copy = pltpu.make_async_remote_copy(
        src_ref=source,
        dst_ref=target,
        send_sem=send,
        recv_sem=recv,
        device_id=device,
        device_id_type=MESH,
    )
    copy.start()
    return copy


def by_rows(rows, work):
    def step(number, carry):
        work(pl.ds(pl.multiple_of(number * 16, 16), 16))
        return carry

    lax.fori_loop(0, rows // 16, step, 0)


class Streams:
    def __init__(self, sems):
        self.sems, self.made = sems, []

    def start(self, source, target):
        copy = pltpu.make_async_copy(source, target, self.sems.at[len(self.made)])
        self.made.append(copy)
        copy.start()
        return copy

    def end(self):
        for copy in self.made:
            copy.wait()


class SquareGather:
    def __init__(self, own, full, send, recv):
        self.own, self.full, self.send, self.recv = own, full, send, recv
        self.rows = own.shape[0]
        self.half = self.rows // 2

    def place(self, rank, part):
        return self.full.at[pl.ds(pl.multiple_of(rank * self.rows + part * self.half, self.half), self.half)]

    def copy(self, index):
        me, side, down, across = sides()
        mine = [self.own.at[pl.ds(part * self.half, self.half)] for part in (0, 1)]
        source, target, peer = (
            (mine[0], self.place(me, 0), side),
            (mine[1], self.place(me, 1), down),
            (mine[1], self.place(me, 1), side),
            (mine[0], self.place(me, 0), down),
            (self.place(side, 0), self.place(side, 0), down),
            (self.place(down, 1), self.place(down, 1), side),
        )[index]
        return pltpu.make_async_remote_copy(
            src_ref=source,
            dst_ref=target,
            send_sem=self.send.at[index],
            recv_sem=self.recv.at[index],
            device_id={"seq": peer},
            device_id_type=MESH,
        )

    def start(self):
        for index in range(4):
            self.copy(index).start()

    def relay(self):
        for index in (0, 1):
            self.copy(index).wait_recv()
            self.copy(4 + index).start()

    def near(self):
        self.copy(2).wait_recv()
        self.copy(3).wait_recv()

    def far(self):
        self.copy(4).wait_recv()
        self.copy(5).wait_recv()

    def finish(self):
        for index in range(6):
            self.copy(index).wait_send()


def block_product(left, right, transposed, tile, store):
    total = right.shape[0] if transposed else right.shape[1]

    def step(number, carry):
        columns = pl.ds(pl.multiple_of(number * tile, tile), tile)
        if transposed:
            store(columns, product_nt(left[...], right[columns, :]))
        else:
            store(columns, product(left[...], right[:, columns]))
        return carry

    lax.fori_loop(0, total // tile, step, 0)


def transposed_product(left, right, out):
    tall = 512 if out.shape[0] % 512 == 0 else 384
    wide = next(size for size in (512, 384, 640, 128) if out.shape[1] % size == 0)
    across = out.shape[1] // wide

    def step(number, carry):
        rows = pl.ds(pl.multiple_of((number // across) * tall, tall), tall)
        columns = pl.ds(pl.multiple_of(lax.rem(number, across) * wide, wide), wide)
        out[rows, columns] = product_tn(left[:, rows], right[:, columns]).astype(out.dtype)
        return carry

    lax.fori_loop(0, (out.shape[0] // tall) * across, step, 0)


def line():
    shards, place = lax.axis_size("wshard"), lax.axis_index("wshard")
    chips = shards // 2
    chip, core = place // 2, lax.rem(place, 2)
    forth = {"wshard": lax.rem(place + 2, shards)}
    back = {"wshard": lax.rem(place + shards - 2, shards)}
    twin = {"wshard": place + 1 - 2 * core}
    return chips, chip, core, forth, back, twin


class LineGather:
    @staticmethod
    def scratch(chips):
        dma = pltpu.SemaphoreType.DMA
        return [dma((3, chips)), dma((2 * chips,)), dma((1,))]

    def __init__(self, own, full, send, recv, local):
        self.own, self.full, self.local = own, full, local.at[0]
        self.sends = (send.at[0], send.at[1], send.at[2])
        self.recv = recv
        self.rows = own.shape[0]
        self.chips, self.chip, self.core, *self.devices = line()

    def place(self, chip, core):
        return self.full.at[pl.ds(pl.multiple_of((2 * chip + core) * self.rows, self.rows), self.rows)]

    def copy(self, way, chip, source=None):
        target = self.place(chip, self.core)
        return pltpu.make_async_remote_copy(
            src_ref=target if source is None else source,
            dst_ref=target,
            send_sem=self.sends[way].at[chip],
            recv_sem=self.recv.at[2 * chip + self.core],
            device_id=self.devices[way],
            device_id_type=MESH,
        )

    def wait_for(self, chip, core):
        target = self.place(chip, core)
        pltpu.make_async_remote_copy(
            src_ref=target,
            dst_ref=target,
            send_sem=self.sends[2].at[0],
            recv_sem=self.recv.at[2 * chip + core],
            device_id=self.devices[2],
            device_id_type=MESH,
        ).wait_recv()

    def start(self):
        @pl.when(self.chip < self.chips - 1)
        def _():
            self.copy(0, self.chip, self.own).start()

        @pl.when(self.chip > 0)
        def _():
            self.copy(1, self.chip, self.own).start()

        self.copy(2, self.chip, self.own).start()
        self.keep().start()

    def keep(self):
        return pltpu.make_async_copy(self.own, self.place(self.chip, self.core), self.local)

    def step(self, number):
        left, right = self.chip - number, self.chip + number

        @pl.when(left >= 0)
        def _():
            self.wait_for(left, self.core)

            @pl.when(self.chip < self.chips - 1)
            def _():
                self.copy(0, left).start()

            self.copy(2, left).start()

        @pl.when(right < self.chips)
        def _():
            self.wait_for(right, self.core)

            @pl.when(self.chip > 0)
            def _():
                self.copy(1, right).start()

            self.copy(2, right).start()

    def finish(self):
        for chip in range(self.chips):
            self.wait_for(chip, 1 - self.core)
            self.copy(2, chip).wait_send()

            @pl.when((chip <= self.chip) & (self.chip < self.chips - 1))
            def _():
                self.copy(0, chip).wait_send()

            @pl.when((chip >= self.chip) & (self.chip > 0))
            def _():
                self.copy(1, chip).wait_send()

        self.keep().wait()


class PartExchange:
    @staticmethod
    def scratch():
        dma = pltpu.SemaphoreType.DMA
        return [dma((4,)), dma((4,)), dma((1,))]

    def __init__(self, parts, out, send, recv, local):
        self.parts, self.out, self.send, self.recv, self.local = parts, out, send, recv, local
        self.rank = lax.axis_index("seq")
        self.core, self.twin = line()[2], line()[5]
        self.others = [{"seq": lax.rem(self.rank + k, 4)} for k in range(1, 4)]
        self.rows = out.shape[2]

    def part(self, rank):
        return self.parts.at[pl.ds(pl.multiple_of((2 * rank + self.core) * self.rows, self.rows), self.rows)]

    def copy(self, index):
        if index == 3:
            source = target = self.out.at[self.core]
        else:
            source = self.part(lax.rem(self.rank + index + 1, 4))
            target = self.out.at[self.core, self.rank]
        return pltpu.make_async_remote_copy(
            src_ref=source,
            dst_ref=target,
            send_sem=self.send.at[index],
            recv_sem=self.recv.at[index],
            device_id=self.twin if index == 3 else self.others[index],
            device_id_type=MESH,
        )

    def keep(self):
        return pltpu.make_async_copy(self.part(self.rank), self.out.at[self.core, self.rank], self.local.at[0])

    def start(self):
        for index in (1, 0, 2):
            self.copy(index).start()
        self.keep().start()

    def relay(self):
        for index in range(3):
            self.copy(index).wait()
        self.keep().wait()
        self.copy(3).start()

    def end(self):
        self.copy(3).wait()


class Regroup:
    @staticmethod
    def scratch(rows, width):
        dma = pltpu.SemaphoreType.DMA
        return [pltpu.VMEM((4, rows, width), jnp.bfloat16), dma((7,)), dma((7,))]

    def __init__(self, piece, out, fours, send, recv):
        self.piece, self.out, self.fours, self.send, self.recv = piece, out, fours, send, recv
        self.rank, self.place = lax.axis_index("seq"), lax.axis_index("wshard")
        self.number = lax.rem(self.place, 4)
        self.others = [{"seq": lax.rem(self.rank + k, 4)} for k in range(1, 4)]
        self.along = [{"wshard": lax.rem(self.place + k, 8)} for k in range(1, 8)]

    def near(self, index):
        return pltpu.make_async_remote_copy(
            src_ref=self.piece,
            dst_ref=self.fours.at[self.rank],
            send_sem=self.send.at[index],
            recv_sem=self.recv.at[index],
            device_id=self.others[index],
            device_id_type=MESH,
        )

    def owner(self, rank):
        return 2 * rank + self.place // 4

    def far(self, rank, number):
        return pltpu.make_async_remote_copy(
            src_ref=self.fours.at[rank],
            dst_ref=self.out.at[number],
            send_sem=self.send.at[3 + rank],
            recv_sem=self.recv.at[3 + number],
            device_id={"wshard": self.owner(rank)},
            device_id_type=MESH,
        )

    def start(self):
        for index in range(3):
            self.near(index).start()
        self.fours[self.rank] = self.piece[...]

    def relay(self):
        for index in range(3):
            self.near(index).wait()
        for rank in range(4):

            @pl.when(self.owner(rank) != self.place)
            def _():
                self.far(rank, self.number).start()

            @pl.when(self.owner(rank) == self.place)
            def _():
                self.out[self.number] = self.fours[rank]

    def end(self):
        for rank in range(4):

            @pl.when(self.owner(rank) != self.place)
            def _():
                self.far(rank, self.number).wait_send()

        for number in range(4):

            @pl.when(4 * lax.rem(self.place, 2) + number != self.place)
            def _():
                self.far(0, number).wait_recv()


class Everywhere:
    def __init__(self, values, out, ranks, total, places, send, recv):
        self.values, self.out, self.ranks, self.total, self.places = values, out, ranks, total, places
        self.send, self.recv = send, recv
        self.groups, self.shards = ranks.shape[0], places.shape[0]
        self.rank, self.place = lax.axis_index("seq"), lax.axis_index("wshard")

    def others(self):
        return [{"seq": lax.rem(self.rank + k, self.groups)} for k in range(1, self.groups)]

    def along(self):
        return [{"wshard": lax.rem(self.place + k, self.shards)} for k in range(1, self.shards)]

    def start(self):
        self.first = [
            push(self.values, self.ranks.at[self.rank], self.send.at[k], self.recv.at[k], other)
            for k, other in enumerate(self.others())
        ]
        self.ranks[self.rank] = self.values[...]

    def relay(self):
        for copy in self.first:
            copy.wait()
        ranks, groups = self.ranks, self.groups
        self.total[...] = (ranks[0] + ranks[1]) + (ranks[2] + ranks[3])
        self.second = [
            push(self.total, self.places.at[self.place], self.send.at[groups + k], self.recv.at[groups + k], other)
            for k, other in enumerate(self.along())
        ]
        self.places[self.place] = self.total[...]

    def end(self):
        for copy in self.second:
            copy.wait()
        sums = [self.places[k] + self.places[k + 1] for k in range(0, self.shards, 2)]
        self.out[...] = (sums[0] + sums[1]) + (sums[2] + sums[3])


def last_gather(values, small, collective_id):
    count = len(values)
    groups = lax.axis_size("seq")
    shards = 2 * groups

    def body(*refs):
        own, small_ref = refs[:count], refs[count]
        full, small_out = refs[count + 1 : 2 * count + 1], refs[2 * count + 1]
        send, recv, local = refs[2 * count + 2 : 2 * count + 5]
        me, side, down, across = sides()
        total = Everywhere(small_ref, small_out, *refs[2 * count + 5 :])
        meet(*total.others(), *total.along())
        jobs = [SquareGather(own[i], full[i], send.at[i], recv.at[i]) for i in range(count)]
        total.start()
        keeps = []
        for i, job in enumerate(jobs):
            job.start()
            rows = own[i].shape[0]
            keep = pltpu.make_async_copy(
                own[i], full[i].at[pl.ds(pl.multiple_of(me * rows, rows), rows)], local.at[i]
            )
            keep.start()
            keeps.append(keep)
        total.relay()
        for job in jobs:
            job.relay()
        total.end()
        for job, keep in zip(jobs, keeps):
            job.near()
            job.far()
            job.finish()
            keep.wait()

    vmem = pl.BlockSpec(memory_space=pltpu.VMEM)
    dma = pltpu.SemaphoreType.DMA
    return pl.pallas_call(
        body,
        in_specs=[vmem] * (count + 1),
        out_specs=[pl.BlockSpec(memory_space=pl.ANY)] * count + [vmem],
        out_shape=[jax.ShapeDtypeStruct((4 * v.shape[0],) + v.shape[1:], v.dtype) for v in values]
        + [jax.ShapeDtypeStruct(small.shape, jnp.float32)],
        scratch_shapes=[
            dma((count, 6)),
            dma((count, 6)),
            dma((count,)),
            pltpu.VMEM((groups,) + small.shape, jnp.float32),
            pltpu.VMEM(small.shape, jnp.float32),
            pltpu.VMEM((shards,) + small.shape, jnp.float32),
            dma((groups + shards,)),
            dma((groups + shards,)),
        ],
        compiler_params=pltpu.CompilerParams(
            collective_id=collective_id, has_side_effects=True, vmem_limit_bytes=VMEM_LIMIT
        ),
        name="last_gather",
    )(*values, small)


def join_units(every_gate, every_up, down, out, part):
    groups, rows, units = every_gate.shape
    steps = 4
    tall = rows // steps

    def body(gate_in, up_in, down_in, out_in, gate_ref, up_ref, down_ref, out_ref):
        for every, to_ref in ((gate_in, gate_ref), (up_in, up_ref)):
            for group in range(groups):
                for block in range(units // part):
                    to = (block * groups + group) * part
                    to_ref[:, to : to + part] = every[group, :, block * part : (block + 1) * part].astype(
                        jnp.float32
                    )
        down_ref[...] = down_in[...].astype(jnp.float32)
        out_ref[...] = out_in[...].astype(jnp.float32)

    def flat(value):
        return pl.BlockSpec((value.shape[0] // steps, value.shape[1]), lambda i: (i, 0))

    wide = jax.ShapeDtypeStruct((rows, groups * units), jnp.float32)
    results = [wide, wide, *(jax.ShapeDtypeStruct(v.shape, jnp.float32) for v in (down, out))]
    return pl.pallas_call(
        body,
        grid=(steps,),
        in_specs=[pl.BlockSpec((groups, tall, units), lambda i: (0, i, 0))] * 2 + [flat(down), flat(out)],
        out_specs=[flat(value) for value in results],
        out_shape=results,
        name="join_units",
    )(every_gate, every_up, down, out)


def join_columns(every, gate, columns, starts, forget_at, heads):
    groups, rows, lanes = every.shape
    own = heads // groups
    steps = 4
    tall = rows // steps

    def body(every_ref, gate_ref, *outs):
        for group in range(groups):
            to = slice(group * columns, (group + 1) * columns)
            for start, out in zip(starts, outs):
                out[:, to] = every_ref[group, :, start : start + columns].astype(jnp.float32)
            outs[-2][:, to] = gate_ref[group].astype(jnp.float32)
            outs[-1][:, group * own : (group + 1) * own] = every_ref[
                group, :, forget_at : forget_at + own
            ].astype(jnp.float32)

    def flat(value):
        return pl.BlockSpec((tall, value.shape[1]), lambda i: (i, 0))

    wide = jax.ShapeDtypeStruct((rows, groups * columns), jnp.float32)
    results = [wide] * (len(starts) + 1) + [jax.ShapeDtypeStruct((rows, heads), jnp.float32)]
    return pl.pallas_call(
        body,
        grid=(steps,),
        in_specs=[pl.BlockSpec((groups, tall, v.shape[2]), lambda i: (0, i, 0)) for v in (every, gate)],
        out_specs=[flat(value) for value in results],
        out_shape=results,
        name="join_columns",
    )(every, gate)


class SquareScatter:
    @staticmethod
    def scratch(rows, width):
        half = rows // 2
        low = jnp.bfloat16
        return [
            pltpu.VMEM((rows, width), low),
            pltpu.VMEM((2, half, width), low),
            pltpu.VMEM((2, half, width), jnp.float32),
            pltpu.VMEM((6, half, width), low),
            pltpu.VMEM((2, half, width), low),
            pltpu.SemaphoreType.DMA((6,)),
            pltpu.SemaphoreType.DMA((6,)),
        ]

    def __init__(self, lefts, rights, transposed, out, far, near, kept, land, carry, send, recv):
        self.lefts, self.rights, self.transposed, self.out = lefts, rights, transposed, out
        self.far, self.near, self.kept, self.land, self.carry = far, near, kept, land, carry
        self.send, self.recv = send, recv
        self.rows, self.width = out.shape
        self.half = self.rows // 2
        self.tile = self.width // 3 if self.width % 384 == 0 else self.width

    def copy(self, index):
        me, side, down, across = sides()
        source = (
            self.far.at[pl.ds(0, self.half)],
            self.far.at[pl.ds(self.half, self.half)],
            self.near.at[0],
            self.near.at[1],
            self.carry.at[0],
            self.carry.at[1],
        )[index]
        return pltpu.make_async_remote_copy(
            src_ref=source,
            dst_ref=self.land.at[index],
            send_sem=self.send.at[index],
            recv_sem=self.recv.at[index],
            device_id={"seq": down if index in (0, 3, 5) else side},
            device_id_type=MESH,
        )

    def partial(self, rank, store):
        at = pl.ds(pl.multiple_of(rank * self.rows, self.rows), self.rows)

        def step(number, carried):
            columns = pl.ds(pl.multiple_of(number * self.tile, self.tile), self.tile)
            value = None
            for a, b in zip(self.lefts, self.rights):
                if self.transposed:
                    term = product_nt(a[at, :], b[columns, :])
                else:
                    term = product(a[at, :], b[:, columns])
                value = term if value is None else value + term
            store(columns, value)
            return carried

        lax.fori_loop(0, self.width // self.tile, step, 0)

    def begin(self):
        me, side, down, across = sides()
        half, far, near, kept = self.half, self.far, self.near, self.kept

        def store_far(columns, value):
            far[:, columns] = value.astype(far.dtype)

        def store_side(columns, value):
            kept[0, :, columns] = value[:half]
            near[0, :, columns] = value[half:].astype(near.dtype)

        def store_down(columns, value):
            near[1, :, columns] = value[:half].astype(near.dtype)
            kept[1, :, columns] = value[half:]

        self.partial(across, store_far)
        self.copy(0).start()
        self.copy(1).start()
        self.partial(side, store_side)
        self.copy(2).start()
        self.partial(down, store_down)
        self.copy(3).start()

    def relay(self):
        for index in (0, 1):
            self.copy(index).wait_recv()

            def add(at, index=index):
                total = self.kept[index, at, :] + self.land[index, at, :].astype(jnp.float32)
                self.carry[index, at, :] = total.astype(self.carry.dtype)

            by_rows(self.half, add)
            self.copy(4 + index).start()

    def own(self):
        out = self.out

        def store_own(columns, value):
            out[:, columns] = value

        self.partial(lax.axis_index("seq"), store_own)

    def end(self):
        for index in (2, 3, 4, 5):
            self.copy(index).wait_recv()
        land, half, out = self.land, self.half, self.out

        def add(at):
            out[at, :] += land[3, at, :].astype(jnp.float32) + land[4, at, :].astype(jnp.float32)

        def add_second(at):
            to = pl.ds(at.start + half, at.size)
            out[to, :] += land[2, at, :].astype(jnp.float32) + land[5, at, :].astype(jnp.float32)

        by_rows(half, add)
        by_rows(half, add_second)
        for index in range(6):
            self.copy(index).wait_send()


class LineScatter:
    @staticmethod
    def scratch(chips, rows, width):
        low = jnp.bfloat16
        dma = pltpu.SemaphoreType.DMA
        return [pltpu.VMEM((chips, rows, width), low)] * 3 + [dma((2, chips)), dma((3, chips))]

    def __init__(self, terms, out, twin_in, forth_in, back_in, send, recv):
        self.terms, self.out, self.twin_in = terms, out, twin_in
        self.forth_in, self.back_in, self.send, self.recv = forth_in, back_in, send, recv
        self.chips, self.chip, self.core, *self.devices = line()
        self.rows = twin_in.shape[1]

    def term(self, chip, core):
        return self.terms.at[pl.ds(pl.multiple_of((2 * chip + core) * self.rows, self.rows), self.rows)]

    def swap(self, chip):
        return pltpu.make_async_remote_copy(
            src_ref=self.term(chip, 1 - self.core),
            dst_ref=self.twin_in.at[chip],
            send_sem=self.send.at[0, chip],
            recv_sem=self.recv.at[0, chip],
            device_id=self.devices[2],
            device_id_type=MESH,
        )

    def hop(self, way, chip):
        return pltpu.make_async_remote_copy(
            src_ref=self.twin_in.at[chip],
            dst_ref=(self.forth_in, self.back_in)[way].at[chip],
            send_sem=self.send.at[1, chip],
            recv_sem=self.recv.at[1 + way, chip],
            device_id=self.devices[way],
            device_id_type=MESH,
        )

    def start(self):
        for chip in (self.chips - 1, 0, *range(1, self.chips - 1)):
            self.swap(chip).start()

    def add(self, chip, ways, out):
        def step(at):
            start = pl.multiple_of((2 * chip + self.core) * self.rows + at.start, at.size)
            total = self.terms[pl.ds(start, at.size), :].astype(jnp.float32)
            total = total + self.twin_in[chip, at, :].astype(jnp.float32)
            for way in ways:
                total = total + (self.forth_in, self.back_in)[way][chip, at, :].astype(jnp.float32)
            out[at, :] = total.astype(out.dtype)

        by_rows(self.rows, step)

    def pass_on(self, way, chip, first):
        self.swap(chip).wait_recv()
        if not first:
            self.hop(way, chip).wait_recv()
        self.add(chip, () if first else (way,), self.twin_in.at[chip])
        self.hop(way, chip).start()

    def slot(self, number):
        last = self.chips - 1
        for chip in range(self.chips):
            forth, back = number - (last - chip), last - (number - chip)
            if 0 <= forth < chip:

                @pl.when(self.chip == forth)
                def _():
                    self.pass_on(0, chip, forth == 0)

            if chip < back <= last:

                @pl.when(self.chip == back)
                def _():
                    self.pass_on(1, chip, back == last)

    def end(self):
        for chip in range(self.chips):

            @pl.when(self.chip == chip)
            def _():
                self.swap(chip).wait_recv()
                ways = [way for way, there in enumerate((chip > 0, chip < self.chips - 1)) if there]
                for way in ways:
                    self.hop(way, chip).wait_recv()
                self.add(chip, ways, self.out)

            self.swap(chip).wait_send()

            @pl.when(self.chip != chip)
            def _():
                self.hop(0, chip).wait_send()


def middle_backward(joined, d_out, offset, col, logit, hidden, w_down, gated, grad_branch, terms_up, share_down,
                    normed, d_pre, head_size, scale, collective_id):
    slots, lanes = joined.shape
    width = w_down.shape[1]
    tokens = slots // 4
    columns = gated.shape[1]
    shards = 2 * lax.axis_size("seq")
    chips = shards // 2
    rows_up = terms_up.shape[0] // shards

    def body(joined_ref, d_out_ref, offset_ref, col_ref, logit_ref, hidden_ref, down_ref, gated_ref, branch_ref,
             up_ref, share_ref, normed_ref, pre_ref,
             grads, bias_grad, lowered, collected, share_up, share_pre, every_down, terms, terms_pre, send, recv, keep, *scratch):
        me, side, down, across = sides()
        line_chips, chip, core, forth, back, twin = line()
        meet({"seq": side}, {"seq": down}, forth, back, twin)
        work = Backward(
            joined_ref, d_out_ref, offset_ref, col_ref, logit_ref, grads, *scratch[:4], head_size, scale
        )
        job = SquareScatter([hidden_ref], [down_ref], False, lowered, *scratch[4:11])
        collect = LineScatter(terms, collected, *scratch[11:16])
        run = LineScatter(up_ref, share_up, *scratch[16:21])
        run_pre = LineScatter(terms_pre, share_pre, *scratch[21:])
        every = SquareGather(share_ref, every_down, send, recv)
        size = share_ref.shape[0]
        kept = pltpu.make_async_copy(
            share_ref, every_down.at[pl.ds(pl.multiple_of(me * size, size), size)], keep.at[0]
        )
        kept.start()
        run.start()
        transposed_product(gated_ref, branch_ref, terms)
        collect.start()
        transposed_product(normed_ref, pre_ref, terms_pre)
        run_pre.start()
        collect.slot(0)
        run.slot(0)
        job.begin()
        run_pre.slot(0)
        work.start()

        def step(pair, carry):
            work.pair(pair)

            @pl.when(pair == 0)
            def _():
                job.relay()
                collect.slot(1)
                run.slot(1)
                run_pre.slot(1)
                every.start()

            @pl.when(pair == 1)
            def _():
                collect.slot(2)
                run.slot(2)
                run_pre.slot(2)

            return carry

        lax.fori_loop(0, work.pairs, step, 0)
        every.relay()
        job.own()
        work.end(bias_grad)
        job.end()
        run.end()
        run_pre.end()
        every.near()
        every.far()
        every.finish()
        kept.wait()
        collect.end()

    vmem = pl.BlockSpec(memory_space=pltpu.VMEM)
    low = jnp.bfloat16
    dma = pltpu.SemaphoreType.DMA
    return pl.pallas_call(
        body,
        in_specs=[vmem] * 13,
        out_specs=[vmem] * 6 + [pl.BlockSpec(memory_space=pl.ANY)],
        out_shape=[
            jax.ShapeDtypeStruct((slots, lanes), low),
            jax.ShapeDtypeStruct((8, PAIR), jnp.float32),
            jax.ShapeDtypeStruct((tokens, width), jnp.float32),
            jax.ShapeDtypeStruct((columns // shards, width), low),
            jax.ShapeDtypeStruct((rows_up, terms_up.shape[1]), low),
            jax.ShapeDtypeStruct((rows_up, columns), low),
            jax.ShapeDtypeStruct((4 * share_down.shape[0], width), low),
        ],
        scratch_shapes=[
            pltpu.VMEM((columns, width), low),
            pltpu.VMEM((width, columns), low),
            dma((6,)),
            dma((6,)),
            dma((1,)),
        ]
        + backward_scratch(slots)
        + SquareScatter.scratch(tokens, width)
        + LineScatter.scratch(chips, columns // shards, width)
        + LineScatter.scratch(chips, rows_up, terms_up.shape[1])
        + LineScatter.scratch(chips, rows_up, columns),
        compiler_params=pltpu.CompilerParams(
            collective_id=collective_id, has_side_effects=True, vmem_limit_bytes=VMEM_LIMIT
        ),
        name="middle_backward",
    )(joined, d_out, offset, col, logit, hidden, w_down, gated, grad_branch, terms_up, share_down, normed, d_pre)


def last_backward(grads, grad_gate_pre, normed, weights, gate_weights, collected, shares, collective_id):
    slots, depth = normed.shape
    front = grads.shape[1]
    count = len(shares)
    tokens = slots // 4
    shards = 2 * lax.axis_size("seq")
    rows = depth // shards

    def body(grads_ref, gate_ref, normed_ref, weights_ref, gate_weights_ref, collected_ref,
             *refs):
        share_refs, refs = refs[:count], refs[count:]
        summed, share, regrouped, *every_refs = refs[: 3 + count]
        terms, send, recv, keep, *scratch = refs[3 + count :]
        me, side, down, across = sides()
        chips, chip, core, forth, back, twin = line()
        regroup = Regroup(collected_ref, regrouped, *scratch[12:])
        meet(*regroup.others, *regroup.along)
        job = SquareScatter(
            [grads_ref, gate_ref],
            [weights_ref, gate_weights_ref],
            True,
            summed,
            *scratch[:7],
        )
        run = LineScatter(terms, share, *scratch[7:12])
        regroup.start()
        every = [
            SquareGather(share_refs[i], every_refs[i], send.at[i], recv.at[i]) for i in range(count)
        ]
        kept = []
        for i in range(count):
            size = share_refs[i].shape[0]
            kept.append(
                pltpu.make_async_copy(
                    share_refs[i],
                    every_refs[i].at[pl.ds(pl.multiple_of(me * size, size), size)],
                    keep.at[i],
                )
            )
            kept[i].start()
            every[i].start()
        transposed_product(normed_ref, grads_ref, terms)
        run.start()
        regroup.relay()
        job.begin()
        run.slot(0)
        for gathering in every:
            gathering.relay()
        job.relay()
        job.own()
        run.slot(1)
        run.slot(2)
        for gathering, copy in zip(every, kept):
            gathering.near()
            gathering.far()
            gathering.finish()
            copy.wait()
        job.end()
        regroup.end()
        run.end()

    vmem = pl.BlockSpec(memory_space=pltpu.VMEM)
    low = jnp.bfloat16
    dma = pltpu.SemaphoreType.DMA
    return pl.pallas_call(
        body,
        in_specs=[vmem] * (6 + count),
        out_specs=[vmem] * 3 + [pl.BlockSpec(memory_space=pl.ANY)] * count,
        out_shape=[
            jax.ShapeDtypeStruct((tokens, depth), jnp.float32),
            jax.ShapeDtypeStruct((rows, front), low),
            jax.ShapeDtypeStruct((4,) + collected.shape, low),
            *(jax.ShapeDtypeStruct((4 * v.shape[0], v.shape[1]), low) for v in shares),
        ],
        scratch_shapes=[
            pltpu.VMEM((depth, front), low),
            dma((count, 6)),
            dma((count, 6)),
            dma((count,)),
        ]
        + SquareScatter.scratch(tokens, depth)
        + LineScatter.scratch(shards // 2, rows, front)
        + Regroup.scratch(*collected.shape),
        compiler_params=pltpu.CompilerParams(
            collective_id=collective_id, has_side_effects=True, vmem_limit_bytes=VMEM_LIMIT
        ),
        name="last_backward",
    )(grads, grad_gate_pre, normed, weights, gate_weights, collected, *shares)


def norm_rows(values, gain):
    scale = lax.rsqrt(jnp.mean(values * values, axis=-1, keepdims=True) + EPS)
    return scale, values * scale * gain


def whole_forward(inputs, gain, cotangent, weights, forget, bias, length, block, w_gate, w_up,
                  head_size, scale, collective_id):
    rows, depth = inputs.shape
    groups = 4
    slots = groups * rows
    chips = groups
    shards = 2 * chips
    mine = weights[0].shape[0]
    columns = depth // groups
    front = 3 * columns + PAIR
    pairs = columns // PAIR
    part = w_gate.shape[1] // (groups * shards)
    units = shards * part
    early = units + units // 2
    low = jnp.bfloat16

    def body(inputs_ref, gain_ref, cot_ref, q_ref, k_ref, v_ref, og_ref, forget_ref, bias_ref, length_ref, block_ref,
             gate_ref, up_ref,
             normed_hbm, cot_full, full_front_hbm, full_gate_hbm, full_out_hbm, full_ffn, joined_hbm, attended_hbm,
             offset, col, logit, gate_pre_hbm, gated_hbm, middle, own_up,
             own_normed, own_front, own_gate, own_ffn, own_out, parts_out, row, picks, cot_send, cot_recv, keep,
             x_send, x_recv, normed, full_front, full_gate, full_out, joined, attended, gate_pre, gated, store_sems,
             *scratch):
        store = Streams(store_sems)
        me, side, down, across = sides()
        line_chips, chip, core, forth, back, twin = line()
        front_line = LineGather(own_front, full_front, *scratch[0:3])
        gate_line = LineGather(own_gate, full_gate, *scratch[3:6])
        ffn_line = LineGather(own_ffn, full_ffn, *scratch[6:9])
        out_line = LineGather(own_out, parts_out, *scratch[9:12])
        exchange = PartExchange(parts_out, full_out, *scratch[12:15])
        job = SquareScatter([gated], [full_out_rows(full_out)], False, middle, *scratch[15:22])
        taken = []
        my_columns = pl.ds(pl.multiple_of(me * columns, columns), columns)
        for index, source in enumerate((q_ref, k_ref, v_ref)):
            taken.append((source.at[:, my_columns], own_front.at[:, pl.ds(index * columns, columns)]))
        taken.append((og_ref.at[:, my_columns], own_gate))
        tall = own_out.shape[0]
        taken.append((block_ref.at[pl.ds(pl.multiple_of(me * tall, tall), tall)], own_out))
        for index, source in enumerate((gate_ref, up_ref)):
            for number in range(shards):
                column = pl.ds(pl.multiple_of((number * groups + me) * part, part), part)
                to = index * units + number * part
                target = own_ffn.at[:, pl.ds(to, part)] if to < early else own_up.at[:, pl.ds(to - early, part)]
                taken.append((source.at[:, column], target))
        taken = [pltpu.make_async_copy(a, b, picks.at[i]) for i, (a, b) in enumerate(taken)]
        for copy in taken:
            copy.start()
        values = inputs_ref[...].astype(jnp.float32)
        own_normed[...] = norm_rows(values, gain_ref[...])[1].astype(low)
        own_front[:, 3 * columns :] = forget_ref[...]
        meet(*exchange.others, forth, back, twin)
        one = SquareGather(own_normed, normed, x_send, x_recv)
        two = SquareGather(cot_ref, cot_full, cot_send, cot_recv)
        one.start()
        for copy in taken:
            copy.wait()
        front_line.start()
        at_me = pl.ds(pl.multiple_of(me * rows, rows), rows)
        kept = pltpu.make_async_copy(cot_ref, cot_full.at[at_me], keep.at[0])
        kept.start()
        normed[at_me, :] = own_normed[...]
        one.relay()
        two.start()
        front_line.step(1)
        front_line.step(2)
        one.near()
        one.far()
        front_line.step(3)
        store.start(normed, normed_hbm)
        front_line.finish()
        store.start(full_front, full_front_hbm)
        one.finish()
        out_line.start()
        gate_line.start()
        two.relay()

        def store_joined(at_columns, value):
            joined[:, at_columns] = value.astype(low)

        block_product(normed, full_front, False, 256, store_joined)
        store.start(joined, joined_hbm)
        work = Forward(joined, bias_ref, length_ref, attended, offset, col, logit, row, head_size, scale)
        offset[...] = jnp.zeros_like(offset)
        out_line.step(1)
        gate_line.step(1)
        work.start()
        out_line.step(2)
        gate_line.step(2)

        def step(pair, carry):
            work.pair(pair)

            @pl.when(pair == 0)
            def _():
                out_line.step(3)
                gate_line.step(3)
                out_line.finish()
                exchange.start()
                ffn_line.start()

            return carry

        lax.fori_loop(0, pairs, step, 0)
        store.start(attended, attended_hbm)
        gate_line.finish()
        store.start(full_gate, full_gate_hbm)
        exchange.relay()

        def store_gate(at_columns, value):
            gate_pre[:, at_columns] = value

        block_product(normed, full_gate, False, PAIR, store_gate)
        gated[...] = (attended[...].astype(jnp.float32) * jax.nn.sigmoid(gate_pre[...])).astype(low)
        store.start(gate_pre, gate_pre_hbm)
        store.start(gated, gated_hbm)
        exchange.end()
        store.start(full_out, full_out_hbm)
        job.begin()
        job.relay()
        ffn_line.step(1)
        job.own()
        two.near()
        two.far()
        two.finish()
        kept.wait()
        ffn_line.step(2)
        job.end()
        middle[...] += inputs_ref[...].astype(jnp.float32)
        ffn_line.step(3)
        ffn_line.finish()
        store.end()

    def shape(size, kind=low):
        return jax.ShapeDtypeStruct(size, kind)

    vmem = pl.BlockSpec(memory_space=pltpu.VMEM)
    anywhere = pl.BlockSpec(memory_space=pl.ANY)
    dma = pltpu.SemaphoreType.DMA
    results = [
        shape((slots, depth)),
        shape((slots, depth)),
        shape((depth, front)),
        shape((depth, columns)),
        shape((2, 4, block.shape[0] // 4, depth)),
        shape((depth, early)),
        shape((slots, front)),
        *Forward.results(slots, pairs),
        shape((slots, columns), jnp.float32),
        shape((slots, columns)),
        shape((rows, depth), jnp.float32),
        shape((mine, 2 * units - early)),
    ]
    kept_here = [results[i] for i in (0, 2, 3, 4, 6, 7, 11, 12)]
    return pl.pallas_call(
        body,
        in_specs=[vmem] * 3 + [anywhere] * 4 + [vmem] * 3 + [anywhere] * 3,
        out_specs=[anywhere] * 8 + [vmem] * 3 + [anywhere] * 2 + [vmem] * 2,
        out_shape=results,
        scratch_shapes=[
            pltpu.VMEM((rows, depth), low),
            pltpu.VMEM((mine, front), low),
            pltpu.VMEM((mine, columns), low),
            pltpu.VMEM((mine, early), low),
            pltpu.VMEM((block.shape[0] // 4, depth), low),
            pltpu.VMEM((shards * block.shape[0] // 4, depth), low),
            pltpu.VMEM((Forward.some, slots), jnp.float32),
            dma((5 + 2 * shards,)),
            dma((6,)),
            dma((6,)),
            dma((1,)),
            dma((6,)),
            dma((6,)),
            *(pltpu.VMEM(value.shape, value.dtype) for value in kept_here),
            dma((len(kept_here),)),
        ]
        + 4 * LineGather.scratch(chips)
        + PartExchange.scratch()
        + SquareScatter.scratch(rows, depth),
        compiler_params=pltpu.CompilerParams(
            collective_id=collective_id, has_side_effects=True, vmem_limit_bytes=VMEM_LIMIT
        ),
        name="whole_forward",
    )(inputs, gain, cotangent, *weights, forget, bias, length, block, w_gate, w_up)


class full_out_rows:
    def __init__(self, ref):
        self.ref = ref
        self.shape = (ref.shape[0] * ref.shape[1] * ref.shape[2], ref.shape[3])

    def __getitem__(self, index):
        taken = self.ref[:, :, :, index[1]]
        return taken.reshape(self.shape[0], taken.shape[3])


def feed_forward(middle, gain, weights, own_up, own_down, cotangent, collective_id):
    rows, depth = middle.shape
    slots = 4 * rows
    units = 4 * own_down.shape[0] * 2
    early = weights.shape[1]
    chips = 4
    low = jnp.bfloat16

    def body(middle_ref, gain_ref, weights_hbm, up_ref, down_ref, cot_hbm,
             normed_hbm, hidden_hbm, full_up_hbm, full_down_hbm, grads_hbm, terms_hbm,
             own_normed, both, send, recv,
             weights_ref, cot_ref, normed, hidden, full_up, full_down, grads, terms, fetch_sems, store_sems, *scratch):
        fetch, store = Streams(fetch_sems), Streams(store_sems)
        weights_in = fetch.start(weights_hbm, weights_ref)
        cot_in = fetch.start(cot_hbm, cot_ref)
        me, side, down, across = sides()
        line_chips, chip, core, forth, back, twin = line()
        up_line = LineGather(up_ref, full_up, *scratch[:3])
        down_line = LineGather(down_ref, full_down, *scratch[3:])
        own_normed[...] = norm_rows(middle_ref[...], gain_ref[...])[1].astype(low)
        meet({"seq": side}, {"seq": down}, forth, back, twin)
        job = SquareGather(own_normed, normed, send, recv)
        job.start()
        up_line.start()

        def rows_of(rank):
            return pl.ds(pl.multiple_of(rank * rows, rows), rows)

        def multiply(rank):
            at = rows_of(rank)

            def store(columns, value):
                both[at, columns] = value

            block_product(normed.at[at], weights_ref, False, 512, store)

        normed[rows_of(me), :] = own_normed[...]
        weights_in.wait()
        multiply(me)
        up_line.step(1)
        job.relay()
        up_line.step(2)
        down_line.start()
        up_line.step(3)
        job.near()
        multiply(side)
        multiply(down)
        job.far()
        down_line.step(1)
        store.start(normed, normed_hbm)
        multiply(across)
        up_line.finish()
        store.start(full_up, full_up_hbm)

        def ahead(number, carry):
            at = rows_of(number)
            both[at, early:] = product(normed[at, :], full_up[...])
            gate, upward = both[at, :units], both[at, units:]
            hidden[at, :] = (gate * jax.nn.sigmoid(gate) * upward).astype(low)
            return carry

        lax.fori_loop(0, 4, ahead, 0)
        down_line.step(2)
        job.finish()
        store.start(hidden, hidden_hbm)
        cot_in.wait()
        transposed_product(hidden, cot_ref, terms)
        store.start(terms, terms_hbm)
        down_line.step(3)
        down_line.finish()
        store.start(full_down, full_down_hbm)

        def behind(number, carry):
            at = rows_of(number)
            grad_hidden = product_nt(cot_ref[at, :], full_down[...])
            gate, upward = both[at, :units], both[at, units:]
            sigma = jax.nn.sigmoid(gate)
            grads[at, :units] = (grad_hidden * upward * sigma * (1.0 + gate * (1.0 - sigma))).astype(low)
            grads[at, units:] = (grad_hidden * gate * sigma).astype(low)
            part(number).start()
            return carry

        def part(number):
            at = rows_of(number)
            return pltpu.make_async_copy(grads.at[at], grads_hbm.at[at], store_sems.at[5 + number])

        lax.fori_loop(0, 4, behind, 0)
        for number in range(4):
            part(number).wait()
        store.end()

    def shape(size, kind=low):
        return jax.ShapeDtypeStruct(size, kind)

    vmem = pl.BlockSpec(memory_space=pltpu.VMEM)
    anywhere = pl.BlockSpec(memory_space=pl.ANY)
    dma = pltpu.SemaphoreType.DMA
    results = [
        shape((slots, depth)),
        shape((slots, units)),
        shape((depth, own_up.shape[1])),
        shape((units, depth)),
        shape((slots, 2 * units)),
        shape((units, depth)),
    ]
    return pl.pallas_call(
        body,
        in_specs=[vmem, vmem, anywhere, vmem, vmem, anywhere],
        out_specs=[anywhere] * 6,
        out_shape=results,
        scratch_shapes=[
            pltpu.VMEM((rows, depth), low),
            pltpu.VMEM((slots, 2 * units), jnp.float32),
            dma((6,)),
            dma((6,)),
            *(pltpu.VMEM(value.shape, value.dtype) for value in (weights, cotangent, *results)),
            dma((2,)),
            dma((9,)),
        ]
        + 2 * LineGather.scratch(chips),
        compiler_params=pltpu.CompilerParams(
            collective_id=collective_id, has_side_effects=True, vmem_limit_bytes=VMEM_LIMIT
        ),
        name="feed_forward",
    )(middle, gain, weights, own_up, own_down, cotangent)


def feed_backward(grads, weights, up_weights, normed, terms_down, w_out, middle, gain, cotangent, attended, gate_pre,
                  collective_id):
    rows, depth = middle.shape
    slots = 4 * rows
    units = grads.shape[1] // 2
    early = weights.shape[1]
    columns = attended.shape[1]
    shards = 2 * lax.axis_size("seq")
    chips = shards // 2
    low = jnp.bfloat16

    def body(grads_hbm, weights_hbm, up_weights_hbm, normed_hbm, down_hbm, out_hbm, middle_hbm, gain_ref, cot_hbm,
             attended_hbm, pre_hbm,
             grad_middle_hbm, grad_gain, branch_hbm, d_attended, d_pre, terms_up_hbm, share_down, share_gate,
             own_branch, summed, terms_gate, send, recv,
             grads_ref, weights_ref, up_weights_ref, normed_ref, down_ref, out_ref, middle_ref, cot_ref,
             attended_ref, pre_ref, grad_middle, branch, terms_up, fetch_sems, store_sems, *scratch):
        fetch, store = Streams(fetch_sems), Streams(store_sems)
        first_in = [
            fetch.start(*both)
            for both in (
                (grads_hbm, grads_ref),
                (weights_hbm, weights_ref),
                (up_weights_hbm, up_weights_ref),
                (down_hbm, down_ref),
            )
        ]
        normed_in = fetch.start(normed_hbm, normed_ref)
        rest_in = [
            fetch.start(*both)
            for both in (
                (middle_hbm, middle_ref),
                (cot_hbm, cot_ref),
                (out_hbm, out_ref),
                (attended_hbm, attended_ref),
                (pre_hbm, pre_ref),
            )
        ]
        me, side, down, across = sides()
        line_chips, chip, core, forth, back, twin = line()
        meet({"seq": side}, {"seq": down}, forth, back, twin)
        first, second = grads_ref.at[:, pl.ds(0, units)], grads_ref.at[:, pl.ds(units, units)]
        job = SquareScatter(
            [grads_ref.at[:, pl.ds(0, early)], grads_ref.at[:, pl.ds(early, 2 * units - early)]],
            [weights_ref, up_weights_ref],
            True,
            summed,
            *scratch[:7],
        )
        run_down = LineScatter(down_ref, share_down, *scratch[7:12])
        run_gate = LineScatter(terms_gate, share_gate, *scratch[12:])
        every = SquareGather(own_branch, branch, send, recv)
        for copy in first_in:
            copy.wait()
        run_down.start()
        job.begin()
        run_down.slot(0)
        normed_in.wait()
        transposed_product(normed_ref, first, terms_gate)
        run_gate.start()
        job.relay()
        run_down.slot(1)
        job.own()
        transposed_product(normed_ref, second, terms_up)
        store.start(terms_up, terms_up_hbm)
        run_down.slot(2)
        run_gate.slot(0)
        for copy in rest_in:
            copy.wait()
        job.end()
        values, change = middle_ref[...], summed[...]
        scale = norm_rows(values, gain_ref[...])[0]
        grad_gain[...] = jnp.sum(change * values * scale, axis=0, keepdims=True)
        change = change * gain_ref[...]
        mean = jnp.mean(change * values, axis=-1, keepdims=True)
        total = cot_ref[...].astype(jnp.float32) + scale * change - values * (scale * scale * scale * mean)
        grad_middle[...] = total
        own_branch[...] = total.astype(low)
        every.start()
        store.start(grad_middle, grad_middle_hbm)

        def rows_of(rank):
            return pl.ds(pl.multiple_of(rank * rows, rows), rows)

        def multiply(rank):
            at = rows_of(rank)
            grad_gated = product_nt(branch[at, :], out_ref[...])
            sigma = jax.nn.sigmoid(pre_ref[at, :])
            d_attended[at, :] = (grad_gated * sigma).astype(low)
            d_pre[at, :] = (
                grad_gated * attended_ref[at, :].astype(jnp.float32) * sigma * (1.0 - sigma)
            ).astype(low)

        branch[rows_of(me), :] = own_branch[...]
        multiply(me)
        run_gate.slot(1)
        every.relay()
        run_gate.slot(2)
        every.near()
        multiply(side)
        multiply(down)
        run_down.end()
        every.far()
        store.start(branch, branch_hbm)
        multiply(across)
        every.finish()
        run_gate.end()
        store.end()

    def shape(size, kind=low):
        return jax.ShapeDtypeStruct(size, kind)

    vmem = pl.BlockSpec(memory_space=pltpu.VMEM)
    anywhere = pl.BlockSpec(memory_space=pl.ANY)
    dma = pltpu.SemaphoreType.DMA
    fetched = (grads, weights, up_weights, normed, terms_down, w_out, middle, cotangent, attended, gate_pre)
    return pl.pallas_call(
        body,
        in_specs=[anywhere] * 7 + [vmem] + [anywhere] * 3,
        out_specs=[anywhere, vmem, anywhere, vmem, vmem, anywhere, vmem, vmem],
        out_shape=[
            shape((rows, depth), jnp.float32),
            shape((1, depth), jnp.float32),
            shape((slots, depth)),
            shape((slots, columns)),
            shape((slots, columns)),
            shape((depth, units)),
            shape((terms_down.shape[0] // shards, depth)),
            shape((depth // shards, units)),
        ],
        scratch_shapes=[
            pltpu.VMEM((rows, depth), low),
            pltpu.VMEM((rows, depth), jnp.float32),
            pltpu.VMEM((depth, units), low),
            dma((6,)),
            dma((6,)),
            *(pltpu.VMEM(value.shape, value.dtype) for value in fetched),
            pltpu.VMEM((rows, depth), jnp.float32),
            pltpu.VMEM((slots, depth), low),
            pltpu.VMEM((depth, units), low),
            dma((len(fetched),)),
            dma((3,)),
        ]
        + SquareScatter.scratch(rows, depth)
        + LineScatter.scratch(chips, terms_down.shape[0] // shards, depth)
        + LineScatter.scratch(chips, depth // shards, units),
        compiler_params=pltpu.CompilerParams(
            collective_id=collective_id, has_side_effects=True, vmem_limit_bytes=VMEM_LIMIT
        ),
        name="feed_backward",
    )(grads, weights, up_weights, normed, terms_down, w_out, middle, gain, cotangent, attended, gate_pre)


def gather(value, axis_name):
    return lax.all_gather(value, axis_name, axis=0, tiled=True)


def scatter(value, axis_name):
    return lax.psum_scatter(value, axis_name, scatter_dimension=0, tiled=True)


def on_device(
    layer_input,
    lengths,
    norm_attn,
    w_query,
    w_key,
    w_value,
    w_ogate,
    w_forget,
    forget_bias,
    w_out,
    norm_ffn,
    w_gate,
    w_up,
    w_down,
    output_grad,
):
    low = jnp.bfloat16
    tokens, width = layer_input.shape[1:]
    heads = forget_bias.shape[0]
    groups = lax.axis_size("seq")
    shards = lax.axis_size("wshard")
    fast = square(groups) and shards == 2 * groups
    local_heads = heads // groups
    head_size = width // heads
    columns = width // groups
    lanes = columns + -columns % PAIR
    front = 3 * lanes + PAIR
    slots = tokens * groups
    hidden_size = w_gate.shape[1]
    part = hidden_size // (groups * shards)
    units = shards * part
    scale = head_size ** (-0.5)
    length = lengths[0]
    seq_rank = lax.axis_index("seq")
    shard_rank = lax.axis_index("wshard")
    per_block = shards // groups
    positions = seq_rank * tokens + jnp.arange(tokens, dtype=jnp.int32)
    valid_slots = (positions < length)[:, None]
    inputs = layer_input[0].astype(jnp.float32)
    cotangent_low = jnp.where(valid_slots, output_grad[0], jnp.zeros((), low))
    cotangent = cotangent_low.astype(jnp.float32)

    def own_columns(weight, size):
        taken = lax.dynamic_slice_in_dim(weight, seq_rank * columns, columns, 1)
        return jnp.pad(taken, ((0, 0), (0, size - columns))) if size > columns else taken

    def own_units(weight):
        split = weight.reshape(weight.shape[0], shards, groups, part)
        mine = lax.dynamic_index_in_dim(split, seq_rank, 2, keepdims=False)
        return mine.reshape(weight.shape[0], units)

    own_forget = lax.dynamic_slice_in_dim(w_forget, seq_rank * local_heads, local_heads, 1)
    own_forget = jnp.pad(own_forget, ((0, 0), (0, PAIR - local_heads)))
    own_bias = lax.dynamic_slice_in_dim(forget_bias, seq_rank * local_heads, local_heads)
    own_bias = jnp.pad(own_bias, (0, PAIR - local_heads))[None]
    length_row = jnp.broadcast_to(lengths[:, None], (1, PAIR))
    mine_down = lax.dynamic_slice_in_dim(w_down, seq_rank * part, part, 0)
    if fast:
        (
            normed_attn, cotangent_all, full_front, full_ogate, full_out, full_ffn,
            joined, attended_low, offset, col, logit, gate_pre, gated, middle, mine_up,
        ) = whole_forward(
            layer_input[0], norm_attn[None], cotangent_low, (w_query, w_key, w_value, w_ogate), own_forget,
            own_bias, length_row, w_out, w_gate, w_up, head_size, scale, 0,
        )
        full_out = full_out.reshape(columns, width)
        normed_ffn, hidden, full_up, full_down, grad_gate_up, terms_down = feed_forward(
            middle, norm_ffn[None], full_ffn, mine_up, mine_down, cotangent_all, 1
        )
        (
            grad_middle, grad_norm_ffn, grad_branch, grad_attended, grad_gate_pre, terms_up, share_down, share_gate,
        ) = feed_backward(
            grad_gate_up, full_ffn, full_up, normed_ffn, terms_down, full_out, middle, norm_ffn[None],
            cotangent_low, attended_low, gate_pre, 2,
        )
        grad_norm_ffn = grad_norm_ffn[0]
        grads, bias_rows, lowered, collected, share_up, share_ogate, grad_down = middle_backward(
            joined, grad_attended, offset, col, logit, hidden, full_down, gated, grad_branch, terms_up, share_down,
            normed_attn, grad_gate_pre, head_size, scale, 3,
        )
        grad_normed_attn, share_attn, grad_out, every_gate, every_ogate = last_backward(
            grads, grad_gate_pre, normed_attn, full_front, full_ogate, collected, (share_gate, share_ogate), 4
        )
        grad_out = grad_out.reshape(columns // per_block, width)
    else:
        mine_front = jnp.concatenate(
            [*(own_columns(w, lanes) for w in (w_query, w_key, w_value)), own_forget], axis=1
        )
        full_front = gather(mine_front, "wshard")
        full_ogate = gather(own_columns(w_ogate, columns), "wshard")
        normed_attn = gather(rms_norm(inputs, norm_attn).astype(low), "seq")
        cotangent_all = gather(cotangent_low, "seq")
        full_out = lax.dynamic_slice_in_dim(gather(w_out, "wshard"), seq_rank * columns, columns, 0)
        full_ffn = gather(jnp.concatenate([own_units(w_gate), own_units(w_up)], axis=1), "wshard")
        joined = product(normed_attn, full_front).astype(low)
        gate_pre = product(normed_attn, full_ogate)
        attended_low, offset, col, logit = attention_fwd(joined, own_bias, length_row, head_size, scale)
        attended = attended_low[:, :columns].astype(jnp.float32)
        gated_full, pull_gate = jax.vjp(gate_product, attended, gate_pre)
        gated = gated_full.astype(low)
        middle = inputs + scatter(product(gated, full_out).astype(low), "seq").astype(jnp.float32)
        normed_ffn_own, pull_ffn_norm = jax.vjp(rms_norm, middle, norm_ffn)
        full_down = gather(mine_down, "wshard")
        normed_ffn = gather(normed_ffn_own.astype(low), "seq")
        gate_up = product(normed_ffn, full_ffn)
        hidden_full, pull_swiglu = jax.vjp(swiglu, gate_up[:, :units], gate_up[:, units:])
        hidden = hidden_full.astype(low)
        grad_hidden = product_nt(cotangent_all, full_down)
        grad_gate_full, grad_up_full = pull_swiglu(grad_hidden)
        grad_gate_up = jnp.concatenate([grad_gate_full.astype(low), grad_up_full.astype(low)], axis=1)
        share_down = scatter(product_tn(hidden, cotangent_all).astype(low), "wshard")
        share_ffn = scatter(product_tn(normed_ffn, grad_gate_up).astype(low), "wshard")
        grad_normed_ffn = scatter(product_nt(grad_gate_up, full_ffn).astype(low), "seq").astype(jnp.float32)
        grad_middle_part, grad_norm_ffn = pull_ffn_norm(grad_normed_ffn)
        grad_middle = cotangent + grad_middle_part
        grad_branch = gather(grad_middle.astype(low), "seq")
        grad_attended_full, grad_gate_pre_full = pull_gate(product_nt(grad_branch, full_out))
        grad_attended = grad_attended_full.astype(low)
        grad_gate_pre = grad_gate_pre_full.astype(low)
        if lanes > columns:
            grad_attended = jnp.pad(grad_attended, ((0, 0), (0, lanes - columns)))
        grads, bias_rows = attention_bwd(joined, grad_attended, offset, col, logit, head_size, scale)
        grad_projected = jnp.concatenate([grads, grad_gate_pre], axis=1)
        share_attn = scatter(product_tn(normed_attn, grad_projected).astype(low), "wshard")
        full_attn = jnp.concatenate([full_front, full_ogate], axis=1)
        grad_normed_attn = scatter(product_nt(grad_projected, full_attn).astype(low), "seq").astype(jnp.float32)
        lowered = scatter(product(hidden, full_down).astype(low), "seq").astype(jnp.float32)
        share_out = scatter(product_tn(gated, grad_branch).astype(low), "wshard")
        rows_out = columns // shards
        pieces_out = lax.all_gather(share_out, "seq", axis=0, tiled=False)
        takes = shards // per_block
        slots_out = jnp.where(
            (jnp.arange(per_block) == shard_rank // takes)[None, :, None, None],
            pieces_out[:, None],
            jnp.zeros((), low),
        ).reshape(shards, rows_out, width)
        moved = lax.all_to_all(slots_out, "wshard", split_axis=0, concat_axis=0, tiled=True)
        moved = moved.reshape(per_block, takes, rows_out, width)
        mine_out = lax.dynamic_index_in_dim(moved, shard_rank % per_block, 0, keepdims=False)
        grad_out = mine_out.reshape(columns // per_block, width).astype(jnp.float32)
    layer_output = (middle + lowered).astype(low)[None]
    grad_bias = lax.dynamic_update_slice_in_dim(
        jnp.zeros((heads,), jnp.float32), bias_rows[:local_heads, 0], seq_rank * local_heads, 0
    )
    unused_normed, pull_attn_norm = jax.vjp(rms_norm, inputs, norm_attn)
    grad_input_part, grad_norm_attn = pull_attn_norm(grad_normed_attn)
    grad_input = (grad_middle + grad_input_part)[None]

    rows = share_attn.shape[0]
    if fast:
        vector = jnp.concatenate([grad_norm_attn, grad_norm_ffn, grad_bias])
        vector = jnp.pad(vector, (0, -vector.shape[0] % 1024)).reshape(-1, 128)
        every_attn, every_up, vector = last_gather([share_attn, share_up], vector, 5)
        vector = vector.reshape(-1)
        small = vector[:width], vector[width : 2 * width], vector[2 * width : 2 * width + heads]
    else:
        every_attn, every_ffn, grad_down = [gather(v, "seq") for v in (share_attn, share_ffn, share_down)]
        small = lax.psum((grad_norm_attn, grad_norm_ffn, grad_bias), ("seq", "wshard"))
    every_attn = every_attn.reshape((groups,) + share_attn.shape)
    if fast:
        grad_w_gate, grad_w_up, grad_down, grad_out = join_units(
            every_gate.reshape((groups,) + share_gate.shape), every_up.reshape((groups,) + share_up.shape),
            grad_down, grad_out, part,
        )
        every_ogate = every_ogate.reshape((groups,) + share_ogate.shape)
        *weight_grads, grad_forget_w = join_columns(
            every_attn, every_ogate, columns, (0, lanes, 2 * lanes), 3 * lanes, heads
        )
    else:

        def join(first):
            taken = every_attn[:, :, first : first + columns]
            return taken.transpose(1, 0, 2).reshape(rows, width).astype(jnp.float32)

        def join_own_units(first):
            taken = every_ffn.reshape((groups,) + share_ffn.shape)[:, :, first * units : (first + 1) * units]
            taken = taken.reshape(groups, rows, shards, part).transpose(1, 2, 0, 3)
            return taken.reshape(rows, hidden_size).astype(jnp.float32)

        weight_grads = [join(first) for first in (0, lanes, 2 * lanes, front)]
        grad_w_gate, grad_w_up = join_own_units(0), join_own_units(1)
        grad_down = grad_down.astype(jnp.float32)
        grad_forget_w = every_attn[:, :, 3 * lanes : 3 * lanes + local_heads]
        grad_forget_w = grad_forget_w.transpose(1, 0, 2).reshape(rows, heads).astype(jnp.float32)
    return (
        layer_output,
        grad_input,
        small[0],
        *weight_grads,
        grad_forget_w,
        small[2],
        grad_out,
        small[1],
        grad_w_gate,
        grad_w_up,
        grad_down,
    )


def solution(mesh):
    return jax.shard_map(
        on_device,
        mesh=mesh,
        in_specs=(
            P("wshard", "seq", None),
            P("wshard"),
            P(),
            P("wshard", None),
            P("wshard", None),
            P("wshard", None),
            P("wshard", None),
            P("wshard", None),
            P(),
            P("wshard", None),
            P(),
            P("wshard", None),
            P("wshard", None),
            P("wshard", None),
            P("wshard", "seq", None),
        ),
        out_specs=(
            P("wshard", "seq", None),
            P("wshard", "seq", None),
            P(),
            P("wshard", None),
            P("wshard", None),
            P("wshard", None),
            P("wshard", None),
            P("wshard", None),
            P(),
            P("wshard", None),
            P(),
            P("wshard", None),
            P("wshard", None),
            P("wshard", None),
        ),
        check_vma=False,
    )
```

```python
import jax
import jax.numpy as jnp
from jax import lax
from jax.experimental import pallas as pl
from jax.experimental.pallas import tpu as pltpu
from jax.sharding import PartitionSpec as P

EPS = 1e-06
NEG_FILL = -1e30
PAIR = 128


def product(left, right):
    return jnp.dot(left, right, preferred_element_type=jnp.float32)


def product_tn(left, right):
    return lax.dot_general(
        left, right, (((0,), (0,)), ((), ())), preferred_element_type=jnp.float32
    )


def product_nt(left, right):
    return lax.dot_general(
        left, right, (((1,), (1,)), ((), ())), preferred_element_type=jnp.float32
    )


def rms_norm(values, gain):
    return values * lax.rsqrt(jnp.mean(values * values, axis=-1, keepdims=True) + EPS) * gain


def gate_product(attended, gate_pre):
    return attended * jax.nn.sigmoid(gate_pre)


def swiglu(gate, upward):
    return jax.nn.silu(gate) * upward


def low_triangle(size):
    rows = lax.broadcasted_iota(jnp.int32, (size, size), 0)
    return rows <= lax.broadcasted_iota(jnp.int32, (size, size), 1)


def exact(left, right):
    return jnp.dot(left, right, precision=lax.Precision.HIGHEST, preferred_element_type=jnp.float32)


class Forward:
    some = 8

    def __init__(self, joined, bias, length, attended, offset, col, logit, row, head_size, scale):
        self.joined, self.bias, self.length = joined, bias, length
        self.attended, self.offset, self.col, self.logit, self.row = attended, offset, col, logit, row
        self.head_size, self.scale = head_size, scale
        self.slots = joined.shape[0]
        self.pairs = (joined.shape[1] // PAIR - 1) // 3
        self.tile = min(256, self.slots)

    @staticmethod
    def results(slots, pairs):
        rows = jax.ShapeDtypeStruct((Forward.some, slots), jnp.float32)
        return [
            jax.ShapeDtypeStruct((slots, pairs * PAIR), jnp.bfloat16),
            rows,
            jax.ShapeDtypeStruct((slots, PAIR), jnp.float32),
            rows,
        ]

    def lanes(self, pair, part=0):
        return pl.ds(pl.multiple_of((part * self.pairs + pair) * PAIR, PAIR), PAIR)

    def start(self):
        slots, tile, some = self.slots, self.tile, self.some
        logits = self.joined[:, 3 * self.pairs * PAIR :].astype(jnp.float32) + self.bias[...]
        logit_rows = logits.T[:some]
        self.logit[...] = logit_rows
        logs = jnp.minimum(logit_rows, 0.0) - jnp.log1p(jnp.exp(-jnp.abs(logit_rows)))
        ones = low_triangle(tile).astype(jnp.float32)
        carry = jnp.zeros((some, 1), jnp.float32)
        for first in range(0, slots, tile):
            sums = exact(logs[:, first : first + tile], ones) + carry
            self.row[:, first : first + tile] = sums
            carry = sums[:, tile - 1 : tile]
        wide = jnp.concatenate([self.row[...], jnp.zeros((PAIR - some, slots), jnp.float32)], axis=0).T
        usable = lax.broadcasted_iota(jnp.int32, (slots, PAIR), 0) < self.length[...]
        self.col[...] = jnp.where(usable, wide, -NEG_FILL)

    def pair(self, pair):
        slots, tile, half = self.slots, self.tile, self.head_size
        key_all = self.joined[:, self.lanes(pair, 1)]
        value_t = self.joined[:, self.lanes(pair, 2)].T
        query_t = (self.joined[:, self.lanes(pair)].astype(jnp.float32) * self.scale).astype(jnp.bfloat16).T
        sub = lax.broadcasted_iota(jnp.int32, (PAIR, tile), 0)
        wide = lax.broadcasted_iota(jnp.int32, (slots, PAIR), 1)
        diag = low_triangle(tile)
        columns = [
            jnp.sum(jnp.where(wide == 2 * pair + a, self.col[...], 0.0), axis=1, keepdims=True) for a in range(2)
        ]
        for number in range(slots // tile):
            first, last = number * tile, (number + 1) * tile
            outs = []
            for a in range(2):
                mine = (sub >= a * half) & (sub < (a + 1) * half)
                at = pl.ds(2 * pair + a, 1)
                query = jnp.where(mine, query_t[:, first:last], jnp.zeros((), query_t.dtype))
                scores = product(key_all[:last], query)
                own_row = self.row[at, first:last]
                scores = scores + (own_row - columns[a][:last])
                tail = jnp.where(diag, scores[first:], NEG_FILL)
                scores = tail if number == 0 else jnp.concatenate([scores[:first], tail], axis=0)
                top = jnp.max(scores, axis=0, keepdims=True)
                weights = jnp.exp(scores - top)
                total = jnp.sum(weights, axis=0, keepdims=True)
                mixed = product(value_t[a * half : (a + 1) * half, :last], weights.astype(jnp.bfloat16))
                outs.append(mixed / total)
                self.offset[at, first:last] = own_row - (top + jnp.log(total))
            self.attended[first:last, self.lanes(pair)] = jnp.concatenate(outs, axis=0).T.astype(jnp.bfloat16)


def attention_fwd(joined, bias, length, head_size, scale):
    slots = joined.shape[0]
    pairs = (joined.shape[1] // PAIR - 1) // 3

    def body(joined_ref, bias_ref, length_ref, attended, offset, col, logit, row):
        work = Forward(joined_ref, bias_ref, length_ref, attended, offset, col, logit, row, head_size, scale)
        work.start()
        offset[...] = jnp.zeros_like(offset)

        def step(pair, carry):
            work.pair(pair)
            return carry

        lax.fori_loop(0, pairs, step, 0)

    vmem = pl.BlockSpec(memory_space=pltpu.VMEM)
    return pl.pallas_call(
        body,
        in_specs=[vmem] * 3,
        out_specs=[vmem] * 4,
        out_shape=Forward.results(slots, pairs),
        scratch_shapes=[pltpu.VMEM((Forward.some, slots), jnp.float32)],
        compiler_params=pltpu.CompilerParams(vmem_limit_bytes=56 << 20),
        cost_estimate=pl.CostEstimate(
            flops=4 * slots * slots * pairs * PAIR, bytes_accessed=8 * slots * pairs * PAIR, transcendentals=0
        ),
        name="attention_fwd",
    )(joined, bias, length)


def backward_scratch(slots):
    return [
        pltpu.VMEM((slots, PAIR), jnp.float32),
        pltpu.VMEM((slots, PAIR), jnp.float32),
        pltpu.VMEM((slots, PAIR), jnp.float32),
        pltpu.VMEM((8, slots), jnp.float32),
    ]


class Backward:
    def __init__(self, joined, d_out, offset, col, logit, grads, dk_acc, dv_acc, dcol, drow, head_size, scale):
        self.joined, self.d_out, self.offset, self.col = joined, d_out, offset, col
        self.logit, self.grads, self.dk_acc, self.dv_acc = logit, grads, dk_acc, dv_acc
        self.dcol, self.drow, self.head_size, self.scale = dcol, drow, head_size, scale
        self.slots = joined.shape[0]
        self.pairs = (joined.shape[1] // PAIR - 1) // 3
        self.tile = min(256, self.slots)

    def start(self):
        self.dcol[...] = jnp.zeros_like(self.dcol)
        self.drow[...] = jnp.zeros_like(self.drow)

    def lanes(self, pair, part=0):
        return pl.ds(pl.multiple_of((part * self.pairs + pair) * PAIR, PAIR), PAIR)

    def pair(self, pair):
        slots, tile, half = self.slots, self.tile, self.head_size
        dk_acc, dv_acc, dcol, drow = self.dk_acc, self.dv_acc, self.dcol, self.drow
        queries = (self.joined[:, self.lanes(pair)].astype(jnp.float32) * self.scale).astype(jnp.bfloat16)
        key_all = self.joined[:, self.lanes(pair, 1)]
        value_all = self.joined[:, self.lanes(pair, 2)]
        d_out = self.d_out[:, self.lanes(pair)]
        query_t, key_t, dout_t = queries.T, key_all.T, d_out.T
        sub = lax.broadcasted_iota(jnp.int32, (PAIR, tile), 0)
        lanes = lax.broadcasted_iota(jnp.int32, (tile, PAIR), 1)
        wide = lax.broadcasted_iota(jnp.int32, (slots, PAIR), 1)
        diag = low_triangle(tile)
        zero = jnp.zeros((), jnp.bfloat16)
        columns = [
            jnp.sum(jnp.where(wide == 2 * pair + a, self.col[...], 0.0), axis=1, keepdims=True) for a in range(2)
        ]
        dk_acc[...] = jnp.zeros_like(dk_acc)
        dv_acc[...] = jnp.zeros_like(dv_acc)
        for number in range(slots // tile):
            first, last = number * tile, (number + 1) * tile
            outs = []
            for a in range(2):
                mine = (sub >= a * half) & (sub < (a + 1) * half)
                own = (lanes >= a * half) & (lanes < (a + 1) * half)
                at = pl.ds(2 * pair + a, 1)
                scores = product(key_all[:last], jnp.where(mine, query_t[:, first:last], zero))
                scores = scores + (self.offset[at, first:last] - columns[a][:last])
                tail = jnp.where(diag, scores[first:], NEG_FILL)
                scores = tail if number == 0 else jnp.concatenate([scores[:first], tail], axis=0)
                probs = jnp.exp(scores)
                d_probs = product(value_all[:last], jnp.where(mine, dout_t[:, first:last], zero))
                dot = jnp.sum(d_probs * probs, axis=0, keepdims=True)
                d_full = probs * (d_probs - dot)
                d_scores = d_full.astype(jnp.bfloat16)
                drow[at, first:last] = jnp.sum(d_full, axis=0, keepdims=True)
                sums = jnp.sum(d_full, axis=1, keepdims=True)
                dcol[:last, :] += jnp.where(wide[:last] == 2 * pair + a, sums, 0.0)
                outs.append(product(key_t[a * half : (a + 1) * half, :last], d_scores) * self.scale)
                dk_acc[:last, :] += product(d_scores, jnp.where(own, queries[first:last, :], zero))
                dv_acc[:last, :] += product(
                    probs.astype(jnp.bfloat16), jnp.where(own, d_out[first:last, :], zero)
                )
            self.grads[first:last, self.lanes(pair)] = jnp.concatenate(outs, axis=0).T.astype(self.grads.dtype)
        self.grads[:, self.lanes(pair, 1)] = dk_acc[...].astype(self.grads.dtype)
        self.grads[:, self.lanes(pair, 2)] = dv_acc[...].astype(self.grads.dtype)

    def end(self, bias_grad):
        slots, tile, some = self.slots, self.tile, 8
        change = self.drow[...] - self.dcol[...].T[:some]
        rows = lax.broadcasted_iota(jnp.int32, (tile, tile), 0)
        ones = (rows >= lax.broadcasted_iota(jnp.int32, (tile, tile), 1)).astype(jnp.float32)
        carry = jnp.zeros((some, 1), jnp.float32)
        pieces = []
        for first in reversed(range(0, slots, tile)):
            sums = exact(change[:, first : first + tile], ones) + carry
            carry = sums[:, :1]
            pieces.insert(0, sums)
        grad = jnp.concatenate(pieces, axis=1) * jax.nn.sigmoid(-self.logit[...])
        heads = lax.broadcasted_iota(jnp.int32, (some, slots), 0)
        grad = jnp.where(heads < 2 * self.pairs, grad, 0.0)
        bias_grad[...] = jnp.broadcast_to(jnp.sum(grad, axis=1, keepdims=True), bias_grad.shape)
        wide = jnp.concatenate([grad, jnp.zeros((PAIR - some, slots), jnp.float32)], axis=0).T
        self.grads[:, 3 * self.pairs * PAIR : (3 * self.pairs + 1) * PAIR] = wide.astype(self.grads.dtype)


def attention_bwd(joined, d_out, offset, col, logit, head_size, scale):
    slots, width = joined.shape
    pairs = (width // PAIR - 1) // 3

    def body(joined_ref, d_out_ref, offset_ref, col_ref, logit_ref, grads, bias_grad, *scratch):
        work = Backward(
            joined_ref, d_out_ref, offset_ref, col_ref, logit_ref, grads, *scratch, head_size, scale
        )
        work.start()

        def step(pair, carry):
            work.pair(pair)
            return carry

        lax.fori_loop(0, pairs, step, 0)
        work.end(bias_grad)

    vmem = pl.BlockSpec(memory_space=pltpu.VMEM)
    return pl.pallas_call(
        body,
        in_specs=[vmem] * 5,
        out_specs=[vmem] * 2,
        out_shape=[
            jax.ShapeDtypeStruct((slots, width), jnp.bfloat16),
            jax.ShapeDtypeStruct((8, PAIR), jnp.float32),
        ],
        scratch_shapes=backward_scratch(slots),
        compiler_params=pltpu.CompilerParams(vmem_limit_bytes=56 << 20),
        cost_estimate=pl.CostEstimate(
            flops=10 * slots * slots * pairs * PAIR, bytes_accessed=14 * slots * pairs * PAIR, transcendentals=0
        ),
        name="attention_bwd",
    )(joined, d_out, offset, col, logit)


MESH = pl.DeviceIdType.MESH
VMEM_LIMIT = 62 << 20


def square(groups):
    return groups == 4


def sides():
    rank = lax.axis_index("seq")
    return rank, rank + 1 - 2 * lax.rem(rank, 2), lax.rem(rank + 2, 4), 3 - rank


def meet(*others):
    barrier = pltpu.get_barrier_semaphore()
    for other in others:
        pl.semaphore_signal(barrier, inc=1, device_id=other, device_id_type=MESH)
    pl.semaphore_wait(barrier, len(others))


def push(source, target, send, recv, device):
    copy = pltpu.make_async_remote_copy(
        src_ref=source,
        dst_ref=target,
        send_sem=send,
        recv_sem=recv,
        device_id=device,
        device_id_type=MESH,
    )
    copy.start()
    return copy


def by_rows(rows, work):
    def step(number, carry):
        work(pl.ds(pl.multiple_of(number * 16, 16), 16))
        return carry

    lax.fori_loop(0, rows // 16, step, 0)


class Streams:
    def __init__(self, sems):
        self.sems, self.made = sems, []

    def start(self, source, target):
        copy = pltpu.make_async_copy(source, target, self.sems.at[len(self.made)])
        self.made.append(copy)
        copy.start()
        return copy

    def end(self):
        for copy in self.made:
            copy.wait()


class SquareGather:
    def __init__(self, own, full, send, recv):
        self.own, self.full, self.send, self.recv = own, full, send, recv
        self.rows = own.shape[0]
        self.half = self.rows // 2

    def place(self, rank, part):
        return self.full.at[pl.ds(pl.multiple_of(rank * self.rows + part * self.half, self.half), self.half)]

    def copy(self, index):
        me, side, down, across = sides()
        mine = [self.own.at[pl.ds(part * self.half, self.half)] for part in (0, 1)]
        source, target, peer = (
            (mine[0], self.place(me, 0), side),
            (mine[1], self.place(me, 1), down),
            (mine[1], self.place(me, 1), side),
            (mine[0], self.place(me, 0), down),
            (self.place(side, 0), self.place(side, 0), down),
            (self.place(down, 1), self.place(down, 1), side),
        )[index]
        return pltpu.make_async_remote_copy(
            src_ref=source,
            dst_ref=target,
            send_sem=self.send.at[index],
            recv_sem=self.recv.at[index],
            device_id={"seq": peer},
            device_id_type=MESH,
        )

    def start(self):
        for index in range(4):
            self.copy(index).start()

    def relay(self):
        for index in (0, 1):
            self.copy(index).wait_recv()
            self.copy(4 + index).start()

    def near(self):
        self.copy(2).wait_recv()
        self.copy(3).wait_recv()

    def far(self):
        self.copy(4).wait_recv()
        self.copy(5).wait_recv()

    def finish(self):
        for index in range(6):
            self.copy(index).wait_send()


def block_product(left, right, transposed, tile, store):
    total = right.shape[0] if transposed else right.shape[1]

    def step(number, carry):
        columns = pl.ds(pl.multiple_of(number * tile, tile), tile)
        if transposed:
            store(columns, product_nt(left[...], right[columns, :]))
        else:
            store(columns, product(left[...], right[:, columns]))
        return carry

    lax.fori_loop(0, total // tile, step, 0)


def transposed_product(left, right, out):
    tall = 512 if out.shape[0] % 512 == 0 else 384
    wide = next(size for size in (512, 384, 640, 128) if out.shape[1] % size == 0)
    across = out.shape[1] // wide

    def step(number, carry):
        rows = pl.ds(pl.multiple_of((number // across) * tall, tall), tall)
        columns = pl.ds(pl.multiple_of(lax.rem(number, across) * wide, wide), wide)
        out[rows, columns] = product_tn(left[:, rows], right[:, columns]).astype(out.dtype)
        return carry

    lax.fori_loop(0, (out.shape[0] // tall) * across, step, 0)


def line():
    shards, place = lax.axis_size("wshard"), lax.axis_index("wshard")
    chips = shards // 2
    chip, core = place // 2, lax.rem(place, 2)
    forth = {"wshard": lax.rem(place + 2, shards)}
    back = {"wshard": lax.rem(place + shards - 2, shards)}
    twin = {"wshard": place + 1 - 2 * core}
    return chips, chip, core, forth, back, twin


class LineGather:
    @staticmethod
    def scratch(chips):
        dma = pltpu.SemaphoreType.DMA
        return [dma((3, chips)), dma((2 * chips,)), dma((1,))]

    def __init__(self, own, full, send, recv, local):
        self.own, self.full, self.local = own, full, local.at[0]
        self.sends = (send.at[0], send.at[1], send.at[2])
        self.recv = recv
        self.rows = own.shape[0]
        self.chips, self.chip, self.core, *self.devices = line()

    def place(self, chip, core):
        return self.full.at[pl.ds(pl.multiple_of((2 * chip + core) * self.rows, self.rows), self.rows)]

    def copy(self, way, chip, source=None):
        target = self.place(chip, self.core)
        return pltpu.make_async_remote_copy(
            src_ref=target if source is None else source,
            dst_ref=target,
            send_sem=self.sends[way].at[chip],
            recv_sem=self.recv.at[2 * chip + self.core],
            device_id=self.devices[way],
            device_id_type=MESH,
        )

    def wait_for(self, chip, core):
        target = self.place(chip, core)
        pltpu.make_async_remote_copy(
            src_ref=target,
            dst_ref=target,
            send_sem=self.sends[2].at[0],
            recv_sem=self.recv.at[2 * chip + core],
            device_id=self.devices[2],
            device_id_type=MESH,
        ).wait_recv()

    def start(self):
        @pl.when(self.chip < self.chips - 1)
        def _():
            self.copy(0, self.chip, self.own).start()

        @pl.when(self.chip > 0)
        def _():
            self.copy(1, self.chip, self.own).start()

        self.copy(2, self.chip, self.own).start()
        self.keep().start()

    def keep(self):
        return pltpu.make_async_copy(self.own, self.place(self.chip, self.core), self.local)

    def step(self, number):
        left, right = self.chip - number, self.chip + number

        @pl.when(left >= 0)
        def _():
            self.wait_for(left, self.core)

            @pl.when(self.chip < self.chips - 1)
            def _():
                self.copy(0, left).start()

            self.copy(2, left).start()

        @pl.when(right < self.chips)
        def _():
            self.wait_for(right, self.core)

            @pl.when(self.chip > 0)
            def _():
                self.copy(1, right).start()

            self.copy(2, right).start()

    def finish(self):
        for chip in range(self.chips):
            self.wait_for(chip, 1 - self.core)
            self.copy(2, chip).wait_send()

            @pl.when((chip <= self.chip) & (self.chip < self.chips - 1))
            def _():
                self.copy(0, chip).wait_send()

            @pl.when((chip >= self.chip) & (self.chip > 0))
            def _():
                self.copy(1, chip).wait_send()

        self.keep().wait()


class PartExchange:
    @staticmethod
    def scratch():
        dma = pltpu.SemaphoreType.DMA
        return [dma((4,)), dma((4,)), dma((1,))]

    def __init__(self, parts, out, send, recv, local):
        self.parts, self.out, self.send, self.recv, self.local = parts, out, send, recv, local
        self.rank = lax.axis_index("seq")
        self.core, self.twin = line()[2], line()[5]
        self.others = [{"seq": lax.rem(self.rank + k, 4)} for k in range(1, 4)]
        self.rows = out.shape[2]

    def part(self, rank):
        return self.parts.at[pl.ds(pl.multiple_of((2 * rank + self.core) * self.rows, self.rows), self.rows)]

    def copy(self, index):
        if index == 3:
            source = target = self.out.at[self.core]
        else:
            source = self.part(lax.rem(self.rank + index + 1, 4))
            target = self.out.at[self.core, self.rank]
        return pltpu.make_async_remote_copy(
            src_ref=source,
            dst_ref=target,
            send_sem=self.send.at[index],
            recv_sem=self.recv.at[index],
            device_id=self.twin if index == 3 else self.others[index],
            device_id_type=MESH,
        )

    def keep(self):
        return pltpu.make_async_copy(self.part(self.rank), self.out.at[self.core, self.rank], self.local.at[0])

    def start(self):
        for index in (1, 0, 2):
            self.copy(index).start()
        self.keep().start()

    def relay(self):
        for index in range(3):
            self.copy(index).wait()
        self.keep().wait()
        self.copy(3).start()

    def end(self):
        self.copy(3).wait()


class Regroup:
    @staticmethod
    def scratch(rows, width):
        dma = pltpu.SemaphoreType.DMA
        return [pltpu.VMEM((4, rows, width), jnp.bfloat16), dma((7,)), dma((7,))]

    def __init__(self, piece, out, fours, send, recv):
        self.piece, self.out, self.fours, self.send, self.recv = piece, out, fours, send, recv
        self.rank, self.place = lax.axis_index("seq"), lax.axis_index("wshard")
        self.number = lax.rem(self.place, 4)
        self.others = [{"seq": lax.rem(self.rank + k, 4)} for k in range(1, 4)]
        self.along = [{"wshard": lax.rem(self.place + k, 8)} for k in range(1, 8)]

    def near(self, index):
        return pltpu.make_async_remote_copy(
            src_ref=self.piece,
            dst_ref=self.fours.at[self.rank],
            send_sem=self.send.at[index],
            recv_sem=self.recv.at[index],
            device_id=self.others[index],
            device_id_type=MESH,
        )

    def owner(self, rank):
        return 2 * rank + self.place // 4

    def far(self, rank, number):
        return pltpu.make_async_remote_copy(
            src_ref=self.fours.at[rank],
            dst_ref=self.out.at[number],
            send_sem=self.send.at[3 + rank],
            recv_sem=self.recv.at[3 + number],
            device_id={"wshard": self.owner(rank)},
            device_id_type=MESH,
        )

    def start(self):
        for index in range(3):
            self.near(index).start()
        self.fours[self.rank] = self.piece[...]

    def relay(self):
        for index in range(3):
            self.near(index).wait()
        for rank in range(4):

            @pl.when(self.owner(rank) != self.place)
            def _():
                self.far(rank, self.number).start()

            @pl.when(self.owner(rank) == self.place)
            def _():
                self.out[self.number] = self.fours[rank]

    def end(self):
        for rank in range(4):

            @pl.when(self.owner(rank) != self.place)
            def _():
                self.far(rank, self.number).wait_send()

        for number in range(4):

            @pl.when(4 * lax.rem(self.place, 2) + number != self.place)
            def _():
                self.far(0, number).wait_recv()


class Everywhere:
    def __init__(self, values, out, ranks, total, places, send, recv):
        self.values, self.out, self.ranks, self.total, self.places = values, out, ranks, total, places
        self.send, self.recv = send, recv
        self.groups, self.shards = ranks.shape[0], places.shape[0]
        self.rank, self.place = lax.axis_index("seq"), lax.axis_index("wshard")

    def others(self):
        return [{"seq": lax.rem(self.rank + k, self.groups)} for k in range(1, self.groups)]

    def along(self):
        return [{"wshard": lax.rem(self.place + k, self.shards)} for k in range(1, self.shards)]

    def start(self):
        self.first = [
            push(self.values, self.ranks.at[self.rank], self.send.at[k], self.recv.at[k], other)
            for k, other in enumerate(self.others())
        ]
        self.ranks[self.rank] = self.values[...]

    def relay(self):
        for copy in self.first:
            copy.wait()
        ranks, groups = self.ranks, self.groups
        self.total[...] = (ranks[0] + ranks[1]) + (ranks[2] + ranks[3])
        self.second = [
            push(self.total, self.places.at[self.place], self.send.at[groups + k], self.recv.at[groups + k], other)
            for k, other in enumerate(self.along())
        ]
        self.places[self.place] = self.total[...]

    def end(self):
        for copy in self.second:
            copy.wait()
        sums = [self.places[k] + self.places[k + 1] for k in range(0, self.shards, 2)]
        self.out[...] = (sums[0] + sums[1]) + (sums[2] + sums[3])


def last_gather(values, small, collective_id):
    count = len(values)
    groups = lax.axis_size("seq")
    shards = 2 * groups

    def body(*refs):
        own, small_ref = refs[:count], refs[count]
        full, small_out = refs[count + 1 : 2 * count + 1], refs[2 * count + 1]
        send, recv, local = refs[2 * count + 2 : 2 * count + 5]
        me, side, down, across = sides()
        total = Everywhere(small_ref, small_out, *refs[2 * count + 5 :])
        meet(*total.others(), *total.along())
        jobs = [SquareGather(own[i], full[i], send.at[i], recv.at[i]) for i in range(count)]
        total.start()
        keeps = []
        for i, job in enumerate(jobs):
            job.start()
            rows = own[i].shape[0]
            keep = pltpu.make_async_copy(
                own[i], full[i].at[pl.ds(pl.multiple_of(me * rows, rows), rows)], local.at[i]
            )
            keep.start()
            keeps.append(keep)
        total.relay()
        for job in jobs:
            job.relay()
        total.end()
        for job, keep in zip(jobs, keeps):
            job.near()
            job.far()
            job.finish()
            keep.wait()

    vmem = pl.BlockSpec(memory_space=pltpu.VMEM)
    dma = pltpu.SemaphoreType.DMA
    return pl.pallas_call(
        body,
        in_specs=[vmem] * (count + 1),
        out_specs=[pl.BlockSpec(memory_space=pl.ANY)] * count + [vmem],
        out_shape=[jax.ShapeDtypeStruct((4 * v.shape[0],) + v.shape[1:], v.dtype) for v in values]
        + [jax.ShapeDtypeStruct(small.shape, jnp.float32)],
        scratch_shapes=[
            dma((count, 6)),
            dma((count, 6)),
            dma((count,)),
            pltpu.VMEM((groups,) + small.shape, jnp.float32),
            pltpu.VMEM(small.shape, jnp.float32),
            pltpu.VMEM((shards,) + small.shape, jnp.float32),
            dma((groups + shards,)),
            dma((groups + shards,)),
        ],
        compiler_params=pltpu.CompilerParams(
            collective_id=collective_id, has_side_effects=True, vmem_limit_bytes=VMEM_LIMIT
        ),
        name="last_gather",
    )(*values, small)


def join_units(every_gate, every_up, down, out, part):
    groups, rows, units = every_gate.shape
    steps = 4
    tall = rows // steps

    def body(gate_in, up_in, down_in, out_in, gate_ref, up_ref, down_ref, out_ref):
        for every, to_ref in ((gate_in, gate_ref), (up_in, up_ref)):
            for group in range(groups):
                for block in range(units // part):
                    to = (block * groups + group) * part
                    to_ref[:, to : to + part] = every[group, :, block * part : (block + 1) * part].astype(
                        jnp.float32
                    )
        down_ref[...] = down_in[...].astype(jnp.float32)
        out_ref[...] = out_in[...].astype(jnp.float32)

    def flat(value):
        return pl.BlockSpec((value.shape[0] // steps, value.shape[1]), lambda i: (i, 0))

    wide = jax.ShapeDtypeStruct((rows, groups * units), jnp.float32)
    results = [wide, wide, *(jax.ShapeDtypeStruct(v.shape, jnp.float32) for v in (down, out))]
    return pl.pallas_call(
        body,
        grid=(steps,),
        in_specs=[pl.BlockSpec((groups, tall, units), lambda i: (0, i, 0))] * 2 + [flat(down), flat(out)],
        out_specs=[flat(value) for value in results],
        out_shape=results,
        name="join_units",
    )(every_gate, every_up, down, out)


def join_columns(every, gate, columns, starts, forget_at, heads):
    groups, rows, lanes = every.shape
    own = heads // groups
    steps = 4
    tall = rows // steps

    def body(every_ref, gate_ref, *outs):
        for group in range(groups):
            to = slice(group * columns, (group + 1) * columns)
            for start, out in zip(starts, outs):
                out[:, to] = every_ref[group, :, start : start + columns].astype(jnp.float32)
            outs[-2][:, to] = gate_ref[group].astype(jnp.float32)
            outs[-1][:, group * own : (group + 1) * own] = every_ref[
                group, :, forget_at : forget_at + own
            ].astype(jnp.float32)

    def flat(value):
        return pl.BlockSpec((tall, value.shape[1]), lambda i: (i, 0))

    wide = jax.ShapeDtypeStruct((rows, groups * columns), jnp.float32)
    results = [wide] * (len(starts) + 1) + [jax.ShapeDtypeStruct((rows, heads), jnp.float32)]
    return pl.pallas_call(
        body,
        grid=(steps,),
        in_specs=[pl.BlockSpec((groups, tall, v.shape[2]), lambda i: (0, i, 0)) for v in (every, gate)],
        out_specs=[flat(value) for value in results],
        out_shape=results,
        name="join_columns",
    )(every, gate)


def norm_rows(values, gain):
    scale = lax.rsqrt(jnp.mean(values * values, axis=-1, keepdims=True) + EPS)
    return scale, values * scale * gain


def whole_forward(inputs, gain, cotangent, weights, forget, bias, length, block, w_gate, w_up,
                  head_size, scale, collective_id):
    rows, depth = inputs.shape
    groups = 4
    slots = groups * rows
    chips = groups
    shards = 2 * chips
    mine = weights[0].shape[0]
    columns = depth // groups
    front = 3 * columns + PAIR
    pairs = columns // PAIR
    part = w_gate.shape[1] // (groups * shards)
    units = shards * part
    early = units + units // 2
    low = jnp.bfloat16

    def body(inputs_ref, gain_ref, cot_ref, q_ref, k_ref, v_ref, og_ref, forget_ref, bias_ref, length_ref, block_ref,
             gate_ref, up_ref,
             normed_hbm, cot_full, full_front_hbm, full_gate_hbm, full_out_hbm, full_ffn, joined_hbm, attended_hbm,
             offset, col, logit, gate_pre_hbm, gated_hbm, middle, own_up,
             own_normed, own_front, own_gate, own_ffn, own_out, parts_out, row, picks, cot_send, cot_recv, keep,
             x_send, x_recv, normed, full_front, full_gate, full_out, joined, attended, gate_pre, gated, store_sems,
             *scratch):
        store = Streams(store_sems)
        me, side, down, across = sides()
        line_chips, chip, core, forth, back, twin = line()
        front_line = LineGather(own_front, full_front, *scratch[0:3])
        gate_line = LineGather(own_gate, full_gate, *scratch[3:6])
        ffn_line = LineGather(own_ffn, full_ffn, *scratch[6:9])
        out_line = LineGather(own_out, parts_out, *scratch[9:12])
        exchange = PartExchange(parts_out, full_out, *scratch[12:15])
        job = SquareScatter([gated], [full_out_rows(full_out)], False, middle, *scratch[15:22])
        taken = []
        my_columns = pl.ds(pl.multiple_of(me * columns, columns), columns)
        for index, source in enumerate((q_ref, k_ref, v_ref)):
            taken.append((source.at[:, my_columns], own_front.at[:, pl.ds(index * columns, columns)]))
        taken.append((og_ref.at[:, my_columns], own_gate))
        tall = own_out.shape[0]
        taken.append((block_ref.at[pl.ds(pl.multiple_of(me * tall, tall), tall)], own_out))
        for index, source in enumerate((gate_ref, up_ref)):
            for number in range(shards):
                column = pl.ds(pl.multiple_of((number * groups + me) * part, part), part)
                to = index * units + number * part
                target = own_ffn.at[:, pl.ds(to, part)] if to < early else own_up.at[:, pl.ds(to - early, part)]
                taken.append((source.at[:, column], target))
        taken = [pltpu.make_async_copy(a, b, picks.at[i]) for i, (a, b) in enumerate(taken)]
        for copy in taken:
            copy.start()
        values = inputs_ref[...].astype(jnp.float32)
        own_normed[...] = norm_rows(values, gain_ref[...])[1].astype(low)
        own_front[:, 3 * columns :] = forget_ref[...]
        meet(*exchange.others, forth, back, twin)
        one = SquareGather(own_normed, normed, x_send, x_recv)
        two = SquareGather(cot_ref, cot_full, cot_send, cot_recv)
        one.start()
        for copy in taken:
            copy.wait()
        front_line.start()
        at_me = pl.ds(pl.multiple_of(me * rows, rows), rows)
        kept = pltpu.make_async_copy(cot_ref, cot_full.at[at_me], keep.at[0])
        kept.start()
        normed[at_me, :] = own_normed[...]
        one.relay()
        two.start()
        front_line.step(1)
        front_line.step(2)
        one.near()
        one.far()
        front_line.step(3)
        store.start(normed, normed_hbm)
        front_line.finish()
        store.start(full_front, full_front_hbm)
        one.finish()
        out_line.start()
        gate_line.start()
        two.relay()

        def store_joined(at_columns, value):
            joined[:, at_columns] = value.astype(low)

        block_product(normed, full_front, False, 256, store_joined)
        store.start(joined, joined_hbm)
        work = Forward(joined, bias_ref, length_ref, attended, offset, col, logit, row, head_size, scale)
        offset[...] = jnp.zeros_like(offset)
        out_line.step(1)
        gate_line.step(1)
        work.start()
        out_line.step(2)
        gate_line.step(2)

        def step(pair, carry):
            work.pair(pair)

            @pl.when(pair == 0)
            def _():
                out_line.step(3)
                gate_line.step(3)
                out_line.finish()
                exchange.start()
                ffn_line.start()

            return carry

        lax.fori_loop(0, pairs, step, 0)
        store.start(attended, attended_hbm)
        gate_line.finish()
        store.start(full_gate, full_gate_hbm)
        exchange.relay()

        def store_gate(at_columns, value):
            gate_pre[:, at_columns] = value

        block_product(normed, full_gate, False, PAIR, store_gate)
        gated[...] = (attended[...].astype(jnp.float32) * jax.nn.sigmoid(gate_pre[...])).astype(low)
        store.start(gate_pre, gate_pre_hbm)
        store.start(gated, gated_hbm)
        exchange.end()
        store.start(full_out, full_out_hbm)
        job.begin()
        job.relay()
        ffn_line.step(1)
        job.own()
        two.near()
        two.far()
        two.finish()
        kept.wait()
        ffn_line.step(2)
        job.end()
        middle[...] += inputs_ref[...].astype(jnp.float32)
        ffn_line.step(3)
        ffn_line.finish()
        store.end()

    def shape(size, kind=low):
        return jax.ShapeDtypeStruct(size, kind)

    vmem = pl.BlockSpec(memory_space=pltpu.VMEM)
    anywhere = pl.BlockSpec(memory_space=pl.ANY)
    dma = pltpu.SemaphoreType.DMA
    results = [
        shape((slots, depth)),
        shape((slots, depth)),
        shape((depth, front)),
        shape((depth, columns)),
        shape((2, 4, block.shape[0] // 4, depth)),
        shape((depth, early)),
        shape((slots, front)),
        *Forward.results(slots, pairs),
        shape((slots, columns), jnp.float32),
        shape((slots, columns)),
        shape((rows, depth), jnp.float32),
        shape((mine, 2 * units - early)),
    ]
    kept_here = [results[i] for i in (0, 2, 3, 4, 6, 7, 11, 12)]
    return pl.pallas_call(
        body,
        in_specs=[vmem] * 3 + [anywhere] * 4 + [vmem] * 3 + [anywhere] * 3,
        out_specs=[anywhere] * 8 + [vmem] * 3 + [anywhere] * 2 + [vmem] * 2,
        out_shape=results,
        scratch_shapes=[
            pltpu.VMEM((rows, depth), low),
            pltpu.VMEM((mine, front), low),
            pltpu.VMEM((mine, columns), low),
            pltpu.VMEM((mine, early), low),
            pltpu.VMEM((block.shape[0] // 4, depth), low),
            pltpu.VMEM((shards * block.shape[0] // 4, depth), low),
            pltpu.VMEM((Forward.some, slots), jnp.float32),
            dma((5 + 2 * shards,)),
            dma((6,)),
            dma((6,)),
            dma((1,)),
            dma((6,)),
            dma((6,)),
            *(pltpu.VMEM(value.shape, value.dtype) for value in kept_here),
            dma((len(kept_here),)),
        ]
        + 4 * LineGather.scratch(chips)
        + PartExchange.scratch()
        + SquareScatter.scratch(rows, depth),
        compiler_params=pltpu.CompilerParams(
            collective_id=collective_id, has_side_effects=True, vmem_limit_bytes=VMEM_LIMIT
        ),
        name="whole_forward",
    )(inputs, gain, cotangent, *weights, forget, bias, length, block, w_gate, w_up)


class full_out_rows:
    def __init__(self, ref):
        self.ref = ref
        self.shape = (ref.shape[0] * ref.shape[1] * ref.shape[2], ref.shape[3])

    def __getitem__(self, index):
        taken = self.ref[:, :, :, index[1]]
        return taken.reshape(self.shape[0], taken.shape[3])


def feed_forward(middle, gain, weights, own_up, own_down, cotangent, collective_id):
    rows, depth = middle.shape
    slots = 4 * rows
    units = 4 * own_down.shape[0] * 2
    early = weights.shape[1]
    chips = 4
    low = jnp.bfloat16

    def body(middle_ref, gain_ref, weights_hbm, up_ref, down_ref, cot_hbm,
             normed_hbm, hidden_hbm, full_up_hbm, full_down_hbm, grads_hbm, terms_hbm,
             own_normed, both, send, recv,
             weights_ref, cot_ref, normed, hidden, full_up, full_down, grads, terms, fetch_sems, store_sems, *scratch):
        fetch, store = Streams(fetch_sems), Streams(store_sems)
        weights_in = fetch.start(weights_hbm, weights_ref)
        cot_in = fetch.start(cot_hbm, cot_ref)
        me, side, down, across = sides()
        line_chips, chip, core, forth, back, twin = line()
        up_line = LineGather(up_ref, full_up, *scratch[:3])
        down_line = LineGather(down_ref, full_down, *scratch[3:])
        own_normed[...] = norm_rows(middle_ref[...], gain_ref[...])[1].astype(low)
        meet({"seq": side}, {"seq": down}, forth, back, twin)
        job = SquareGather(own_normed, normed, send, recv)
        job.start()
        up_line.start()

        def rows_of(rank):
            return pl.ds(pl.multiple_of(rank * rows, rows), rows)

        def multiply(rank):
            at = rows_of(rank)

            def store(columns, value):
                both[at, columns] = value

            block_product(normed.at[at], weights_ref, False, 512, store)

        normed[rows_of(me), :] = own_normed[...]
        weights_in.wait()
        multiply(me)
        up_line.step(1)
        job.relay()
        up_line.step(2)
        down_line.start()
        up_line.step(3)
        job.near()
        multiply(side)
        multiply(down)
        job.far()
        down_line.step(1)
        store.start(normed, normed_hbm)
        multiply(across)
        up_line.finish()
        store.start(full_up, full_up_hbm)

        def ahead(number, carry):
            at = rows_of(number)
            both[at, early:] = product(normed[at, :], full_up[...])
            gate, upward = both[at, :units], both[at, units:]
            hidden[at, :] = (gate * jax.nn.sigmoid(gate) * upward).astype(low)
            return carry

        lax.fori_loop(0, 4, ahead, 0)
        down_line.step(2)
        job.finish()
        store.start(hidden, hidden_hbm)
        cot_in.wait()
        transposed_product(hidden, cot_ref, terms)
        store.start(terms, terms_hbm)
        down_line.step(3)
        down_line.finish()
        store.start(full_down, full_down_hbm)

        def behind(number, carry):
            at = rows_of(number)
            grad_hidden = product_nt(cot_ref[at, :], full_down[...])
            gate, upward = both[at, :units], both[at, units:]
            sigma = jax.nn.sigmoid(gate)
            grads[at, :units] = (grad_hidden * upward * sigma * (1.0 + gate * (1.0 - sigma))).astype(low)
            grads[at, units:] = (grad_hidden * gate * sigma).astype(low)
            part(number).start()
            return carry

        def part(number):
            at = rows_of(number)
            return pltpu.make_async_copy(grads.at[at], grads_hbm.at[at], store_sems.at[5 + number])

        lax.fori_loop(0, 4, behind, 0)
        for number in range(4):
            part(number).wait()
        store.end()

    def shape(size, kind=low):
        return jax.ShapeDtypeStruct(size, kind)

    vmem = pl.BlockSpec(memory_space=pltpu.VMEM)
    anywhere = pl.BlockSpec(memory_space=pl.ANY)
    dma = pltpu.SemaphoreType.DMA
    results = [
        shape((slots, depth)),
        shape((slots, units)),
        shape((depth, own_up.shape[1])),
        shape((units, depth)),
        shape((slots, 2 * units)),
        shape((units, depth)),
    ]
    return pl.pallas_call(
        body,
        in_specs=[vmem, vmem, anywhere, vmem, vmem, anywhere],
        out_specs=[anywhere] * 6,
        out_shape=results,
        scratch_shapes=[
            pltpu.VMEM((rows, depth), low),
            pltpu.VMEM((slots, 2 * units), jnp.float32),
            dma((6,)),
            dma((6,)),
            *(pltpu.VMEM(value.shape, value.dtype) for value in (weights, cotangent, *results)),
            dma((2,)),
            dma((9,)),
        ]
        + 2 * LineGather.scratch(chips),
        compiler_params=pltpu.CompilerParams(
            collective_id=collective_id, has_side_effects=True, vmem_limit_bytes=VMEM_LIMIT
        ),
        name="feed_forward",
    )(middle, gain, weights, own_up, own_down, cotangent)


def feed_backward(grads, weights, up_weights, normed, terms_down, w_out, middle, gain, cotangent, attended, gate_pre,
                  collective_id):
    rows, depth = middle.shape
    slots = 4 * rows
    units = grads.shape[1] // 2
    early = weights.shape[1]
    columns = attended.shape[1]
    shards = 2 * lax.axis_size("seq")
    chips = shards // 2
    low = jnp.bfloat16

    def body(grads_hbm, weights_hbm, up_weights_hbm, normed_hbm, down_hbm, out_hbm, middle_hbm, gain_ref, cot_hbm,
             attended_hbm, pre_hbm,
             grad_middle_hbm, grad_gain, branch_hbm, d_attended, d_pre, terms_up_hbm, share_down, share_gate,
             own_branch, summed, terms_gate, send, recv,
             grads_ref, weights_ref, up_weights_ref, normed_ref, down_ref, out_ref, middle_ref, cot_ref,
             attended_ref, pre_ref, grad_middle, branch, terms_up, fetch_sems, store_sems, *scratch):
        fetch, store = Streams(fetch_sems), Streams(store_sems)
        first_in = [
            fetch.start(*both)
            for both in (
                (grads_hbm, grads_ref),
                (weights_hbm, weights_ref),
                (up_weights_hbm, up_weights_ref),
                (down_hbm, down_ref),
            )
        ]
        normed_in = fetch.start(normed_hbm, normed_ref)
        rest_in = [
            fetch.start(*both)
            for both in (
                (middle_hbm, middle_ref),
                (cot_hbm, cot_ref),
                (out_hbm, out_ref),
                (attended_hbm, attended_ref),
                (pre_hbm, pre_ref),
            )
        ]
        me, side, down, across = sides()
        line_chips, chip, core, forth, back, twin = line()
        meet({"seq": side}, {"seq": down}, forth, back, twin)
        first, second = grads_ref.at[:, pl.ds(0, units)], grads_ref.at[:, pl.ds(units, units)]
        job = SquareScatter(
            [grads_ref.at[:, pl.ds(0, early)], grads_ref.at[:, pl.ds(early, 2 * units - early)]],
            [weights_ref, up_weights_ref],
            True,
            summed,
            *scratch[:7],
        )
        run_down = LineScatter(down_ref, share_down, *scratch[7:12])
        run_gate = LineScatter(terms_gate, share_gate, *scratch[12:])
        every = SquareGather(own_branch, branch, send, recv)
        for copy in first_in:
            copy.wait()
        run_down.start()
        job.begin()
        run_down.slot(0)
        normed_in.wait()
        transposed_product(normed_ref, first, terms_gate)
        run_gate.start()
        job.relay()
        run_down.slot(1)
        job.own()
        transposed_product(normed_ref, second, terms_up)
        store.start(terms_up, terms_up_hbm)
        run_down.slot(2)
        run_gate.slot(0)
        for copy in rest_in:
            copy.wait()
        job.end()
        values, change = middle_ref[...], summed[...]
        scale = norm_rows(values, gain_ref[...])[0]
        grad_gain[...] = jnp.sum(change * values * scale, axis=0, keepdims=True)
        change = change * gain_ref[...]
        mean = jnp.mean(change * values, axis=-1, keepdims=True)
        total = cot_ref[...].astype(jnp.float32) + scale * change - values * (scale * scale * scale * mean)
        grad_middle[...] = total
        own_branch[...] = total.astype(low)
        every.start()
        store.start(grad_middle, grad_middle_hbm)

        def rows_of(rank):
            return pl.ds(pl.multiple_of(rank * rows, rows), rows)

        def multiply(rank):
            at = rows_of(rank)
            grad_gated = product_nt(branch[at, :], out_ref[...])
            sigma = jax.nn.sigmoid(pre_ref[at, :])
            d_attended[at, :] = (grad_gated * sigma).astype(low)
            d_pre[at, :] = (
                grad_gated * attended_ref[at, :].astype(jnp.float32) * sigma * (1.0 - sigma)
            ).astype(low)

        branch[rows_of(me), :] = own_branch[...]
        multiply(me)
        run_gate.slot(1)
        every.relay()
        run_gate.slot(2)
        every.near()
        multiply(side)
        multiply(down)
        run_down.end()
        every.far()
        store.start(branch, branch_hbm)
        multiply(across)
        every.finish()
        run_gate.end()
        store.end()

    def shape(size, kind=low):
        return jax.ShapeDtypeStruct(size, kind)

    vmem = pl.BlockSpec(memory_space=pltpu.VMEM)
    anywhere = pl.BlockSpec(memory_space=pl.ANY)
    dma = pltpu.SemaphoreType.DMA
    fetched = (grads, weights, up_weights, normed, terms_down, w_out, middle, cotangent, attended, gate_pre)
    return pl.pallas_call(
        body,
        in_specs=[anywhere] * 7 + [vmem] + [anywhere] * 3,
        out_specs=[anywhere, vmem, anywhere, vmem, vmem, anywhere, vmem, vmem],
        out_shape=[
            shape((rows, depth), jnp.float32),
            shape((1, depth), jnp.float32),
            shape((slots, depth)),
            shape((slots, columns)),
            shape((slots, columns)),
            shape((depth, units)),
            shape((terms_down.shape[0] // shards, depth)),
            shape((depth // shards, units)),
        ],
        scratch_shapes=[
            pltpu.VMEM((rows, depth), low),
            pltpu.VMEM((rows, depth), jnp.float32),
            pltpu.VMEM((depth, units), low),
            dma((6,)),
            dma((6,)),
            *(pltpu.VMEM(value.shape, value.dtype) for value in fetched),
            pltpu.VMEM((rows, depth), jnp.float32),
            pltpu.VMEM((slots, depth), low),
            pltpu.VMEM((depth, units), low),
            dma((len(fetched),)),
            dma((3,)),
        ]
        + SquareScatter.scratch(rows, depth)
        + LineScatter.scratch(chips, terms_down.shape[0] // shards, depth)
        + LineScatter.scratch(chips, depth // shards, units),
        compiler_params=pltpu.CompilerParams(
            collective_id=collective_id, has_side_effects=True, vmem_limit_bytes=VMEM_LIMIT
        ),
        name="feed_backward",
    )(grads, weights, up_weights, normed, terms_down, w_out, middle, gain, cotangent, attended, gate_pre)


class SquareScatter:
    @staticmethod
    def scratch(rows, width):
        half = rows // 2
        low = jnp.bfloat16
        return [
            pltpu.VMEM((rows, width), low),
            pltpu.VMEM((2, half, width), low),
            pltpu.VMEM((2, half, width), jnp.float32),
            pltpu.VMEM((6, half, width), low),
            pltpu.VMEM((2, half, width), low),
            pltpu.SemaphoreType.DMA((6,)),
            pltpu.SemaphoreType.DMA((6,)),
        ]

    def __init__(self, lefts, rights, transposed, out, far, near, kept, land, carry, send, recv):
        self.lefts, self.rights, self.transposed, self.out = lefts, rights, transposed, out
        self.far, self.near, self.kept, self.land, self.carry = far, near, kept, land, carry
        self.send, self.recv = send, recv
        self.rows, self.width = out.shape
        self.half = self.rows // 2
        self.tile = self.width // 3 if self.width % 384 == 0 else self.width

    def copy(self, index):
        me, side, down, across = sides()
        source = (
            self.far.at[pl.ds(0, self.half)],
            self.far.at[pl.ds(self.half, self.half)],
            self.near.at[0],
            self.near.at[1],
            self.carry.at[0],
            self.carry.at[1],
        )[index]
        return pltpu.make_async_remote_copy(
            src_ref=source,
            dst_ref=self.land.at[index],
            send_sem=self.send.at[index],
            recv_sem=self.recv.at[index],
            device_id={"seq": down if index in (0, 3, 5) else side},
            device_id_type=MESH,
        )

    def partial(self, rank, store):
        at = pl.ds(pl.multiple_of(rank * self.rows, self.rows), self.rows)

        def step(number, carried):
            columns = pl.ds(pl.multiple_of(number * self.tile, self.tile), self.tile)
            value = None
            for a, b in zip(self.lefts, self.rights):
                if self.transposed:
                    term = product_nt(a[at, :], b[columns, :])
                else:
                    term = product(a[at, :], b[:, columns])
                value = term if value is None else value + term
            store(columns, value)
            return carried

        lax.fori_loop(0, self.width // self.tile, step, 0)

    def begin(self):
        me, side, down, across = sides()
        half, far, near, kept = self.half, self.far, self.near, self.kept

        def store_far(columns, value):
            far[:, columns] = value.astype(far.dtype)

        def store_side(columns, value):
            kept[0, :, columns] = value[:half]
            near[0, :, columns] = value[half:].astype(near.dtype)

        def store_down(columns, value):
            near[1, :, columns] = value[:half].astype(near.dtype)
            kept[1, :, columns] = value[half:]

        self.partial(across, store_far)
        self.copy(0).start()
        self.copy(1).start()
        self.partial(side, store_side)
        self.copy(2).start()
        self.partial(down, store_down)
        self.copy(3).start()

    def relay(self):
        for index in (0, 1):
            self.copy(index).wait_recv()

            def add(at, index=index):
                total = self.kept[index, at, :] + self.land[index, at, :].astype(jnp.float32)
                self.carry[index, at, :] = total.astype(self.carry.dtype)

            by_rows(self.half, add)
            self.copy(4 + index).start()

    def own(self):
        out = self.out

        def store_own(columns, value):
            out[:, columns] = value

        self.partial(lax.axis_index("seq"), store_own)

    def end(self):
        for index in (2, 3, 4, 5):
            self.copy(index).wait_recv()
        land, half, out = self.land, self.half, self.out

        def add(at):
            out[at, :] += land[3, at, :].astype(jnp.float32) + land[4, at, :].astype(jnp.float32)

        def add_second(at):
            to = pl.ds(at.start + half, at.size)
            out[to, :] += land[2, at, :].astype(jnp.float32) + land[5, at, :].astype(jnp.float32)

        by_rows(half, add)
        by_rows(half, add_second)
        for index in range(6):
            self.copy(index).wait_send()


class LineScatter:
    @staticmethod
    def scratch(chips, rows, width):
        low = jnp.bfloat16
        dma = pltpu.SemaphoreType.DMA
        return [pltpu.VMEM((chips, rows, width), low)] * 3 + [dma((2, chips)), dma((3, chips))]

    def __init__(self, terms, out, twin_in, forth_in, back_in, send, recv):
        self.terms, self.out, self.twin_in = terms, out, twin_in
        self.forth_in, self.back_in, self.send, self.recv = forth_in, back_in, send, recv
        self.chips, self.chip, self.core, *self.devices = line()
        self.rows = twin_in.shape[1]

    def term(self, chip, core):
        return self.terms.at[pl.ds(pl.multiple_of((2 * chip + core) * self.rows, self.rows), self.rows)]

    def swap(self, chip):
        return pltpu.make_async_remote_copy(
            src_ref=self.term(chip, 1 - self.core),
            dst_ref=self.twin_in.at[chip],
            send_sem=self.send.at[0, chip],
            recv_sem=self.recv.at[0, chip],
            device_id=self.devices[2],
            device_id_type=MESH,
        )

    def hop(self, way, chip):
        return pltpu.make_async_remote_copy(
            src_ref=self.twin_in.at[chip],
            dst_ref=(self.forth_in, self.back_in)[way].at[chip],
            send_sem=self.send.at[1, chip],
            recv_sem=self.recv.at[1 + way, chip],
            device_id=self.devices[way],
            device_id_type=MESH,
        )

    def start(self):
        for chip in (self.chips - 1, 0, *range(1, self.chips - 1)):
            self.swap(chip).start()

    def add(self, chip, ways, out):
        def step(at):
            start = pl.multiple_of((2 * chip + self.core) * self.rows + at.start, at.size)
            total = self.terms[pl.ds(start, at.size), :].astype(jnp.float32)
            total = total + self.twin_in[chip, at, :].astype(jnp.float32)
            for way in ways:
                total = total + (self.forth_in, self.back_in)[way][chip, at, :].astype(jnp.float32)
            out[at, :] = total.astype(out.dtype)

        by_rows(self.rows, step)

    def pass_on(self, way, chip, first):
        self.swap(chip).wait_recv()
        if not first:
            self.hop(way, chip).wait_recv()
        self.add(chip, () if first else (way,), self.twin_in.at[chip])
        self.hop(way, chip).start()

    def slot(self, number):
        last = self.chips - 1
        for chip in range(self.chips):
            forth, back = number - (last - chip), last - (number - chip)
            if 0 <= forth < chip:

                @pl.when(self.chip == forth)
                def _():
                    self.pass_on(0, chip, forth == 0)

            if chip < back <= last:

                @pl.when(self.chip == back)
                def _():
                    self.pass_on(1, chip, back == last)

    def end(self):
        for chip in range(self.chips):

            @pl.when(self.chip == chip)
            def _():
                self.swap(chip).wait_recv()
                ways = [way for way, there in enumerate((chip > 0, chip < self.chips - 1)) if there]
                for way in ways:
                    self.hop(way, chip).wait_recv()
                self.add(chip, ways, self.out)

            self.swap(chip).wait_send()

            @pl.when(self.chip != chip)
            def _():
                self.hop(0, chip).wait_send()


def middle_backward(joined, d_out, offset, col, logit, hidden, w_down, gated, grad_branch, terms_up, shares,
                    normed, d_pre, middle, head_size, scale, collective_id):
    slots, lanes = joined.shape
    width = w_down.shape[1]
    tokens = slots // 4
    columns = gated.shape[1]
    shards = 2 * lax.axis_size("seq")
    chips = shards // 2
    rows_up = terms_up.shape[0] // shards
    fetched = (terms_up, gated, grad_branch, normed, d_pre, hidden, w_down, joined, d_out, middle)

    def body(*refs):
        sources, refs = refs[:10], refs[10:]
        (offset_ref, col_ref, logit_ref, *share_refs), refs = refs[:5], refs[5:]
        (grads, bias_grad, layer_output, collected, share_up, share_pre, *every_refs), refs = refs[:8], refs[8:]
        buffers, refs = refs[:10], refs[10:]
        terms, terms_pre, lowered, send, recv, keep, fetch_sems, *scratch = refs
        up_ref, gated_ref, branch_ref, normed_ref, pre_ref, hidden_ref, down_ref, joined_ref, d_out_ref = buffers[:9]
        fetch = Streams(fetch_sems)
        comes = [fetch.start(source, buffer) for source, buffer in zip(sources, buffers)]
        me, side, down, across = sides()
        line_chips, chip, core, forth, back, twin = line()
        meet({"seq": side}, {"seq": down}, forth, back, twin)
        work = Backward(
            joined_ref, d_out_ref, offset_ref, col_ref, logit_ref, grads, *scratch[:4], head_size, scale
        )
        job = SquareScatter([hidden_ref], [down_ref], False, lowered, *scratch[4:11])
        collect = LineScatter(terms, collected, *scratch[11:16])
        run = LineScatter(up_ref, share_up, *scratch[16:21])
        run_pre = LineScatter(terms_pre, share_pre, *scratch[21:])
        every = [SquareGather(share_refs[i], every_refs[i], send.at[i], recv.at[i]) for i in range(2)]
        every[0].start()
        comes[0].wait()
        run.start()
        kept = []
        for i in range(2):
            size = share_refs[i].shape[0]
            kept.append(
                pltpu.make_async_copy(
                    share_refs[i],
                    every_refs[i].at[pl.ds(pl.multiple_of(me * size, size), size)],
                    keep.at[i],
                )
            )
            kept[i].start()
        comes[1].wait()
        comes[2].wait()
        transposed_product(gated_ref, branch_ref, terms)
        collect.start()
        run.slot(0)
        comes[3].wait()
        comes[4].wait()
        transposed_product(normed_ref, pre_ref, terms_pre)
        run_pre.start()
        collect.slot(0)
        for copy in comes[5:]:
            copy.wait()
        job.begin()
        run_pre.slot(0)
        work.start()

        def step(pair, carry):
            work.pair(pair)

            @pl.when(pair == 0)
            def _():
                run.slot(1)
                job.relay()
                every[0].relay()
                every[1].start()
                collect.slot(1)
                run_pre.slot(1)

            @pl.when(pair == 1)
            def _():
                run.slot(2)
                collect.slot(2)
                run_pre.slot(2)
                every[1].relay()

            return carry

        lax.fori_loop(0, work.pairs, step, 0)
        job.own()
        work.end(bias_grad)
        job.end()
        layer_output[...] = (buffers[9][...] + lowered[...]).astype(layer_output.dtype)
        run.end()
        collect.end()
        run_pre.end()
        for gathering, copy in zip(every, kept):
            gathering.near()
            gathering.far()
            gathering.finish()
            copy.wait()

    vmem = pl.BlockSpec(memory_space=pltpu.VMEM)
    anywhere = pl.BlockSpec(memory_space=pl.ANY)
    low = jnp.bfloat16
    dma = pltpu.SemaphoreType.DMA
    return pl.pallas_call(
        body,
        in_specs=[anywhere] * 10 + [vmem] * 5,
        out_specs=[vmem] * 6 + [anywhere] * 2,
        out_shape=[
            jax.ShapeDtypeStruct((slots, lanes), low),
            jax.ShapeDtypeStruct((8, PAIR), jnp.float32),
            jax.ShapeDtypeStruct((tokens, width), low),
            jax.ShapeDtypeStruct((columns // shards, width), low),
            jax.ShapeDtypeStruct((rows_up, terms_up.shape[1]), low),
            jax.ShapeDtypeStruct((rows_up, columns), low),
            *(jax.ShapeDtypeStruct((4 * v.shape[0], v.shape[1]), low) for v in shares),
        ],
        scratch_shapes=[
            *(pltpu.VMEM(value.shape, value.dtype) for value in fetched),
            pltpu.VMEM((columns, width), low),
            pltpu.VMEM((width, columns), low),
            pltpu.VMEM((tokens, width), jnp.float32),
            dma((2, 6)),
            dma((2, 6)),
            dma((2,)),
            dma((10,)),
        ]
        + backward_scratch(slots)
        + SquareScatter.scratch(tokens, width)
        + LineScatter.scratch(chips, columns // shards, width)
        + LineScatter.scratch(chips, rows_up, terms_up.shape[1])
        + LineScatter.scratch(chips, rows_up, columns),
        compiler_params=pltpu.CompilerParams(
            collective_id=collective_id, has_side_effects=True, vmem_limit_bytes=VMEM_LIMIT
        ),
        name="middle_backward",
    )(*fetched, offset, col, logit, *shares)


def last_backward(grads, d_pre, normed, weights, gate_weights, collected, shares, inputs, gain, grad_middle,
                  collective_id):
    slots, depth = normed.shape
    front = grads.shape[1]
    tokens = slots // 4
    shards = 2 * lax.axis_size("seq")
    rows = depth // shards
    fetched = (normed, grads, d_pre, weights, gate_weights, inputs, grad_middle)

    def body(*refs):
        sources, refs = refs[:7], refs[7:]
        (collected_ref, gain_ref, *share_refs), refs = refs[:4], refs[4:]
        (grad_input, grad_gain, share, regrouped, *every_refs), refs = refs[:6], refs[6:]
        buffers, refs = refs[:7], refs[7:]
        terms, summed, send, recv, keep, fetch_sems, *scratch = refs
        normed_ref, grads_ref, pre_ref, weights_ref, gate_weights_ref, inputs_ref, middle_ref = buffers
        fetch = Streams(fetch_sems)
        comes = [fetch.start(source, buffer) for source, buffer in zip(sources, buffers)]
        me, side, down, across = sides()
        regroup = Regroup(collected_ref, regrouped, *scratch[12:])
        meet(*regroup.others, *regroup.along)
        job = SquareScatter([grads_ref, pre_ref], [weights_ref, gate_weights_ref], True, summed, *scratch[:7])
        run = LineScatter(terms, share, *scratch[7:12])
        regroup.start()
        every = [SquareGather(share_refs[i], every_refs[i], send.at[i], recv.at[i]) for i in range(2)]
        every[0].start()
        kept = []
        for i in range(2):
            size = share_refs[i].shape[0]
            kept.append(
                pltpu.make_async_copy(
                    share_refs[i],
                    every_refs[i].at[pl.ds(pl.multiple_of(me * size, size), size)],
                    keep.at[i],
                )
            )
            kept[i].start()
        comes[0].wait()
        comes[1].wait()
        transposed_product(normed_ref, grads_ref, terms)
        run.start()
        every[0].relay()
        regroup.relay()
        run.slot(0)
        for copy in comes[2:]:
            copy.wait()
        job.begin()
        every[1].start()
        job.relay()
        run.slot(1)
        job.own()
        every[1].relay()
        run.slot(2)
        job.end()
        values, change = inputs_ref[...].astype(jnp.float32), summed[...]
        scale = norm_rows(values, gain_ref[...])[0]
        grad_gain[...] = jnp.sum(change * values * scale, axis=0, keepdims=True)
        change = change * gain_ref[...]
        mean = jnp.mean(change * values, axis=-1, keepdims=True)
        grad_input[...] = middle_ref[...] + scale * change - values * (scale * scale * scale * mean)
        for gathering, copy in zip(every, kept):
            gathering.near()
            gathering.far()
            gathering.finish()
            copy.wait()
        regroup.end()
        run.end()

    vmem = pl.BlockSpec(memory_space=pltpu.VMEM)
    anywhere = pl.BlockSpec(memory_space=pl.ANY)
    low = jnp.bfloat16
    dma = pltpu.SemaphoreType.DMA
    return pl.pallas_call(
        body,
        in_specs=[anywhere] * 7 + [vmem] * 4,
        out_specs=[vmem] * 4 + [anywhere] * 2,
        out_shape=[
            jax.ShapeDtypeStruct((tokens, depth), jnp.float32),
            jax.ShapeDtypeStruct((1, depth), jnp.float32),
            jax.ShapeDtypeStruct((rows, front), low),
            jax.ShapeDtypeStruct((4,) + collected.shape, low),
            *(jax.ShapeDtypeStruct((4 * v.shape[0], v.shape[1]), low) for v in shares),
        ],
        scratch_shapes=[
            *(pltpu.VMEM(value.shape, value.dtype) for value in fetched),
            pltpu.VMEM((depth, front), low),
            pltpu.VMEM((tokens, depth), jnp.float32),
            dma((2, 6)),
            dma((2, 6)),
            dma((2,)),
            dma((7,)),
        ]
        + SquareScatter.scratch(tokens, depth)
        + LineScatter.scratch(shards // 2, rows, front)
        + Regroup.scratch(*collected.shape),
        compiler_params=pltpu.CompilerParams(
            collective_id=collective_id, has_side_effects=True, vmem_limit_bytes=VMEM_LIMIT
        ),
        name="last_backward",
    )(*fetched, collected, gain, *shares)


def gather(value, axis_name):
    return lax.all_gather(value, axis_name, axis=0, tiled=True)


def scatter(value, axis_name):
    return lax.psum_scatter(value, axis_name, scatter_dimension=0, tiled=True)


def on_device(
    layer_input,
    lengths,
    norm_attn,
    w_query,
    w_key,
    w_value,
    w_ogate,
    w_forget,
    forget_bias,
    w_out,
    norm_ffn,
    w_gate,
    w_up,
    w_down,
    output_grad,
):
    low = jnp.bfloat16
    tokens, width = layer_input.shape[1:]
    heads = forget_bias.shape[0]
    groups = lax.axis_size("seq")
    shards = lax.axis_size("wshard")
    fast = square(groups) and shards == 2 * groups
    local_heads = heads // groups
    head_size = width // heads
    columns = width // groups
    lanes = columns + -columns % PAIR
    front = 3 * lanes + PAIR
    slots = tokens * groups
    hidden_size = w_gate.shape[1]
    part = hidden_size // (groups * shards)
    units = shards * part
    scale = head_size ** (-0.5)
    length = lengths[0]
    seq_rank = lax.axis_index("seq")
    shard_rank = lax.axis_index("wshard")
    per_block = shards // groups
    positions = seq_rank * tokens + jnp.arange(tokens, dtype=jnp.int32)
    valid_slots = (positions < length)[:, None]
    inputs = layer_input[0].astype(jnp.float32)
    cotangent_low = jnp.where(valid_slots, output_grad[0], jnp.zeros((), low))
    cotangent = cotangent_low.astype(jnp.float32)

    def own_columns(weight, size):
        taken = lax.dynamic_slice_in_dim(weight, seq_rank * columns, columns, 1)
        return jnp.pad(taken, ((0, 0), (0, size - columns))) if size > columns else taken

    def own_units(weight):
        split = weight.reshape(weight.shape[0], shards, groups, part)
        mine = lax.dynamic_index_in_dim(split, seq_rank, 2, keepdims=False)
        return mine.reshape(weight.shape[0], units)

    own_forget = lax.dynamic_slice_in_dim(w_forget, seq_rank * local_heads, local_heads, 1)
    own_forget = jnp.pad(own_forget, ((0, 0), (0, PAIR - local_heads)))
    own_bias = lax.dynamic_slice_in_dim(forget_bias, seq_rank * local_heads, local_heads)
    own_bias = jnp.pad(own_bias, (0, PAIR - local_heads))[None]
    length_row = jnp.broadcast_to(lengths[:, None], (1, PAIR))
    mine_down = lax.dynamic_slice_in_dim(w_down, seq_rank * part, part, 0)
    if fast:
        (
            normed_attn, cotangent_all, full_front, full_ogate, full_out, full_ffn,
            joined, attended_low, offset, col, logit, gate_pre, gated, middle, mine_up,
        ) = whole_forward(
            layer_input[0], norm_attn[None], cotangent_low, (w_query, w_key, w_value, w_ogate), own_forget,
            own_bias, length_row, w_out, w_gate, w_up, head_size, scale, 0,
        )
        full_out = full_out.reshape(columns, width)
        normed_ffn, hidden, full_up, full_down, grad_gate_up, terms_down = feed_forward(
            middle, norm_ffn[None], full_ffn, mine_up, mine_down, cotangent_all, 1
        )
        (
            grad_middle, grad_norm_ffn, grad_branch, grad_attended, grad_gate_pre, terms_up, share_down, share_gate,
        ) = feed_backward(
            grad_gate_up, full_ffn, full_up, normed_ffn, terms_down, full_out, middle, norm_ffn[None],
            cotangent_low, attended_low, gate_pre, 2,
        )
        grad_norm_ffn = grad_norm_ffn[0]
        grads, bias_rows, layer_output, collected, share_up, share_ogate, grad_down, every_gate = middle_backward(
            joined, grad_attended, offset, col, logit, hidden, full_down, gated, grad_branch, terms_up,
            (share_down, share_gate), normed_attn, grad_gate_pre, middle, head_size, scale, 3,
        )
        grad_input, grad_norm_attn, share_attn, grad_out, every_ogate, every_up = last_backward(
            grads, grad_gate_pre, normed_attn, full_front, full_ogate, collected, (share_ogate, share_up),
            layer_input[0], norm_attn[None], grad_middle, 4,
        )
        grad_norm_attn = grad_norm_attn[0]
        grad_out = grad_out.reshape(columns // per_block, width)
    else:
        mine_front = jnp.concatenate(
            [*(own_columns(w, lanes) for w in (w_query, w_key, w_value)), own_forget], axis=1
        )
        full_front = gather(mine_front, "wshard")
        full_ogate = gather(own_columns(w_ogate, columns), "wshard")
        normed_attn = gather(rms_norm(inputs, norm_attn).astype(low), "seq")
        cotangent_all = gather(cotangent_low, "seq")
        full_out = lax.dynamic_slice_in_dim(gather(w_out, "wshard"), seq_rank * columns, columns, 0)
        full_ffn = gather(jnp.concatenate([own_units(w_gate), own_units(w_up)], axis=1), "wshard")
        joined = product(normed_attn, full_front).astype(low)
        gate_pre = product(normed_attn, full_ogate)
        attended_low, offset, col, logit = attention_fwd(joined, own_bias, length_row, head_size, scale)
        attended = attended_low[:, :columns].astype(jnp.float32)
        gated_full, pull_gate = jax.vjp(gate_product, attended, gate_pre)
        gated = gated_full.astype(low)
        middle = inputs + scatter(product(gated, full_out).astype(low), "seq").astype(jnp.float32)
        normed_ffn_own, pull_ffn_norm = jax.vjp(rms_norm, middle, norm_ffn)
        full_down = gather(mine_down, "wshard")
        normed_ffn = gather(normed_ffn_own.astype(low), "seq")
        gate_up = product(normed_ffn, full_ffn)
        hidden_full, pull_swiglu = jax.vjp(swiglu, gate_up[:, :units], gate_up[:, units:])
        hidden = hidden_full.astype(low)
        grad_hidden = product_nt(cotangent_all, full_down)
        grad_gate_full, grad_up_full = pull_swiglu(grad_hidden)
        grad_gate_up = jnp.concatenate([grad_gate_full.astype(low), grad_up_full.astype(low)], axis=1)
        share_down = scatter(product_tn(hidden, cotangent_all).astype(low), "wshard")
        share_ffn = scatter(product_tn(normed_ffn, grad_gate_up).astype(low), "wshard")
        grad_normed_ffn = scatter(product_nt(grad_gate_up, full_ffn).astype(low), "seq").astype(jnp.float32)
        grad_middle_part, grad_norm_ffn = pull_ffn_norm(grad_normed_ffn)
        grad_middle = cotangent + grad_middle_part
        grad_branch = gather(grad_middle.astype(low), "seq")
        grad_attended_full, grad_gate_pre_full = pull_gate(product_nt(grad_branch, full_out))
        grad_attended = grad_attended_full.astype(low)
        grad_gate_pre = grad_gate_pre_full.astype(low)
        if lanes > columns:
            grad_attended = jnp.pad(grad_attended, ((0, 0), (0, lanes - columns)))
        grads, bias_rows = attention_bwd(joined, grad_attended, offset, col, logit, head_size, scale)
        grad_projected = jnp.concatenate([grads, grad_gate_pre], axis=1)
        share_attn = scatter(product_tn(normed_attn, grad_projected).astype(low), "wshard")
        full_attn = jnp.concatenate([full_front, full_ogate], axis=1)
        grad_normed_attn = scatter(product_nt(grad_projected, full_attn).astype(low), "seq").astype(jnp.float32)
        lowered = scatter(product(hidden, full_down).astype(low), "seq").astype(jnp.float32)
        share_out = scatter(product_tn(gated, grad_branch).astype(low), "wshard")
        rows_out = columns // shards
        pieces_out = lax.all_gather(share_out, "seq", axis=0, tiled=False)
        takes = shards // per_block
        slots_out = jnp.where(
            (jnp.arange(per_block) == shard_rank // takes)[None, :, None, None],
            pieces_out[:, None],
            jnp.zeros((), low),
        ).reshape(shards, rows_out, width)
        moved = lax.all_to_all(slots_out, "wshard", split_axis=0, concat_axis=0, tiled=True)
        moved = moved.reshape(per_block, takes, rows_out, width)
        mine_out = lax.dynamic_index_in_dim(moved, shard_rank % per_block, 0, keepdims=False)
        grad_out = mine_out.reshape(columns // per_block, width).astype(jnp.float32)
        layer_output = (middle + lowered).astype(low)
        unused_normed, pull_attn_norm = jax.vjp(rms_norm, inputs, norm_attn)
        grad_input_part, grad_norm_attn = pull_attn_norm(grad_normed_attn)
        grad_input = grad_middle + grad_input_part
    grad_bias = lax.dynamic_update_slice_in_dim(
        jnp.zeros((heads,), jnp.float32), bias_rows[:local_heads, 0], seq_rank * local_heads, 0
    )

    rows = share_attn.shape[0]
    if fast:
        vector = jnp.concatenate([grad_norm_attn, grad_norm_ffn, grad_bias])
        vector = jnp.pad(vector, (0, -vector.shape[0] % 1024)).reshape(-1, 128)
        every_attn, vector = last_gather([share_attn], vector, 5)
        vector = vector.reshape(-1)
        small = vector[:width], vector[width : 2 * width], vector[2 * width : 2 * width + heads]
    else:
        every_attn, every_ffn, grad_down = [gather(v, "seq") for v in (share_attn, share_ffn, share_down)]
        small = lax.psum((grad_norm_attn, grad_norm_ffn, grad_bias), ("seq", "wshard"))
    every_attn = every_attn.reshape((groups,) + share_attn.shape)
    if fast:
        grad_w_gate, grad_w_up, grad_down, grad_out = join_units(
            every_gate.reshape((groups,) + share_gate.shape), every_up.reshape((groups,) + share_up.shape),
            grad_down, grad_out, part,
        )
        every_ogate = every_ogate.reshape((groups,) + share_ogate.shape)
        *weight_grads, grad_forget_w = join_columns(
            every_attn, every_ogate, columns, (0, lanes, 2 * lanes), 3 * lanes, heads
        )
    else:

        def join(first):
            taken = every_attn[:, :, first : first + columns]
            return taken.transpose(1, 0, 2).reshape(rows, width).astype(jnp.float32)

        def join_own_units(first):
            taken = every_ffn.reshape((groups,) + share_ffn.shape)[:, :, first * units : (first + 1) * units]
            taken = taken.reshape(groups, rows, shards, part).transpose(1, 2, 0, 3)
            return taken.reshape(rows, hidden_size).astype(jnp.float32)

        weight_grads = [join(first) for first in (0, lanes, 2 * lanes, front)]
        grad_w_gate, grad_w_up = join_own_units(0), join_own_units(1)
        grad_down = grad_down.astype(jnp.float32)
        grad_forget_w = every_attn[:, :, 3 * lanes : 3 * lanes + local_heads]
        grad_forget_w = grad_forget_w.transpose(1, 0, 2).reshape(rows, heads).astype(jnp.float32)
    return (
        layer_output[None],
        grad_input[None],
        small[0],
        *weight_grads,
        grad_forget_w,
        small[2],
        grad_out,
        small[1],
        grad_w_gate,
        grad_w_up,
        grad_down,
    )


def solution(mesh):
    return jax.shard_map(
        on_device,
        mesh=mesh,
        in_specs=(
            P("wshard", "seq", None),
            P("wshard"),
            P(),
            P("wshard", None),
            P("wshard", None),
            P("wshard", None),
            P("wshard", None),
            P("wshard", None),
            P(),
            P("wshard", None),
            P(),
            P("wshard", None),
            P("wshard", None),
            P("wshard", None),
            P("wshard", "seq", None),
        ),
        out_specs=(
            P("wshard", "seq", None),
            P("wshard", "seq", None),
            P(),
            P("wshard", None),
            P("wshard", None),
            P("wshard", None),
            P("wshard", None),
            P("wshard", None),
            P(),
            P("wshard", None),
            P(),
            P("wshard", None),
            P("wshard", None),
            P("wshard", None),
        ),
        check_vma=False,
    )
```

```python
import jax
import jax.numpy as jnp
from jax import lax
from jax.experimental import pallas as pl
from jax.experimental.pallas import tpu as pltpu
from jax.sharding import PartitionSpec as P

EPS = 1e-06
NEG_FILL = -1e30
PAIR = 128


def product(left, right):
    return jnp.dot(left, right, preferred_element_type=jnp.float32)


def product_tn(left, right):
    return lax.dot_general(
        left, right, (((0,), (0,)), ((), ())), preferred_element_type=jnp.float32
    )


def product_nt(left, right):
    return lax.dot_general(
        left, right, (((1,), (1,)), ((), ())), preferred_element_type=jnp.float32
    )


def rms_norm(values, gain):
    return values * lax.rsqrt(jnp.mean(values * values, axis=-1, keepdims=True) + EPS) * gain


def gate_product(attended, gate_pre):
    return attended * jax.nn.sigmoid(gate_pre)


def swiglu(gate, upward):
    return jax.nn.silu(gate) * upward


def low_triangle(size):
    rows = lax.broadcasted_iota(jnp.int32, (size, size), 0)
    return rows <= lax.broadcasted_iota(jnp.int32, (size, size), 1)


def exact(left, right):
    return jnp.dot(left, right, precision=lax.Precision.HIGHEST, preferred_element_type=jnp.float32)


class Forward:
    some = 8

    def __init__(self, joined, bias, length, attended, offset, col, logit, row, head_size, scale):
        self.joined, self.bias, self.length = joined, bias, length
        self.attended, self.offset, self.col, self.logit, self.row = attended, offset, col, logit, row
        self.head_size, self.scale = head_size, scale
        self.slots = joined.shape[0]
        self.pairs = (joined.shape[1] // PAIR - 1) // 3
        self.tile = min(256, self.slots)

    @staticmethod
    def results(slots, pairs):
        rows = jax.ShapeDtypeStruct((Forward.some, slots), jnp.float32)
        return [
            jax.ShapeDtypeStruct((slots, pairs * PAIR), jnp.bfloat16),
            rows,
            jax.ShapeDtypeStruct((slots, PAIR), jnp.float32),
            rows,
        ]

    def lanes(self, pair, part=0):
        return pl.ds(pl.multiple_of((part * self.pairs + pair) * PAIR, PAIR), PAIR)

    def start(self):
        slots, tile, some = self.slots, self.tile, self.some
        logits = self.joined[:, 3 * self.pairs * PAIR :].astype(jnp.float32) + self.bias[...]
        logit_rows = logits.T[:some]
        self.logit[...] = logit_rows
        logs = jnp.minimum(logit_rows, 0.0) - jnp.log1p(jnp.exp(-jnp.abs(logit_rows)))
        ones = low_triangle(tile).astype(jnp.float32)
        carry = jnp.zeros((some, 1), jnp.float32)
        for first in range(0, slots, tile):
            sums = exact(logs[:, first : first + tile], ones) + carry
            self.row[:, first : first + tile] = sums
            carry = sums[:, tile - 1 : tile]
        wide = jnp.concatenate([self.row[...], jnp.zeros((PAIR - some, slots), jnp.float32)], axis=0).T
        usable = lax.broadcasted_iota(jnp.int32, (slots, PAIR), 0) < self.length[...]
        self.col[...] = jnp.where(usable, wide, -NEG_FILL)

    def pair(self, pair):
        slots, tile, half = self.slots, self.tile, self.head_size
        key_all = self.joined[:, self.lanes(pair, 1)]
        value_t = self.joined[:, self.lanes(pair, 2)].T
        query_t = (self.joined[:, self.lanes(pair)].astype(jnp.float32) * self.scale).astype(jnp.bfloat16).T
        sub = lax.broadcasted_iota(jnp.int32, (PAIR, tile), 0)
        wide = lax.broadcasted_iota(jnp.int32, (slots, PAIR), 1)
        diag = low_triangle(tile)
        columns = [
            jnp.sum(jnp.where(wide == 2 * pair + a, self.col[...], 0.0), axis=1, keepdims=True) for a in range(2)
        ]
        for number in range(slots // tile):
            first, last = number * tile, (number + 1) * tile
            outs = []
            for a in range(2):
                mine = (sub >= a * half) & (sub < (a + 1) * half)
                at = pl.ds(2 * pair + a, 1)
                query = jnp.where(mine, query_t[:, first:last], jnp.zeros((), query_t.dtype))
                scores = product(key_all[:last], query)
                own_row = self.row[at, first:last]
                scores = scores + (own_row - columns[a][:last])
                tail = jnp.where(diag, scores[first:], NEG_FILL)
                scores = tail if number == 0 else jnp.concatenate([scores[:first], tail], axis=0)
                top = jnp.max(scores, axis=0, keepdims=True)
                weights = jnp.exp(scores - top)
                total = jnp.sum(weights, axis=0, keepdims=True)
                mixed = product(value_t[a * half : (a + 1) * half, :last], weights.astype(jnp.bfloat16))
                outs.append(mixed / total)
                self.offset[at, first:last] = own_row - (top + jnp.log(total))
            self.attended[first:last, self.lanes(pair)] = jnp.concatenate(outs, axis=0).T.astype(jnp.bfloat16)


def attention_fwd(joined, bias, length, head_size, scale):
    slots = joined.shape[0]
    pairs = (joined.shape[1] // PAIR - 1) // 3

    def body(joined_ref, bias_ref, length_ref, attended, offset, col, logit, row):
        work = Forward(joined_ref, bias_ref, length_ref, attended, offset, col, logit, row, head_size, scale)
        work.start()
        offset[...] = jnp.zeros_like(offset)

        def step(pair, carry):
            work.pair(pair)
            return carry

        lax.fori_loop(0, pairs, step, 0)

    vmem = pl.BlockSpec(memory_space=pltpu.VMEM)
    return pl.pallas_call(
        body,
        in_specs=[vmem] * 3,
        out_specs=[vmem] * 4,
        out_shape=Forward.results(slots, pairs),
        scratch_shapes=[pltpu.VMEM((Forward.some, slots), jnp.float32)],
        compiler_params=pltpu.CompilerParams(vmem_limit_bytes=56 << 20),
        cost_estimate=pl.CostEstimate(
            flops=4 * slots * slots * pairs * PAIR, bytes_accessed=8 * slots * pairs * PAIR, transcendentals=0
        ),
        name="attention_fwd",
    )(joined, bias, length)


def backward_scratch(slots):
    return [
        pltpu.VMEM((slots, PAIR), jnp.float32),
        pltpu.VMEM((slots, PAIR), jnp.float32),
        pltpu.VMEM((slots, PAIR), jnp.float32),
        pltpu.VMEM((8, slots), jnp.float32),
    ]


class Backward:
    def __init__(self, joined, d_out, offset, col, logit, grads, dk_acc, dv_acc, dcol, drow, head_size, scale):
        self.joined, self.d_out, self.offset, self.col = joined, d_out, offset, col
        self.logit, self.grads, self.dk_acc, self.dv_acc = logit, grads, dk_acc, dv_acc
        self.dcol, self.drow, self.head_size, self.scale = dcol, drow, head_size, scale
        self.slots = joined.shape[0]
        self.pairs = (joined.shape[1] // PAIR - 1) // 3
        self.tile = min(256, self.slots)

    def start(self):
        self.dcol[...] = jnp.zeros_like(self.dcol)
        self.drow[...] = jnp.zeros_like(self.drow)

    def lanes(self, pair, part=0):
        return pl.ds(pl.multiple_of((part * self.pairs + pair) * PAIR, PAIR), PAIR)

    def pair(self, pair):
        slots, tile, half = self.slots, self.tile, self.head_size
        dk_acc, dv_acc, dcol, drow = self.dk_acc, self.dv_acc, self.dcol, self.drow
        queries = (self.joined[:, self.lanes(pair)].astype(jnp.float32) * self.scale).astype(jnp.bfloat16)
        key_all = self.joined[:, self.lanes(pair, 1)]
        value_all = self.joined[:, self.lanes(pair, 2)]
        d_out = self.d_out[:, self.lanes(pair)]
        query_t, key_t, dout_t = queries.T, key_all.T, d_out.T
        sub = lax.broadcasted_iota(jnp.int32, (PAIR, tile), 0)
        lanes = lax.broadcasted_iota(jnp.int32, (tile, PAIR), 1)
        wide = lax.broadcasted_iota(jnp.int32, (slots, PAIR), 1)
        diag = low_triangle(tile)
        zero = jnp.zeros((), jnp.bfloat16)
        columns = [
            jnp.sum(jnp.where(wide == 2 * pair + a, self.col[...], 0.0), axis=1, keepdims=True) for a in range(2)
        ]
        dk_acc[...] = jnp.zeros_like(dk_acc)
        dv_acc[...] = jnp.zeros_like(dv_acc)
        for number in range(slots // tile):
            first, last = number * tile, (number + 1) * tile
            outs = []
            for a in range(2):
                mine = (sub >= a * half) & (sub < (a + 1) * half)
                own = (lanes >= a * half) & (lanes < (a + 1) * half)
                at = pl.ds(2 * pair + a, 1)
                scores = product(key_all[:last], jnp.where(mine, query_t[:, first:last], zero))
                scores = scores + (self.offset[at, first:last] - columns[a][:last])
                tail = jnp.where(diag, scores[first:], NEG_FILL)
                scores = tail if number == 0 else jnp.concatenate([scores[:first], tail], axis=0)
                probs = jnp.exp(scores)
                d_probs = product(value_all[:last], jnp.where(mine, dout_t[:, first:last], zero))
                dot = jnp.sum(d_probs * probs, axis=0, keepdims=True)
                d_full = probs * (d_probs - dot)
                d_scores = d_full.astype(jnp.bfloat16)
                drow[at, first:last] = jnp.sum(d_full, axis=0, keepdims=True)
                sums = jnp.sum(d_full, axis=1, keepdims=True)
                dcol[:last, :] += jnp.where(wide[:last] == 2 * pair + a, sums, 0.0)
                outs.append(product(key_t[a * half : (a + 1) * half, :last], d_scores) * self.scale)
                dk_acc[:last, :] += product(d_scores, jnp.where(own, queries[first:last, :], zero))
                dv_acc[:last, :] += product(
                    probs.astype(jnp.bfloat16), jnp.where(own, d_out[first:last, :], zero)
                )
            self.grads[first:last, self.lanes(pair)] = jnp.concatenate(outs, axis=0).T.astype(self.grads.dtype)
        self.grads[:, self.lanes(pair, 1)] = dk_acc[...].astype(self.grads.dtype)
        self.grads[:, self.lanes(pair, 2)] = dv_acc[...].astype(self.grads.dtype)

    def end(self, bias_grad):
        slots, tile, some = self.slots, self.tile, 8
        change = self.drow[...] - self.dcol[...].T[:some]
        rows = lax.broadcasted_iota(jnp.int32, (tile, tile), 0)
        ones = (rows >= lax.broadcasted_iota(jnp.int32, (tile, tile), 1)).astype(jnp.float32)
        carry = jnp.zeros((some, 1), jnp.float32)
        pieces = []
        for first in reversed(range(0, slots, tile)):
            sums = exact(change[:, first : first + tile], ones) + carry
            carry = sums[:, :1]
            pieces.insert(0, sums)
        grad = jnp.concatenate(pieces, axis=1) * jax.nn.sigmoid(-self.logit[...])
        heads = lax.broadcasted_iota(jnp.int32, (some, slots), 0)
        grad = jnp.where(heads < 2 * self.pairs, grad, 0.0)
        bias_grad[...] = jnp.broadcast_to(jnp.sum(grad, axis=1, keepdims=True), bias_grad.shape)
        wide = jnp.concatenate([grad, jnp.zeros((PAIR - some, slots), jnp.float32)], axis=0).T
        self.grads[:, 3 * self.pairs * PAIR : (3 * self.pairs + 1) * PAIR] = wide.astype(self.grads.dtype)


def attention_bwd(joined, d_out, offset, col, logit, head_size, scale):
    slots, width = joined.shape
    pairs = (width // PAIR - 1) // 3

    def body(joined_ref, d_out_ref, offset_ref, col_ref, logit_ref, grads, bias_grad, *scratch):
        work = Backward(
            joined_ref, d_out_ref, offset_ref, col_ref, logit_ref, grads, *scratch, head_size, scale
        )
        work.start()

        def step(pair, carry):
            work.pair(pair)
            return carry

        lax.fori_loop(0, pairs, step, 0)
        work.end(bias_grad)

    vmem = pl.BlockSpec(memory_space=pltpu.VMEM)
    return pl.pallas_call(
        body,
        in_specs=[vmem] * 5,
        out_specs=[vmem] * 2,
        out_shape=[
            jax.ShapeDtypeStruct((slots, width), jnp.bfloat16),
            jax.ShapeDtypeStruct((8, PAIR), jnp.float32),
        ],
        scratch_shapes=backward_scratch(slots),
        compiler_params=pltpu.CompilerParams(vmem_limit_bytes=56 << 20),
        cost_estimate=pl.CostEstimate(
            flops=10 * slots * slots * pairs * PAIR, bytes_accessed=14 * slots * pairs * PAIR, transcendentals=0
        ),
        name="attention_bwd",
    )(joined, d_out, offset, col, logit)


MESH = pl.DeviceIdType.MESH
VMEM_LIMIT = 62 << 20


def square(groups):
    return groups == 4


def sides():
    rank = lax.axis_index("seq")
    return rank, rank + 1 - 2 * lax.rem(rank, 2), lax.rem(rank + 2, 4), 3 - rank


def meet(*others):
    barrier = pltpu.get_barrier_semaphore()
    for other in others:
        pl.semaphore_signal(barrier, inc=1, device_id=other, device_id_type=MESH)
    pl.semaphore_wait(barrier, len(others))


def push(source, target, send, recv, device):
    copy = pltpu.make_async_remote_copy(
        src_ref=source,
        dst_ref=target,
        send_sem=send,
        recv_sem=recv,
        device_id=device,
        device_id_type=MESH,
    )
    copy.start()
    return copy


def by_rows(rows, work):
    def step(number, carry):
        work(pl.ds(pl.multiple_of(number * 16, 16), 16))
        return carry

    lax.fori_loop(0, rows // 16, step, 0)


class Streams:
    def __init__(self, sems):
        self.sems, self.made = sems, []

    def start(self, source, target):
        copy = pltpu.make_async_copy(source, target, self.sems.at[len(self.made)])
        self.made.append(copy)
        copy.start()
        return copy

    def end(self):
        for copy in self.made:
            copy.wait()


class SquareGather:
    def __init__(self, own, full, send, recv):
        self.own, self.full, self.send, self.recv = own, full, send, recv
        self.rows = own.shape[0]
        self.half = self.rows // 2

    def place(self, rank, part):
        return self.full.at[pl.ds(pl.multiple_of(rank * self.rows + part * self.half, self.half), self.half)]

    def copy(self, index):
        me, side, down, across = sides()
        mine = [self.own.at[pl.ds(part * self.half, self.half)] for part in (0, 1)]
        source, target, peer = (
            (mine[0], self.place(me, 0), side),
            (mine[1], self.place(me, 1), down),
            (mine[1], self.place(me, 1), side),
            (mine[0], self.place(me, 0), down),
            (self.place(side, 0), self.place(side, 0), down),
            (self.place(down, 1), self.place(down, 1), side),
        )[index]
        return pltpu.make_async_remote_copy(
            src_ref=source,
            dst_ref=target,
            send_sem=self.send.at[index],
            recv_sem=self.recv.at[index],
            device_id={"seq": peer},
            device_id_type=MESH,
        )

    def start(self):
        for index in range(4):
            self.copy(index).start()

    def relay(self):
        for index in (0, 1):
            self.copy(index).wait_recv()
            self.copy(4 + index).start()

    def near(self):
        self.copy(2).wait_recv()
        self.copy(3).wait_recv()

    def far(self):
        self.copy(4).wait_recv()
        self.copy(5).wait_recv()

    def finish(self):
        for index in range(6):
            self.copy(index).wait_send()


def block_product(left, right, transposed, tile, store):
    total = right.shape[0] if transposed else right.shape[1]

    def step(number, carry):
        columns = pl.ds(pl.multiple_of(number * tile, tile), tile)
        if transposed:
            store(columns, product_nt(left[...], right[columns, :]))
        else:
            store(columns, product(left[...], right[:, columns]))
        return carry

    lax.fori_loop(0, total // tile, step, 0)


def transposed_product(left, right, out):
    tall = 512 if out.shape[0] % 512 == 0 else 384
    wide = next(size for size in (512, 384, 640, 128) if out.shape[1] % size == 0)
    across = out.shape[1] // wide

    def step(number, carry):
        rows = pl.ds(pl.multiple_of((number // across) * tall, tall), tall)
        columns = pl.ds(pl.multiple_of(lax.rem(number, across) * wide, wide), wide)
        out[rows, columns] = product_tn(left[:, rows], right[:, columns]).astype(out.dtype)
        return carry

    lax.fori_loop(0, (out.shape[0] // tall) * across, step, 0)


def line():
    shards, place = lax.axis_size("wshard"), lax.axis_index("wshard")
    chips = shards // 2
    chip, core = place // 2, lax.rem(place, 2)
    forth = {"wshard": lax.rem(place + 2, shards)}
    back = {"wshard": lax.rem(place + shards - 2, shards)}
    twin = {"wshard": place + 1 - 2 * core}
    return chips, chip, core, forth, back, twin


class LineGather:
    @staticmethod
    def scratch(chips):
        dma = pltpu.SemaphoreType.DMA
        return [dma((3, chips)), dma((2 * chips,)), dma((1,))]

    def __init__(self, own, full, send, recv, local):
        self.own, self.full, self.local = own, full, local.at[0]
        self.sends = (send.at[0], send.at[1], send.at[2])
        self.recv = recv
        self.rows = own.shape[0]
        self.chips, self.chip, self.core, *self.devices = line()

    def place(self, chip, core):
        return self.full.at[pl.ds(pl.multiple_of((2 * chip + core) * self.rows, self.rows), self.rows)]

    def copy(self, way, chip, source=None):
        target = self.place(chip, self.core)
        return pltpu.make_async_remote_copy(
            src_ref=target if source is None else source,
            dst_ref=target,
            send_sem=self.sends[way].at[chip],
            recv_sem=self.recv.at[2 * chip + self.core],
            device_id=self.devices[way],
            device_id_type=MESH,
        )

    def wait_for(self, chip, core):
        target = self.place(chip, core)
        pltpu.make_async_remote_copy(
            src_ref=target,
            dst_ref=target,
            send_sem=self.sends[2].at[0],
            recv_sem=self.recv.at[2 * chip + core],
            device_id=self.devices[2],
            device_id_type=MESH,
        ).wait_recv()

    def start(self):
        @pl.when(self.chip < self.chips - 1)
        def _():
            self.copy(0, self.chip, self.own).start()

        @pl.when(self.chip > 0)
        def _():
            self.copy(1, self.chip, self.own).start()

        self.copy(2, self.chip, self.own).start()
        self.keep().start()

    def keep(self):
        return pltpu.make_async_copy(self.own, self.place(self.chip, self.core), self.local)

    def step(self, number):
        left, right = self.chip - number, self.chip + number

        @pl.when(left >= 0)
        def _():
            self.wait_for(left, self.core)

            @pl.when(self.chip < self.chips - 1)
            def _():
                self.copy(0, left).start()

            self.copy(2, left).start()

        @pl.when(right < self.chips)
        def _():
            self.wait_for(right, self.core)

            @pl.when(self.chip > 0)
            def _():
                self.copy(1, right).start()

            self.copy(2, right).start()

    def finish(self):
        for chip in range(self.chips):
            self.wait_for(chip, 1 - self.core)
            self.copy(2, chip).wait_send()

            @pl.when((chip <= self.chip) & (self.chip < self.chips - 1))
            def _():
                self.copy(0, chip).wait_send()

            @pl.when((chip >= self.chip) & (self.chip > 0))
            def _():
                self.copy(1, chip).wait_send()

        self.keep().wait()


class PartExchange:
    @staticmethod
    def scratch():
        dma = pltpu.SemaphoreType.DMA
        return [dma((4,)), dma((4,)), dma((1,))]

    def __init__(self, parts, out, send, recv, local):
        self.parts, self.out, self.send, self.recv, self.local = parts, out, send, recv, local
        self.rank = lax.axis_index("seq")
        self.core, self.twin = line()[2], line()[5]
        self.others = [{"seq": lax.rem(self.rank + k, 4)} for k in range(1, 4)]
        self.rows = out.shape[2]

    def part(self, rank):
        return self.parts.at[pl.ds(pl.multiple_of((2 * rank + self.core) * self.rows, self.rows), self.rows)]

    def copy(self, index):
        if index == 3:
            source = target = self.out.at[self.core]
        else:
            source = self.part(lax.rem(self.rank + index + 1, 4))
            target = self.out.at[self.core, self.rank]
        return pltpu.make_async_remote_copy(
            src_ref=source,
            dst_ref=target,
            send_sem=self.send.at[index],
            recv_sem=self.recv.at[index],
            device_id=self.twin if index == 3 else self.others[index],
            device_id_type=MESH,
        )

    def keep(self):
        return pltpu.make_async_copy(self.part(self.rank), self.out.at[self.core, self.rank], self.local.at[0])

    def start(self):
        for index in (1, 0, 2):
            self.copy(index).start()
        self.keep().start()

    def relay(self):
        for index in range(3):
            self.copy(index).wait()
        self.keep().wait()
        self.copy(3).start()

    def end(self):
        self.copy(3).wait()


class Regroup:
    @staticmethod
    def scratch(rows, width):
        dma = pltpu.SemaphoreType.DMA
        return [pltpu.VMEM((4, rows, width), jnp.bfloat16), dma((7,)), dma((7,))]

    def __init__(self, piece, out, fours, send, recv):
        self.piece, self.out, self.fours, self.send, self.recv = piece, out, fours, send, recv
        self.rank, self.place = lax.axis_index("seq"), lax.axis_index("wshard")
        self.number = lax.rem(self.place, 4)
        self.others = [{"seq": lax.rem(self.rank + k, 4)} for k in range(1, 4)]
        self.along = [{"wshard": lax.rem(self.place + k, 8)} for k in range(1, 8)]

    def near(self, index):
        return pltpu.make_async_remote_copy(
            src_ref=self.piece,
            dst_ref=self.fours.at[self.rank],
            send_sem=self.send.at[index],
            recv_sem=self.recv.at[index],
            device_id=self.others[index],
            device_id_type=MESH,
        )

    def owner(self, rank):
        return 2 * rank + self.place // 4

    def far(self, rank, number):
        return pltpu.make_async_remote_copy(
            src_ref=self.fours.at[rank],
            dst_ref=self.out.at[number],
            send_sem=self.send.at[3 + rank],
            recv_sem=self.recv.at[3 + number],
            device_id={"wshard": self.owner(rank)},
            device_id_type=MESH,
        )

    def start(self):
        for index in range(3):
            self.near(index).start()
        self.fours[self.rank] = self.piece[...]

    def relay(self):
        for index in range(3):
            self.near(index).wait()
        for rank in range(4):

            @pl.when(self.owner(rank) != self.place)
            def _():
                self.far(rank, self.number).start()

            @pl.when(self.owner(rank) == self.place)
            def _():
                self.out[self.number] = self.fours[rank]

    def end(self):
        for rank in range(4):

            @pl.when(self.owner(rank) != self.place)
            def _():
                self.far(rank, self.number).wait_send()

        for number in range(4):

            @pl.when(4 * lax.rem(self.place, 2) + number != self.place)
            def _():
                self.far(0, number).wait_recv()


class Everywhere:
    def __init__(self, values, out, ranks, total, places, send, recv):
        self.values, self.out, self.ranks, self.total, self.places = values, out, ranks, total, places
        self.send, self.recv = send, recv
        self.groups, self.shards = ranks.shape[0], places.shape[0]
        self.rank, self.place = lax.axis_index("seq"), lax.axis_index("wshard")

    def others(self):
        return [{"seq": lax.rem(self.rank + k, self.groups)} for k in range(1, self.groups)]

    def along(self):
        return [{"wshard": lax.rem(self.place + k, self.shards)} for k in range(1, self.shards)]

    def start(self):
        self.first = [
            push(self.values, self.ranks.at[self.rank], self.send.at[k], self.recv.at[k], other)
            for k, other in enumerate(self.others())
        ]
        self.ranks[self.rank] = self.values[...]

    def relay(self):
        for copy in self.first:
            copy.wait()
        ranks, groups = self.ranks, self.groups
        self.total[...] = (ranks[0] + ranks[1]) + (ranks[2] + ranks[3])
        self.second = [
            push(self.total, self.places.at[self.place], self.send.at[groups + k], self.recv.at[groups + k], other)
            for k, other in enumerate(self.along())
        ]
        self.places[self.place] = self.total[...]

    def end(self):
        for copy in self.second:
            copy.wait()
        sums = [self.places[k] + self.places[k + 1] for k in range(0, self.shards, 2)]
        self.out[...] = (sums[0] + sums[1]) + (sums[2] + sums[3])


def last_gather(values, small, collective_id):
    count = len(values)
    groups = lax.axis_size("seq")
    shards = 2 * groups

    def body(*refs):
        own, small_ref = refs[:count], refs[count]
        full, small_out = refs[count + 1 : 2 * count + 1], refs[2 * count + 1]
        send, recv, local = refs[2 * count + 2 : 2 * count + 5]
        me, side, down, across = sides()
        total = Everywhere(small_ref, small_out, *refs[2 * count + 5 :])
        meet(*total.others(), *total.along())
        jobs = [SquareGather(own[i], full[i], send.at[i], recv.at[i]) for i in range(count)]
        total.start()
        keeps = []
        for i, job in enumerate(jobs):
            job.start()
            rows = own[i].shape[0]
            keep = pltpu.make_async_copy(
                own[i], full[i].at[pl.ds(pl.multiple_of(me * rows, rows), rows)], local.at[i]
            )
            keep.start()
            keeps.append(keep)
        total.relay()
        for job in jobs:
            job.relay()
        total.end()
        for job, keep in zip(jobs, keeps):
            job.near()
            job.far()
            job.finish()
            keep.wait()

    vmem = pl.BlockSpec(memory_space=pltpu.VMEM)
    dma = pltpu.SemaphoreType.DMA
    return pl.pallas_call(
        body,
        in_specs=[vmem] * (count + 1),
        out_specs=[pl.BlockSpec(memory_space=pl.ANY)] * count + [vmem],
        out_shape=[jax.ShapeDtypeStruct((4 * v.shape[0],) + v.shape[1:], v.dtype) for v in values]
        + [jax.ShapeDtypeStruct(small.shape, jnp.float32)],
        scratch_shapes=[
            dma((count, 6)),
            dma((count, 6)),
            dma((count,)),
            pltpu.VMEM((groups,) + small.shape, jnp.float32),
            pltpu.VMEM(small.shape, jnp.float32),
            pltpu.VMEM((shards,) + small.shape, jnp.float32),
            dma((groups + shards,)),
            dma((groups + shards,)),
        ],
        compiler_params=pltpu.CompilerParams(
            collective_id=collective_id, has_side_effects=True, vmem_limit_bytes=VMEM_LIMIT
        ),
        name="last_gather",
    )(*values, small)


def join_shares(every, gate, every_gate, every_up, down, out, columns, starts, forget_at, heads, part):
    groups, rows, lanes = every.shape
    units = every_gate.shape[2]
    own = heads // groups
    steps = 4
    tall = rows // steps

    def body(every_ref, gate_ref, wide_gate, wide_up, down_in, out_in, *outs):
        firsts = len(starts)
        for group in range(groups):
            to = slice(group * columns, (group + 1) * columns)
            for start, result in zip(starts, outs):
                result[:, to] = every_ref[group, :, start : start + columns].astype(jnp.float32)
            outs[firsts][:, to] = gate_ref[group].astype(jnp.float32)
            outs[firsts + 1][:, group * own : (group + 1) * own] = every_ref[
                group, :, forget_at : forget_at + own
            ].astype(jnp.float32)
            for source, result in ((wide_gate, outs[firsts + 2]), (wide_up, outs[firsts + 3])):
                for block in range(units // part):
                    at = (block * groups + group) * part
                    result[:, at : at + part] = source[group, :, block * part : (block + 1) * part].astype(
                        jnp.float32
                    )
        outs[firsts + 4][...] = down_in[...].astype(jnp.float32)
        outs[firsts + 5][...] = out_in[...].astype(jnp.float32)

    def flat(value):
        return pl.BlockSpec((value.shape[0] // steps, value.shape[1]), lambda i: (i, 0))

    def ranks(value):
        return pl.BlockSpec((groups, tall, value.shape[2]), lambda i: (0, i, 0))

    def shape(size):
        return jax.ShapeDtypeStruct(size, jnp.float32)

    results = [shape((rows, groups * columns))] * (len(starts) + 1) + [
        shape((rows, heads)),
        shape((rows, groups * units)),
        shape((rows, groups * units)),
        shape(down.shape),
        shape(out.shape),
    ]
    return pl.pallas_call(
        body,
        grid=(steps,),
        in_specs=[ranks(v) for v in (every, gate, every_gate, every_up)] + [flat(down), flat(out)],
        out_specs=[flat(value) for value in results],
        out_shape=results,
        compiler_params=pltpu.CompilerParams(vmem_limit_bytes=56 << 20),
        name="join_shares",
    )(every, gate, every_gate, every_up, down, out)


def norm_rows(values, gain):
    scale = lax.rsqrt(jnp.mean(values * values, axis=-1, keepdims=True) + EPS)
    return scale, values * scale * gain


def whole_forward(inputs, gain, cotangent, weights, forget, bias, length, block, w_gate, w_up,
                  head_size, scale, collective_id):
    rows, depth = inputs.shape
    groups = 4
    slots = groups * rows
    chips = groups
    shards = 2 * chips
    mine = weights[0].shape[0]
    columns = depth // groups
    front = 3 * columns + PAIR
    pairs = columns // PAIR
    part = w_gate.shape[1] // (groups * shards)
    units = shards * part
    early = units + units // 2
    low = jnp.bfloat16

    def body(inputs_ref, gain_ref, cot_ref, q_ref, k_ref, v_ref, og_ref, forget_ref, bias_ref, length_ref, block_ref,
             gate_ref, up_ref,
             normed_hbm, cot_full, full_front_hbm, full_gate_hbm, full_out_hbm, full_ffn, joined_hbm, attended_hbm,
             offset, col, logit, gate_pre_hbm, gated_hbm, middle, own_up,
             own_normed, own_front, own_gate, own_ffn, own_out, parts_out, own_cot, row, picks, cot_send, cot_recv, keep,
             x_send, x_recv, normed, full_front, full_gate, full_out, joined, attended, gate_pre, gated, store_sems,
             *scratch):
        store = Streams(store_sems)
        me, side, down, across = sides()
        line_chips, chip, core, forth, back, twin = line()
        halves = (pl.ds(0, 2 * columns), pl.ds(2 * columns, front - 2 * columns))
        first_line = LineGather(own_front.at[:, halves[0]], full_front.at[:, halves[0]], *scratch[0:3])
        second_line = LineGather(own_front.at[:, halves[1]], full_front.at[:, halves[1]], *scratch[22:25])
        gate_line = LineGather(own_gate, full_gate, *scratch[3:6])
        ffn_line = LineGather(own_ffn, full_ffn, *scratch[6:9])
        out_line = LineGather(own_out, parts_out, *scratch[9:12])
        exchange = PartExchange(parts_out, full_out, *scratch[12:15])
        job = SquareScatter([gated], [full_out_rows(full_out)], False, middle, *scratch[15:22])
        taken = []
        my_columns = pl.ds(pl.multiple_of(me * columns, columns), columns)
        for index, source in enumerate((q_ref, k_ref, v_ref)):
            taken.append((source.at[:, my_columns], own_front.at[:, pl.ds(index * columns, columns)]))
        taken.append((og_ref.at[:, my_columns], own_gate))
        tall = own_out.shape[0]
        taken.append((block_ref.at[pl.ds(pl.multiple_of(me * tall, tall), tall)], own_out))
        for index, source in enumerate((gate_ref, up_ref)):
            for number in range(shards):
                column = pl.ds(pl.multiple_of((number * groups + me) * part, part), part)
                to = index * units + number * part
                target = own_ffn.at[:, pl.ds(to, part)] if to < early else own_up.at[:, pl.ds(to - early, part)]
                taken.append((source.at[:, column], target))
        taken = [pltpu.make_async_copy(a, b, picks.at[i]) for i, (a, b) in enumerate(taken)]
        for copy in taken:
            copy.start()
        values = inputs_ref[...].astype(jnp.float32)
        own_normed[...] = norm_rows(values, gain_ref[...])[1].astype(low)
        own_front[:, 3 * columns :] = forget_ref[...]
        positions = me * rows + lax.broadcasted_iota(jnp.int32, (rows, depth), 0)
        own_cot[...] = jnp.where(positions < length_ref[:, :1], cot_ref[...], jnp.zeros((), low))
        meet(*exchange.others, forth, back, twin)
        one = SquareGather(own_normed, normed, x_send, x_recv)
        two = SquareGather(own_cot, cot_full, cot_send, cot_recv)
        one.start()
        for copy in taken:
            copy.wait()
        first_line.start()
        second_line.start()
        at_me = pl.ds(pl.multiple_of(me * rows, rows), rows)
        kept = pltpu.make_async_copy(own_cot, cot_full.at[at_me], keep.at[0])
        kept.start()
        normed[at_me, :] = own_normed[...]
        one.relay()
        two.start()
        first_line.step(1)
        second_line.step(1)
        first_line.step(2)
        second_line.step(2)
        one.near()
        one.far()
        first_line.step(3)
        second_line.step(3)
        store.start(normed, normed_hbm)
        out_line.start()
        gate_line.start()
        two.relay()
        first_line.finish()

        def product_of(columns_of_front):
            view = joined.at[:, columns_of_front]

            def store_joined(at_columns, value):
                view[:, at_columns] = value.astype(low)

            block_product(normed, full_front.at[:, columns_of_front], False, 256, store_joined)

        product_of(halves[0])
        second_line.finish()
        product_of(halves[1])
        store.start(full_front, full_front_hbm)
        one.finish()
        store.start(joined, joined_hbm)
        work = Forward(joined, bias_ref, length_ref, attended, offset, col, logit, row, head_size, scale)
        offset[...] = jnp.zeros_like(offset)
        out_line.step(1)
        gate_line.step(1)
        work.start()

        def step(pair, carry):
            work.pair(pair)

            @pl.when(pair == 0)
            def _():
                out_line.step(2)
                gate_line.step(2)

            @pl.when(pair == 1)
            def _():
                out_line.step(3)
                out_line.finish()
                exchange.start()
                gate_line.step(3)
                ffn_line.start()

            return carry

        lax.fori_loop(0, pairs, step, 0)
        store.start(attended, attended_hbm)
        gate_line.finish()
        store.start(full_gate, full_gate_hbm)

        def store_gate(at_columns, value):
            gate_pre[:, at_columns] = value

        block_product(normed, full_gate, False, PAIR, store_gate)
        gated[...] = (attended[...].astype(jnp.float32) * jax.nn.sigmoid(gate_pre[...])).astype(low)
        exchange.relay()
        store.start(gate_pre, gate_pre_hbm)
        store.start(gated, gated_hbm)
        exchange.end()
        store.start(full_out, full_out_hbm)
        job.begin()
        ffn_line.step(1)
        job.relay()
        job.own()
        two.near()
        two.far()
        two.finish()
        kept.wait()
        ffn_line.step(2)
        job.end()
        middle[...] += inputs_ref[...].astype(jnp.float32)
        ffn_line.step(3)
        ffn_line.finish()
        store.end()

    def shape(size, kind=low):
        return jax.ShapeDtypeStruct(size, kind)

    vmem = pl.BlockSpec(memory_space=pltpu.VMEM)
    anywhere = pl.BlockSpec(memory_space=pl.ANY)
    dma = pltpu.SemaphoreType.DMA
    results = [
        shape((slots, depth)),
        shape((slots, depth)),
        shape((depth, front)),
        shape((depth, columns)),
        shape((2, 4, block.shape[0] // 4, depth)),
        shape((depth, early)),
        shape((slots, front)),
        *Forward.results(slots, pairs),
        shape((slots, columns), jnp.float32),
        shape((slots, columns)),
        shape((rows, depth), jnp.float32),
        shape((mine, 2 * units - early)),
    ]
    kept_here = [results[i] for i in (0, 2, 3, 4, 6, 7, 11, 12)]
    return pl.pallas_call(
        body,
        in_specs=[vmem] * 3 + [anywhere] * 4 + [vmem] * 3 + [anywhere] * 3,
        out_specs=[anywhere] * 8 + [vmem] * 3 + [anywhere] * 2 + [vmem] * 2,
        out_shape=results,
        scratch_shapes=[
            pltpu.VMEM((rows, depth), low),
            pltpu.VMEM((mine, front), low),
            pltpu.VMEM((mine, columns), low),
            pltpu.VMEM((mine, early), low),
            pltpu.VMEM((block.shape[0] // 4, depth), low),
            pltpu.VMEM((shards * block.shape[0] // 4, depth), low),
            pltpu.VMEM((rows, depth), low),
            pltpu.VMEM((Forward.some, slots), jnp.float32),
            dma((5 + 2 * shards,)),
            dma((6,)),
            dma((6,)),
            dma((1,)),
            dma((6,)),
            dma((6,)),
            *(pltpu.VMEM(value.shape, value.dtype) for value in kept_here),
            dma((len(kept_here),)),
        ]
        + 4 * LineGather.scratch(chips)
        + PartExchange.scratch()
        + SquareScatter.scratch(rows, depth)
        + LineGather.scratch(chips),
        compiler_params=pltpu.CompilerParams(
            collective_id=collective_id, has_side_effects=True, vmem_limit_bytes=VMEM_LIMIT
        ),
        name="whole_forward",
    )(inputs, gain, cotangent, *weights, forget, bias, length, block, w_gate, w_up)


class full_out_rows:
    def __init__(self, ref):
        self.ref = ref
        self.shape = (ref.shape[0] * ref.shape[1] * ref.shape[2], ref.shape[3])

    def __getitem__(self, index):
        taken = self.ref[:, :, :, index[1]]
        return taken.reshape(self.shape[0], taken.shape[3])


def feed_forward(middle, gain, weights, own_up, own_down, cotangent, collective_id):
    rows, depth = middle.shape
    slots = 4 * rows
    units = 4 * own_down.shape[0] * 2
    early = weights.shape[1]
    chips = 4
    low = jnp.bfloat16

    def body(middle_ref, gain_ref, weights_hbm, up_ref, down_ref, cot_hbm,
             normed_hbm, hidden_hbm, full_up_hbm, full_down_hbm, grads_hbm, terms_hbm,
             own_normed, both, send, recv,
             weights_ref, cot_ref, normed, hidden, full_up, full_down, grads, terms, fetch_sems, store_sems, *scratch):
        fetch, store = Streams(fetch_sems), Streams(store_sems)
        weights_in = fetch.start(weights_hbm, weights_ref)
        cot_in = fetch.start(cot_hbm, cot_ref)
        me, side, down, across = sides()
        line_chips, chip, core, forth, back, twin = line()
        up_line = LineGather(up_ref, full_up, *scratch[:3])
        down_line = LineGather(down_ref, full_down, *scratch[3:])
        own_normed[...] = norm_rows(middle_ref[...], gain_ref[...])[1].astype(low)
        meet({"seq": side}, {"seq": down}, forth, back, twin)
        job = SquareGather(own_normed, normed, send, recv)
        job.start()
        up_line.start()

        def rows_of(rank):
            return pl.ds(pl.multiple_of(rank * rows, rows), rows)

        def multiply(rank):
            at = rows_of(rank)

            def store(columns, value):
                both[at, columns] = value

            block_product(normed.at[at], weights_ref, False, 512, store)

        normed[rows_of(me), :] = own_normed[...]
        weights_in.wait()
        multiply(me)
        up_line.step(1)
        job.relay()
        up_line.step(2)
        down_line.start()
        up_line.step(3)
        job.near()
        multiply(side)
        multiply(down)
        job.far()
        down_line.step(1)
        store.start(normed, normed_hbm)
        multiply(across)
        up_line.finish()
        store.start(full_up, full_up_hbm)

        def ahead(number, carry):
            at = rows_of(number)
            both[at, early:] = product(normed[at, :], full_up[...])
            gate, upward = both[at, :units], both[at, units:]
            hidden[at, :] = (gate * jax.nn.sigmoid(gate) * upward).astype(low)
            return carry

        lax.fori_loop(0, 4, ahead, 0)
        down_line.step(2)
        job.finish()
        store.start(hidden, hidden_hbm)
        cot_in.wait()
        transposed_product(hidden, cot_ref, terms)
        store.start(terms, terms_hbm)
        down_line.step(3)
        down_line.finish()
        store.start(full_down, full_down_hbm)

        def behind(number, carry):
            at = rows_of(number)
            grad_hidden = product_nt(cot_ref[at, :], full_down[...])
            gate, upward = both[at, :units], both[at, units:]
            sigma = jax.nn.sigmoid(gate)
            grads[at, :units] = (grad_hidden * upward * sigma * (1.0 + gate * (1.0 - sigma))).astype(low)
            grads[at, units:] = (grad_hidden * gate * sigma).astype(low)
            part(number).start()
            return carry

        def part(number):
            at = rows_of(number)
            return pltpu.make_async_copy(grads.at[at], grads_hbm.at[at], store_sems.at[5 + number])

        lax.fori_loop(0, 4, behind, 0)
        for number in range(4):
            part(number).wait()
        store.end()

    def shape(size, kind=low):
        return jax.ShapeDtypeStruct(size, kind)

    vmem = pl.BlockSpec(memory_space=pltpu.VMEM)
    anywhere = pl.BlockSpec(memory_space=pl.ANY)
    dma = pltpu.SemaphoreType.DMA
    results = [
        shape((slots, depth)),
        shape((slots, units)),
        shape((depth, own_up.shape[1])),
        shape((units, depth)),
        shape((slots, 2 * units)),
        shape((units, depth)),
    ]
    return pl.pallas_call(
        body,
        in_specs=[vmem, vmem, anywhere, vmem, vmem, anywhere],
        out_specs=[anywhere] * 6,
        out_shape=results,
        scratch_shapes=[
            pltpu.VMEM((rows, depth), low),
            pltpu.VMEM((slots, 2 * units), jnp.float32),
            dma((6,)),
            dma((6,)),
            *(pltpu.VMEM(value.shape, value.dtype) for value in (weights, cotangent, *results)),
            dma((2,)),
            dma((9,)),
        ]
        + 2 * LineGather.scratch(chips),
        compiler_params=pltpu.CompilerParams(
            collective_id=collective_id, has_side_effects=True, vmem_limit_bytes=VMEM_LIMIT
        ),
        name="feed_forward",
    )(middle, gain, weights, own_up, own_down, cotangent)


def feed_backward(grads, weights, up_weights, normed, terms_down, w_out, middle, gain, cotangent, attended, gate_pre,
                  collective_id):
    rows, depth = middle.shape
    slots = 4 * rows
    units = grads.shape[1] // 2
    early = weights.shape[1]
    columns = attended.shape[1]
    shards = 2 * lax.axis_size("seq")
    chips = shards // 2
    low = jnp.bfloat16

    def body(grads_hbm, weights_hbm, up_weights_hbm, normed_hbm, down_hbm, out_hbm, middle_hbm, gain_ref, cot_hbm,
             attended_hbm, pre_hbm,
             grad_middle_hbm, grad_gain, branch_hbm, d_attended, d_pre, terms_up_hbm, share_down, share_gate,
             own_branch, summed, terms_gate, send, recv,
             grads_ref, weights_ref, up_weights_ref, normed_ref, down_ref, out_ref, middle_ref, cot_ref,
             attended_ref, pre_ref, grad_middle, branch, terms_up, fetch_sems, store_sems, *scratch):
        fetch, store = Streams(fetch_sems), Streams(store_sems)
        own_rows = pl.ds(pl.multiple_of(lax.axis_index("seq") * rows, rows), rows)
        first_in = [
            fetch.start(*both)
            for both in (
                (grads_hbm, grads_ref),
                (weights_hbm, weights_ref),
                (up_weights_hbm, up_weights_ref),
                (down_hbm, down_ref),
            )
        ]
        normed_in = fetch.start(normed_hbm, normed_ref)
        rest_in = [
            fetch.start(*both)
            for both in (
                (middle_hbm, middle_ref),
                (cot_hbm.at[own_rows], cot_ref),
                (out_hbm, out_ref),
                (attended_hbm, attended_ref),
                (pre_hbm, pre_ref),
            )
        ]
        me, side, down, across = sides()
        line_chips, chip, core, forth, back, twin = line()
        meet({"seq": side}, {"seq": down}, forth, back, twin)
        first, second = grads_ref.at[:, pl.ds(0, units)], grads_ref.at[:, pl.ds(units, units)]
        job = SquareScatter(
            [grads_ref.at[:, pl.ds(0, early)], grads_ref.at[:, pl.ds(early, 2 * units - early)]],
            [weights_ref, up_weights_ref],
            True,
            summed,
            *scratch[:7],
        )
        run_down = LineScatter(down_ref, share_down, *scratch[7:12])
        run_gate = LineScatter(terms_gate, share_gate, *scratch[12:])
        every = SquareGather(own_branch, branch, send, recv)
        for copy in first_in:
            copy.wait()
        run_down.start()
        job.begin()
        run_down.slot(0)
        normed_in.wait()
        transposed_product(normed_ref, first, terms_gate)
        run_gate.start()
        job.relay()
        run_down.slot(1)
        job.own()
        transposed_product(normed_ref, second, terms_up)
        store.start(terms_up, terms_up_hbm)
        run_down.slot(2)
        run_gate.slot(0)
        for copy in rest_in:
            copy.wait()
        job.end()
        values, change = middle_ref[...], summed[...]
        scale = norm_rows(values, gain_ref[...])[0]
        grad_gain[...] = jnp.sum(change * values * scale, axis=0, keepdims=True)
        change = change * gain_ref[...]
        mean = jnp.mean(change * values, axis=-1, keepdims=True)
        total = cot_ref[...].astype(jnp.float32) + scale * change - values * (scale * scale * scale * mean)
        grad_middle[...] = total
        own_branch[...] = total.astype(low)
        every.start()
        store.start(grad_middle, grad_middle_hbm)

        def rows_of(rank):
            return pl.ds(pl.multiple_of(rank * rows, rows), rows)

        def multiply(rank):
            at = rows_of(rank)
            grad_gated = product_nt(branch[at, :], out_ref[...])
            sigma = jax.nn.sigmoid(pre_ref[at, :])
            d_attended[at, :] = (grad_gated * sigma).astype(low)
            d_pre[at, :] = (
                grad_gated * attended_ref[at, :].astype(jnp.float32) * sigma * (1.0 - sigma)
            ).astype(low)

        branch[rows_of(me), :] = own_branch[...]
        multiply(me)
        run_gate.slot(1)
        every.relay()
        run_gate.slot(2)
        every.near()
        multiply(side)
        multiply(down)
        run_down.end()
        every.far()
        store.start(branch, branch_hbm)
        multiply(across)
        every.finish()
        run_gate.end()
        store.end()

    def shape(size, kind=low):
        return jax.ShapeDtypeStruct(size, kind)

    vmem = pl.BlockSpec(memory_space=pltpu.VMEM)
    anywhere = pl.BlockSpec(memory_space=pl.ANY)
    dma = pltpu.SemaphoreType.DMA
    own_shape = jax.ShapeDtypeStruct((rows, depth), low)
    fetched = (grads, weights, up_weights, normed, terms_down, w_out, middle, own_shape, attended, gate_pre)
    return pl.pallas_call(
        body,
        in_specs=[anywhere] * 7 + [vmem] + [anywhere] * 3,
        out_specs=[anywhere, vmem, anywhere, vmem, vmem, anywhere, vmem, vmem],
        out_shape=[
            shape((rows, depth), jnp.float32),
            shape((1, depth), jnp.float32),
            shape((slots, depth)),
            shape((slots, columns)),
            shape((slots, columns)),
            shape((depth, units)),
            shape((terms_down.shape[0] // shards, depth)),
            shape((depth // shards, units)),
        ],
        scratch_shapes=[
            pltpu.VMEM((rows, depth), low),
            pltpu.VMEM((rows, depth), jnp.float32),
            pltpu.VMEM((depth, units), low),
            dma((6,)),
            dma((6,)),
            *(pltpu.VMEM(value.shape, value.dtype) for value in fetched),
            pltpu.VMEM((rows, depth), jnp.float32),
            pltpu.VMEM((slots, depth), low),
            pltpu.VMEM((depth, units), low),
            dma((len(fetched),)),
            dma((3,)),
        ]
        + SquareScatter.scratch(rows, depth)
        + LineScatter.scratch(chips, terms_down.shape[0] // shards, depth)
        + LineScatter.scratch(chips, depth // shards, units),
        compiler_params=pltpu.CompilerParams(
            collective_id=collective_id, has_side_effects=True, vmem_limit_bytes=VMEM_LIMIT
        ),
        name="feed_backward",
    )(grads, weights, up_weights, normed, terms_down, w_out, middle, gain, cotangent, attended, gate_pre)


class SquareScatter:
    @staticmethod
    def scratch(rows, width):
        half = rows // 2
        low = jnp.bfloat16
        return [
            pltpu.VMEM((rows, width), low),
            pltpu.VMEM((2, half, width), low),
            pltpu.VMEM((2, half, width), jnp.float32),
            pltpu.VMEM((6, half, width), low),
            pltpu.VMEM((2, half, width), low),
            pltpu.SemaphoreType.DMA((6,)),
            pltpu.SemaphoreType.DMA((6,)),
        ]

    def __init__(self, lefts, rights, transposed, out, far, near, kept, land, carry, send, recv):
        self.lefts, self.rights, self.transposed, self.out = lefts, rights, transposed, out
        self.far, self.near, self.kept, self.land, self.carry = far, near, kept, land, carry
        self.send, self.recv = send, recv
        self.rows, self.width = out.shape
        self.half = self.rows // 2
        self.tile = self.width // 3 if self.width % 384 == 0 else self.width

    def copy(self, index):
        me, side, down, across = sides()
        source = (
            self.far.at[pl.ds(0, self.half)],
            self.far.at[pl.ds(self.half, self.half)],
            self.near.at[0],
            self.near.at[1],
            self.carry.at[0],
            self.carry.at[1],
        )[index]
        return pltpu.make_async_remote_copy(
            src_ref=source,
            dst_ref=self.land.at[index],
            send_sem=self.send.at[index],
            recv_sem=self.recv.at[index],
            device_id={"seq": down if index in (0, 3, 5) else side},
            device_id_type=MESH,
        )

    def partial(self, rank, store):
        at = pl.ds(pl.multiple_of(rank * self.rows, self.rows), self.rows)

        def step(number, carried):
            columns = pl.ds(pl.multiple_of(number * self.tile, self.tile), self.tile)
            value = None
            for a, b in zip(self.lefts, self.rights):
                if self.transposed:
                    term = product_nt(a[at, :], b[columns, :])
                else:
                    term = product(a[at, :], b[:, columns])
                value = term if value is None else value + term
            store(columns, value)
            return carried

        lax.fori_loop(0, self.width // self.tile, step, 0)

    def begin(self):
        me, side, down, across = sides()
        half, far, near, kept = self.half, self.far, self.near, self.kept

        def store_far(columns, value):
            far[:, columns] = value.astype(far.dtype)

        def store_side(columns, value):
            kept[0, :, columns] = value[:half]
            near[0, :, columns] = value[half:].astype(near.dtype)

        def store_down(columns, value):
            near[1, :, columns] = value[:half].astype(near.dtype)
            kept[1, :, columns] = value[half:]

        self.partial(across, store_far)
        self.copy(0).start()
        self.copy(1).start()
        self.partial(side, store_side)
        self.copy(2).start()
        self.partial(down, store_down)
        self.copy(3).start()

    def relay(self):
        for index in (0, 1):
            self.copy(index).wait_recv()

            def add(at, index=index):
                total = self.kept[index, at, :] + self.land[index, at, :].astype(jnp.float32)
                self.carry[index, at, :] = total.astype(self.carry.dtype)

            by_rows(self.half, add)
            self.copy(4 + index).start()

    def own(self):
        out = self.out

        def store_own(columns, value):
            out[:, columns] = value

        self.partial(lax.axis_index("seq"), store_own)

    def end(self):
        for index in (2, 3, 4, 5):
            self.copy(index).wait_recv()
        land, half, out = self.land, self.half, self.out

        def add(at):
            out[at, :] += land[3, at, :].astype(jnp.float32) + land[4, at, :].astype(jnp.float32)

        def add_second(at):
            to = pl.ds(at.start + half, at.size)
            out[to, :] += land[2, at, :].astype(jnp.float32) + land[5, at, :].astype(jnp.float32)

        by_rows(half, add)
        by_rows(half, add_second)
        for index in range(6):
            self.copy(index).wait_send()


class LineScatter:
    @staticmethod
    def scratch(chips, rows, width):
        low = jnp.bfloat16
        dma = pltpu.SemaphoreType.DMA
        return [pltpu.VMEM((chips, rows, width), low)] * 3 + [dma((2, chips)), dma((3, chips))]

    def __init__(self, terms, out, twin_in, forth_in, back_in, send, recv):
        self.terms, self.out, self.twin_in = terms, out, twin_in
        self.forth_in, self.back_in, self.send, self.recv = forth_in, back_in, send, recv
        self.chips, self.chip, self.core, *self.devices = line()
        self.rows = twin_in.shape[1]

    def term(self, chip, core):
        return self.terms.at[pl.ds(pl.multiple_of((2 * chip + core) * self.rows, self.rows), self.rows)]

    def swap(self, chip):
        return pltpu.make_async_remote_copy(
            src_ref=self.term(chip, 1 - self.core),
            dst_ref=self.twin_in.at[chip],
            send_sem=self.send.at[0, chip],
            recv_sem=self.recv.at[0, chip],
            device_id=self.devices[2],
            device_id_type=MESH,
        )

    def hop(self, way, chip):
        return pltpu.make_async_remote_copy(
            src_ref=self.twin_in.at[chip],
            dst_ref=(self.forth_in, self.back_in)[way].at[chip],
            send_sem=self.send.at[1, chip],
            recv_sem=self.recv.at[1 + way, chip],
            device_id=self.devices[way],
            device_id_type=MESH,
        )

    def start(self):
        for chip in (self.chips - 1, 0, *range(1, self.chips - 1)):
            self.swap(chip).start()

    def add(self, chip, ways, out):
        def step(at):
            start = pl.multiple_of((2 * chip + self.core) * self.rows + at.start, at.size)
            total = self.terms[pl.ds(start, at.size), :].astype(jnp.float32)
            total = total + self.twin_in[chip, at, :].astype(jnp.float32)
            for way in ways:
                total = total + (self.forth_in, self.back_in)[way][chip, at, :].astype(jnp.float32)
            out[at, :] = total.astype(out.dtype)

        by_rows(self.rows, step)

    def pass_on(self, way, chip, first):
        self.swap(chip).wait_recv()
        if not first:
            self.hop(way, chip).wait_recv()
        self.add(chip, () if first else (way,), self.twin_in.at[chip])
        self.hop(way, chip).start()

    def slot(self, number):
        last = self.chips - 1
        for chip in range(self.chips):
            forth, back = number - (last - chip), last - (number - chip)
            if 0 <= forth < chip:

                @pl.when(self.chip == forth)
                def _():
                    self.pass_on(0, chip, forth == 0)

            if chip < back <= last:

                @pl.when(self.chip == back)
                def _():
                    self.pass_on(1, chip, back == last)

    def end(self):
        for chip in range(self.chips):

            @pl.when(self.chip == chip)
            def _():
                self.swap(chip).wait_recv()
                ways = [way for way, there in enumerate((chip > 0, chip < self.chips - 1)) if there]
                for way in ways:
                    self.hop(way, chip).wait_recv()
                self.add(chip, ways, self.out)

            self.swap(chip).wait_send()

            @pl.when(self.chip != chip)
            def _():
                self.hop(0, chip).wait_send()


def middle_backward(joined, d_out, offset, col, logit, hidden, w_down, gated, grad_branch, terms_up, shares,
                    normed, d_pre, middle, head_size, scale, collective_id):
    slots, lanes = joined.shape
    width = w_down.shape[1]
    tokens = slots // 4
    columns = gated.shape[1]
    shards = 2 * lax.axis_size("seq")
    chips = shards // 2
    rows_up = terms_up.shape[0] // shards
    fetched = (terms_up, hidden, w_down, gated, grad_branch, normed, d_pre, joined, d_out, middle)

    def body(*refs):
        sources, refs = refs[:10], refs[10:]
        (offset_ref, col_ref, logit_ref, *share_refs), refs = refs[:5], refs[5:]
        (grads, bias_grad, layer_output, collected, share_up, share_pre, *every_refs), refs = refs[:8], refs[8:]
        buffers, refs = refs[:10], refs[10:]
        terms, terms_pre, lowered, send, recv, keep, fetch_sems, *scratch = refs
        up_ref, hidden_ref, down_ref, gated_ref, branch_ref, normed_ref, pre_ref, joined_ref, d_out_ref = buffers[:9]
        fetch = Streams(fetch_sems)
        comes = [fetch.start(source, buffer) for source, buffer in zip(sources, buffers)]
        me, side, down, across = sides()
        line_chips, chip, core, forth, back, twin = line()
        meet({"seq": side}, {"seq": down}, forth, back, twin)
        work = Backward(
            joined_ref, d_out_ref, offset_ref, col_ref, logit_ref, grads, *scratch[:4], head_size, scale
        )
        job = SquareScatter([hidden_ref], [down_ref], False, lowered, *scratch[4:11])
        collect = LineScatter(terms, collected, *scratch[11:16])
        run = LineScatter(up_ref, share_up, *scratch[16:21])
        run_pre = LineScatter(terms_pre, share_pre, *scratch[21:])
        every = [SquareGather(share_refs[i], every_refs[i], send.at[i], recv.at[i]) for i in range(2)]
        every[0].start()
        comes[0].wait()
        run.start()
        kept = []
        for i in range(2):
            size = share_refs[i].shape[0]
            kept.append(
                pltpu.make_async_copy(
                    share_refs[i],
                    every_refs[i].at[pl.ds(pl.multiple_of(me * size, size), size)],
                    keep.at[i],
                )
            )
            kept[i].start()
        comes[1].wait()
        comes[2].wait()
        job.begin()
        run.slot(0)
        comes[3].wait()
        comes[4].wait()
        transposed_product(gated_ref, branch_ref, terms)
        collect.start()
        comes[5].wait()
        comes[6].wait()
        transposed_product(normed_ref, pre_ref, terms_pre)
        run_pre.start()
        collect.slot(0)
        for copy in comes[7:]:
            copy.wait()
        run_pre.slot(0)
        work.start()

        def step(pair, carry):
            work.pair(pair)

            @pl.when(pair == 0)
            def _():
                run.slot(1)
                job.relay()
                every[0].relay()
                every[1].start()
                collect.slot(1)
                run_pre.slot(1)

            @pl.when(pair == 1)
            def _():
                run.slot(2)
                collect.slot(2)
                run_pre.slot(2)
                every[1].relay()

            return carry

        lax.fori_loop(0, work.pairs, step, 0)
        job.own()
        work.end(bias_grad)
        job.end()
        layer_output[...] = (buffers[9][...] + lowered[...]).astype(layer_output.dtype)
        run.end()
        collect.end()
        run_pre.end()
        for gathering, copy in zip(every, kept):
            gathering.near()
            gathering.far()
            gathering.finish()
            copy.wait()

    vmem = pl.BlockSpec(memory_space=pltpu.VMEM)
    anywhere = pl.BlockSpec(memory_space=pl.ANY)
    low = jnp.bfloat16
    dma = pltpu.SemaphoreType.DMA
    return pl.pallas_call(
        body,
        in_specs=[anywhere] * 10 + [vmem] * 5,
        out_specs=[vmem] * 6 + [anywhere] * 2,
        out_shape=[
            jax.ShapeDtypeStruct((slots, lanes), low),
            jax.ShapeDtypeStruct((8, PAIR), jnp.float32),
            jax.ShapeDtypeStruct((tokens, width), low),
            jax.ShapeDtypeStruct((columns // shards, width), low),
            jax.ShapeDtypeStruct((rows_up, terms_up.shape[1]), low),
            jax.ShapeDtypeStruct((rows_up, columns), low),
            *(jax.ShapeDtypeStruct((4 * v.shape[0], v.shape[1]), low) for v in shares),
        ],
        scratch_shapes=[
            *(pltpu.VMEM(value.shape, value.dtype) for value in fetched),
            pltpu.VMEM((columns, width), low),
            pltpu.VMEM((width, columns), low),
            pltpu.VMEM((tokens, width), jnp.float32),
            dma((2, 6)),
            dma((2, 6)),
            dma((2,)),
            dma((10,)),
        ]
        + backward_scratch(slots)
        + SquareScatter.scratch(tokens, width)
        + LineScatter.scratch(chips, columns // shards, width)
        + LineScatter.scratch(chips, rows_up, terms_up.shape[1])
        + LineScatter.scratch(chips, rows_up, columns),
        compiler_params=pltpu.CompilerParams(
            collective_id=collective_id, has_side_effects=True, vmem_limit_bytes=VMEM_LIMIT
        ),
        name="middle_backward",
    )(*fetched, offset, col, logit, *shares)


def last_backward(grads, d_pre, normed, weights, gate_weights, collected, shares, inputs, gain, grad_middle,
                  collective_id):
    slots, depth = normed.shape
    front = grads.shape[1]
    tokens = slots // 4
    shards = 2 * lax.axis_size("seq")
    rows = depth // shards
    fetched = (normed, grads, d_pre, weights, gate_weights, inputs, grad_middle)

    def body(*refs):
        sources, refs = refs[:7], refs[7:]
        (collected_ref, gain_ref, *share_refs), refs = refs[:4], refs[4:]
        (grad_input, grad_gain, share, regrouped, *every_refs), refs = refs[:6], refs[6:]
        buffers, refs = refs[:7], refs[7:]
        terms, summed, send, recv, keep, fetch_sems, *scratch = refs
        normed_ref, grads_ref, pre_ref, weights_ref, gate_weights_ref, inputs_ref, middle_ref = buffers
        fetch = Streams(fetch_sems)
        comes = [fetch.start(source, buffer) for source, buffer in zip(sources, buffers)]
        me, side, down, across = sides()
        regroup = Regroup(collected_ref, regrouped, *scratch[12:])
        meet(*regroup.others, *regroup.along)
        job = SquareScatter([grads_ref, pre_ref], [weights_ref, gate_weights_ref], True, summed, *scratch[:7])
        run = LineScatter(terms, share, *scratch[7:12])
        regroup.start()
        every = [SquareGather(share_refs[i], every_refs[i], send.at[i], recv.at[i]) for i in range(2)]
        every[0].start()
        kept = []
        for i in range(2):
            size = share_refs[i].shape[0]
            kept.append(
                pltpu.make_async_copy(
                    share_refs[i],
                    every_refs[i].at[pl.ds(pl.multiple_of(me * size, size), size)],
                    keep.at[i],
                )
            )
            kept[i].start()
        comes[0].wait()
        comes[1].wait()
        transposed_product(normed_ref, grads_ref, terms)
        run.start()
        every[0].relay()
        regroup.relay()
        run.slot(0)
        for copy in comes[2:]:
            copy.wait()
        job.begin()
        every[1].start()
        job.relay()
        run.slot(1)
        job.own()
        every[1].relay()
        run.slot(2)
        job.end()
        values, change = inputs_ref[...].astype(jnp.float32), summed[...]
        scale = norm_rows(values, gain_ref[...])[0]
        grad_gain[...] = jnp.sum(change * values * scale, axis=0, keepdims=True)
        change = change * gain_ref[...]
        mean = jnp.mean(change * values, axis=-1, keepdims=True)
        grad_input[...] = middle_ref[...] + scale * change - values * (scale * scale * scale * mean)
        for gathering, copy in zip(every, kept):
            gathering.near()
            gathering.far()
            gathering.finish()
            copy.wait()
        regroup.end()
        run.end()

    vmem = pl.BlockSpec(memory_space=pltpu.VMEM)
    anywhere = pl.BlockSpec(memory_space=pl.ANY)
    low = jnp.bfloat16
    dma = pltpu.SemaphoreType.DMA
    return pl.pallas_call(
        body,
        in_specs=[anywhere] * 7 + [vmem] * 4,
        out_specs=[vmem] * 4 + [anywhere] * 2,
        out_shape=[
            jax.ShapeDtypeStruct((tokens, depth), jnp.float32),
            jax.ShapeDtypeStruct((1, depth), jnp.float32),
            jax.ShapeDtypeStruct((rows, front), low),
            jax.ShapeDtypeStruct((4,) + collected.shape, low),
            *(jax.ShapeDtypeStruct((4 * v.shape[0], v.shape[1]), low) for v in shares),
        ],
        scratch_shapes=[
            *(pltpu.VMEM(value.shape, value.dtype) for value in fetched),
            pltpu.VMEM((depth, front), low),
            pltpu.VMEM((tokens, depth), jnp.float32),
            dma((2, 6)),
            dma((2, 6)),
            dma((2,)),
            dma((7,)),
        ]
        + SquareScatter.scratch(tokens, depth)
        + LineScatter.scratch(shards // 2, rows, front)
        + Regroup.scratch(*collected.shape),
        compiler_params=pltpu.CompilerParams(
            collective_id=collective_id, has_side_effects=True, vmem_limit_bytes=VMEM_LIMIT
        ),
        name="last_backward",
    )(*fetched, collected, gain, *shares)


def gather(value, axis_name):
    return lax.all_gather(value, axis_name, axis=0, tiled=True)


def scatter(value, axis_name):
    return lax.psum_scatter(value, axis_name, scatter_dimension=0, tiled=True)


def on_device(
    layer_input,
    lengths,
    norm_attn,
    w_query,
    w_key,
    w_value,
    w_ogate,
    w_forget,
    forget_bias,
    w_out,
    norm_ffn,
    w_gate,
    w_up,
    w_down,
    output_grad,
):
    low = jnp.bfloat16
    tokens, width = layer_input.shape[1:]
    heads = forget_bias.shape[0]
    groups = lax.axis_size("seq")
    shards = lax.axis_size("wshard")
    fast = square(groups) and shards == 2 * groups
    local_heads = heads // groups
    head_size = width // heads
    columns = width // groups
    lanes = columns + -columns % PAIR
    front = 3 * lanes + PAIR
    slots = tokens * groups
    hidden_size = w_gate.shape[1]
    part = hidden_size // (groups * shards)
    units = shards * part
    scale = head_size ** (-0.5)
    length = lengths[0]
    seq_rank = lax.axis_index("seq")
    shard_rank = lax.axis_index("wshard")
    per_block = shards // groups
    positions = seq_rank * tokens + jnp.arange(tokens, dtype=jnp.int32)
    valid_slots = (positions < length)[:, None]
    inputs = layer_input[0].astype(jnp.float32)
    cotangent_low = jnp.where(valid_slots, output_grad[0], jnp.zeros((), low))
    cotangent = cotangent_low.astype(jnp.float32)

    def own_columns(weight, size):
        taken = lax.dynamic_slice_in_dim(weight, seq_rank * columns, columns, 1)
        return jnp.pad(taken, ((0, 0), (0, size - columns))) if size > columns else taken

    def own_units(weight):
        split = weight.reshape(weight.shape[0], shards, groups, part)
        mine = lax.dynamic_index_in_dim(split, seq_rank, 2, keepdims=False)
        return mine.reshape(weight.shape[0], units)

    own_forget = lax.dynamic_slice_in_dim(w_forget, seq_rank * local_heads, local_heads, 1)
    own_forget = jnp.pad(own_forget, ((0, 0), (0, PAIR - local_heads)))
    own_bias = lax.dynamic_slice_in_dim(forget_bias, seq_rank * local_heads, local_heads)
    own_bias = jnp.pad(own_bias, (0, PAIR - local_heads))[None]
    length_row = jnp.broadcast_to(lengths[:, None], (1, PAIR))
    mine_down = lax.dynamic_slice_in_dim(w_down, seq_rank * part, part, 0)
    if fast:
        (
            normed_attn, cotangent_all, full_front, full_ogate, full_out, full_ffn,
            joined, attended_low, offset, col, logit, gate_pre, gated, middle, mine_up,
        ) = whole_forward(
            layer_input[0], norm_attn[None], output_grad[0], (w_query, w_key, w_value, w_ogate), own_forget,
            own_bias, length_row, w_out, w_gate, w_up, head_size, scale, 0,
        )
        full_out = full_out.reshape(columns, width)
        normed_ffn, hidden, full_up, full_down, grad_gate_up, terms_down = feed_forward(
            middle, norm_ffn[None], full_ffn, mine_up, mine_down, cotangent_all, 1
        )
        (
            grad_middle, grad_norm_ffn, grad_branch, grad_attended, grad_gate_pre, terms_up, share_down, share_gate,
        ) = feed_backward(
            grad_gate_up, full_ffn, full_up, normed_ffn, terms_down, full_out, middle, norm_ffn[None],
            cotangent_all, attended_low, gate_pre, 2,
        )
        grad_norm_ffn = grad_norm_ffn[0]
        grads, bias_rows, layer_output, collected, share_up, share_ogate, grad_down, every_gate = middle_backward(
            joined, grad_attended, offset, col, logit, hidden, full_down, gated, grad_branch, terms_up,
            (share_down, share_gate), normed_attn, grad_gate_pre, middle, head_size, scale, 3,
        )
        grad_input, grad_norm_attn, share_attn, grad_out, every_ogate, every_up = last_backward(
            grads, grad_gate_pre, normed_attn, full_front, full_ogate, collected, (share_ogate, share_up),
            layer_input[0], norm_attn[None], grad_middle, 4,
        )
        grad_norm_attn = grad_norm_attn[0]
        grad_out = grad_out.reshape(columns // per_block, width)
    else:
        mine_front = jnp.concatenate(
            [*(own_columns(w, lanes) for w in (w_query, w_key, w_value)), own_forget], axis=1
        )
        full_front = gather(mine_front, "wshard")
        full_ogate = gather(own_columns(w_ogate, columns), "wshard")
        normed_attn = gather(rms_norm(inputs, norm_attn).astype(low), "seq")
        cotangent_all = gather(cotangent_low, "seq")
        full_out = lax.dynamic_slice_in_dim(gather(w_out, "wshard"), seq_rank * columns, columns, 0)
        full_ffn = gather(jnp.concatenate([own_units(w_gate), own_units(w_up)], axis=1), "wshard")
        joined = product(normed_attn, full_front).astype(low)
        gate_pre = product(normed_attn, full_ogate)
        attended_low, offset, col, logit = attention_fwd(joined, own_bias, length_row, head_size, scale)
        attended = attended_low[:, :columns].astype(jnp.float32)
        gated_full, pull_gate = jax.vjp(gate_product, attended, gate_pre)
        gated = gated_full.astype(low)
        middle = inputs + scatter(product(gated, full_out).astype(low), "seq").astype(jnp.float32)
        normed_ffn_own, pull_ffn_norm = jax.vjp(rms_norm, middle, norm_ffn)
        full_down = gather(mine_down, "wshard")
        normed_ffn = gather(normed_ffn_own.astype(low), "seq")
        gate_up = product(normed_ffn, full_ffn)
        hidden_full, pull_swiglu = jax.vjp(swiglu, gate_up[:, :units], gate_up[:, units:])
        hidden = hidden_full.astype(low)
        grad_hidden = product_nt(cotangent_all, full_down)
        grad_gate_full, grad_up_full = pull_swiglu(grad_hidden)
        grad_gate_up = jnp.concatenate([grad_gate_full.astype(low), grad_up_full.astype(low)], axis=1)
        share_down = scatter(product_tn(hidden, cotangent_all).astype(low), "wshard")
        share_ffn = scatter(product_tn(normed_ffn, grad_gate_up).astype(low), "wshard")
        grad_normed_ffn = scatter(product_nt(grad_gate_up, full_ffn).astype(low), "seq").astype(jnp.float32)
        grad_middle_part, grad_norm_ffn = pull_ffn_norm(grad_normed_ffn)
        grad_middle = cotangent + grad_middle_part
        grad_branch = gather(grad_middle.astype(low), "seq")
        grad_attended_full, grad_gate_pre_full = pull_gate(product_nt(grad_branch, full_out))
        grad_attended = grad_attended_full.astype(low)
        grad_gate_pre = grad_gate_pre_full.astype(low)
        if lanes > columns:
            grad_attended = jnp.pad(grad_attended, ((0, 0), (0, lanes - columns)))
        grads, bias_rows = attention_bwd(joined, grad_attended, offset, col, logit, head_size, scale)
        grad_projected = jnp.concatenate([grads, grad_gate_pre], axis=1)
        share_attn = scatter(product_tn(normed_attn, grad_projected).astype(low), "wshard")
        full_attn = jnp.concatenate([full_front, full_ogate], axis=1)
        grad_normed_attn = scatter(product_nt(grad_projected, full_attn).astype(low), "seq").astype(jnp.float32)
        lowered = scatter(product(hidden, full_down).astype(low), "seq").astype(jnp.float32)
        share_out = scatter(product_tn(gated, grad_branch).astype(low), "wshard")
        rows_out = columns // shards
        pieces_out = lax.all_gather(share_out, "seq", axis=0, tiled=False)
        takes = shards // per_block
        slots_out = jnp.where(
            (jnp.arange(per_block) == shard_rank // takes)[None, :, None, None],
            pieces_out[:, None],
            jnp.zeros((), low),
        ).reshape(shards, rows_out, width)
        moved = lax.all_to_all(slots_out, "wshard", split_axis=0, concat_axis=0, tiled=True)
        moved = moved.reshape(per_block, takes, rows_out, width)
        mine_out = lax.dynamic_index_in_dim(moved, shard_rank % per_block, 0, keepdims=False)
        grad_out = mine_out.reshape(columns // per_block, width).astype(jnp.float32)
        layer_output = (middle + lowered).astype(low)
        unused_normed, pull_attn_norm = jax.vjp(rms_norm, inputs, norm_attn)
        grad_input_part, grad_norm_attn = pull_attn_norm(grad_normed_attn)
        grad_input = grad_middle + grad_input_part
    grad_bias = lax.dynamic_update_slice_in_dim(
        jnp.zeros((heads,), jnp.float32), bias_rows[:local_heads, 0], seq_rank * local_heads, 0
    )

    rows = share_attn.shape[0]
    if fast:
        vector = jnp.concatenate([grad_norm_attn, grad_norm_ffn, grad_bias])
        vector = jnp.pad(vector, (0, -vector.shape[0] % 1024)).reshape(-1, 128)
        every_attn, vector = last_gather([share_attn], vector, 5)
        vector = vector.reshape(-1)
        small = vector[:width], vector[width : 2 * width], vector[2 * width : 2 * width + heads]
    else:
        every_attn, every_ffn, grad_down = [gather(v, "seq") for v in (share_attn, share_ffn, share_down)]
        small = lax.psum((grad_norm_attn, grad_norm_ffn, grad_bias), ("seq", "wshard"))
    every_attn = every_attn.reshape((groups,) + share_attn.shape)
    if fast:
        *weight_grads, grad_forget_w, grad_w_gate, grad_w_up, grad_down, grad_out = join_shares(
            every_attn,
            every_ogate.reshape((groups,) + share_ogate.shape),
            every_gate.reshape((groups,) + share_gate.shape),
            every_up.reshape((groups,) + share_up.shape),
            grad_down,
            grad_out,
            columns,
            (0, lanes, 2 * lanes),
            3 * lanes,
            heads,
            part,
        )
    else:

        def join(first):
            taken = every_attn[:, :, first : first + columns]
            return taken.transpose(1, 0, 2).reshape(rows, width).astype(jnp.float32)

        def join_own_units(first):
            taken = every_ffn.reshape((groups,) + share_ffn.shape)[:, :, first * units : (first + 1) * units]
            taken = taken.reshape(groups, rows, shards, part).transpose(1, 2, 0, 3)
            return taken.reshape(rows, hidden_size).astype(jnp.float32)

        weight_grads = [join(first) for first in (0, lanes, 2 * lanes, front)]
        grad_w_gate, grad_w_up = join_own_units(0), join_own_units(1)
        grad_down = grad_down.astype(jnp.float32)
        grad_forget_w = every_attn[:, :, 3 * lanes : 3 * lanes + local_heads]
        grad_forget_w = grad_forget_w.transpose(1, 0, 2).reshape(rows, heads).astype(jnp.float32)
    return (
        layer_output[None],
        grad_input[None],
        small[0],
        *weight_grads,
        grad_forget_w,
        small[2],
        grad_out,
        small[1],
        grad_w_gate,
        grad_w_up,
        grad_down,
    )


def solution(mesh):
    return jax.shard_map(
        on_device,
        mesh=mesh,
        in_specs=(
            P("wshard", "seq", None),
            P("wshard"),
            P(),
            P("wshard", None),
            P("wshard", None),
            P("wshard", None),
            P("wshard", None),
            P("wshard", None),
            P(),
            P("wshard", None),
            P(),
            P("wshard", None),
            P("wshard", None),
            P("wshard", None),
            P("wshard", "seq", None),
        ),
        out_specs=(
            P("wshard", "seq", None),
            P("wshard", "seq", None),
            P(),
            P("wshard", None),
            P("wshard", None),
            P("wshard", None),
            P("wshard", None),
            P("wshard", None),
            P(),
            P("wshard", None),
            P(),
            P("wshard", None),
            P("wshard", None),
            P("wshard", None),
        ),
        check_vma=False,
    )
```

```python
import jax
import jax.numpy as jnp
from jax import lax
from jax.experimental import pallas as pl
from jax.experimental.pallas import tpu as pltpu
from jax.sharding import PartitionSpec as P

EPS = 1e-06
NEG_FILL = -1e30
PAIR = 128


def product(left, right):
    return jnp.dot(left, right, preferred_element_type=jnp.float32)


def product_tn(left, right):
    return lax.dot_general(
        left, right, (((0,), (0,)), ((), ())), preferred_element_type=jnp.float32
    )


def product_nt(left, right):
    return lax.dot_general(
        left, right, (((1,), (1,)), ((), ())), preferred_element_type=jnp.float32
    )


def rms_norm(values, gain):
    return values * lax.rsqrt(jnp.mean(values * values, axis=-1, keepdims=True) + EPS) * gain


def gate_product(attended, gate_pre):
    return attended * jax.nn.sigmoid(gate_pre)


def swiglu(gate, upward):
    return jax.nn.silu(gate) * upward


def low_triangle(size):
    rows = lax.broadcasted_iota(jnp.int32, (size, size), 0)
    return rows <= lax.broadcasted_iota(jnp.int32, (size, size), 1)


def exact(left, right):
    return jnp.dot(left, right, precision=lax.Precision.HIGHEST, preferred_element_type=jnp.float32)


class Forward:
    some = 8

    def __init__(self, joined, bias, length, attended, offset, col, logit, row, head_size, scale):
        self.joined, self.bias, self.length = joined, bias, length
        self.attended, self.offset, self.col, self.logit, self.row = attended, offset, col, logit, row
        self.head_size, self.scale = head_size, scale
        self.slots = joined.shape[0]
        self.pairs = (joined.shape[1] // PAIR - 1) // 3
        self.tile = min(256, self.slots)

    @staticmethod
    def results(slots, pairs):
        rows = jax.ShapeDtypeStruct((Forward.some, slots), jnp.float32)
        return [
            jax.ShapeDtypeStruct((slots, pairs * PAIR), jnp.bfloat16),
            rows,
            jax.ShapeDtypeStruct((slots, PAIR), jnp.float32),
            rows,
        ]

    def lanes(self, pair, part=0):
        return pl.ds(pl.multiple_of((part * self.pairs + pair) * PAIR, PAIR), PAIR)

    def start(self):
        slots, tile, some = self.slots, self.tile, self.some
        logits = self.joined[:, 3 * self.pairs * PAIR :].astype(jnp.float32) + self.bias[...]
        logit_rows = logits.T[:some]
        self.logit[...] = logit_rows
        logs = jnp.minimum(logit_rows, 0.0) - jnp.log1p(jnp.exp(-jnp.abs(logit_rows)))
        ones = low_triangle(tile).astype(jnp.float32)
        carry = jnp.zeros((some, 1), jnp.float32)
        for first in range(0, slots, tile):
            sums = exact(logs[:, first : first + tile], ones) + carry
            self.row[:, first : first + tile] = sums
            carry = sums[:, tile - 1 : tile]
        wide = jnp.concatenate([self.row[...], jnp.zeros((PAIR - some, slots), jnp.float32)], axis=0).T
        usable = lax.broadcasted_iota(jnp.int32, (slots, PAIR), 0) < self.length[...]
        self.col[...] = jnp.where(usable, wide, -NEG_FILL)

    def pair(self, pair):
        slots, tile, half = self.slots, self.tile, self.head_size
        key_all = self.joined[:, self.lanes(pair, 1)]
        value_t = self.joined[:, self.lanes(pair, 2)].T
        query_t = (self.joined[:, self.lanes(pair)].astype(jnp.float32) * self.scale).astype(jnp.bfloat16).T
        sub = lax.broadcasted_iota(jnp.int32, (PAIR, tile), 0)
        wide = lax.broadcasted_iota(jnp.int32, (slots, PAIR), 1)
        diag = low_triangle(tile)
        columns = [
            jnp.sum(jnp.where(wide == 2 * pair + a, self.col[...], 0.0), axis=1, keepdims=True) for a in range(2)
        ]
        for number in range(slots // tile):
            first, last = number * tile, (number + 1) * tile
            outs = []
            for a in range(2):
                mine = (sub >= a * half) & (sub < (a + 1) * half)
                at = pl.ds(2 * pair + a, 1)
                query = jnp.where(mine, query_t[:, first:last], jnp.zeros((), query_t.dtype))
                scores = product(key_all[:last], query)
                own_row = self.row[at, first:last]
                scores = scores + (own_row - columns[a][:last])
                tail = jnp.where(diag, scores[first:], NEG_FILL)
                scores = tail if number == 0 else jnp.concatenate([scores[:first], tail], axis=0)
                top = jnp.max(scores, axis=0, keepdims=True)
                weights = jnp.exp(scores - top)
                total = jnp.sum(weights, axis=0, keepdims=True)
                mixed = product(value_t[a * half : (a + 1) * half, :last], weights.astype(jnp.bfloat16))
                outs.append(mixed / total)
                self.offset[at, first:last] = own_row - (top + jnp.log(total))
            self.attended[first:last, self.lanes(pair)] = jnp.concatenate(outs, axis=0).T.astype(jnp.bfloat16)


def attention_fwd(joined, bias, length, head_size, scale):
    slots = joined.shape[0]
    pairs = (joined.shape[1] // PAIR - 1) // 3

    def body(joined_ref, bias_ref, length_ref, attended, offset, col, logit, row):
        work = Forward(joined_ref, bias_ref, length_ref, attended, offset, col, logit, row, head_size, scale)
        work.start()
        offset[...] = jnp.zeros_like(offset)

        def step(pair, carry):
            work.pair(pair)
            return carry

        lax.fori_loop(0, pairs, step, 0)

    vmem = pl.BlockSpec(memory_space=pltpu.VMEM)
    return pl.pallas_call(
        body,
        in_specs=[vmem] * 3,
        out_specs=[vmem] * 4,
        out_shape=Forward.results(slots, pairs),
        scratch_shapes=[pltpu.VMEM((Forward.some, slots), jnp.float32)],
        compiler_params=pltpu.CompilerParams(vmem_limit_bytes=56 << 20),
        cost_estimate=pl.CostEstimate(
            flops=4 * slots * slots * pairs * PAIR, bytes_accessed=8 * slots * pairs * PAIR, transcendentals=0
        ),
        name="attention_fwd",
    )(joined, bias, length)


def backward_scratch(slots):
    return [
        pltpu.VMEM((slots, PAIR), jnp.float32),
        pltpu.VMEM((slots, PAIR), jnp.float32),
        pltpu.VMEM((slots, PAIR), jnp.float32),
        pltpu.VMEM((8, slots), jnp.float32),
    ]


class Backward:
    def __init__(self, joined, d_out, offset, col, logit, grads, dk_acc, dv_acc, dcol, drow, head_size, scale):
        self.joined, self.d_out, self.offset, self.col = joined, d_out, offset, col
        self.logit, self.grads, self.dk_acc, self.dv_acc = logit, grads, dk_acc, dv_acc
        self.dcol, self.drow, self.head_size, self.scale = dcol, drow, head_size, scale
        self.slots = joined.shape[0]
        self.pairs = (joined.shape[1] // PAIR - 1) // 3
        self.tile = min(256, self.slots)

    def start(self):
        self.dcol[...] = jnp.zeros_like(self.dcol)
        self.drow[...] = jnp.zeros_like(self.drow)

    def lanes(self, pair, part=0):
        return pl.ds(pl.multiple_of((part * self.pairs + pair) * PAIR, PAIR), PAIR)

    def pair(self, pair):
        slots, tile, half = self.slots, self.tile, self.head_size
        dk_acc, dv_acc, dcol, drow = self.dk_acc, self.dv_acc, self.dcol, self.drow
        queries = (self.joined[:, self.lanes(pair)].astype(jnp.float32) * self.scale).astype(jnp.bfloat16)
        key_all = self.joined[:, self.lanes(pair, 1)]
        value_all = self.joined[:, self.lanes(pair, 2)]
        d_out = self.d_out[:, self.lanes(pair)]
        query_t, key_t, dout_t = queries.T, key_all.T, d_out.T
        sub = lax.broadcasted_iota(jnp.int32, (PAIR, tile), 0)
        lanes = lax.broadcasted_iota(jnp.int32, (tile, PAIR), 1)
        wide = lax.broadcasted_iota(jnp.int32, (slots, PAIR), 1)
        diag = low_triangle(tile)
        zero = jnp.zeros((), jnp.bfloat16)
        columns = [
            jnp.sum(jnp.where(wide == 2 * pair + a, self.col[...], 0.0), axis=1, keepdims=True) for a in range(2)
        ]
        dk_acc[...] = jnp.zeros_like(dk_acc)
        dv_acc[...] = jnp.zeros_like(dv_acc)
        for number in range(slots // tile):
            first, last = number * tile, (number + 1) * tile
            outs = []
            for a in range(2):
                mine = (sub >= a * half) & (sub < (a + 1) * half)
                own = (lanes >= a * half) & (lanes < (a + 1) * half)
                at = pl.ds(2 * pair + a, 1)
                scores = product(key_all[:last], jnp.where(mine, query_t[:, first:last], zero))
                scores = scores + (self.offset[at, first:last] - columns[a][:last])
                tail = jnp.where(diag, scores[first:], NEG_FILL)
                scores = tail if number == 0 else jnp.concatenate([scores[:first], tail], axis=0)
                probs = jnp.exp(scores)
                d_probs = product(value_all[:last], jnp.where(mine, dout_t[:, first:last], zero))
                dot = jnp.sum(d_probs * probs, axis=0, keepdims=True)
                d_full = probs * (d_probs - dot)
                d_scores = d_full.astype(jnp.bfloat16)
                drow[at, first:last] = jnp.sum(d_full, axis=0, keepdims=True)
                sums = jnp.sum(d_full, axis=1, keepdims=True)
                dcol[:last, :] += jnp.where(wide[:last] == 2 * pair + a, sums, 0.0)
                outs.append(product(key_t[a * half : (a + 1) * half, :last], d_scores) * self.scale)
                dk_acc[:last, :] += product(d_scores, jnp.where(own, queries[first:last, :], zero))
                dv_acc[:last, :] += product(
                    probs.astype(jnp.bfloat16), jnp.where(own, d_out[first:last, :], zero)
                )
            self.grads[first:last, self.lanes(pair)] = jnp.concatenate(outs, axis=0).T.astype(self.grads.dtype)
        self.grads[:, self.lanes(pair, 1)] = dk_acc[...].astype(self.grads.dtype)
        self.grads[:, self.lanes(pair, 2)] = dv_acc[...].astype(self.grads.dtype)

    def end(self, bias_grad):
        slots, tile, some = self.slots, self.tile, 8
        change = self.drow[...] - self.dcol[...].T[:some]
        rows = lax.broadcasted_iota(jnp.int32, (tile, tile), 0)
        ones = (rows >= lax.broadcasted_iota(jnp.int32, (tile, tile), 1)).astype(jnp.float32)
        carry = jnp.zeros((some, 1), jnp.float32)
        pieces = []
        for first in reversed(range(0, slots, tile)):
            sums = exact(change[:, first : first + tile], ones) + carry
            carry = sums[:, :1]
            pieces.insert(0, sums)
        grad = jnp.concatenate(pieces, axis=1) * jax.nn.sigmoid(-self.logit[...])
        heads = lax.broadcasted_iota(jnp.int32, (some, slots), 0)
        grad = jnp.where(heads < 2 * self.pairs, grad, 0.0)
        bias_grad[...] = jnp.broadcast_to(jnp.sum(grad, axis=1, keepdims=True), bias_grad.shape)
        wide = jnp.concatenate([grad, jnp.zeros((PAIR - some, slots), jnp.float32)], axis=0).T
        self.grads[:, 3 * self.pairs * PAIR : (3 * self.pairs + 1) * PAIR] = wide.astype(self.grads.dtype)


def attention_bwd(joined, d_out, offset, col, logit, head_size, scale):
    slots, width = joined.shape
    pairs = (width // PAIR - 1) // 3

    def body(joined_ref, d_out_ref, offset_ref, col_ref, logit_ref, grads, bias_grad, *scratch):
        work = Backward(
            joined_ref, d_out_ref, offset_ref, col_ref, logit_ref, grads, *scratch, head_size, scale
        )
        work.start()

        def step(pair, carry):
            work.pair(pair)
            return carry

        lax.fori_loop(0, pairs, step, 0)
        work.end(bias_grad)

    vmem = pl.BlockSpec(memory_space=pltpu.VMEM)
    return pl.pallas_call(
        body,
        in_specs=[vmem] * 5,
        out_specs=[vmem] * 2,
        out_shape=[
            jax.ShapeDtypeStruct((slots, width), jnp.bfloat16),
            jax.ShapeDtypeStruct((8, PAIR), jnp.float32),
        ],
        scratch_shapes=backward_scratch(slots),
        compiler_params=pltpu.CompilerParams(vmem_limit_bytes=56 << 20),
        cost_estimate=pl.CostEstimate(
            flops=10 * slots * slots * pairs * PAIR, bytes_accessed=14 * slots * pairs * PAIR, transcendentals=0
        ),
        name="attention_bwd",
    )(joined, d_out, offset, col, logit)


MESH = pl.DeviceIdType.MESH
VMEM_LIMIT = 62 << 20


def square(groups):
    return groups == 4


def sides():
    rank = lax.axis_index("seq")
    return rank, rank + 1 - 2 * lax.rem(rank, 2), lax.rem(rank + 2, 4), 3 - rank


def meet(*others):
    barrier = pltpu.get_barrier_semaphore()
    for other in others:
        pl.semaphore_signal(barrier, inc=1, device_id=other, device_id_type=MESH)
    pl.semaphore_wait(barrier, len(others))


def push(source, target, send, recv, device):
    copy = pltpu.make_async_remote_copy(
        src_ref=source,
        dst_ref=target,
        send_sem=send,
        recv_sem=recv,
        device_id=device,
        device_id_type=MESH,
    )
    copy.start()
    return copy


def by_rows(rows, work):
    def step(number, carry):
        work(pl.ds(pl.multiple_of(number * 16, 16), 16))
        return carry

    lax.fori_loop(0, rows // 16, step, 0)


class Streams:
    def __init__(self, sems):
        self.sems, self.made = sems, []

    def start(self, source, target):
        copy = pltpu.make_async_copy(source, target, self.sems.at[len(self.made)])
        self.made.append(copy)
        copy.start()
        return copy

    def end(self):
        for copy in self.made:
            copy.wait()


class SquareGather:
    def __init__(self, own, full, send, recv):
        self.own, self.full, self.send, self.recv = own, full, send, recv
        self.rows = own.shape[0]
        self.half = self.rows // 2

    def place(self, rank, part):
        return self.full.at[pl.ds(pl.multiple_of(rank * self.rows + part * self.half, self.half), self.half)]

    def copy(self, index):
        me, side, down, across = sides()
        mine = [self.own.at[pl.ds(part * self.half, self.half)] for part in (0, 1)]
        source, target, peer = (
            (mine[0], self.place(me, 0), side),
            (mine[1], self.place(me, 1), down),
            (mine[1], self.place(me, 1), side),
            (mine[0], self.place(me, 0), down),
            (self.place(side, 0), self.place(side, 0), down),
            (self.place(down, 1), self.place(down, 1), side),
        )[index]
        return pltpu.make_async_remote_copy(
            src_ref=source,
            dst_ref=target,
            send_sem=self.send.at[index],
            recv_sem=self.recv.at[index],
            device_id={"seq": peer},
            device_id_type=MESH,
        )

    def start(self):
        for index in range(4):
            self.copy(index).start()

    def relay(self):
        for index in (0, 1):
            self.copy(index).wait_recv()
            self.copy(4 + index).start()

    def near(self):
        self.copy(2).wait_recv()
        self.copy(3).wait_recv()

    def far(self):
        self.copy(4).wait_recv()
        self.copy(5).wait_recv()

    def finish(self):
        for index in range(6):
            self.copy(index).wait_send()


def block_product(left, right, transposed, tile, store):
    total = right.shape[0] if transposed else right.shape[1]

    def step(number, carry):
        columns = pl.ds(pl.multiple_of(number * tile, tile), tile)
        if transposed:
            store(columns, product_nt(left[...], right[columns, :]))
        else:
            store(columns, product(left[...], right[:, columns]))
        return carry

    lax.fori_loop(0, total // tile, step, 0)


def transposed_product(left, right, out):
    tall = 512 if out.shape[0] % 512 == 0 else 384
    wide = next(size for size in (512, 384, 640, 128) if out.shape[1] % size == 0)
    across = out.shape[1] // wide

    def step(number, carry):
        rows = pl.ds(pl.multiple_of((number // across) * tall, tall), tall)
        columns = pl.ds(pl.multiple_of(lax.rem(number, across) * wide, wide), wide)
        out[rows, columns] = product_tn(left[:, rows], right[:, columns]).astype(out.dtype)
        return carry

    lax.fori_loop(0, (out.shape[0] // tall) * across, step, 0)


def line():
    shards, place = lax.axis_size("wshard"), lax.axis_index("wshard")
    chips = shards // 2
    chip, core = place // 2, lax.rem(place, 2)
    forth = {"wshard": lax.rem(place + 2, shards)}
    back = {"wshard": lax.rem(place + shards - 2, shards)}
    twin = {"wshard": place + 1 - 2 * core}
    return chips, chip, core, forth, back, twin


class LineGather:
    @staticmethod
    def scratch(chips):
        dma = pltpu.SemaphoreType.DMA
        return [dma((3, chips)), dma((2 * chips,)), dma((1,))]

    def __init__(self, own, full, send, recv, local):
        self.own, self.full, self.local = own, full, local.at[0]
        self.sends = (send.at[0], send.at[1], send.at[2])
        self.recv = recv
        self.rows = own.shape[0]
        self.chips, self.chip, self.core, *self.devices = line()

    def place(self, chip, core):
        return self.full.at[pl.ds(pl.multiple_of((2 * chip + core) * self.rows, self.rows), self.rows)]

    def copy(self, way, chip, source=None):
        target = self.place(chip, self.core)
        return pltpu.make_async_remote_copy(
            src_ref=target if source is None else source,
            dst_ref=target,
            send_sem=self.sends[way].at[chip],
            recv_sem=self.recv.at[2 * chip + self.core],
            device_id=self.devices[way],
            device_id_type=MESH,
        )

    def wait_for(self, chip, core):
        target = self.place(chip, core)
        pltpu.make_async_remote_copy(
            src_ref=target,
            dst_ref=target,
            send_sem=self.sends[2].at[0],
            recv_sem=self.recv.at[2 * chip + core],
            device_id=self.devices[2],
            device_id_type=MESH,
        ).wait_recv()

    def start(self):
        @pl.when(self.chip < self.chips - 1)
        def _():
            self.copy(0, self.chip, self.own).start()

        @pl.when(self.chip > 0)
        def _():
            self.copy(1, self.chip, self.own).start()

        self.copy(2, self.chip, self.own).start()
        self.keep().start()

    def keep(self):
        return pltpu.make_async_copy(self.own, self.place(self.chip, self.core), self.local)

    def step(self, number):
        left, right = self.chip - number, self.chip + number

        @pl.when(left >= 0)
        def _():
            self.wait_for(left, self.core)

            @pl.when(self.chip < self.chips - 1)
            def _():
                self.copy(0, left).start()

            self.copy(2, left).start()

        @pl.when(right < self.chips)
        def _():
            self.wait_for(right, self.core)

            @pl.when(self.chip > 0)
            def _():
                self.copy(1, right).start()

            self.copy(2, right).start()

    def finish(self):
        for chip in range(self.chips):
            self.wait_for(chip, 1 - self.core)
            self.copy(2, chip).wait_send()

            @pl.when((chip <= self.chip) & (self.chip < self.chips - 1))
            def _():
                self.copy(0, chip).wait_send()

            @pl.when((chip >= self.chip) & (self.chip > 0))
            def _():
                self.copy(1, chip).wait_send()

        self.keep().wait()


class PartExchange:
    @staticmethod
    def scratch():
        dma = pltpu.SemaphoreType.DMA
        return [dma((4,)), dma((4,)), dma((1,))]

    def __init__(self, parts, out, send, recv, local):
        self.parts, self.out, self.send, self.recv, self.local = parts, out, send, recv, local
        self.rank = lax.axis_index("seq")
        self.core, self.twin = line()[2], line()[5]
        self.others = [{"seq": lax.rem(self.rank + k, 4)} for k in range(1, 4)]
        self.rows = out.shape[2]

    def part(self, rank):
        return self.parts.at[pl.ds(pl.multiple_of((2 * rank + self.core) * self.rows, self.rows), self.rows)]

    def copy(self, index):
        if index == 3:
            source = target = self.out.at[self.core]
        else:
            source = self.part(lax.rem(self.rank + index + 1, 4))
            target = self.out.at[self.core, self.rank]
        return pltpu.make_async_remote_copy(
            src_ref=source,
            dst_ref=target,
            send_sem=self.send.at[index],
            recv_sem=self.recv.at[index],
            device_id=self.twin if index == 3 else self.others[index],
            device_id_type=MESH,
        )

    def keep(self):
        return pltpu.make_async_copy(self.part(self.rank), self.out.at[self.core, self.rank], self.local.at[0])

    def start(self):
        for index in (1, 0, 2):
            self.copy(index).start()
        self.keep().start()

    def relay(self):
        for index in range(3):
            self.copy(index).wait()
        self.keep().wait()
        self.copy(3).start()

    def end(self):
        self.copy(3).wait()


class Regroup:
    @staticmethod
    def scratch(rows, width):
        dma = pltpu.SemaphoreType.DMA
        return [pltpu.VMEM((4, rows, width), jnp.bfloat16), dma((7,)), dma((7,))]

    def __init__(self, piece, out, fours, send, recv):
        self.piece, self.out, self.fours, self.send, self.recv = piece, out, fours, send, recv
        self.rank, self.place = lax.axis_index("seq"), lax.axis_index("wshard")
        self.number = lax.rem(self.place, 4)
        self.others = [{"seq": lax.rem(self.rank + k, 4)} for k in range(1, 4)]
        self.along = [{"wshard": lax.rem(self.place + k, 8)} for k in range(1, 8)]

    def near(self, index):
        return pltpu.make_async_remote_copy(
            src_ref=self.piece,
            dst_ref=self.fours.at[self.rank],
            send_sem=self.send.at[index],
            recv_sem=self.recv.at[index],
            device_id=self.others[index],
            device_id_type=MESH,
        )

    def owner(self, rank):
        return 2 * rank + self.place // 4

    def far(self, rank, number):
        return pltpu.make_async_remote_copy(
            src_ref=self.fours.at[rank],
            dst_ref=self.out.at[number],
            send_sem=self.send.at[3 + rank],
            recv_sem=self.recv.at[3 + number],
            device_id={"wshard": self.owner(rank)},
            device_id_type=MESH,
        )

    def start(self):
        for index in range(3):
            self.near(index).start()
        self.fours[self.rank] = self.piece[...]

    def relay(self):
        for index in range(3):
            self.near(index).wait()
        for rank in range(4):

            @pl.when(self.owner(rank) != self.place)
            def _():
                self.far(rank, self.number).start()

            @pl.when(self.owner(rank) == self.place)
            def _():
                self.out[self.number] = self.fours[rank]

    def end(self):
        for rank in range(4):

            @pl.when(self.owner(rank) != self.place)
            def _():
                self.far(rank, self.number).wait_send()

        for number in range(4):

            @pl.when(4 * lax.rem(self.place, 2) + number != self.place)
            def _():
                self.far(0, number).wait_recv()


class Everywhere:
    def __init__(self, values, out, ranks, total, places, send, recv):
        self.values, self.out, self.ranks, self.total, self.places = values, out, ranks, total, places
        self.send, self.recv = send, recv
        self.groups, self.shards = ranks.shape[0], places.shape[0]
        self.rank, self.place = lax.axis_index("seq"), lax.axis_index("wshard")

    def others(self):
        return [{"seq": lax.rem(self.rank + k, self.groups)} for k in range(1, self.groups)]

    def along(self):
        return [{"wshard": lax.rem(self.place + k, self.shards)} for k in range(1, self.shards)]

    def start(self):
        self.first = [
            push(self.values, self.ranks.at[self.rank], self.send.at[k], self.recv.at[k], other)
            for k, other in enumerate(self.others())
        ]
        self.ranks[self.rank] = self.values[...]

    def relay(self):
        for copy in self.first:
            copy.wait()
        ranks, groups = self.ranks, self.groups
        self.total[...] = (ranks[0] + ranks[1]) + (ranks[2] + ranks[3])
        self.second = [
            push(self.total, self.places.at[self.place], self.send.at[groups + k], self.recv.at[groups + k], other)
            for k, other in enumerate(self.along())
        ]
        self.places[self.place] = self.total[...]

    def end(self):
        for copy in self.second:
            copy.wait()
        sums = [self.places[k] + self.places[k + 1] for k in range(0, self.shards, 2)]
        self.out[...] = (sums[0] + sums[1]) + (sums[2] + sums[3])


def last_gather(values, small, collective_id):
    count = len(values)
    groups = lax.axis_size("seq")
    shards = 2 * groups

    def body(*refs):
        own, small_ref = refs[:count], refs[count]
        full, small_out = refs[count + 1 : 2 * count + 1], refs[2 * count + 1]
        send, recv, local = refs[2 * count + 2 : 2 * count + 5]
        me, side, down, across = sides()
        total = Everywhere(small_ref, small_out, *refs[2 * count + 5 :])
        meet(*total.others(), *total.along())
        jobs = [SquareGather(own[i], full[i], send.at[i], recv.at[i]) for i in range(count)]
        total.start()
        keeps = []
        for i, job in enumerate(jobs):
            job.start()
            rows = own[i].shape[0]
            keep = pltpu.make_async_copy(
                own[i], full[i].at[pl.ds(pl.multiple_of(me * rows, rows), rows)], local.at[i]
            )
            keep.start()
            keeps.append(keep)
        total.relay()
        for job in jobs:
            job.relay()
        total.end()
        for job, keep in zip(jobs, keeps):
            job.near()
            job.far()
            job.finish()
            keep.wait()

    vmem = pl.BlockSpec(memory_space=pltpu.VMEM)
    dma = pltpu.SemaphoreType.DMA
    return pl.pallas_call(
        body,
        in_specs=[vmem] * (count + 1),
        out_specs=[pl.BlockSpec(memory_space=pl.ANY)] * count + [vmem],
        out_shape=[jax.ShapeDtypeStruct((4 * v.shape[0],) + v.shape[1:], v.dtype) for v in values]
        + [jax.ShapeDtypeStruct(small.shape, jnp.float32)],
        scratch_shapes=[
            dma((count, 6)),
            dma((count, 6)),
            dma((count,)),
            pltpu.VMEM((groups,) + small.shape, jnp.float32),
            pltpu.VMEM(small.shape, jnp.float32),
            pltpu.VMEM((shards,) + small.shape, jnp.float32),
            dma((groups + shards,)),
            dma((groups + shards,)),
        ],
        compiler_params=pltpu.CompilerParams(
            collective_id=collective_id, has_side_effects=True, vmem_limit_bytes=VMEM_LIMIT
        ),
        name="last_gather",
    )(*values, small)


def join_shares(every, gate, every_gate, every_up, down, out, columns, starts, forget_at, heads, part):
    groups, rows, lanes = every.shape
    units = every_gate.shape[2]
    own = heads // groups
    steps = 4
    tall = rows // steps

    def body(every_ref, gate_ref, wide_gate, wide_up, down_in, out_in, *outs):
        firsts = len(starts)
        for group in range(groups):
            to = slice(group * columns, (group + 1) * columns)
            for start, result in zip(starts, outs):
                result[:, to] = every_ref[group, :, start : start + columns].astype(jnp.float32)
            outs[firsts][:, to] = gate_ref[group].astype(jnp.float32)
            outs[firsts + 1][:, group * own : (group + 1) * own] = every_ref[
                group, :, forget_at : forget_at + own
            ].astype(jnp.float32)
            for source, result in ((wide_gate, outs[firsts + 2]), (wide_up, outs[firsts + 3])):
                for block in range(units // part):
                    at = (block * groups + group) * part
                    result[:, at : at + part] = source[group, :, block * part : (block + 1) * part].astype(
                        jnp.float32
                    )
        outs[firsts + 4][...] = down_in[...].astype(jnp.float32)
        outs[firsts + 5][...] = out_in[...].astype(jnp.float32)

    def flat(value):
        return pl.BlockSpec((value.shape[0] // steps, value.shape[1]), lambda i: (i, 0))

    def ranks(value):
        return pl.BlockSpec((groups, tall, value.shape[2]), lambda i: (0, i, 0))

    def shape(size):
        return jax.ShapeDtypeStruct(size, jnp.float32)

    results = [shape((rows, groups * columns))] * (len(starts) + 1) + [
        shape((rows, heads)),
        shape((rows, groups * units)),
        shape((rows, groups * units)),
        shape(down.shape),
        shape(out.shape),
    ]
    return pl.pallas_call(
        body,
        grid=(steps,),
        in_specs=[ranks(v) for v in (every, gate, every_gate, every_up)] + [flat(down), flat(out)],
        out_specs=[flat(value) for value in results],
        out_shape=results,
        compiler_params=pltpu.CompilerParams(vmem_limit_bytes=56 << 20),
        name="join_shares",
    )(every, gate, every_gate, every_up, down, out)


def norm_rows(values, gain):
    scale = lax.rsqrt(jnp.mean(values * values, axis=-1, keepdims=True) + EPS)
    return scale, values * scale * gain


def whole_forward(inputs, gain, cotangent, weights, forget, bias, length, block, w_gate, w_up,
                  head_size, scale, collective_id):
    rows, depth = inputs.shape
    groups = 4
    slots = groups * rows
    chips = groups
    shards = 2 * chips
    mine = weights[0].shape[0]
    columns = depth // groups
    front = 3 * columns + PAIR
    pairs = columns // PAIR
    part = w_gate.shape[1] // (groups * shards)
    units = shards * part
    early = units + units // 2
    low = jnp.bfloat16

    def body(inputs_ref, gain_ref, cot_ref, q_ref, k_ref, v_ref, og_ref, forget_ref, bias_ref, length_ref, block_ref,
             gate_ref, up_ref,
             normed_hbm, cot_full, full_front_hbm, full_gate_hbm, full_out_hbm, full_ffn, joined_hbm, attended_hbm,
             offset, col, logit, gate_pre_hbm, gated_hbm, middle, own_up,
             own_normed, own_front, own_gate, own_ffn, own_out, parts_out, own_cot, row, picks, cot_send, cot_recv, keep,
             x_send, x_recv, normed, full_front, full_gate, full_out, joined, attended, gate_pre, gated, store_sems,
             *scratch):
        store = Streams(store_sems)
        me, side, down, across = sides()
        line_chips, chip, core, forth, back, twin = line()
        halves = (pl.ds(0, 2 * columns), pl.ds(2 * columns, front - 2 * columns))
        first_line = LineGather(own_front.at[:, halves[0]], full_front.at[:, halves[0]], *scratch[0:3])
        second_line = LineGather(own_front.at[:, halves[1]], full_front.at[:, halves[1]], *scratch[22:25])
        gate_line = LineGather(own_gate, full_gate, *scratch[3:6])
        ffn_line = LineGather(own_ffn, full_ffn, *scratch[6:9])
        out_line = LineGather(own_out, parts_out, *scratch[9:12])
        exchange = PartExchange(parts_out, full_out, *scratch[12:15])
        job = SquareScatter([gated], [full_out_rows(full_out)], False, middle, *scratch[15:22])
        taken = []
        my_columns = pl.ds(pl.multiple_of(me * columns, columns), columns)
        for index, source in enumerate((q_ref, k_ref, v_ref)):
            taken.append((source.at[:, my_columns], own_front.at[:, pl.ds(index * columns, columns)]))
        taken.append((og_ref.at[:, my_columns], own_gate))
        tall = own_out.shape[0]
        taken.append((block_ref.at[pl.ds(pl.multiple_of(me * tall, tall), tall)], own_out))
        for index, source in enumerate((gate_ref, up_ref)):
            for number in range(shards):
                column = pl.ds(pl.multiple_of((number * groups + me) * part, part), part)
                to = index * units + number * part
                target = own_ffn.at[:, pl.ds(to, part)] if to < early else own_up.at[:, pl.ds(to - early, part)]
                taken.append((source.at[:, column], target))
        taken = [pltpu.make_async_copy(a, b, picks.at[i]) for i, (a, b) in enumerate(taken)]
        for copy in taken:
            copy.start()
        values = inputs_ref[...].astype(jnp.float32)
        own_normed[...] = norm_rows(values, gain_ref[...])[1].astype(low)
        own_front[:, 3 * columns :] = forget_ref[...]
        positions = me * rows + lax.broadcasted_iota(jnp.int32, (rows, depth), 0)
        own_cot[...] = jnp.where(positions < length_ref[:, :1], cot_ref[...], jnp.zeros((), low))
        meet(*exchange.others, forth, back, twin)
        one = SquareGather(own_normed, normed, x_send, x_recv)
        two = SquareGather(own_cot, cot_full, cot_send, cot_recv)
        one.start()
        for copy in taken:
            copy.wait()
        first_line.start()
        second_line.start()
        at_me = pl.ds(pl.multiple_of(me * rows, rows), rows)
        kept = pltpu.make_async_copy(own_cot, cot_full.at[at_me], keep.at[0])
        kept.start()
        normed[at_me, :] = own_normed[...]
        one.relay()
        two.start()
        first_line.step(1)
        second_line.step(1)
        first_line.step(2)
        second_line.step(2)
        one.near()
        one.far()
        first_line.step(3)
        second_line.step(3)
        store.start(normed, normed_hbm)
        out_line.start()
        gate_line.start()
        two.relay()
        first_line.finish()

        def product_of(columns_of_front):
            view = joined.at[:, columns_of_front]

            def store_joined(at_columns, value):
                view[:, at_columns] = value.astype(low)

            block_product(normed, full_front.at[:, columns_of_front], False, 256, store_joined)

        product_of(halves[0])
        second_line.finish()
        product_of(halves[1])
        store.start(full_front, full_front_hbm)
        one.finish()
        store.start(joined, joined_hbm)
        work = Forward(joined, bias_ref, length_ref, attended, offset, col, logit, row, head_size, scale)
        offset[...] = jnp.zeros_like(offset)
        out_line.step(1)
        gate_line.step(1)
        work.start()

        def step(pair, carry):
            work.pair(pair)

            @pl.when(pair == 0)
            def _():
                out_line.step(2)
                gate_line.step(2)

            @pl.when(pair == 1)
            def _():
                out_line.step(3)
                out_line.finish()
                exchange.start()
                gate_line.step(3)
                ffn_line.start()

            return carry

        lax.fori_loop(0, pairs, step, 0)
        store.start(attended, attended_hbm)
        gate_line.finish()
        store.start(full_gate, full_gate_hbm)

        def store_gate(at_columns, value):
            gate_pre[:, at_columns] = value

        block_product(normed, full_gate, False, PAIR, store_gate)
        gated[...] = (attended[...].astype(jnp.float32) * jax.nn.sigmoid(gate_pre[...])).astype(low)
        exchange.relay()
        store.start(gate_pre, gate_pre_hbm)
        store.start(gated, gated_hbm)
        exchange.end()
        store.start(full_out, full_out_hbm)
        job.begin()
        ffn_line.step(1)
        job.relay()
        job.own()
        two.near()
        two.far()
        two.finish()
        kept.wait()
        ffn_line.step(2)
        job.end()
        middle[...] += inputs_ref[...].astype(jnp.float32)
        ffn_line.step(3)
        ffn_line.finish()
        store.end()

    def shape(size, kind=low):
        return jax.ShapeDtypeStruct(size, kind)

    vmem = pl.BlockSpec(memory_space=pltpu.VMEM)
    anywhere = pl.BlockSpec(memory_space=pl.ANY)
    dma = pltpu.SemaphoreType.DMA
    results = [
        shape((slots, depth)),
        shape((slots, depth)),
        shape((depth, front)),
        shape((depth, columns)),
        shape((2, 4, block.shape[0] // 4, depth)),
        shape((depth, early)),
        shape((slots, front)),
        *Forward.results(slots, pairs),
        shape((slots, columns), jnp.float32),
        shape((slots, columns)),
        shape((rows, depth), jnp.float32),
        shape((mine, 2 * units - early)),
    ]
    kept_here = [results[i] for i in (0, 2, 3, 4, 6, 7, 11, 12)]
    return pl.pallas_call(
        body,
        in_specs=[vmem] * 3 + [anywhere] * 4 + [vmem] * 3 + [anywhere] * 3,
        out_specs=[anywhere] * 8 + [vmem] * 3 + [anywhere] * 2 + [vmem] * 2,
        out_shape=results,
        scratch_shapes=[
            pltpu.VMEM((rows, depth), low),
            pltpu.VMEM((mine, front), low),
            pltpu.VMEM((mine, columns), low),
            pltpu.VMEM((mine, early), low),
            pltpu.VMEM((block.shape[0] // 4, depth), low),
            pltpu.VMEM((shards * block.shape[0] // 4, depth), low),
            pltpu.VMEM((rows, depth), low),
            pltpu.VMEM((Forward.some, slots), jnp.float32),
            dma((5 + 2 * shards,)),
            dma((6,)),
            dma((6,)),
            dma((1,)),
            dma((6,)),
            dma((6,)),
            *(pltpu.VMEM(value.shape, value.dtype) for value in kept_here),
            dma((len(kept_here),)),
        ]
        + 4 * LineGather.scratch(chips)
        + PartExchange.scratch()
        + SquareScatter.scratch(rows, depth)
        + LineGather.scratch(chips),
        compiler_params=pltpu.CompilerParams(
            collective_id=collective_id, has_side_effects=True, vmem_limit_bytes=VMEM_LIMIT
        ),
        name="whole_forward",
    )(inputs, gain, cotangent, *weights, forget, bias, length, block, w_gate, w_up)


class full_out_rows:
    def __init__(self, ref):
        self.ref = ref
        self.shape = (ref.shape[0] * ref.shape[1] * ref.shape[2], ref.shape[3])

    def __getitem__(self, index):
        taken = self.ref[:, :, :, index[1]]
        return taken.reshape(self.shape[0], taken.shape[3])


def feed_forward(middle, gain, weights, own_up, own_down, cotangent, collective_id):
    rows, depth = middle.shape
    slots = 4 * rows
    units = 4 * own_down.shape[0] * 2
    early = weights.shape[1]
    chips = 4
    low = jnp.bfloat16

    def body(middle_ref, gain_ref, weights_hbm, up_ref, down_ref, cot_hbm,
             normed_hbm, hidden_hbm, full_up_hbm, full_down_hbm, grads_hbm, terms_hbm,
             own_normed, both, send, recv,
             weights_ref, cot_ref, normed, hidden, full_up, full_down, grads, terms, fetch_sems, store_sems, *scratch):
        fetch, store = Streams(fetch_sems), Streams(store_sems)
        weights_in = fetch.start(weights_hbm, weights_ref)
        cot_in = fetch.start(cot_hbm, cot_ref)
        me, side, down, across = sides()
        line_chips, chip, core, forth, back, twin = line()
        up_line = LineGather(up_ref, full_up, *scratch[:3])
        down_line = LineGather(down_ref, full_down, *scratch[3:])
        own_normed[...] = norm_rows(middle_ref[...], gain_ref[...])[1].astype(low)
        meet({"seq": side}, {"seq": down}, forth, back, twin)
        job = SquareGather(own_normed, normed, send, recv)
        up_line.start()
        down_line.start()
        job.start()

        def rows_of(rank):
            return pl.ds(pl.multiple_of(rank * rows, rows), rows)

        def multiply(rank):
            at = rows_of(rank)

            def store(columns, value):
                both[at, columns] = value

            block_product(normed.at[at], weights_ref, False, 512, store)

        normed[rows_of(me), :] = own_normed[...]
        weights_in.wait()
        multiply(me)
        up_line.step(1)
        job.relay()
        down_line.step(1)
        up_line.step(2)
        job.near()
        multiply(side)
        up_line.step(3)
        multiply(down)
        job.far()
        store.start(normed, normed_hbm)
        down_line.step(2)
        multiply(across)
        job.finish()
        up_line.finish()
        store.start(full_up, full_up_hbm)

        def ahead(number, carry):
            at = rows_of(number)
            both[at, early:] = product(normed[at, :], full_up[...])
            gate, upward = both[at, :units], both[at, units:]
            hidden[at, :] = (gate * jax.nn.sigmoid(gate) * upward).astype(low)
            return carry

        lax.fori_loop(0, 4, ahead, 0)
        store.start(hidden, hidden_hbm)
        down_line.step(3)
        cot_in.wait()
        transposed_product(hidden, cot_ref, terms)
        store.start(terms, terms_hbm)
        down_line.finish()
        store.start(full_down, full_down_hbm)

        def behind(number, carry):
            at = rows_of(number)
            grad_hidden = product_nt(cot_ref[at, :], full_down[...])
            gate, upward = both[at, :units], both[at, units:]
            sigma = jax.nn.sigmoid(gate)
            grads[at, :units] = (grad_hidden * upward * sigma * (1.0 + gate * (1.0 - sigma))).astype(low)
            grads[at, units:] = (grad_hidden * gate * sigma).astype(low)
            part(number).start()
            return carry

        def part(number):
            at = rows_of(number)
            return pltpu.make_async_copy(grads.at[at], grads_hbm.at[at], store_sems.at[5 + number])

        lax.fori_loop(0, 4, behind, 0)
        for number in range(4):
            part(number).wait()
        store.end()

    def shape(size, kind=low):
        return jax.ShapeDtypeStruct(size, kind)

    vmem = pl.BlockSpec(memory_space=pltpu.VMEM)
    anywhere = pl.BlockSpec(memory_space=pl.ANY)
    dma = pltpu.SemaphoreType.DMA
    results = [
        shape((slots, depth)),
        shape((slots, units)),
        shape((depth, own_up.shape[1])),
        shape((units, depth)),
        shape((slots, 2 * units)),
        shape((units, depth)),
    ]
    return pl.pallas_call(
        body,
        in_specs=[vmem, vmem, anywhere, vmem, vmem, anywhere],
        out_specs=[anywhere] * 6,
        out_shape=results,
        scratch_shapes=[
            pltpu.VMEM((rows, depth), low),
            pltpu.VMEM((slots, 2 * units), jnp.float32),
            dma((6,)),
            dma((6,)),
            *(pltpu.VMEM(value.shape, value.dtype) for value in (weights, cotangent, *results)),
            dma((2,)),
            dma((9,)),
        ]
        + 2 * LineGather.scratch(chips),
        compiler_params=pltpu.CompilerParams(
            collective_id=collective_id, has_side_effects=True, vmem_limit_bytes=VMEM_LIMIT
        ),
        name="feed_forward",
    )(middle, gain, weights, own_up, own_down, cotangent)


def feed_backward(grads, weights, up_weights, normed, terms_down, w_out, middle, gain, cotangent, attended, gate_pre,
                  collective_id):
    rows, depth = middle.shape
    slots = 4 * rows
    units = grads.shape[1] // 2
    early = weights.shape[1]
    columns = attended.shape[1]
    shards = 2 * lax.axis_size("seq")
    chips = shards // 2
    low = jnp.bfloat16

    def body(grads_hbm, weights_hbm, up_weights_hbm, normed_hbm, down_hbm, out_hbm, middle_hbm, gain_ref, cot_hbm,
             attended_hbm, pre_hbm,
             grad_middle_hbm, grad_gain, branch_hbm, d_attended, d_pre, terms_up_hbm, share_down, share_gate,
             own_branch, summed, terms_gate, send, recv,
             grads_ref, weights_ref, up_weights_ref, normed_ref, down_ref, out_ref, middle_ref, cot_ref,
             attended_ref, pre_ref, grad_middle, branch, terms_up, fetch_sems, store_sems, *scratch):
        fetch, store = Streams(fetch_sems), Streams(store_sems)
        own_rows = pl.ds(pl.multiple_of(lax.axis_index("seq") * rows, rows), rows)
        first_in = [
            fetch.start(*both)
            for both in (
                (down_hbm, down_ref),
                (grads_hbm, grads_ref),
                (weights_hbm, weights_ref),
                (up_weights_hbm, up_weights_ref),
            )
        ]
        normed_in = fetch.start(normed_hbm, normed_ref)
        rest_in = [
            fetch.start(*both)
            for both in (
                (middle_hbm, middle_ref),
                (cot_hbm.at[own_rows], cot_ref),
                (out_hbm, out_ref),
                (attended_hbm, attended_ref),
                (pre_hbm, pre_ref),
            )
        ]
        me, side, down, across = sides()
        line_chips, chip, core, forth, back, twin = line()
        meet({"seq": side}, {"seq": down}, forth, back, twin)
        first, second = grads_ref.at[:, pl.ds(0, units)], grads_ref.at[:, pl.ds(units, units)]
        job = SquareScatter(
            [grads_ref.at[:, pl.ds(0, early)], grads_ref.at[:, pl.ds(early, 2 * units - early)]],
            [weights_ref, up_weights_ref],
            True,
            summed,
            *scratch[:7],
        )
        run_down = LineScatter(down_ref, share_down, *scratch[7:12])
        run_gate = LineScatter(terms_gate, share_gate, *scratch[12:])
        every = SquareGather(own_branch, branch, send, recv)
        first_in[0].wait()
        run_down.start()
        for copy in first_in[1:]:
            copy.wait()
        job.begin_far()
        run_down.slot(0)
        job.begin_near()
        normed_in.wait()
        transposed_product(normed_ref, first, terms_gate)
        run_gate.start()
        job.relay()
        run_down.slot(1)
        run_gate.slot(0)
        job.own()
        transposed_product(normed_ref, second, terms_up)
        store.start(terms_up, terms_up_hbm)
        run_down.slot(2)
        for copy in rest_in:
            copy.wait()
        job.end()
        values, change = middle_ref[...], summed[...]
        scale = norm_rows(values, gain_ref[...])[0]
        grad_gain[...] = jnp.sum(change * values * scale, axis=0, keepdims=True)
        change = change * gain_ref[...]
        mean = jnp.mean(change * values, axis=-1, keepdims=True)
        total = cot_ref[...].astype(jnp.float32) + scale * change - values * (scale * scale * scale * mean)
        grad_middle[...] = total
        own_branch[...] = total.astype(low)
        every.start()
        store.start(grad_middle, grad_middle_hbm)

        def rows_of(rank):
            return pl.ds(pl.multiple_of(rank * rows, rows), rows)

        def multiply(rank):
            at = rows_of(rank)
            grad_gated = product_nt(branch[at, :], out_ref[...])
            sigma = jax.nn.sigmoid(pre_ref[at, :])
            d_attended[at, :] = (grad_gated * sigma).astype(low)
            d_pre[at, :] = (
                grad_gated * attended_ref[at, :].astype(jnp.float32) * sigma * (1.0 - sigma)
            ).astype(low)

        branch[rows_of(me), :] = own_branch[...]
        multiply(me)
        run_gate.slot(1)
        every.relay()
        run_gate.slot(2)
        every.near()
        multiply(side)
        multiply(down)
        run_down.end()
        every.far()
        store.start(branch, branch_hbm)
        multiply(across)
        every.finish()
        run_gate.end()
        store.end()

    def shape(size, kind=low):
        return jax.ShapeDtypeStruct(size, kind)

    vmem = pl.BlockSpec(memory_space=pltpu.VMEM)
    anywhere = pl.BlockSpec(memory_space=pl.ANY)
    dma = pltpu.SemaphoreType.DMA
    own_shape = jax.ShapeDtypeStruct((rows, depth), low)
    fetched = (grads, weights, up_weights, normed, terms_down, w_out, middle, own_shape, attended, gate_pre)
    return pl.pallas_call(
        body,
        in_specs=[anywhere] * 7 + [vmem] + [anywhere] * 3,
        out_specs=[anywhere, vmem, anywhere, vmem, vmem, anywhere, vmem, vmem],
        out_shape=[
            shape((rows, depth), jnp.float32),
            shape((1, depth), jnp.float32),
            shape((slots, depth)),
            shape((slots, columns)),
            shape((slots, columns)),
            shape((depth, units)),
            shape((terms_down.shape[0] // shards, depth)),
            shape((depth // shards, units)),
        ],
        scratch_shapes=[
            pltpu.VMEM((rows, depth), low),
            pltpu.VMEM((rows, depth), jnp.float32),
            pltpu.VMEM((depth, units), low),
            dma((6,)),
            dma((6,)),
            *(pltpu.VMEM(value.shape, value.dtype) for value in fetched),
            pltpu.VMEM((rows, depth), jnp.float32),
            pltpu.VMEM((slots, depth), low),
            pltpu.VMEM((depth, units), low),
            dma((len(fetched),)),
            dma((3,)),
        ]
        + SquareScatter.scratch(rows, depth)
        + LineScatter.scratch(chips, terms_down.shape[0] // shards, depth)
        + LineScatter.scratch(chips, depth // shards, units),
        compiler_params=pltpu.CompilerParams(
            collective_id=collective_id, has_side_effects=True, vmem_limit_bytes=VMEM_LIMIT
        ),
        name="feed_backward",
    )(grads, weights, up_weights, normed, terms_down, w_out, middle, gain, cotangent, attended, gate_pre)


class SquareScatter:
    @staticmethod
    def scratch(rows, width):
        half = rows // 2
        low = jnp.bfloat16
        return [
            pltpu.VMEM((rows, width), low),
            pltpu.VMEM((2, half, width), low),
            pltpu.VMEM((2, half, width), jnp.float32),
            pltpu.VMEM((6, half, width), low),
            pltpu.VMEM((2, half, width), low),
            pltpu.SemaphoreType.DMA((6,)),
            pltpu.SemaphoreType.DMA((6,)),
        ]

    def __init__(self, lefts, rights, transposed, out, far, near, kept, land, carry, send, recv):
        self.lefts, self.rights, self.transposed, self.out = lefts, rights, transposed, out
        self.far, self.near, self.kept, self.land, self.carry = far, near, kept, land, carry
        self.send, self.recv = send, recv
        self.rows, self.width = out.shape
        self.half = self.rows // 2
        self.tile = self.width // 3 if self.width % 384 == 0 else self.width

    def copy(self, index):
        me, side, down, across = sides()
        source = (
            self.far.at[pl.ds(0, self.half)],
            self.far.at[pl.ds(self.half, self.half)],
            self.near.at[0],
            self.near.at[1],
            self.carry.at[0],
            self.carry.at[1],
        )[index]
        return pltpu.make_async_remote_copy(
            src_ref=source,
            dst_ref=self.land.at[index],
            send_sem=self.send.at[index],
            recv_sem=self.recv.at[index],
            device_id={"seq": down if index in (0, 3, 5) else side},
            device_id_type=MESH,
        )

    def partial(self, rank, store):
        at = pl.ds(pl.multiple_of(rank * self.rows, self.rows), self.rows)

        def step(number, carried):
            columns = pl.ds(pl.multiple_of(number * self.tile, self.tile), self.tile)
            value = None
            for a, b in zip(self.lefts, self.rights):
                if self.transposed:
                    term = product_nt(a[at, :], b[columns, :])
                else:
                    term = product(a[at, :], b[:, columns])
                value = term if value is None else value + term
            store(columns, value)
            return carried

        lax.fori_loop(0, self.width // self.tile, step, 0)

    def begin(self):
        self.begin_far()
        self.begin_near()

    def begin_far(self):
        me, side, down, across = sides()
        far = self.far

        def store_far(columns, value):
            far[:, columns] = value.astype(far.dtype)

        self.partial(across, store_far)
        self.copy(0).start()
        self.copy(1).start()

    def begin_near(self):
        me, side, down, across = sides()
        half, near, kept = self.half, self.near, self.kept

        def store_side(columns, value):
            kept[0, :, columns] = value[:half]
            near[0, :, columns] = value[half:].astype(near.dtype)

        def store_down(columns, value):
            near[1, :, columns] = value[:half].astype(near.dtype)
            kept[1, :, columns] = value[half:]

        self.partial(side, store_side)
        self.copy(2).start()
        self.partial(down, store_down)
        self.copy(3).start()

    def relay(self):
        for index in (0, 1):
            self.copy(index).wait_recv()

            def add(at, index=index):
                total = self.kept[index, at, :] + self.land[index, at, :].astype(jnp.float32)
                self.carry[index, at, :] = total.astype(self.carry.dtype)

            by_rows(self.half, add)
            self.copy(4 + index).start()

    def own(self):
        out = self.out

        def store_own(columns, value):
            out[:, columns] = value

        self.partial(lax.axis_index("seq"), store_own)

    def end(self):
        for index in (2, 3, 4, 5):
            self.copy(index).wait_recv()
        land, half, out = self.land, self.half, self.out

        def add(at):
            out[at, :] += land[3, at, :].astype(jnp.float32) + land[4, at, :].astype(jnp.float32)

        def add_second(at):
            to = pl.ds(at.start + half, at.size)
            out[to, :] += land[2, at, :].astype(jnp.float32) + land[5, at, :].astype(jnp.float32)

        by_rows(half, add)
        by_rows(half, add_second)
        for index in range(6):
            self.copy(index).wait_send()


class LineScatter:
    @staticmethod
    def scratch(chips, rows, width):
        low = jnp.bfloat16
        dma = pltpu.SemaphoreType.DMA
        return [pltpu.VMEM((chips, rows, width), low)] * 3 + [dma((2, chips)), dma((3, chips))]

    def __init__(self, terms, out, twin_in, forth_in, back_in, send, recv):
        self.terms, self.out, self.twin_in = terms, out, twin_in
        self.forth_in, self.back_in, self.send, self.recv = forth_in, back_in, send, recv
        self.chips, self.chip, self.core, *self.devices = line()
        self.rows = twin_in.shape[1]

    def term(self, chip, core):
        return self.terms.at[pl.ds(pl.multiple_of((2 * chip + core) * self.rows, self.rows), self.rows)]

    def swap(self, chip):
        return pltpu.make_async_remote_copy(
            src_ref=self.term(chip, 1 - self.core),
            dst_ref=self.twin_in.at[chip],
            send_sem=self.send.at[0, chip],
            recv_sem=self.recv.at[0, chip],
            device_id=self.devices[2],
            device_id_type=MESH,
        )

    def hop(self, way, chip):
        return pltpu.make_async_remote_copy(
            src_ref=self.twin_in.at[chip],
            dst_ref=(self.forth_in, self.back_in)[way].at[chip],
            send_sem=self.send.at[1, chip],
            recv_sem=self.recv.at[1 + way, chip],
            device_id=self.devices[way],
            device_id_type=MESH,
        )

    def start(self):
        for chip in (self.chips - 1, 0, *range(1, self.chips - 1)):
            self.swap(chip).start()

    def add(self, chip, ways, out):
        def step(at):
            start = pl.multiple_of((2 * chip + self.core) * self.rows + at.start, at.size)
            total = self.terms[pl.ds(start, at.size), :].astype(jnp.float32)
            total = total + self.twin_in[chip, at, :].astype(jnp.float32)
            for way in ways:
                total = total + (self.forth_in, self.back_in)[way][chip, at, :].astype(jnp.float32)
            out[at, :] = total.astype(out.dtype)

        by_rows(self.rows, step)

    def pass_on(self, way, chip, first):
        self.swap(chip).wait_recv()
        if not first:
            self.hop(way, chip).wait_recv()
        self.add(chip, () if first else (way,), self.twin_in.at[chip])
        self.hop(way, chip).start()

    def slot(self, number):
        last = self.chips - 1
        for chip in range(self.chips):
            forth, back = number - (last - chip), last - (number - chip)
            if 0 <= forth < chip:

                @pl.when(self.chip == forth)
                def _():
                    self.pass_on(0, chip, forth == 0)

            if chip < back <= last:

                @pl.when(self.chip == back)
                def _():
                    self.pass_on(1, chip, back == last)

    def end(self):
        for chip in range(self.chips):

            @pl.when(self.chip == chip)
            def _():
                self.swap(chip).wait_recv()
                ways = [way for way, there in enumerate((chip > 0, chip < self.chips - 1)) if there]
                for way in ways:
                    self.hop(way, chip).wait_recv()
                self.add(chip, ways, self.out)

            self.swap(chip).wait_send()

            @pl.when(self.chip != chip)
            def _():
                self.hop(0, chip).wait_send()


def middle_backward(joined, d_out, offset, col, logit, hidden, w_down, gated, grad_branch, terms_up, shares,
                    normed, d_pre, middle, head_size, scale, collective_id):
    slots, lanes = joined.shape
    width = w_down.shape[1]
    tokens = slots // 4
    columns = gated.shape[1]
    shards = 2 * lax.axis_size("seq")
    chips = shards // 2
    rows_up = terms_up.shape[0] // shards
    fetched = (terms_up, hidden, w_down, gated, grad_branch, normed, d_pre, joined, d_out, middle)

    def body(*refs):
        sources, refs = refs[:10], refs[10:]
        (offset_ref, col_ref, logit_ref, *share_refs), refs = refs[:5], refs[5:]
        (grads, bias_grad, layer_output, collected, share_up, share_pre, *every_refs), refs = refs[:8], refs[8:]
        buffers, refs = refs[:10], refs[10:]
        terms, terms_pre, lowered, send, recv, keep, fetch_sems, *scratch = refs
        up_ref, hidden_ref, down_ref, gated_ref, branch_ref, normed_ref, pre_ref, joined_ref, d_out_ref = buffers[:9]
        fetch = Streams(fetch_sems)
        comes = [fetch.start(source, buffer) for source, buffer in zip(sources, buffers)]
        me, side, down, across = sides()
        line_chips, chip, core, forth, back, twin = line()
        meet({"seq": side}, {"seq": down}, forth, back, twin)
        work = Backward(
            joined_ref, d_out_ref, offset_ref, col_ref, logit_ref, grads, *scratch[:4], head_size, scale
        )
        job = SquareScatter([hidden_ref], [down_ref], False, lowered, *scratch[4:11])
        collect = LineScatter(terms, collected, *scratch[11:16])
        run = LineScatter(up_ref, share_up, *scratch[16:21])
        run_pre = LineScatter(terms_pre, share_pre, *scratch[21:])
        every = [SquareGather(share_refs[i], every_refs[i], send.at[i], recv.at[i]) for i in range(2)]
        every[0].start()
        comes[0].wait()
        run.start()
        kept = []
        for i in range(2):
            size = share_refs[i].shape[0]
            kept.append(
                pltpu.make_async_copy(
                    share_refs[i],
                    every_refs[i].at[pl.ds(pl.multiple_of(me * size, size), size)],
                    keep.at[i],
                )
            )
            kept[i].start()
        comes[1].wait()
        comes[2].wait()
        job.begin()
        run.slot(0)
        comes[3].wait()
        comes[4].wait()
        transposed_product(gated_ref, branch_ref, terms)
        collect.start()
        comes[5].wait()
        comes[6].wait()
        transposed_product(normed_ref, pre_ref, terms_pre)
        run_pre.start()
        collect.slot(0)
        for copy in comes[7:]:
            copy.wait()
        run_pre.slot(0)
        work.start()

        def step(pair, carry):
            work.pair(pair)

            @pl.when(pair == 0)
            def _():
                run.slot(1)
                job.relay()
                every[0].relay()
                every[1].start()
                collect.slot(1)
                run_pre.slot(1)

            @pl.when(pair == 1)
            def _():
                run.slot(2)
                collect.slot(2)
                run_pre.slot(2)
                every[1].relay()

            return carry

        lax.fori_loop(0, work.pairs, step, 0)
        job.own()
        work.end(bias_grad)
        job.end()
        layer_output[...] = (buffers[9][...] + lowered[...]).astype(layer_output.dtype)
        run.end()
        collect.end()
        run_pre.end()
        for gathering, copy in zip(every, kept):
            gathering.near()
            gathering.far()
            gathering.finish()
            copy.wait()

    vmem = pl.BlockSpec(memory_space=pltpu.VMEM)
    anywhere = pl.BlockSpec(memory_space=pl.ANY)
    low = jnp.bfloat16
    dma = pltpu.SemaphoreType.DMA
    return pl.pallas_call(
        body,
        in_specs=[anywhere] * 10 + [vmem] * 5,
        out_specs=[vmem] * 6 + [anywhere] * 2,
        out_shape=[
            jax.ShapeDtypeStruct((slots, lanes), low),
            jax.ShapeDtypeStruct((8, PAIR), jnp.float32),
            jax.ShapeDtypeStruct((tokens, width), low),
            jax.ShapeDtypeStruct((columns // shards, width), low),
            jax.ShapeDtypeStruct((rows_up, terms_up.shape[1]), low),
            jax.ShapeDtypeStruct((rows_up, columns), low),
            *(jax.ShapeDtypeStruct((4 * v.shape[0], v.shape[1]), low) for v in shares),
        ],
        scratch_shapes=[
            *(pltpu.VMEM(value.shape, value.dtype) for value in fetched),
            pltpu.VMEM((columns, width), low),
            pltpu.VMEM((width, columns), low),
            pltpu.VMEM((tokens, width), jnp.float32),
            dma((2, 6)),
            dma((2, 6)),
            dma((2,)),
            dma((10,)),
        ]
        + backward_scratch(slots)
        + SquareScatter.scratch(tokens, width)
        + LineScatter.scratch(chips, columns // shards, width)
        + LineScatter.scratch(chips, rows_up, terms_up.shape[1])
        + LineScatter.scratch(chips, rows_up, columns),
        compiler_params=pltpu.CompilerParams(
            collective_id=collective_id, has_side_effects=True, vmem_limit_bytes=VMEM_LIMIT
        ),
        name="middle_backward",
    )(*fetched, offset, col, logit, *shares)


def last_backward(grads, d_pre, normed, weights, gate_weights, collected, shares, inputs, gain, grad_middle,
                  collective_id):
    slots, depth = normed.shape
    front = grads.shape[1]
    tokens = slots // 4
    shards = 2 * lax.axis_size("seq")
    rows = depth // shards
    fetched = (normed, grads, d_pre, weights, gate_weights, inputs, grad_middle)

    def body(*refs):
        sources, refs = refs[:7], refs[7:]
        (collected_ref, gain_ref, *share_refs), refs = refs[:4], refs[4:]
        (grad_input, grad_gain, share, regrouped, *every_refs), refs = refs[:6], refs[6:]
        buffers, refs = refs[:7], refs[7:]
        terms, summed, send, recv, keep, fetch_sems, *scratch = refs
        normed_ref, grads_ref, pre_ref, weights_ref, gate_weights_ref, inputs_ref, middle_ref = buffers
        fetch = Streams(fetch_sems)
        comes = [fetch.start(source, buffer) for source, buffer in zip(sources, buffers)]
        me, side, down, across = sides()
        regroup = Regroup(collected_ref, regrouped, *scratch[12:])
        meet(*regroup.others, *regroup.along)
        job = SquareScatter([grads_ref, pre_ref], [weights_ref, gate_weights_ref], True, summed, *scratch[:7])
        run = LineScatter(terms, share, *scratch[7:12])
        regroup.start()
        every = [SquareGather(share_refs[i], every_refs[i], send.at[i], recv.at[i]) for i in range(2)]
        every[0].start()
        kept = []
        for i in range(2):
            size = share_refs[i].shape[0]
            kept.append(
                pltpu.make_async_copy(
                    share_refs[i],
                    every_refs[i].at[pl.ds(pl.multiple_of(me * size, size), size)],
                    keep.at[i],
                )
            )
            kept[i].start()
        comes[0].wait()
        comes[1].wait()
        transposed_product(normed_ref, grads_ref, terms)
        run.start()
        every[0].relay()
        regroup.relay()
        run.slot(0)
        for copy in comes[2:]:
            copy.wait()
        job.begin()
        every[1].start()
        job.relay()
        run.slot(1)
        job.own()
        every[1].relay()
        run.slot(2)
        job.end()
        values, change = inputs_ref[...].astype(jnp.float32), summed[...]
        scale = norm_rows(values, gain_ref[...])[0]
        grad_gain[...] = jnp.sum(change * values * scale, axis=0, keepdims=True)
        change = change * gain_ref[...]
        mean = jnp.mean(change * values, axis=-1, keepdims=True)
        grad_input[...] = middle_ref[...] + scale * change - values * (scale * scale * scale * mean)
        for gathering, copy in zip(every, kept):
            gathering.near()
            gathering.far()
            gathering.finish()
            copy.wait()
        regroup.end()
        run.end()

    vmem = pl.BlockSpec(memory_space=pltpu.VMEM)
    anywhere = pl.BlockSpec(memory_space=pl.ANY)
    low = jnp.bfloat16
    dma = pltpu.SemaphoreType.DMA
    return pl.pallas_call(
        body,
        in_specs=[anywhere] * 7 + [vmem] * 4,
        out_specs=[vmem] * 4 + [anywhere] * 2,
        out_shape=[
            jax.ShapeDtypeStruct((tokens, depth), jnp.float32),
            jax.ShapeDtypeStruct((1, depth), jnp.float32),
            jax.ShapeDtypeStruct((rows, front), low),
            jax.ShapeDtypeStruct((4,) + collected.shape, low),
            *(jax.ShapeDtypeStruct((4 * v.shape[0], v.shape[1]), low) for v in shares),
        ],
        scratch_shapes=[
            *(pltpu.VMEM(value.shape, value.dtype) for value in fetched),
            pltpu.VMEM((depth, front), low),
            pltpu.VMEM((tokens, depth), jnp.float32),
            dma((2, 6)),
            dma((2, 6)),
            dma((2,)),
            dma((7,)),
        ]
        + SquareScatter.scratch(tokens, depth)
        + LineScatter.scratch(shards // 2, rows, front)
        + Regroup.scratch(*collected.shape),
        compiler_params=pltpu.CompilerParams(
            collective_id=collective_id, has_side_effects=True, vmem_limit_bytes=VMEM_LIMIT
        ),
        name="last_backward",
    )(*fetched, collected, gain, *shares)


def gather(value, axis_name):
    return lax.all_gather(value, axis_name, axis=0, tiled=True)


def scatter(value, axis_name):
    return lax.psum_scatter(value, axis_name, scatter_dimension=0, tiled=True)


def on_device(
    layer_input,
    lengths,
    norm_attn,
    w_query,
    w_key,
    w_value,
    w_ogate,
    w_forget,
    forget_bias,
    w_out,
    norm_ffn,
    w_gate,
    w_up,
    w_down,
    output_grad,
):
    low = jnp.bfloat16
    tokens, width = layer_input.shape[1:]
    heads = forget_bias.shape[0]
    groups = lax.axis_size("seq")
    shards = lax.axis_size("wshard")
    fast = square(groups) and shards == 2 * groups
    local_heads = heads // groups
    head_size = width // heads
    columns = width // groups
    lanes = columns + -columns % PAIR
    front = 3 * lanes + PAIR
    slots = tokens * groups
    hidden_size = w_gate.shape[1]
    part = hidden_size // (groups * shards)
    units = shards * part
    scale = head_size ** (-0.5)
    length = lengths[0]
    seq_rank = lax.axis_index("seq")
    shard_rank = lax.axis_index("wshard")
    per_block = shards // groups
    positions = seq_rank * tokens + jnp.arange(tokens, dtype=jnp.int32)
    valid_slots = (positions < length)[:, None]
    inputs = layer_input[0].astype(jnp.float32)
    cotangent_low = jnp.where(valid_slots, output_grad[0], jnp.zeros((), low))
    cotangent = cotangent_low.astype(jnp.float32)

    def own_columns(weight, size):
        taken = lax.dynamic_slice_in_dim(weight, seq_rank * columns, columns, 1)
        return jnp.pad(taken, ((0, 0), (0, size - columns))) if size > columns else taken

    def own_units(weight):
        split = weight.reshape(weight.shape[0], shards, groups, part)
        mine = lax.dynamic_index_in_dim(split, seq_rank, 2, keepdims=False)
        return mine.reshape(weight.shape[0], units)

    own_forget = lax.dynamic_slice_in_dim(w_forget, seq_rank * local_heads, local_heads, 1)
    own_forget = jnp.pad(own_forget, ((0, 0), (0, PAIR - local_heads)))
    own_bias = lax.dynamic_slice_in_dim(forget_bias, seq_rank * local_heads, local_heads)
    own_bias = jnp.pad(own_bias, (0, PAIR - local_heads))[None]
    length_row = jnp.broadcast_to(lengths[:, None], (1, PAIR))
    mine_down = lax.dynamic_slice_in_dim(w_down, seq_rank * part, part, 0)
    if fast:
        (
            normed_attn, cotangent_all, full_front, full_ogate, full_out, full_ffn,
            joined, attended_low, offset, col, logit, gate_pre, gated, middle, mine_up,
        ) = whole_forward(
            layer_input[0], norm_attn[None], output_grad[0], (w_query, w_key, w_value, w_ogate), own_forget,
            own_bias, length_row, w_out, w_gate, w_up, head_size, scale, 0,
        )
        full_out = full_out.reshape(columns, width)
        normed_ffn, hidden, full_up, full_down, grad_gate_up, terms_down = feed_forward(
            middle, norm_ffn[None], full_ffn, mine_up, mine_down, cotangent_all, 1
        )
        (
            grad_middle, grad_norm_ffn, grad_branch, grad_attended, grad_gate_pre, terms_up, share_down, share_gate,
        ) = feed_backward(
            grad_gate_up, full_ffn, full_up, normed_ffn, terms_down, full_out, middle, norm_ffn[None],
            cotangent_all, attended_low, gate_pre, 2,
        )
        grad_norm_ffn = grad_norm_ffn[0]
        grads, bias_rows, layer_output, collected, share_up, share_ogate, grad_down, every_gate = middle_backward(
            joined, grad_attended, offset, col, logit, hidden, full_down, gated, grad_branch, terms_up,
            (share_down, share_gate), normed_attn, grad_gate_pre, middle, head_size, scale, 3,
        )
        grad_input, grad_norm_attn, share_attn, grad_out, every_ogate, every_up = last_backward(
            grads, grad_gate_pre, normed_attn, full_front, full_ogate, collected, (share_ogate, share_up),
            layer_input[0], norm_attn[None], grad_middle, 4,
        )
        grad_norm_attn = grad_norm_attn[0]
        grad_out = grad_out.reshape(columns // per_block, width)
    else:
        mine_front = jnp.concatenate(
            [*(own_columns(w, lanes) for w in (w_query, w_key, w_value)), own_forget], axis=1
        )
        full_front = gather(mine_front, "wshard")
        full_ogate = gather(own_columns(w_ogate, columns), "wshard")
        normed_attn = gather(rms_norm(inputs, norm_attn).astype(low), "seq")
        cotangent_all = gather(cotangent_low, "seq")
        full_out = lax.dynamic_slice_in_dim(gather(w_out, "wshard"), seq_rank * columns, columns, 0)
        full_ffn = gather(jnp.concatenate([own_units(w_gate), own_units(w_up)], axis=1), "wshard")
        joined = product(normed_attn, full_front).astype(low)
        gate_pre = product(normed_attn, full_ogate)
        attended_low, offset, col, logit = attention_fwd(joined, own_bias, length_row, head_size, scale)
        attended = attended_low[:, :columns].astype(jnp.float32)
        gated_full, pull_gate = jax.vjp(gate_product, attended, gate_pre)
        gated = gated_full.astype(low)
        middle = inputs + scatter(product(gated, full_out).astype(low), "seq").astype(jnp.float32)
        normed_ffn_own, pull_ffn_norm = jax.vjp(rms_norm, middle, norm_ffn)
        full_down = gather(mine_down, "wshard")
        normed_ffn = gather(normed_ffn_own.astype(low), "seq")
        gate_up = product(normed_ffn, full_ffn)
        hidden_full, pull_swiglu = jax.vjp(swiglu, gate_up[:, :units], gate_up[:, units:])
        hidden = hidden_full.astype(low)
        grad_hidden = product_nt(cotangent_all, full_down)
        grad_gate_full, grad_up_full = pull_swiglu(grad_hidden)
        grad_gate_up = jnp.concatenate([grad_gate_full.astype(low), grad_up_full.astype(low)], axis=1)
        share_down = scatter(product_tn(hidden, cotangent_all).astype(low), "wshard")
        share_ffn = scatter(product_tn(normed_ffn, grad_gate_up).astype(low), "wshard")
        grad_normed_ffn = scatter(product_nt(grad_gate_up, full_ffn).astype(low), "seq").astype(jnp.float32)
        grad_middle_part, grad_norm_ffn = pull_ffn_norm(grad_normed_ffn)
        grad_middle = cotangent + grad_middle_part
        grad_branch = gather(grad_middle.astype(low), "seq")
        grad_attended_full, grad_gate_pre_full = pull_gate(product_nt(grad_branch, full_out))
        grad_attended = grad_attended_full.astype(low)
        grad_gate_pre = grad_gate_pre_full.astype(low)
        if lanes > columns:
            grad_attended = jnp.pad(grad_attended, ((0, 0), (0, lanes - columns)))
        grads, bias_rows = attention_bwd(joined, grad_attended, offset, col, logit, head_size, scale)
        grad_projected = jnp.concatenate([grads, grad_gate_pre], axis=1)
        share_attn = scatter(product_tn(normed_attn, grad_projected).astype(low), "wshard")
        full_attn = jnp.concatenate([full_front, full_ogate], axis=1)
        grad_normed_attn = scatter(product_nt(grad_projected, full_attn).astype(low), "seq").astype(jnp.float32)
        lowered = scatter(product(hidden, full_down).astype(low), "seq").astype(jnp.float32)
        share_out = scatter(product_tn(gated, grad_branch).astype(low), "wshard")
        rows_out = columns // shards
        pieces_out = lax.all_gather(share_out, "seq", axis=0, tiled=False)
        takes = shards // per_block
        slots_out = jnp.where(
            (jnp.arange(per_block) == shard_rank // takes)[None, :, None, None],
            pieces_out[:, None],
            jnp.zeros((), low),
        ).reshape(shards, rows_out, width)
        moved = lax.all_to_all(slots_out, "wshard", split_axis=0, concat_axis=0, tiled=True)
        moved = moved.reshape(per_block, takes, rows_out, width)
        mine_out = lax.dynamic_index_in_dim(moved, shard_rank % per_block, 0, keepdims=False)
        grad_out = mine_out.reshape(columns // per_block, width).astype(jnp.float32)
        layer_output = (middle + lowered).astype(low)
        unused_normed, pull_attn_norm = jax.vjp(rms_norm, inputs, norm_attn)
        grad_input_part, grad_norm_attn = pull_attn_norm(grad_normed_attn)
        grad_input = grad_middle + grad_input_part
    grad_bias = lax.dynamic_update_slice_in_dim(
        jnp.zeros((heads,), jnp.float32), bias_rows[:local_heads, 0], seq_rank * local_heads, 0
    )

    rows = share_attn.shape[0]
    if fast:
        vector = jnp.concatenate([grad_norm_attn, grad_norm_ffn, grad_bias])
        vector = jnp.pad(vector, (0, -vector.shape[0] % 1024)).reshape(-1, 128)
        every_attn, vector = last_gather([share_attn], vector, 5)
        vector = vector.reshape(-1)
        small = vector[:width], vector[width : 2 * width], vector[2 * width : 2 * width + heads]
    else:
        every_attn, every_ffn, grad_down = [gather(v, "seq") for v in (share_attn, share_ffn, share_down)]
        small = lax.psum((grad_norm_attn, grad_norm_ffn, grad_bias), ("seq", "wshard"))
    every_attn = every_attn.reshape((groups,) + share_attn.shape)
    if fast:
        *weight_grads, grad_forget_w, grad_w_gate, grad_w_up, grad_down, grad_out = join_shares(
            every_attn,
            every_ogate.reshape((groups,) + share_ogate.shape),
            every_gate.reshape((groups,) + share_gate.shape),
            every_up.reshape((groups,) + share_up.shape),
            grad_down,
            grad_out,
            columns,
            (0, lanes, 2 * lanes),
            3 * lanes,
            heads,
            part,
        )
    else:

        def join(first):
            taken = every_attn[:, :, first : first + columns]
            return taken.transpose(1, 0, 2).reshape(rows, width).astype(jnp.float32)

        def join_own_units(first):
            taken = every_ffn.reshape((groups,) + share_ffn.shape)[:, :, first * units : (first + 1) * units]
            taken = taken.reshape(groups, rows, shards, part).transpose(1, 2, 0, 3)
            return taken.reshape(rows, hidden_size).astype(jnp.float32)

        weight_grads = [join(first) for first in (0, lanes, 2 * lanes, front)]
        grad_w_gate, grad_w_up = join_own_units(0), join_own_units(1)
        grad_down = grad_down.astype(jnp.float32)
        grad_forget_w = every_attn[:, :, 3 * lanes : 3 * lanes + local_heads]
        grad_forget_w = grad_forget_w.transpose(1, 0, 2).reshape(rows, heads).astype(jnp.float32)
    return (
        layer_output[None],
        grad_input[None],
        small[0],
        *weight_grads,
        grad_forget_w,
        small[2],
        grad_out,
        small[1],
        grad_w_gate,
        grad_w_up,
        grad_down,
    )


def solution(mesh):
    return jax.shard_map(
        on_device,
        mesh=mesh,
        in_specs=(
            P("wshard", "seq", None),
            P("wshard"),
            P(),
            P("wshard", None),
            P("wshard", None),
            P("wshard", None),
            P("wshard", None),
            P("wshard", None),
            P(),
            P("wshard", None),
            P(),
            P("wshard", None),
            P("wshard", None),
            P("wshard", None),
            P("wshard", "seq", None),
        ),
        out_specs=(
            P("wshard", "seq", None),
            P("wshard", "seq", None),
            P(),
            P("wshard", None),
            P("wshard", None),
            P("wshard", None),
            P("wshard", None),
            P("wshard", None),
            P(),
            P("wshard", None),
            P(),
            P("wshard", None),
            P("wshard", None),
            P("wshard", None),
        ),
        check_vma=False,
    )
```

```python
import jax
import jax.numpy as jnp
from jax import lax
from jax.experimental import pallas as pl
from jax.experimental.pallas import tpu as pltpu
from jax.sharding import PartitionSpec as P

EPS = 1e-06
NEG_FILL = -1e30
PAIR = 128


def product(left, right):
    return jnp.dot(left, right, preferred_element_type=jnp.float32)


def product_tn(left, right):
    return lax.dot_general(
        left, right, (((0,), (0,)), ((), ())), preferred_element_type=jnp.float32
    )


def product_nt(left, right):
    return lax.dot_general(
        left, right, (((1,), (1,)), ((), ())), preferred_element_type=jnp.float32
    )


def rms_norm(values, gain):
    return values * lax.rsqrt(jnp.mean(values * values, axis=-1, keepdims=True) + EPS) * gain


def gate_product(attended, gate_pre):
    return attended * jax.nn.sigmoid(gate_pre)


def swiglu(gate, upward):
    return jax.nn.silu(gate) * upward


def low_triangle(size):
    rows = lax.broadcasted_iota(jnp.int32, (size, size), 0)
    return rows <= lax.broadcasted_iota(jnp.int32, (size, size), 1)


def exact(left, right):
    return jnp.dot(left, right, precision=lax.Precision.HIGHEST, preferred_element_type=jnp.float32)


class Forward:
    some = 8

    def __init__(self, joined, bias, length, attended, offset, col, logit, row, head_size, scale):
        self.joined, self.bias, self.length = joined, bias, length
        self.attended, self.offset, self.col, self.logit, self.row = attended, offset, col, logit, row
        self.head_size, self.scale = head_size, scale
        self.slots = joined.shape[0]
        self.pairs = (joined.shape[1] // PAIR - 1) // 3
        self.tile = min(256, self.slots)

    @staticmethod
    def results(slots, pairs):
        rows = jax.ShapeDtypeStruct((Forward.some, slots), jnp.float32)
        return [
            jax.ShapeDtypeStruct((slots, pairs * PAIR), jnp.bfloat16),
            rows,
            jax.ShapeDtypeStruct((slots, PAIR), jnp.float32),
            rows,
        ]

    def lanes(self, pair, part=0):
        return pl.ds(pl.multiple_of((part * self.pairs + pair) * PAIR, PAIR), PAIR)

    def start(self):
        slots, tile, some = self.slots, self.tile, self.some
        logits = self.joined[:, 3 * self.pairs * PAIR :].astype(jnp.float32) + self.bias[...]
        logit_rows = logits.T[:some]
        self.logit[...] = logit_rows
        logs = jnp.minimum(logit_rows, 0.0) - jnp.log1p(jnp.exp(-jnp.abs(logit_rows)))
        ones = low_triangle(tile).astype(jnp.float32)
        carry = jnp.zeros((some, 1), jnp.float32)
        for first in range(0, slots, tile):
            sums = exact(logs[:, first : first + tile], ones) + carry
            self.row[:, first : first + tile] = sums
            carry = sums[:, tile - 1 : tile]
        wide = jnp.concatenate([self.row[...], jnp.zeros((PAIR - some, slots), jnp.float32)], axis=0).T
        usable = lax.broadcasted_iota(jnp.int32, (slots, PAIR), 0) < self.length[...]
        self.col[...] = jnp.where(usable, wide, -NEG_FILL)

    def pair(self, pair):
        slots, tile, half = self.slots, self.tile, self.head_size
        key_all = self.joined[:, self.lanes(pair, 1)]
        value_t = self.joined[:, self.lanes(pair, 2)].T
        query_t = (self.joined[:, self.lanes(pair)].astype(jnp.float32) * self.scale).astype(jnp.bfloat16).T
        sub = lax.broadcasted_iota(jnp.int32, (PAIR, tile), 0)
        wide = lax.broadcasted_iota(jnp.int32, (slots, PAIR), 1)
        diag = low_triangle(tile)
        columns = [
            jnp.sum(jnp.where(wide == 2 * pair + a, self.col[...], 0.0), axis=1, keepdims=True) for a in range(2)
        ]
        for number in range(slots // tile):
            first, last = number * tile, (number + 1) * tile
            outs = []
            for a in range(2):
                mine = (sub >= a * half) & (sub < (a + 1) * half)
                at = pl.ds(2 * pair + a, 1)
                query = jnp.where(mine, query_t[:, first:last], jnp.zeros((), query_t.dtype))
                scores = product(key_all[:last], query)
                own_row = self.row[at, first:last]
                scores = scores + (own_row - columns[a][:last])
                tail = jnp.where(diag, scores[first:], NEG_FILL)
                scores = tail if number == 0 else jnp.concatenate([scores[:first], tail], axis=0)
                top = jnp.max(scores, axis=0, keepdims=True)
                weights = jnp.exp(scores - top)
                total = jnp.sum(weights, axis=0, keepdims=True)
                mixed = product(value_t[a * half : (a + 1) * half, :last], weights.astype(jnp.bfloat16))
                outs.append(mixed / total)
                self.offset[at, first:last] = own_row - (top + jnp.log(total))
            self.attended[first:last, self.lanes(pair)] = jnp.concatenate(outs, axis=0).T.astype(jnp.bfloat16)


def attention_fwd(joined, bias, length, head_size, scale):
    slots = joined.shape[0]
    pairs = (joined.shape[1] // PAIR - 1) // 3

    def body(joined_ref, bias_ref, length_ref, attended, offset, col, logit, row):
        work = Forward(joined_ref, bias_ref, length_ref, attended, offset, col, logit, row, head_size, scale)
        work.start()
        offset[...] = jnp.zeros_like(offset)

        def step(pair, carry):
            work.pair(pair)
            return carry

        lax.fori_loop(0, pairs, step, 0)

    vmem = pl.BlockSpec(memory_space=pltpu.VMEM)
    return pl.pallas_call(
        body,
        in_specs=[vmem] * 3,
        out_specs=[vmem] * 4,
        out_shape=Forward.results(slots, pairs),
        scratch_shapes=[pltpu.VMEM((Forward.some, slots), jnp.float32)],
        compiler_params=pltpu.CompilerParams(vmem_limit_bytes=56 << 20),
        cost_estimate=pl.CostEstimate(
            flops=4 * slots * slots * pairs * PAIR, bytes_accessed=8 * slots * pairs * PAIR, transcendentals=0
        ),
        name="attention_fwd",
    )(joined, bias, length)


def backward_scratch(slots):
    return [
        pltpu.VMEM((slots, PAIR), jnp.float32),
        pltpu.VMEM((slots, PAIR), jnp.float32),
        pltpu.VMEM((slots, PAIR), jnp.float32),
        pltpu.VMEM((8, slots), jnp.float32),
    ]


class Backward:
    def __init__(self, joined, d_out, offset, col, logit, grads, dk_acc, dv_acc, dcol, drow, head_size, scale):
        self.joined, self.d_out, self.offset, self.col = joined, d_out, offset, col
        self.logit, self.grads, self.dk_acc, self.dv_acc = logit, grads, dk_acc, dv_acc
        self.dcol, self.drow, self.head_size, self.scale = dcol, drow, head_size, scale
        self.slots = joined.shape[0]
        self.pairs = (joined.shape[1] // PAIR - 1) // 3
        self.tile = min(256, self.slots)

    def start(self):
        self.dcol[...] = jnp.zeros_like(self.dcol)
        self.drow[...] = jnp.zeros_like(self.drow)

    def lanes(self, pair, part=0):
        return pl.ds(pl.multiple_of((part * self.pairs + pair) * PAIR, PAIR), PAIR)

    def pair(self, pair):
        slots, tile, half = self.slots, self.tile, self.head_size
        dk_acc, dv_acc, dcol, drow = self.dk_acc, self.dv_acc, self.dcol, self.drow
        queries = (self.joined[:, self.lanes(pair)].astype(jnp.float32) * self.scale).astype(jnp.bfloat16)
        key_all = self.joined[:, self.lanes(pair, 1)]
        value_all = self.joined[:, self.lanes(pair, 2)]
        d_out = self.d_out[:, self.lanes(pair)]
        query_t, key_t, dout_t = queries.T, key_all.T, d_out.T
        sub = lax.broadcasted_iota(jnp.int32, (PAIR, tile), 0)
        lanes = lax.broadcasted_iota(jnp.int32, (tile, PAIR), 1)
        wide = lax.broadcasted_iota(jnp.int32, (slots, PAIR), 1)
        diag = low_triangle(tile)
        zero = jnp.zeros((), jnp.bfloat16)
        columns = [
            jnp.sum(jnp.where(wide == 2 * pair + a, self.col[...], 0.0), axis=1, keepdims=True) for a in range(2)
        ]
        dk_acc[...] = jnp.zeros_like(dk_acc)
        dv_acc[...] = jnp.zeros_like(dv_acc)
        for number in range(slots // tile):
            first, last = number * tile, (number + 1) * tile
            outs = []
            for a in range(2):
                mine = (sub >= a * half) & (sub < (a + 1) * half)
                own = (lanes >= a * half) & (lanes < (a + 1) * half)
                at = pl.ds(2 * pair + a, 1)
                scores = product(key_all[:last], jnp.where(mine, query_t[:, first:last], zero))
                scores = scores + (self.offset[at, first:last] - columns[a][:last])
                tail = jnp.where(diag, scores[first:], NEG_FILL)
                scores = tail if number == 0 else jnp.concatenate([scores[:first], tail], axis=0)
                probs = jnp.exp(scores)
                d_probs = product(value_all[:last], jnp.where(mine, dout_t[:, first:last], zero))
                dot = jnp.sum(d_probs * probs, axis=0, keepdims=True)
                d_full = probs * (d_probs - dot)
                d_scores = d_full.astype(jnp.bfloat16)
                drow[at, first:last] = jnp.sum(d_full, axis=0, keepdims=True)
                sums = jnp.sum(d_full, axis=1, keepdims=True)
                dcol[:last, :] += jnp.where(wide[:last] == 2 * pair + a, sums, 0.0)
                outs.append(product(key_t[a * half : (a + 1) * half, :last], d_scores) * self.scale)
                dk_acc[:last, :] += product(d_scores, jnp.where(own, queries[first:last, :], zero))
                dv_acc[:last, :] += product(
                    probs.astype(jnp.bfloat16), jnp.where(own, d_out[first:last, :], zero)
                )
            self.grads[first:last, self.lanes(pair)] = jnp.concatenate(outs, axis=0).T.astype(self.grads.dtype)
        self.grads[:, self.lanes(pair, 1)] = dk_acc[...].astype(self.grads.dtype)
        self.grads[:, self.lanes(pair, 2)] = dv_acc[...].astype(self.grads.dtype)

    def end(self, bias_grad):
        slots, tile, some = self.slots, self.tile, 8
        change = self.drow[...] - self.dcol[...].T[:some]
        rows = lax.broadcasted_iota(jnp.int32, (tile, tile), 0)
        ones = (rows >= lax.broadcasted_iota(jnp.int32, (tile, tile), 1)).astype(jnp.float32)
        carry = jnp.zeros((some, 1), jnp.float32)
        pieces = []
        for first in reversed(range(0, slots, tile)):
            sums = exact(change[:, first : first + tile], ones) + carry
            carry = sums[:, :1]
            pieces.insert(0, sums)
        grad = jnp.concatenate(pieces, axis=1) * jax.nn.sigmoid(-self.logit[...])
        heads = lax.broadcasted_iota(jnp.int32, (some, slots), 0)
        grad = jnp.where(heads < 2 * self.pairs, grad, 0.0)
        bias_grad[...] = jnp.broadcast_to(jnp.sum(grad, axis=1, keepdims=True), bias_grad.shape)
        wide = jnp.concatenate([grad, jnp.zeros((PAIR - some, slots), jnp.float32)], axis=0).T
        self.grads[:, 3 * self.pairs * PAIR : (3 * self.pairs + 1) * PAIR] = wide.astype(self.grads.dtype)


def attention_bwd(joined, d_out, offset, col, logit, head_size, scale):
    slots, width = joined.shape
    pairs = (width // PAIR - 1) // 3

    def body(joined_ref, d_out_ref, offset_ref, col_ref, logit_ref, grads, bias_grad, *scratch):
        work = Backward(
            joined_ref, d_out_ref, offset_ref, col_ref, logit_ref, grads, *scratch, head_size, scale
        )
        work.start()

        def step(pair, carry):
            work.pair(pair)
            return carry

        lax.fori_loop(0, pairs, step, 0)
        work.end(bias_grad)

    vmem = pl.BlockSpec(memory_space=pltpu.VMEM)
    return pl.pallas_call(
        body,
        in_specs=[vmem] * 5,
        out_specs=[vmem] * 2,
        out_shape=[
            jax.ShapeDtypeStruct((slots, width), jnp.bfloat16),
            jax.ShapeDtypeStruct((8, PAIR), jnp.float32),
        ],
        scratch_shapes=backward_scratch(slots),
        compiler_params=pltpu.CompilerParams(vmem_limit_bytes=56 << 20),
        cost_estimate=pl.CostEstimate(
            flops=10 * slots * slots * pairs * PAIR, bytes_accessed=14 * slots * pairs * PAIR, transcendentals=0
        ),
        name="attention_bwd",
    )(joined, d_out, offset, col, logit)


MESH = pl.DeviceIdType.MESH
VMEM_LIMIT = 62 << 20


def square(groups):
    return groups == 4


def sides():
    rank = lax.axis_index("seq")
    return rank, rank + 1 - 2 * lax.rem(rank, 2), lax.rem(rank + 2, 4), 3 - rank


def meet(*others):
    barrier = pltpu.get_barrier_semaphore()
    for other in others:
        pl.semaphore_signal(barrier, inc=1, device_id=other, device_id_type=MESH)
    pl.semaphore_wait(barrier, len(others))


def push(source, target, send, recv, device):
    copy = pltpu.make_async_remote_copy(
        src_ref=source,
        dst_ref=target,
        send_sem=send,
        recv_sem=recv,
        device_id=device,
        device_id_type=MESH,
    )
    copy.start()
    return copy


def by_rows(rows, work):
    def step(number, carry):
        work(pl.ds(pl.multiple_of(number * 16, 16), 16))
        return carry

    lax.fori_loop(0, rows // 16, step, 0)


class Streams:
    def __init__(self, sems):
        self.sems, self.made = sems, []

    def start(self, source, target):
        copy = pltpu.make_async_copy(source, target, self.sems.at[len(self.made)])
        self.made.append(copy)
        copy.start()
        return copy

    def end(self):
        for copy in self.made:
            copy.wait()


class SquareGather:
    def __init__(self, own, full, send, recv):
        self.own, self.full, self.send, self.recv = own, full, send, recv
        self.rows = own.shape[0]
        self.half = self.rows // 2

    def place(self, rank, part):
        return self.full.at[pl.ds(pl.multiple_of(rank * self.rows + part * self.half, self.half), self.half)]

    def copy(self, index):
        me, side, down, across = sides()
        mine = [self.own.at[pl.ds(part * self.half, self.half)] for part in (0, 1)]
        source, target, peer = (
            (mine[0], self.place(me, 0), side),
            (mine[1], self.place(me, 1), down),
            (mine[1], self.place(me, 1), side),
            (mine[0], self.place(me, 0), down),
            (self.place(side, 0), self.place(side, 0), down),
            (self.place(down, 1), self.place(down, 1), side),
        )[index]
        return pltpu.make_async_remote_copy(
            src_ref=source,
            dst_ref=target,
            send_sem=self.send.at[index],
            recv_sem=self.recv.at[index],
            device_id={"seq": peer},
            device_id_type=MESH,
        )

    def start(self):
        for index in range(4):
            self.copy(index).start()

    def relay(self):
        for index in (0, 1):
            self.copy(index).wait_recv()
            self.copy(4 + index).start()

    def near(self):
        self.copy(2).wait_recv()
        self.copy(3).wait_recv()

    def far(self):
        self.copy(4).wait_recv()
        self.copy(5).wait_recv()

    def finish(self):
        for index in range(6):
            self.copy(index).wait_send()


def block_product(left, right, transposed, tile, store):
    total = right.shape[0] if transposed else right.shape[1]

    def step(number, carry):
        columns = pl.ds(pl.multiple_of(number * tile, tile), tile)
        if transposed:
            store(columns, product_nt(left[...], right[columns, :]))
        else:
            store(columns, product(left[...], right[:, columns]))
        return carry

    lax.fori_loop(0, total // tile, step, 0)


def transposed_product(left, right, out):
    tall = 512 if out.shape[0] % 512 == 0 else 384
    wide = next(size for size in (512, 384, 640, 128) if out.shape[1] % size == 0)
    across = out.shape[1] // wide

    def step(number, carry):
        rows = pl.ds(pl.multiple_of((number // across) * tall, tall), tall)
        columns = pl.ds(pl.multiple_of(lax.rem(number, across) * wide, wide), wide)
        out[rows, columns] = product_tn(left[:, rows], right[:, columns]).astype(out.dtype)
        return carry

    lax.fori_loop(0, (out.shape[0] // tall) * across, step, 0)


def line():
    shards, place = lax.axis_size("wshard"), lax.axis_index("wshard")
    chips = shards // 2
    chip, core = place // 2, lax.rem(place, 2)
    forth = {"wshard": lax.rem(place + 2, shards)}
    back = {"wshard": lax.rem(place + shards - 2, shards)}
    twin = {"wshard": place + 1 - 2 * core}
    return chips, chip, core, forth, back, twin


class LineGather:
    @staticmethod
    def scratch(chips):
        dma = pltpu.SemaphoreType.DMA
        return [dma((3, chips)), dma((2 * chips,)), dma((1,))]

    def __init__(self, own, full, send, recv, local):
        self.own, self.full, self.local = own, full, local.at[0]
        self.sends = (send.at[0], send.at[1], send.at[2])
        self.recv = recv
        self.rows = own.shape[0]
        self.chips, self.chip, self.core, *self.devices = line()

    def place(self, chip, core):
        return self.full.at[pl.ds(pl.multiple_of((2 * chip + core) * self.rows, self.rows), self.rows)]

    def copy(self, way, chip, source=None):
        target = self.place(chip, self.core)
        return pltpu.make_async_remote_copy(
            src_ref=target if source is None else source,
            dst_ref=target,
            send_sem=self.sends[way].at[chip],
            recv_sem=self.recv.at[2 * chip + self.core],
            device_id=self.devices[way],
            device_id_type=MESH,
        )

    def wait_for(self, chip, core):
        target = self.place(chip, core)
        pltpu.make_async_remote_copy(
            src_ref=target,
            dst_ref=target,
            send_sem=self.sends[2].at[0],
            recv_sem=self.recv.at[2 * chip + core],
            device_id=self.devices[2],
            device_id_type=MESH,
        ).wait_recv()

    def start(self):
        @pl.when(self.chip < self.chips - 1)
        def _():
            self.copy(0, self.chip, self.own).start()

        @pl.when(self.chip > 0)
        def _():
            self.copy(1, self.chip, self.own).start()

        self.copy(2, self.chip, self.own).start()
        self.keep().start()

    def keep(self):
        return pltpu.make_async_copy(self.own, self.place(self.chip, self.core), self.local)

    def step(self, number):
        left, right = self.chip - number, self.chip + number

        @pl.when(left >= 0)
        def _():
            self.wait_for(left, self.core)

            @pl.when(self.chip < self.chips - 1)
            def _():
                self.copy(0, left).start()

            self.copy(2, left).start()

        @pl.when(right < self.chips)
        def _():
            self.wait_for(right, self.core)

            @pl.when(self.chip > 0)
            def _():
                self.copy(1, right).start()

            self.copy(2, right).start()

    def finish(self):
        for chip in range(self.chips):
            self.wait_for(chip, 1 - self.core)
            self.copy(2, chip).wait_send()

            @pl.when((chip <= self.chip) & (self.chip < self.chips - 1))
            def _():
                self.copy(0, chip).wait_send()

            @pl.when((chip >= self.chip) & (self.chip > 0))
            def _():
                self.copy(1, chip).wait_send()

        self.keep().wait()


class PartExchange:
    @staticmethod
    def scratch():
        dma = pltpu.SemaphoreType.DMA
        return [dma((4,)), dma((4,)), dma((1,))]

    def __init__(self, parts, out, send, recv, local):
        self.parts, self.out, self.send, self.recv, self.local = parts, out, send, recv, local
        self.rank = lax.axis_index("seq")
        self.core, self.twin = line()[2], line()[5]
        self.others = [{"seq": lax.rem(self.rank + k, 4)} for k in range(1, 4)]
        self.rows = out.shape[2]

    def part(self, rank):
        return self.parts.at[pl.ds(pl.multiple_of((2 * rank + self.core) * self.rows, self.rows), self.rows)]

    def copy(self, index):
        if index == 3:
            source = target = self.out.at[self.core]
        else:
            source = self.part(lax.rem(self.rank + index + 1, 4))
            target = self.out.at[self.core, self.rank]
        return pltpu.make_async_remote_copy(
            src_ref=source,
            dst_ref=target,
            send_sem=self.send.at[index],
            recv_sem=self.recv.at[index],
            device_id=self.twin if index == 3 else self.others[index],
            device_id_type=MESH,
        )

    def keep(self):
        return pltpu.make_async_copy(self.part(self.rank), self.out.at[self.core, self.rank], self.local.at[0])

    def start(self):
        for index in (1, 0, 2):
            self.copy(index).start()
        self.keep().start()

    def relay(self):
        for index in range(3):
            self.copy(index).wait()
        self.keep().wait()
        self.copy(3).start()

    def end(self):
        self.copy(3).wait()


class Regroup:
    @staticmethod
    def scratch(rows, width):
        dma = pltpu.SemaphoreType.DMA
        return [pltpu.VMEM((4, rows, width), jnp.bfloat16), dma((7,)), dma((7,))]

    def __init__(self, piece, out, fours, send, recv):
        self.piece, self.out, self.fours, self.send, self.recv = piece, out, fours, send, recv
        self.rank, self.place = lax.axis_index("seq"), lax.axis_index("wshard")
        self.number = lax.rem(self.place, 4)
        self.others = [{"seq": lax.rem(self.rank + k, 4)} for k in range(1, 4)]
        self.along = [{"wshard": lax.rem(self.place + k, 8)} for k in range(1, 8)]

    def near(self, index):
        return pltpu.make_async_remote_copy(
            src_ref=self.piece,
            dst_ref=self.fours.at[self.rank],
            send_sem=self.send.at[index],
            recv_sem=self.recv.at[index],
            device_id=self.others[index],
            device_id_type=MESH,
        )

    def owner(self, rank):
        return 2 * rank + self.place // 4

    def far(self, rank, number):
        return pltpu.make_async_remote_copy(
            src_ref=self.fours.at[rank],
            dst_ref=self.out.at[number],
            send_sem=self.send.at[3 + rank],
            recv_sem=self.recv.at[3 + number],
            device_id={"wshard": self.owner(rank)},
            device_id_type=MESH,
        )

    def start(self):
        for index in range(3):
            self.near(index).start()
        self.fours[self.rank] = self.piece[...]

    def relay(self):
        for index in range(3):
            self.near(index).wait()
        for rank in range(4):

            @pl.when(self.owner(rank) != self.place)
            def _():
                self.far(rank, self.number).start()

            @pl.when(self.owner(rank) == self.place)
            def _():
                self.out[self.number] = self.fours[rank]

    def end(self):
        for rank in range(4):

            @pl.when(self.owner(rank) != self.place)
            def _():
                self.far(rank, self.number).wait_send()

        for number in range(4):

            @pl.when(4 * lax.rem(self.place, 2) + number != self.place)
            def _():
                self.far(0, number).wait_recv()


class Everywhere:
    @staticmethod
    def scratch(shape):
        dma = pltpu.SemaphoreType.DMA
        return [
            pltpu.VMEM((4,) + shape, jnp.float32),
            pltpu.VMEM(shape, jnp.float32),
            pltpu.VMEM((8,) + shape, jnp.float32),
            dma((12,)),
            dma((12,)),
        ]

    def __init__(self, values, out, ranks, total, places, send, recv):
        self.values, self.out, self.ranks, self.total, self.places = values, out, ranks, total, places
        self.send, self.recv = send, recv
        self.groups, self.shards = ranks.shape[0], places.shape[0]
        self.rank, self.place = lax.axis_index("seq"), lax.axis_index("wshard")

    def others(self):
        return [{"seq": lax.rem(self.rank + k, self.groups)} for k in range(1, self.groups)]

    def along(self):
        return [{"wshard": lax.rem(self.place + k, self.shards)} for k in range(1, self.shards)]

    def start(self):
        self.first = [
            push(self.values, self.ranks.at[self.rank], self.send.at[k], self.recv.at[k], other)
            for k, other in enumerate(self.others())
        ]
        self.ranks[self.rank] = self.values[...]

    def relay(self):
        for copy in self.first:
            copy.wait()
        ranks, groups = self.ranks, self.groups
        self.total[...] = (ranks[0] + ranks[1]) + (ranks[2] + ranks[3])
        self.second = [
            push(self.total, self.places.at[self.place], self.send.at[groups + k], self.recv.at[groups + k], other)
            for k, other in enumerate(self.along())
        ]
        self.places[self.place] = self.total[...]

    def end(self):
        for copy in self.second:
            copy.wait()
        sums = [self.places[k] + self.places[k + 1] for k in range(0, self.shards, 2)]
        self.out[...] = (sums[0] + sums[1]) + (sums[2] + sums[3])


def join_shares(every, gate, every_gate, every_up, down, out, columns, starts, forget_at, heads, part):
    groups, rows, lanes = every.shape
    units = every_gate.shape[2]
    own = heads // groups
    steps = 4
    tall = rows // steps

    def body(every_ref, gate_ref, wide_gate, wide_up, down_in, out_in, *outs):
        firsts = len(starts)
        for group in range(groups):
            to = slice(group * columns, (group + 1) * columns)
            for start, result in zip(starts, outs):
                result[:, to] = every_ref[group, :, start : start + columns].astype(jnp.float32)
            outs[firsts][:, to] = gate_ref[group].astype(jnp.float32)
            outs[firsts + 1][:, group * own : (group + 1) * own] = every_ref[
                group, :, forget_at : forget_at + own
            ].astype(jnp.float32)
            for source, result in ((wide_gate, outs[firsts + 2]), (wide_up, outs[firsts + 3])):
                for block in range(units // part):
                    at = (block * groups + group) * part
                    result[:, at : at + part] = source[group, :, block * part : (block + 1) * part].astype(
                        jnp.float32
                    )
        outs[firsts + 4][...] = down_in[...].astype(jnp.float32)
        outs[firsts + 5][...] = out_in[...].astype(jnp.float32)

    def flat(value):
        return pl.BlockSpec((value.shape[0] // steps, value.shape[1]), lambda i: (i, 0))

    def ranks(value):
        return pl.BlockSpec((groups, tall, value.shape[2]), lambda i: (0, i, 0))

    def shape(size):
        return jax.ShapeDtypeStruct(size, jnp.float32)

    results = [shape((rows, groups * columns))] * (len(starts) + 1) + [
        shape((rows, heads)),
        shape((rows, groups * units)),
        shape((rows, groups * units)),
        shape(down.shape),
        shape(out.shape),
    ]
    return pl.pallas_call(
        body,
        grid=(steps,),
        in_specs=[ranks(v) for v in (every, gate, every_gate, every_up)] + [flat(down), flat(out)],
        out_specs=[flat(value) for value in results],
        out_shape=results,
        compiler_params=pltpu.CompilerParams(vmem_limit_bytes=56 << 20),
        name="join_shares",
    )(every, gate, every_gate, every_up, down, out)


def norm_rows(values, gain):
    scale = lax.rsqrt(jnp.mean(values * values, axis=-1, keepdims=True) + EPS)
    return scale, values * scale * gain


def whole_forward(inputs, gain, cotangent, weights, forget, bias, length, block, w_gate, w_up,
                  head_size, scale, collective_id):
    rows, depth = inputs.shape
    groups = 4
    slots = groups * rows
    chips = groups
    shards = 2 * chips
    mine = weights[0].shape[0]
    columns = depth // groups
    front = 3 * columns + PAIR
    pairs = columns // PAIR
    part = w_gate.shape[1] // (groups * shards)
    units = shards * part
    early = units + units // 2
    low = jnp.bfloat16

    def body(inputs_ref, gain_ref, cot_ref, q_ref, k_ref, v_ref, og_ref, forget_ref, bias_ref, length_ref, block_ref,
             gate_ref, up_ref,
             normed_hbm, cot_full, full_front_hbm, full_gate_hbm, full_out_hbm, full_ffn, joined_hbm, attended_hbm,
             offset, col, logit, gate_pre_hbm, gated_hbm, middle, own_up,
             own_normed, own_front, own_gate, own_ffn, own_out, parts_out, own_cot, row, picks, cot_send, cot_recv, keep,
             x_send, x_recv, normed, full_front, full_gate, full_out, joined, attended, gate_pre, gated, store_sems,
             *scratch):
        store = Streams(store_sems)
        me, side, down, across = sides()
        line_chips, chip, core, forth, back, twin = line()
        halves = (pl.ds(0, 2 * columns), pl.ds(2 * columns, front - 2 * columns))
        first_line = LineGather(own_front.at[:, halves[0]], full_front.at[:, halves[0]], *scratch[0:3])
        second_line = LineGather(own_front.at[:, halves[1]], full_front.at[:, halves[1]], *scratch[22:25])
        gate_line = LineGather(own_gate, full_gate, *scratch[3:6])
        ffn_line = LineGather(own_ffn, full_ffn, *scratch[6:9])
        out_line = LineGather(own_out, parts_out, *scratch[9:12])
        exchange = PartExchange(parts_out, full_out, *scratch[12:15])
        job = SquareScatter([gated], [full_out_rows(full_out)], False, middle, *scratch[15:22])
        taken = []
        my_columns = pl.ds(pl.multiple_of(me * columns, columns), columns)
        for index, source in enumerate((q_ref, k_ref, v_ref)):
            taken.append((source.at[:, my_columns], own_front.at[:, pl.ds(index * columns, columns)]))
        taken.append((og_ref.at[:, my_columns], own_gate))
        tall = own_out.shape[0]
        taken.append((block_ref.at[pl.ds(pl.multiple_of(me * tall, tall), tall)], own_out))
        for index, source in enumerate((gate_ref, up_ref)):
            for number in range(shards):
                column = pl.ds(pl.multiple_of((number * groups + me) * part, part), part)
                to = index * units + number * part
                target = own_ffn.at[:, pl.ds(to, part)] if to < early else own_up.at[:, pl.ds(to - early, part)]
                taken.append((source.at[:, column], target))
        taken = [pltpu.make_async_copy(a, b, picks.at[i]) for i, (a, b) in enumerate(taken)]
        for copy in taken:
            copy.start()
        values = inputs_ref[...].astype(jnp.float32)
        own_normed[...] = norm_rows(values, gain_ref[...])[1].astype(low)
        own_front[:, 3 * columns :] = forget_ref[...]
        positions = me * rows + lax.broadcasted_iota(jnp.int32, (rows, depth), 0)
        own_cot[...] = jnp.where(positions < length_ref[:, :1], cot_ref[...], jnp.zeros((), low))
        meet(*exchange.others, forth, back, twin)
        one = SquareGather(own_normed, normed, x_send, x_recv)
        two = SquareGather(own_cot, cot_full, cot_send, cot_recv)
        one.start()
        for copy in taken:
            copy.wait()
        first_line.start()
        second_line.start()
        at_me = pl.ds(pl.multiple_of(me * rows, rows), rows)
        kept = pltpu.make_async_copy(own_cot, cot_full.at[at_me], keep.at[0])
        kept.start()
        normed[at_me, :] = own_normed[...]
        one.relay()
        two.start()
        first_line.step(1)
        second_line.step(1)
        first_line.step(2)
        second_line.step(2)
        one.near()
        one.far()
        first_line.step(3)
        second_line.step(3)
        store.start(normed, normed_hbm)
        out_line.start()
        gate_line.start()
        two.relay()
        first_line.finish()

        def product_of(columns_of_front):
            view = joined.at[:, columns_of_front]

            def store_joined(at_columns, value):
                view[:, at_columns] = value.astype(low)

            block_product(normed, full_front.at[:, columns_of_front], False, 256, store_joined)

        product_of(halves[0])
        second_line.finish()
        product_of(halves[1])
        store.start(full_front, full_front_hbm)
        one.finish()
        store.start(joined, joined_hbm)
        work = Forward(joined, bias_ref, length_ref, attended, offset, col, logit, row, head_size, scale)
        offset[...] = jnp.zeros_like(offset)
        out_line.step(1)
        gate_line.step(1)
        work.start()

        def step(pair, carry):
            work.pair(pair)

            @pl.when(pair == 0)
            def _():
                out_line.step(2)
                gate_line.step(2)

            @pl.when(pair == 1)
            def _():
                out_line.step(3)
                out_line.finish()
                exchange.start()
                gate_line.step(3)
                ffn_line.start()

            return carry

        lax.fori_loop(0, pairs, step, 0)
        store.start(attended, attended_hbm)
        gate_line.finish()
        store.start(full_gate, full_gate_hbm)

        def store_gate(at_columns, value):
            gate_pre[:, at_columns] = value

        block_product(normed, full_gate, False, PAIR, store_gate)
        gated[...] = (attended[...].astype(jnp.float32) * jax.nn.sigmoid(gate_pre[...])).astype(low)
        exchange.relay()
        store.start(gate_pre, gate_pre_hbm)
        store.start(gated, gated_hbm)
        exchange.end()
        store.start(full_out, full_out_hbm)
        job.begin()
        ffn_line.step(1)
        job.relay()
        job.own()
        two.near()
        two.far()
        two.finish()
        kept.wait()
        ffn_line.step(2)
        job.end()
        middle[...] += inputs_ref[...].astype(jnp.float32)
        ffn_line.step(3)
        ffn_line.finish()
        store.end()

    def shape(size, kind=low):
        return jax.ShapeDtypeStruct(size, kind)

    vmem = pl.BlockSpec(memory_space=pltpu.VMEM)
    anywhere = pl.BlockSpec(memory_space=pl.ANY)
    dma = pltpu.SemaphoreType.DMA
    results = [
        shape((slots, depth)),
        shape((slots, depth)),
        shape((depth, front)),
        shape((depth, columns)),
        shape((2, 4, block.shape[0] // 4, depth)),
        shape((depth, early)),
        shape((slots, front)),
        *Forward.results(slots, pairs),
        shape((slots, columns), jnp.float32),
        shape((slots, columns)),
        shape((rows, depth), jnp.float32),
        shape((mine, 2 * units - early)),
    ]
    kept_here = [results[i] for i in (0, 2, 3, 4, 6, 7, 11, 12)]
    return pl.pallas_call(
        body,
        in_specs=[vmem] * 3 + [anywhere] * 4 + [vmem] * 3 + [anywhere] * 3,
        out_specs=[anywhere] * 8 + [vmem] * 3 + [anywhere] * 2 + [vmem] * 2,
        out_shape=results,
        scratch_shapes=[
            pltpu.VMEM((rows, depth), low),
            pltpu.VMEM((mine, front), low),
            pltpu.VMEM((mine, columns), low),
            pltpu.VMEM((mine, early), low),
            pltpu.VMEM((block.shape[0] // 4, depth), low),
            pltpu.VMEM((shards * block.shape[0] // 4, depth), low),
            pltpu.VMEM((rows, depth), low),
            pltpu.VMEM((Forward.some, slots), jnp.float32),
            dma((5 + 2 * shards,)),
            dma((6,)),
            dma((6,)),
            dma((1,)),
            dma((6,)),
            dma((6,)),
            *(pltpu.VMEM(value.shape, value.dtype) for value in kept_here),
            dma((len(kept_here),)),
        ]
        + 4 * LineGather.scratch(chips)
        + PartExchange.scratch()
        + SquareScatter.scratch(rows, depth)
        + LineGather.scratch(chips),
        compiler_params=pltpu.CompilerParams(
            collective_id=collective_id, has_side_effects=True, vmem_limit_bytes=VMEM_LIMIT
        ),
        name="whole_forward",
    )(inputs, gain, cotangent, *weights, forget, bias, length, block, w_gate, w_up)


class full_out_rows:
    def __init__(self, ref):
        self.ref = ref
        self.shape = (ref.shape[0] * ref.shape[1] * ref.shape[2], ref.shape[3])

    def __getitem__(self, index):
        taken = self.ref[:, :, :, index[1]]
        return taken.reshape(self.shape[0], taken.shape[3])


def feed_forward(middle, gain, weights, own_up, own_down, cotangent, collective_id):
    rows, depth = middle.shape
    slots = 4 * rows
    units = 4 * own_down.shape[0] * 2
    early = weights.shape[1]
    chips = 4
    low = jnp.bfloat16

    def body(middle_ref, gain_ref, weights_hbm, up_ref, down_ref, cot_hbm,
             normed_hbm, hidden_hbm, full_up_hbm, full_down_hbm, grads_hbm, terms_hbm,
             own_normed, both, send, recv,
             weights_ref, cot_ref, normed, hidden, full_up, full_down, grads, terms, fetch_sems, store_sems, *scratch):
        fetch, store = Streams(fetch_sems), Streams(store_sems)
        weights_in = fetch.start(weights_hbm, weights_ref)
        cot_in = fetch.start(cot_hbm, cot_ref)
        me, side, down, across = sides()
        line_chips, chip, core, forth, back, twin = line()
        up_line = LineGather(up_ref, full_up, *scratch[:3])
        down_line = LineGather(down_ref, full_down, *scratch[3:])
        own_normed[...] = norm_rows(middle_ref[...], gain_ref[...])[1].astype(low)
        meet({"seq": side}, {"seq": down}, forth, back, twin)
        job = SquareGather(own_normed, normed, send, recv)
        up_line.start()
        down_line.start()
        job.start()

        def rows_of(rank):
            return pl.ds(pl.multiple_of(rank * rows, rows), rows)

        def multiply(rank):
            at = rows_of(rank)

            def store(columns, value):
                both[at, columns] = value

            block_product(normed.at[at], weights_ref, False, 512, store)

        normed[rows_of(me), :] = own_normed[...]
        weights_in.wait()
        multiply(me)
        up_line.step(1)
        job.relay()
        down_line.step(1)
        up_line.step(2)
        job.near()
        multiply(side)
        up_line.step(3)
        multiply(down)
        job.far()
        store.start(normed, normed_hbm)
        down_line.step(2)
        multiply(across)
        job.finish()
        up_line.finish()
        store.start(full_up, full_up_hbm)

        def ahead(number, carry):
            at = rows_of(number)
            both[at, early:] = product(normed[at, :], full_up[...])
            gate, upward = both[at, :units], both[at, units:]
            hidden[at, :] = (gate * jax.nn.sigmoid(gate) * upward).astype(low)
            return carry

        lax.fori_loop(0, 4, ahead, 0)
        store.start(hidden, hidden_hbm)
        down_line.step(3)
        cot_in.wait()
        transposed_product(hidden, cot_ref, terms)
        store.start(terms, terms_hbm)
        down_line.finish()
        store.start(full_down, full_down_hbm)

        def behind(number, carry):
            at = rows_of(number)
            grad_hidden = product_nt(cot_ref[at, :], full_down[...])
            gate, upward = both[at, :units], both[at, units:]
            sigma = jax.nn.sigmoid(gate)
            grads[at, :units] = (grad_hidden * upward * sigma * (1.0 + gate * (1.0 - sigma))).astype(low)
            grads[at, units:] = (grad_hidden * gate * sigma).astype(low)
            part(number).start()
            return carry

        def part(number):
            at = rows_of(number)
            return pltpu.make_async_copy(grads.at[at], grads_hbm.at[at], store_sems.at[5 + number])

        lax.fori_loop(0, 4, behind, 0)
        for number in range(4):
            part(number).wait()
        store.end()

    def shape(size, kind=low):
        return jax.ShapeDtypeStruct(size, kind)

    vmem = pl.BlockSpec(memory_space=pltpu.VMEM)
    anywhere = pl.BlockSpec(memory_space=pl.ANY)
    dma = pltpu.SemaphoreType.DMA
    results = [
        shape((slots, depth)),
        shape((slots, units)),
        shape((depth, own_up.shape[1])),
        shape((units, depth)),
        shape((slots, 2 * units)),
        shape((units, depth)),
    ]
    return pl.pallas_call(
        body,
        in_specs=[vmem, vmem, anywhere, vmem, vmem, anywhere],
        out_specs=[anywhere] * 6,
        out_shape=results,
        scratch_shapes=[
            pltpu.VMEM((rows, depth), low),
            pltpu.VMEM((slots, 2 * units), jnp.float32),
            dma((6,)),
            dma((6,)),
            *(pltpu.VMEM(value.shape, value.dtype) for value in (weights, cotangent, *results)),
            dma((2,)),
            dma((9,)),
        ]
        + 2 * LineGather.scratch(chips),
        compiler_params=pltpu.CompilerParams(
            collective_id=collective_id, has_side_effects=True, vmem_limit_bytes=VMEM_LIMIT
        ),
        name="feed_forward",
    )(middle, gain, weights, own_up, own_down, cotangent)


def feed_backward(grads, weights, up_weights, normed, terms_down, w_out, middle, gain, cotangent, attended, gate_pre,
                  collective_id):
    rows, depth = middle.shape
    slots = 4 * rows
    units = grads.shape[1] // 2
    early = weights.shape[1]
    columns = attended.shape[1]
    shards = 2 * lax.axis_size("seq")
    chips = shards // 2
    low = jnp.bfloat16

    def body(grads_hbm, weights_hbm, up_weights_hbm, normed_hbm, down_hbm, out_hbm, middle_hbm, gain_ref, cot_hbm,
             attended_hbm, pre_hbm,
             grad_middle_hbm, grad_gain, branch_hbm, d_attended, d_pre, terms_up_hbm, share_down, share_gate,
             own_branch, summed, terms_gate, send, recv,
             grads_ref, weights_ref, up_weights_ref, normed_ref, down_ref, out_ref, middle_ref, cot_ref,
             attended_ref, pre_ref, grad_middle, branch, terms_up, fetch_sems, store_sems, *scratch):
        fetch, store = Streams(fetch_sems), Streams(store_sems)
        own_rows = pl.ds(pl.multiple_of(lax.axis_index("seq") * rows, rows), rows)
        first_in = [
            fetch.start(*both)
            for both in (
                (down_hbm, down_ref),
                (grads_hbm, grads_ref),
                (weights_hbm, weights_ref),
                (up_weights_hbm, up_weights_ref),
            )
        ]
        normed_in = fetch.start(normed_hbm, normed_ref)
        rest_in = [
            fetch.start(*both)
            for both in (
                (middle_hbm, middle_ref),
                (cot_hbm.at[own_rows], cot_ref),
                (out_hbm, out_ref),
                (attended_hbm, attended_ref),
                (pre_hbm, pre_ref),
            )
        ]
        me, side, down, across = sides()
        line_chips, chip, core, forth, back, twin = line()
        meet({"seq": side}, {"seq": down}, forth, back, twin)
        first, second = grads_ref.at[:, pl.ds(0, units)], grads_ref.at[:, pl.ds(units, units)]
        job = SquareScatter(
            [grads_ref.at[:, pl.ds(0, early)], grads_ref.at[:, pl.ds(early, 2 * units - early)]],
            [weights_ref, up_weights_ref],
            True,
            summed,
            *scratch[:7],
        )
        run_down = LineScatter(down_ref, share_down, *scratch[7:12])
        run_gate = LineScatter(terms_gate, share_gate, *scratch[12:])
        every = SquareGather(own_branch, branch, send, recv)
        first_in[0].wait()
        run_down.start()
        for copy in first_in[1:]:
            copy.wait()
        job.begin_far()
        run_down.slot(0)
        job.begin_near()
        normed_in.wait()
        transposed_product(normed_ref, first, terms_gate)
        run_gate.start()
        job.relay()
        run_down.slot(1)
        run_gate.slot(0)
        job.own()
        transposed_product(normed_ref, second, terms_up)
        store.start(terms_up, terms_up_hbm)
        run_down.slot(2)
        for copy in rest_in:
            copy.wait()
        job.end()
        values, change = middle_ref[...], summed[...]
        scale = norm_rows(values, gain_ref[...])[0]
        grad_gain[...] = jnp.sum(change * values * scale, axis=0, keepdims=True)
        change = change * gain_ref[...]
        mean = jnp.mean(change * values, axis=-1, keepdims=True)
        total = cot_ref[...].astype(jnp.float32) + scale * change - values * (scale * scale * scale * mean)
        grad_middle[...] = total
        own_branch[...] = total.astype(low)
        every.start()
        store.start(grad_middle, grad_middle_hbm)

        def rows_of(rank):
            return pl.ds(pl.multiple_of(rank * rows, rows), rows)

        def multiply(rank):
            at = rows_of(rank)
            grad_gated = product_nt(branch[at, :], out_ref[...])
            sigma = jax.nn.sigmoid(pre_ref[at, :])
            d_attended[at, :] = (grad_gated * sigma).astype(low)
            d_pre[at, :] = (
                grad_gated * attended_ref[at, :].astype(jnp.float32) * sigma * (1.0 - sigma)
            ).astype(low)

        branch[rows_of(me), :] = own_branch[...]
        multiply(me)
        run_gate.slot(1)
        every.relay()
        run_gate.slot(2)
        every.near()
        multiply(side)
        multiply(down)
        run_down.end()
        every.far()
        store.start(branch, branch_hbm)
        multiply(across)
        every.finish()
        run_gate.end()
        store.end()

    def shape(size, kind=low):
        return jax.ShapeDtypeStruct(size, kind)

    vmem = pl.BlockSpec(memory_space=pltpu.VMEM)
    anywhere = pl.BlockSpec(memory_space=pl.ANY)
    dma = pltpu.SemaphoreType.DMA
    own_shape = jax.ShapeDtypeStruct((rows, depth), low)
    fetched = (grads, weights, up_weights, normed, terms_down, w_out, middle, own_shape, attended, gate_pre)
    return pl.pallas_call(
        body,
        in_specs=[anywhere] * 7 + [vmem] + [anywhere] * 3,
        out_specs=[anywhere, vmem, anywhere, vmem, vmem, anywhere, vmem, vmem],
        out_shape=[
            shape((rows, depth), jnp.float32),
            shape((1, depth), jnp.float32),
            shape((slots, depth)),
            shape((slots, columns)),
            shape((slots, columns)),
            shape((depth, units)),
            shape((terms_down.shape[0] // shards, depth)),
            shape((depth // shards, units)),
        ],
        scratch_shapes=[
            pltpu.VMEM((rows, depth), low),
            pltpu.VMEM((rows, depth), jnp.float32),
            pltpu.VMEM((depth, units), low),
            dma((6,)),
            dma((6,)),
            *(pltpu.VMEM(value.shape, value.dtype) for value in fetched),
            pltpu.VMEM((rows, depth), jnp.float32),
            pltpu.VMEM((slots, depth), low),
            pltpu.VMEM((depth, units), low),
            dma((len(fetched),)),
            dma((3,)),
        ]
        + SquareScatter.scratch(rows, depth)
        + LineScatter.scratch(chips, terms_down.shape[0] // shards, depth)
        + LineScatter.scratch(chips, depth // shards, units),
        compiler_params=pltpu.CompilerParams(
            collective_id=collective_id, has_side_effects=True, vmem_limit_bytes=VMEM_LIMIT
        ),
        name="feed_backward",
    )(grads, weights, up_weights, normed, terms_down, w_out, middle, gain, cotangent, attended, gate_pre)


class SquareScatter:
    @staticmethod
    def scratch(rows, width):
        half = rows // 2
        low = jnp.bfloat16
        return [
            pltpu.VMEM((rows, width), low),
            pltpu.VMEM((2, half, width), low),
            pltpu.VMEM((2, half, width), jnp.float32),
            pltpu.VMEM((6, half, width), low),
            pltpu.VMEM((2, half, width), low),
            pltpu.SemaphoreType.DMA((6,)),
            pltpu.SemaphoreType.DMA((6,)),
        ]

    def __init__(self, lefts, rights, transposed, out, far, near, kept, land, carry, send, recv):
        self.lefts, self.rights, self.transposed, self.out = lefts, rights, transposed, out
        self.far, self.near, self.kept, self.land, self.carry = far, near, kept, land, carry
        self.send, self.recv = send, recv
        self.rows, self.width = out.shape
        self.half = self.rows // 2
        self.tile = self.width // 3 if self.width % 384 == 0 else self.width

    def copy(self, index):
        me, side, down, across = sides()
        source = (
            self.far.at[pl.ds(0, self.half)],
            self.far.at[pl.ds(self.half, self.half)],
            self.near.at[0],
            self.near.at[1],
            self.carry.at[0],
            self.carry.at[1],
        )[index]
        return pltpu.make_async_remote_copy(
            src_ref=source,
            dst_ref=self.land.at[index],
            send_sem=self.send.at[index],
            recv_sem=self.recv.at[index],
            device_id={"seq": down if index in (0, 3, 5) else side},
            device_id_type=MESH,
        )

    def partial(self, rank, store):
        at = pl.ds(pl.multiple_of(rank * self.rows, self.rows), self.rows)

        def step(number, carried):
            columns = pl.ds(pl.multiple_of(number * self.tile, self.tile), self.tile)
            value = None
            for a, b in zip(self.lefts, self.rights):
                if self.transposed:
                    term = product_nt(a[at, :], b[columns, :])
                else:
                    term = product(a[at, :], b[:, columns])
                value = term if value is None else value + term
            store(columns, value)
            return carried

        lax.fori_loop(0, self.width // self.tile, step, 0)

    def begin(self):
        self.begin_far()
        self.begin_near()

    def begin_far(self):
        me, side, down, across = sides()
        far = self.far

        def store_far(columns, value):
            far[:, columns] = value.astype(far.dtype)

        self.partial(across, store_far)
        self.copy(0).start()
        self.copy(1).start()

    def begin_near(self):
        me, side, down, across = sides()
        half, near, kept = self.half, self.near, self.kept

        def store_side(columns, value):
            kept[0, :, columns] = value[:half]
            near[0, :, columns] = value[half:].astype(near.dtype)

        def store_down(columns, value):
            near[1, :, columns] = value[:half].astype(near.dtype)
            kept[1, :, columns] = value[half:]

        self.partial(side, store_side)
        self.copy(2).start()
        self.partial(down, store_down)
        self.copy(3).start()

    def relay(self):
        for index in (0, 1):
            self.copy(index).wait_recv()

            def add(at, index=index):
                total = self.kept[index, at, :] + self.land[index, at, :].astype(jnp.float32)
                self.carry[index, at, :] = total.astype(self.carry.dtype)

            by_rows(self.half, add)
            self.copy(4 + index).start()

    def own(self):
        out = self.out

        def store_own(columns, value):
            out[:, columns] = value

        self.partial(lax.axis_index("seq"), store_own)

    def end(self):
        for index in (2, 3, 4, 5):
            self.copy(index).wait_recv()
        land, half, out = self.land, self.half, self.out

        def add(at):
            out[at, :] += land[3, at, :].astype(jnp.float32) + land[4, at, :].astype(jnp.float32)

        def add_second(at):
            to = pl.ds(at.start + half, at.size)
            out[to, :] += land[2, at, :].astype(jnp.float32) + land[5, at, :].astype(jnp.float32)

        by_rows(half, add)
        by_rows(half, add_second)
        for index in range(6):
            self.copy(index).wait_send()


class LineScatter:
    @staticmethod
    def scratch(chips, rows, width):
        low = jnp.bfloat16
        dma = pltpu.SemaphoreType.DMA
        return [pltpu.VMEM((chips, rows, width), low)] * 3 + [dma((2, chips)), dma((3, chips))]

    def __init__(self, terms, out, twin_in, forth_in, back_in, send, recv):
        self.terms, self.out, self.twin_in = terms, out, twin_in
        self.forth_in, self.back_in, self.send, self.recv = forth_in, back_in, send, recv
        self.chips, self.chip, self.core, *self.devices = line()
        self.rows = twin_in.shape[1]

    def term(self, chip, core):
        return self.terms.at[pl.ds(pl.multiple_of((2 * chip + core) * self.rows, self.rows), self.rows)]

    def swap(self, chip):
        return pltpu.make_async_remote_copy(
            src_ref=self.term(chip, 1 - self.core),
            dst_ref=self.twin_in.at[chip],
            send_sem=self.send.at[0, chip],
            recv_sem=self.recv.at[0, chip],
            device_id=self.devices[2],
            device_id_type=MESH,
        )

    def hop(self, way, chip):
        return pltpu.make_async_remote_copy(
            src_ref=self.twin_in.at[chip],
            dst_ref=(self.forth_in, self.back_in)[way].at[chip],
            send_sem=self.send.at[1, chip],
            recv_sem=self.recv.at[1 + way, chip],
            device_id=self.devices[way],
            device_id_type=MESH,
        )

    def start(self):
        for chip in (self.chips - 1, 0, *range(1, self.chips - 1)):
            self.swap(chip).start()

    def add(self, chip, ways, out):
        def step(at):
            start = pl.multiple_of((2 * chip + self.core) * self.rows + at.start, at.size)
            total = self.terms[pl.ds(start, at.size), :].astype(jnp.float32)
            total = total + self.twin_in[chip, at, :].astype(jnp.float32)
            for way in ways:
                total = total + (self.forth_in, self.back_in)[way][chip, at, :].astype(jnp.float32)
            out[at, :] = total.astype(out.dtype)

        by_rows(self.rows, step)

    def pass_on(self, way, chip, first):
        self.swap(chip).wait_recv()
        if not first:
            self.hop(way, chip).wait_recv()
        self.add(chip, () if first else (way,), self.twin_in.at[chip])
        self.hop(way, chip).start()

    def slot(self, number):
        last = self.chips - 1
        for chip in range(self.chips):
            forth, back = number - (last - chip), last - (number - chip)
            if 0 <= forth < chip:

                @pl.when(self.chip == forth)
                def _():
                    self.pass_on(0, chip, forth == 0)

            if chip < back <= last:

                @pl.when(self.chip == back)
                def _():
                    self.pass_on(1, chip, back == last)

    def end(self):
        for chip in range(self.chips):

            @pl.when(self.chip == chip)
            def _():
                self.swap(chip).wait_recv()
                ways = [way for way, there in enumerate((chip > 0, chip < self.chips - 1)) if there]
                for way in ways:
                    self.hop(way, chip).wait_recv()
                self.add(chip, ways, self.out)

            self.swap(chip).wait_send()

            @pl.when(self.chip != chip)
            def _():
                self.hop(0, chip).wait_send()


def middle_backward(joined, d_out, offset, col, logit, hidden, w_down, gated, grad_branch, terms_up, shares,
                    normed, d_pre, middle, head_size, scale, collective_id):
    slots, lanes = joined.shape
    width = w_down.shape[1]
    tokens = slots // 4
    columns = gated.shape[1]
    shards = 2 * lax.axis_size("seq")
    chips = shards // 2
    rows_up = terms_up.shape[0] // shards
    fetched = (terms_up, hidden, w_down, gated, grad_branch, normed, d_pre, joined, d_out, middle)

    def body(*refs):
        sources, refs = refs[:10], refs[10:]
        (offset_ref, col_ref, logit_ref, *share_refs), refs = refs[:5], refs[5:]
        (grads, bias_grad, layer_output, collected, share_up, share_pre, *every_refs), refs = refs[:8], refs[8:]
        buffers, refs = refs[:10], refs[10:]
        terms, terms_pre, lowered, send, recv, keep, fetch_sems, *scratch = refs
        up_ref, hidden_ref, down_ref, gated_ref, branch_ref, normed_ref, pre_ref, joined_ref, d_out_ref = buffers[:9]
        fetch = Streams(fetch_sems)
        comes = [fetch.start(source, buffer) for source, buffer in zip(sources, buffers)]
        me, side, down, across = sides()
        line_chips, chip, core, forth, back, twin = line()
        meet({"seq": side}, {"seq": down}, forth, back, twin)
        work = Backward(
            joined_ref, d_out_ref, offset_ref, col_ref, logit_ref, grads, *scratch[:4], head_size, scale
        )
        job = SquareScatter([hidden_ref], [down_ref], False, lowered, *scratch[4:11])
        collect = LineScatter(terms, collected, *scratch[11:16])
        run = LineScatter(up_ref, share_up, *scratch[16:21])
        run_pre = LineScatter(terms_pre, share_pre, *scratch[21:])
        every = [SquareGather(share_refs[i], every_refs[i], send.at[i], recv.at[i]) for i in range(2)]
        every[0].start()
        comes[0].wait()
        run.start()
        kept = []
        for i in range(2):
            size = share_refs[i].shape[0]
            kept.append(
                pltpu.make_async_copy(
                    share_refs[i],
                    every_refs[i].at[pl.ds(pl.multiple_of(me * size, size), size)],
                    keep.at[i],
                )
            )
            kept[i].start()
        comes[1].wait()
        comes[2].wait()
        job.begin_far()
        run.slot(0)
        job.begin_near()
        comes[3].wait()
        comes[4].wait()
        transposed_product(gated_ref, branch_ref, terms)
        collect.start()
        comes[5].wait()
        comes[6].wait()
        transposed_product(normed_ref, pre_ref, terms_pre)
        run_pre.start()
        collect.slot(0)
        for copy in comes[7:]:
            copy.wait()
        run_pre.slot(0)
        work.start()

        def step(pair, carry):
            work.pair(pair)

            @pl.when(pair == 0)
            def _():
                run.slot(1)
                job.relay()
                every[0].relay()
                every[1].start()
                collect.slot(1)
                run_pre.slot(1)

            @pl.when(pair == 1)
            def _():
                run.slot(2)
                collect.slot(2)
                run_pre.slot(2)
                every[1].relay()

            return carry

        lax.fori_loop(0, work.pairs, step, 0)
        job.own()
        work.end(bias_grad)
        job.end()
        layer_output[...] = (buffers[9][...] + lowered[...]).astype(layer_output.dtype)
        run.end()
        collect.end()
        run_pre.end()
        for gathering, copy in zip(every, kept):
            gathering.near()
            gathering.far()
            gathering.finish()
            copy.wait()

    vmem = pl.BlockSpec(memory_space=pltpu.VMEM)
    anywhere = pl.BlockSpec(memory_space=pl.ANY)
    low = jnp.bfloat16
    dma = pltpu.SemaphoreType.DMA
    return pl.pallas_call(
        body,
        in_specs=[anywhere] * 10 + [vmem] * 5,
        out_specs=[vmem] * 6 + [anywhere] * 2,
        out_shape=[
            jax.ShapeDtypeStruct((slots, lanes), low),
            jax.ShapeDtypeStruct((8, PAIR), jnp.float32),
            jax.ShapeDtypeStruct((tokens, width), low),
            jax.ShapeDtypeStruct((columns // shards, width), low),
            jax.ShapeDtypeStruct((rows_up, terms_up.shape[1]), low),
            jax.ShapeDtypeStruct((rows_up, columns), low),
            *(jax.ShapeDtypeStruct((4 * v.shape[0], v.shape[1]), low) for v in shares),
        ],
        scratch_shapes=[
            *(pltpu.VMEM(value.shape, value.dtype) for value in fetched),
            pltpu.VMEM((columns, width), low),
            pltpu.VMEM((width, columns), low),
            pltpu.VMEM((tokens, width), jnp.float32),
            dma((2, 6)),
            dma((2, 6)),
            dma((2,)),
            dma((10,)),
        ]
        + backward_scratch(slots)
        + SquareScatter.scratch(tokens, width)
        + LineScatter.scratch(chips, columns // shards, width)
        + LineScatter.scratch(chips, rows_up, terms_up.shape[1])
        + LineScatter.scratch(chips, rows_up, columns),
        compiler_params=pltpu.CompilerParams(
            collective_id=collective_id, has_side_effects=True, vmem_limit_bytes=VMEM_LIMIT
        ),
        name="middle_backward",
    )(*fetched, offset, col, logit, *shares)


def last_backward(grads, d_pre, normed, weights, gate_weights, collected, shares, inputs, gain, grad_middle,
                  small, collective_id):
    slots, depth = normed.shape
    front = grads.shape[1]
    tokens = slots // 4
    shards = 2 * lax.axis_size("seq")
    rows = depth // shards
    fetched = (normed, grads, d_pre, weights, gate_weights, inputs, grad_middle)

    def body(*refs):
        sources, refs = refs[:7], refs[7:]
        (collected_ref, gain_ref, small_ref, *share_refs), refs = refs[:5], refs[5:]
        (grad_input, small_out, regrouped, *every_refs), refs = refs[:6], refs[6:]
        buffers, refs = refs[:7], refs[7:]
        terms, summed, share, small_own, send, recv, keep, fetch_sems, *scratch = refs
        normed_ref, grads_ref, pre_ref, weights_ref, gate_weights_ref, inputs_ref, middle_ref = buffers
        fetch = Streams(fetch_sems)
        comes = [fetch.start(source, buffer) for source, buffer in zip(sources, buffers)]
        me, side, down, across = sides()
        regroup = Regroup(collected_ref, regrouped, *scratch[12:15])
        total = Everywhere(small_own, small_out, *scratch[20:])
        meet(*regroup.others, *regroup.along)
        job = SquareScatter([grads_ref, pre_ref], [weights_ref, gate_weights_ref], True, summed, *scratch[:7])
        halves = (pl.ds(0, front // 2), pl.ds(front // 2, front // 2))
        runs = [
            LineScatter(terms.at[:, half], share.at[:, half], *scratch[at : at + 5])
            for half, at in zip(halves, (7, 15))
        ]
        regroup.start()
        every = [SquareGather(share_refs[i], every_refs[i], send.at[i], recv.at[i]) for i in range(2)]
        every[0].start()
        every[1].start()
        kept = []
        for i in range(2):
            size = share_refs[i].shape[0]
            kept.append(
                pltpu.make_async_copy(
                    share_refs[i],
                    every_refs[i].at[pl.ds(pl.multiple_of(me * size, size), size)],
                    keep.at[i],
                )
            )
            kept[i].start()
        comes[0].wait()
        comes[1].wait()
        for half, run in zip(halves, runs):
            transposed_product(normed_ref, grads_ref.at[:, half], terms.at[:, half])
            run.start()
        runs[0].slot(0)
        for copy in comes[2:]:
            copy.wait()
        job.begin_far()
        runs[1].slot(0)
        regroup.relay()
        runs[0].slot(1)
        job.begin_near()
        runs[1].slot(1)
        every[0].relay()
        job.relay()
        runs[0].slot(2)
        every[1].relay()
        runs[1].slot(2)
        job.own()
        job.end()
        values, change = inputs_ref[...].astype(jnp.float32), summed[...]
        scale = norm_rows(values, gain_ref[...])[0]
        small_own[...] = small_ref[...]
        small_own[:, :depth] = jnp.sum(change * values * scale, axis=0, keepdims=True)
        total.start()
        change = change * gain_ref[...]
        mean = jnp.mean(change * values, axis=-1, keepdims=True)
        grad_input[...] = middle_ref[...] + scale * change - values * (scale * scale * scale * mean)
        for run in runs:
            run.end()
        every.append(SquareGather(share, every_refs[2], send.at[2], recv.at[2]))
        every[2].start()
        size = share.shape[0]
        kept.append(
            pltpu.make_async_copy(
                share, every_refs[2].at[pl.ds(pl.multiple_of(me * size, size), size)], keep.at[2]
            )
        )
        kept[2].start()
        total.relay()
        every[2].relay()
        regroup.end()
        total.end()
        for gathering, copy in zip(every, kept):
            gathering.near()
            gathering.far()
            gathering.finish()
            copy.wait()

    vmem = pl.BlockSpec(memory_space=pltpu.VMEM)
    anywhere = pl.BlockSpec(memory_space=pl.ANY)
    low = jnp.bfloat16
    dma = pltpu.SemaphoreType.DMA
    return pl.pallas_call(
        body,
        in_specs=[anywhere] * 7 + [vmem] * 5,
        out_specs=[vmem] * 3 + [anywhere] * 3,
        out_shape=[
            jax.ShapeDtypeStruct((tokens, depth), jnp.float32),
            jax.ShapeDtypeStruct(small.shape, jnp.float32),
            jax.ShapeDtypeStruct((4,) + collected.shape, low),
            *(jax.ShapeDtypeStruct((4 * v.shape[0], v.shape[1]), low) for v in shares),
            jax.ShapeDtypeStruct((4 * rows, front), low),
        ],
        scratch_shapes=[
            *(pltpu.VMEM(value.shape, value.dtype) for value in fetched),
            pltpu.VMEM((depth, front), low),
            pltpu.VMEM((tokens, depth), jnp.float32),
            pltpu.VMEM((rows, front), low),
            pltpu.VMEM(small.shape, jnp.float32),
            dma((3, 6)),
            dma((3, 6)),
            dma((3,)),
            dma((7,)),
        ]
        + SquareScatter.scratch(tokens, depth)
        + LineScatter.scratch(shards // 2, rows, front // 2)
        + Regroup.scratch(*collected.shape)
        + LineScatter.scratch(shards // 2, rows, front // 2)
        + Everywhere.scratch(small.shape),
        compiler_params=pltpu.CompilerParams(
            collective_id=collective_id, has_side_effects=True, vmem_limit_bytes=VMEM_LIMIT
        ),
        name="last_backward",
    )(*fetched, collected, gain, small, *shares)


def gather(value, axis_name):
    return lax.all_gather(value, axis_name, axis=0, tiled=True)


def scatter(value, axis_name):
    return lax.psum_scatter(value, axis_name, scatter_dimension=0, tiled=True)


def on_device(
    layer_input,
    lengths,
    norm_attn,
    w_query,
    w_key,
    w_value,
    w_ogate,
    w_forget,
    forget_bias,
    w_out,
    norm_ffn,
    w_gate,
    w_up,
    w_down,
    output_grad,
):
    low = jnp.bfloat16
    tokens, width = layer_input.shape[1:]
    heads = forget_bias.shape[0]
    groups = lax.axis_size("seq")
    shards = lax.axis_size("wshard")
    fast = square(groups) and shards == 2 * groups
    local_heads = heads // groups
    head_size = width // heads
    columns = width // groups
    lanes = columns + -columns % PAIR
    front = 3 * lanes + PAIR
    slots = tokens * groups
    hidden_size = w_gate.shape[1]
    part = hidden_size // (groups * shards)
    units = shards * part
    scale = head_size ** (-0.5)
    length = lengths[0]
    seq_rank = lax.axis_index("seq")
    shard_rank = lax.axis_index("wshard")
    per_block = shards // groups
    positions = seq_rank * tokens + jnp.arange(tokens, dtype=jnp.int32)
    valid_slots = (positions < length)[:, None]
    inputs = layer_input[0].astype(jnp.float32)
    cotangent_low = jnp.where(valid_slots, output_grad[0], jnp.zeros((), low))
    cotangent = cotangent_low.astype(jnp.float32)

    def own_columns(weight, size):
        taken = lax.dynamic_slice_in_dim(weight, seq_rank * columns, columns, 1)
        return jnp.pad(taken, ((0, 0), (0, size - columns))) if size > columns else taken

    def own_units(weight):
        split = weight.reshape(weight.shape[0], shards, groups, part)
        mine = lax.dynamic_index_in_dim(split, seq_rank, 2, keepdims=False)
        return mine.reshape(weight.shape[0], units)

    def own_bias_grad(bias_rows):
        return lax.dynamic_update_slice_in_dim(
            jnp.zeros((heads,), jnp.float32), bias_rows[:local_heads, 0], seq_rank * local_heads, 0
        )

    own_forget = lax.dynamic_slice_in_dim(w_forget, seq_rank * local_heads, local_heads, 1)
    own_forget = jnp.pad(own_forget, ((0, 0), (0, PAIR - local_heads)))
    own_bias = lax.dynamic_slice_in_dim(forget_bias, seq_rank * local_heads, local_heads)
    own_bias = jnp.pad(own_bias, (0, PAIR - local_heads))[None]
    length_row = jnp.broadcast_to(lengths[:, None], (1, PAIR))
    mine_down = lax.dynamic_slice_in_dim(w_down, seq_rank * part, part, 0)
    if fast:
        (
            normed_attn, cotangent_all, full_front, full_ogate, full_out, full_ffn,
            joined, attended_low, offset, col, logit, gate_pre, gated, middle, mine_up,
        ) = whole_forward(
            layer_input[0], norm_attn[None], output_grad[0], (w_query, w_key, w_value, w_ogate), own_forget,
            own_bias, length_row, w_out, w_gate, w_up, head_size, scale, 0,
        )
        full_out = full_out.reshape(columns, width)
        normed_ffn, hidden, full_up, full_down, grad_gate_up, terms_down = feed_forward(
            middle, norm_ffn[None], full_ffn, mine_up, mine_down, cotangent_all, 1
        )
        (
            grad_middle, grad_norm_ffn, grad_branch, grad_attended, grad_gate_pre, terms_up, share_down, share_gate,
        ) = feed_backward(
            grad_gate_up, full_ffn, full_up, normed_ffn, terms_down, full_out, middle, norm_ffn[None],
            cotangent_all, attended_low, gate_pre, 2,
        )
        grad_norm_ffn = grad_norm_ffn[0]
        grads, bias_rows, layer_output, collected, share_up, share_ogate, grad_down, every_gate = middle_backward(
            joined, grad_attended, offset, col, logit, hidden, full_down, gated, grad_branch, terms_up,
            (share_down, share_gate), normed_attn, grad_gate_pre, middle, head_size, scale, 3,
        )
        vector = jnp.concatenate([jnp.zeros((width,), jnp.float32), grad_norm_ffn, own_bias_grad(bias_rows)])
        vector = jnp.pad(vector, (0, -vector.shape[0] % PAIR))[None]
        grad_input, vector, grad_out, every_ogate, every_up, every_attn = last_backward(
            grads, grad_gate_pre, normed_attn, full_front, full_ogate, collected, (share_ogate, share_up),
            layer_input[0], norm_attn[None], grad_middle, vector, 4,
        )
        small = vector[0, :width], vector[0, width : 2 * width], vector[0, 2 * width : 2 * width + heads]
        grad_out = grad_out.reshape(columns // per_block, width)
    else:
        mine_front = jnp.concatenate(
            [*(own_columns(w, lanes) for w in (w_query, w_key, w_value)), own_forget], axis=1
        )
        full_front = gather(mine_front, "wshard")
        full_ogate = gather(own_columns(w_ogate, columns), "wshard")
        normed_attn = gather(rms_norm(inputs, norm_attn).astype(low), "seq")
        cotangent_all = gather(cotangent_low, "seq")
        full_out = lax.dynamic_slice_in_dim(gather(w_out, "wshard"), seq_rank * columns, columns, 0)
        full_ffn = gather(jnp.concatenate([own_units(w_gate), own_units(w_up)], axis=1), "wshard")
        joined = product(normed_attn, full_front).astype(low)
        gate_pre = product(normed_attn, full_ogate)
        attended_low, offset, col, logit = attention_fwd(joined, own_bias, length_row, head_size, scale)
        attended = attended_low[:, :columns].astype(jnp.float32)
        gated_full, pull_gate = jax.vjp(gate_product, attended, gate_pre)
        gated = gated_full.astype(low)
        middle = inputs + scatter(product(gated, full_out).astype(low), "seq").astype(jnp.float32)
        normed_ffn_own, pull_ffn_norm = jax.vjp(rms_norm, middle, norm_ffn)
        full_down = gather(mine_down, "wshard")
        normed_ffn = gather(normed_ffn_own.astype(low), "seq")
        gate_up = product(normed_ffn, full_ffn)
        hidden_full, pull_swiglu = jax.vjp(swiglu, gate_up[:, :units], gate_up[:, units:])
        hidden = hidden_full.astype(low)
        grad_hidden = product_nt(cotangent_all, full_down)
        grad_gate_full, grad_up_full = pull_swiglu(grad_hidden)
        grad_gate_up = jnp.concatenate([grad_gate_full.astype(low), grad_up_full.astype(low)], axis=1)
        share_down = scatter(product_tn(hidden, cotangent_all).astype(low), "wshard")
        share_ffn = scatter(product_tn(normed_ffn, grad_gate_up).astype(low), "wshard")
        grad_normed_ffn = scatter(product_nt(grad_gate_up, full_ffn).astype(low), "seq").astype(jnp.float32)
        grad_middle_part, grad_norm_ffn = pull_ffn_norm(grad_normed_ffn)
        grad_middle = cotangent + grad_middle_part
        grad_branch = gather(grad_middle.astype(low), "seq")
        grad_attended_full, grad_gate_pre_full = pull_gate(product_nt(grad_branch, full_out))
        grad_attended = grad_attended_full.astype(low)
        grad_gate_pre = grad_gate_pre_full.astype(low)
        if lanes > columns:
            grad_attended = jnp.pad(grad_attended, ((0, 0), (0, lanes - columns)))
        grads, bias_rows = attention_bwd(joined, grad_attended, offset, col, logit, head_size, scale)
        grad_projected = jnp.concatenate([grads, grad_gate_pre], axis=1)
        share_attn = scatter(product_tn(normed_attn, grad_projected).astype(low), "wshard")
        full_attn = jnp.concatenate([full_front, full_ogate], axis=1)
        grad_normed_attn = scatter(product_nt(grad_projected, full_attn).astype(low), "seq").astype(jnp.float32)
        lowered = scatter(product(hidden, full_down).astype(low), "seq").astype(jnp.float32)
        share_out = scatter(product_tn(gated, grad_branch).astype(low), "wshard")
        rows_out = columns // shards
        pieces_out = lax.all_gather(share_out, "seq", axis=0, tiled=False)
        takes = shards // per_block
        slots_out = jnp.where(
            (jnp.arange(per_block) == shard_rank // takes)[None, :, None, None],
            pieces_out[:, None],
            jnp.zeros((), low),
        ).reshape(shards, rows_out, width)
        moved = lax.all_to_all(slots_out, "wshard", split_axis=0, concat_axis=0, tiled=True)
        moved = moved.reshape(per_block, takes, rows_out, width)
        mine_out = lax.dynamic_index_in_dim(moved, shard_rank % per_block, 0, keepdims=False)
        grad_out = mine_out.reshape(columns // per_block, width).astype(jnp.float32)
        layer_output = (middle + lowered).astype(low)
        unused_normed, pull_attn_norm = jax.vjp(rms_norm, inputs, norm_attn)
        grad_input_part, grad_norm_attn = pull_attn_norm(grad_normed_attn)
        grad_input = grad_middle + grad_input_part
    if not fast:
        every_attn, every_ffn, grad_down = [gather(v, "seq") for v in (share_attn, share_ffn, share_down)]
        small = lax.psum((grad_norm_attn, grad_norm_ffn, own_bias_grad(bias_rows)), ("seq", "wshard"))
    rows = width // shards
    every_attn = every_attn.reshape(groups, rows, every_attn.shape[1])
    if fast:
        *weight_grads, grad_forget_w, grad_w_gate, grad_w_up, grad_down, grad_out = join_shares(
            every_attn,
            every_ogate.reshape((groups,) + share_ogate.shape),
            every_gate.reshape((groups,) + share_gate.shape),
            every_up.reshape((groups,) + share_up.shape),
            grad_down,
            grad_out,
            columns,
            (0, lanes, 2 * lanes),
            3 * lanes,
            heads,
            part,
        )
    else:

        def join(first):
            taken = every_attn[:, :, first : first + columns]
            return taken.transpose(1, 0, 2).reshape(rows, width).astype(jnp.float32)

        def join_own_units(first):
            taken = every_ffn.reshape((groups,) + share_ffn.shape)[:, :, first * units : (first + 1) * units]
            taken = taken.reshape(groups, rows, shards, part).transpose(1, 2, 0, 3)
            return taken.reshape(rows, hidden_size).astype(jnp.float32)

        weight_grads = [join(first) for first in (0, lanes, 2 * lanes, front)]
        grad_w_gate, grad_w_up = join_own_units(0), join_own_units(1)
        grad_down = grad_down.astype(jnp.float32)
        grad_forget_w = every_attn[:, :, 3 * lanes : 3 * lanes + local_heads]
        grad_forget_w = grad_forget_w.transpose(1, 0, 2).reshape(rows, heads).astype(jnp.float32)
    return (
        layer_output[None],
        grad_input[None],
        small[0],
        *weight_grads,
        grad_forget_w,
        small[2],
        grad_out,
        small[1],
        grad_w_gate,
        grad_w_up,
        grad_down,
    )


def solution(mesh):
    return jax.shard_map(
        on_device,
        mesh=mesh,
        in_specs=(
            P("wshard", "seq", None),
            P("wshard"),
            P(),
            P("wshard", None),
            P("wshard", None),
            P("wshard", None),
            P("wshard", None),
            P("wshard", None),
            P(),
            P("wshard", None),
            P(),
            P("wshard", None),
            P("wshard", None),
            P("wshard", None),
            P("wshard", "seq", None),
        ),
        out_specs=(
            P("wshard", "seq", None),
            P("wshard", "seq", None),
            P(),
            P("wshard", None),
            P("wshard", None),
            P("wshard", None),
            P("wshard", None),
            P("wshard", None),
            P(),
            P("wshard", None),
            P(),
            P("wshard", None),
            P("wshard", None),
            P("wshard", None),
        ),
        check_vma=False,
    )
```

```python
import jax
import jax.numpy as jnp
from jax import lax
from jax.experimental import pallas as pl
from jax.experimental.pallas import tpu as pltpu
from jax.sharding import PartitionSpec as P

EPS = 1e-06
NEG_FILL = -1e30
PAIR = 128


def product(left, right):
    return jnp.dot(left, right, preferred_element_type=jnp.float32)


def product_tn(left, right):
    return lax.dot_general(
        left, right, (((0,), (0,)), ((), ())), preferred_element_type=jnp.float32
    )


def product_nt(left, right):
    return lax.dot_general(
        left, right, (((1,), (1,)), ((), ())), preferred_element_type=jnp.float32
    )


def rms_norm(values, gain):
    return values * lax.rsqrt(jnp.mean(values * values, axis=-1, keepdims=True) + EPS) * gain


def gate_product(attended, gate_pre):
    return attended * jax.nn.sigmoid(gate_pre)


def swiglu(gate, upward):
    return jax.nn.silu(gate) * upward


def low_triangle(size):
    rows = lax.broadcasted_iota(jnp.int32, (size, size), 0)
    return rows <= lax.broadcasted_iota(jnp.int32, (size, size), 1)


def exact(left, right):
    return jnp.dot(left, right, precision=lax.Precision.HIGHEST, preferred_element_type=jnp.float32)


class Forward:
    some = 8

    def __init__(self, joined, bias, length, attended, offset, col, logit, row, head_size, scale):
        self.joined, self.bias, self.length = joined, bias, length
        self.attended, self.offset, self.col, self.logit, self.row = attended, offset, col, logit, row
        self.head_size, self.scale = head_size, scale
        self.slots = joined.shape[0]
        self.pairs = (joined.shape[1] // PAIR - 1) // 3
        self.tile = min(256, self.slots)

    @staticmethod
    def results(slots, pairs):
        rows = jax.ShapeDtypeStruct((Forward.some, slots), jnp.float32)
        return [
            jax.ShapeDtypeStruct((slots, pairs * PAIR), jnp.bfloat16),
            rows,
            jax.ShapeDtypeStruct((slots, PAIR), jnp.float32),
            rows,
        ]

    def lanes(self, pair, part=0):
        return pl.ds(pl.multiple_of((part * self.pairs + pair) * PAIR, PAIR), PAIR)

    def start(self):
        slots, tile, some = self.slots, self.tile, self.some
        logits = self.joined[:, 3 * self.pairs * PAIR :].astype(jnp.float32) + self.bias[...]
        logit_rows = logits.T[:some]
        self.logit[...] = logit_rows
        logs = jnp.minimum(logit_rows, 0.0) - jnp.log1p(jnp.exp(-jnp.abs(logit_rows)))
        ones = low_triangle(tile).astype(jnp.float32)
        carry = jnp.zeros((some, 1), jnp.float32)
        for first in range(0, slots, tile):
            sums = exact(logs[:, first : first + tile], ones) + carry
            self.row[:, first : first + tile] = sums
            carry = sums[:, tile - 1 : tile]
        wide = jnp.concatenate([self.row[...], jnp.zeros((PAIR - some, slots), jnp.float32)], axis=0).T
        usable = lax.broadcasted_iota(jnp.int32, (slots, PAIR), 0) < self.length[...]
        self.col[...] = jnp.where(usable, wide, -NEG_FILL)

    def pair(self, pair):
        slots, tile, half = self.slots, self.tile, self.head_size
        key_all = self.joined[:, self.lanes(pair, 1)]
        value_t = self.joined[:, self.lanes(pair, 2)].T
        query_t = (self.joined[:, self.lanes(pair)].astype(jnp.float32) * self.scale).astype(jnp.bfloat16).T
        sub = lax.broadcasted_iota(jnp.int32, (PAIR, tile), 0)
        wide = lax.broadcasted_iota(jnp.int32, (slots, PAIR), 1)
        diag = low_triangle(tile)
        columns = [
            jnp.sum(jnp.where(wide == 2 * pair + a, self.col[...], 0.0), axis=1, keepdims=True) for a in range(2)
        ]
        for number in range(slots // tile):
            first, last = number * tile, (number + 1) * tile
            outs = []
            for a in range(2):
                mine = (sub >= a * half) & (sub < (a + 1) * half)
                at = pl.ds(2 * pair + a, 1)
                query = jnp.where(mine, query_t[:, first:last], jnp.zeros((), query_t.dtype))
                scores = product(key_all[:last], query)
                own_row = self.row[at, first:last]
                scores = scores + (own_row - columns[a][:last])
                tail = jnp.where(diag, scores[first:], NEG_FILL)
                scores = tail if number == 0 else jnp.concatenate([scores[:first], tail], axis=0)
                top = jnp.max(scores, axis=0, keepdims=True)
                weights = jnp.exp(scores - top)
                total = jnp.sum(weights, axis=0, keepdims=True)
                mixed = product(value_t[a * half : (a + 1) * half, :last], weights.astype(jnp.bfloat16))
                outs.append(mixed / total)
                self.offset[at, first:last] = own_row - (top + jnp.log(total))
            self.attended[first:last, self.lanes(pair)] = jnp.concatenate(outs, axis=0).T.astype(jnp.bfloat16)


def attention_fwd(joined, bias, length, head_size, scale):
    slots = joined.shape[0]
    pairs = (joined.shape[1] // PAIR - 1) // 3

    def body(joined_ref, bias_ref, length_ref, attended, offset, col, logit, row):
        work = Forward(joined_ref, bias_ref, length_ref, attended, offset, col, logit, row, head_size, scale)
        work.start()
        offset[...] = jnp.zeros_like(offset)

        def step(pair, carry):
            work.pair(pair)
            return carry

        lax.fori_loop(0, pairs, step, 0)

    vmem = pl.BlockSpec(memory_space=pltpu.VMEM)
    return pl.pallas_call(
        body,
        in_specs=[vmem] * 3,
        out_specs=[vmem] * 4,
        out_shape=Forward.results(slots, pairs),
        scratch_shapes=[pltpu.VMEM((Forward.some, slots), jnp.float32)],
        compiler_params=pltpu.CompilerParams(vmem_limit_bytes=56 << 20),
        cost_estimate=pl.CostEstimate(
            flops=4 * slots * slots * pairs * PAIR, bytes_accessed=8 * slots * pairs * PAIR, transcendentals=0
        ),
        name="attention_fwd",
    )(joined, bias, length)


def backward_scratch(slots):
    return [
        pltpu.VMEM((slots, PAIR), jnp.float32),
        pltpu.VMEM((slots, PAIR), jnp.float32),
        pltpu.VMEM((slots, PAIR), jnp.float32),
        pltpu.VMEM((8, slots), jnp.float32),
    ]


class Backward:
    def __init__(self, joined, d_out, offset, col, logit, grads, dk_acc, dv_acc, dcol, drow, head_size, scale):
        self.joined, self.d_out, self.offset, self.col = joined, d_out, offset, col
        self.logit, self.grads, self.dk_acc, self.dv_acc = logit, grads, dk_acc, dv_acc
        self.dcol, self.drow, self.head_size, self.scale = dcol, drow, head_size, scale
        self.slots = joined.shape[0]
        self.pairs = (joined.shape[1] // PAIR - 1) // 3
        self.tile = min(256, self.slots)

    def start(self):
        self.dcol[...] = jnp.zeros_like(self.dcol)
        self.drow[...] = jnp.zeros_like(self.drow)

    def lanes(self, pair, part=0):
        return pl.ds(pl.multiple_of((part * self.pairs + pair) * PAIR, PAIR), PAIR)

    def pair(self, pair):
        slots, tile, half = self.slots, self.tile, self.head_size
        dk_acc, dv_acc, dcol, drow = self.dk_acc, self.dv_acc, self.dcol, self.drow
        queries = (self.joined[:, self.lanes(pair)].astype(jnp.float32) * self.scale).astype(jnp.bfloat16)
        key_all = self.joined[:, self.lanes(pair, 1)]
        value_all = self.joined[:, self.lanes(pair, 2)]
        d_out = self.d_out[:, self.lanes(pair)]
        query_t, key_t, dout_t = queries.T, key_all.T, d_out.T
        sub = lax.broadcasted_iota(jnp.int32, (PAIR, tile), 0)
        lanes = lax.broadcasted_iota(jnp.int32, (tile, PAIR), 1)
        wide = lax.broadcasted_iota(jnp.int32, (slots, PAIR), 1)
        diag = low_triangle(tile)
        zero = jnp.zeros((), jnp.bfloat16)
        columns = [
            jnp.sum(jnp.where(wide == 2 * pair + a, self.col[...], 0.0), axis=1, keepdims=True) for a in range(2)
        ]
        dk_acc[...] = jnp.zeros_like(dk_acc)
        dv_acc[...] = jnp.zeros_like(dv_acc)
        for number in range(slots // tile):
            first, last = number * tile, (number + 1) * tile
            outs = []
            for a in range(2):
                mine = (sub >= a * half) & (sub < (a + 1) * half)
                own = (lanes >= a * half) & (lanes < (a + 1) * half)
                at = pl.ds(2 * pair + a, 1)
                scores = product(key_all[:last], jnp.where(mine, query_t[:, first:last], zero))
                scores = scores + (self.offset[at, first:last] - columns[a][:last])
                tail = jnp.where(diag, scores[first:], NEG_FILL)
                scores = tail if number == 0 else jnp.concatenate([scores[:first], tail], axis=0)
                probs = jnp.exp(scores)
                d_probs = product(value_all[:last], jnp.where(mine, dout_t[:, first:last], zero))
                dot = jnp.sum(d_probs * probs, axis=0, keepdims=True)
                d_full = probs * (d_probs - dot)
                d_scores = d_full.astype(jnp.bfloat16)
                drow[at, first:last] = jnp.sum(d_full, axis=0, keepdims=True)
                sums = jnp.sum(d_full, axis=1, keepdims=True)
                dcol[:last, :] += jnp.where(wide[:last] == 2 * pair + a, sums, 0.0)
                outs.append(product(key_t[a * half : (a + 1) * half, :last], d_scores) * self.scale)
                dk_acc[:last, :] += product(d_scores, jnp.where(own, queries[first:last, :], zero))
                dv_acc[:last, :] += product(
                    probs.astype(jnp.bfloat16), jnp.where(own, d_out[first:last, :], zero)
                )
            self.grads[first:last, self.lanes(pair)] = jnp.concatenate(outs, axis=0).T.astype(self.grads.dtype)
        self.grads[:, self.lanes(pair, 1)] = dk_acc[...].astype(self.grads.dtype)
        self.grads[:, self.lanes(pair, 2)] = dv_acc[...].astype(self.grads.dtype)

    def end(self, bias_grad):
        slots, tile, some = self.slots, self.tile, 8
        change = self.drow[...] - self.dcol[...].T[:some]
        rows = lax.broadcasted_iota(jnp.int32, (tile, tile), 0)
        ones = (rows >= lax.broadcasted_iota(jnp.int32, (tile, tile), 1)).astype(jnp.float32)
        carry = jnp.zeros((some, 1), jnp.float32)
        pieces = []
        for first in reversed(range(0, slots, tile)):
            sums = exact(change[:, first : first + tile], ones) + carry
            carry = sums[:, :1]
            pieces.insert(0, sums)
        grad = jnp.concatenate(pieces, axis=1) * jax.nn.sigmoid(-self.logit[...])
        heads = lax.broadcasted_iota(jnp.int32, (some, slots), 0)
        grad = jnp.where(heads < 2 * self.pairs, grad, 0.0)
        bias_grad[...] = jnp.broadcast_to(jnp.sum(grad, axis=1, keepdims=True), bias_grad.shape)
        wide = jnp.concatenate([grad, jnp.zeros((PAIR - some, slots), jnp.float32)], axis=0).T
        self.grads[:, 3 * self.pairs * PAIR : (3 * self.pairs + 1) * PAIR] = wide.astype(self.grads.dtype)


def attention_bwd(joined, d_out, offset, col, logit, head_size, scale):
    slots, width = joined.shape
    pairs = (width // PAIR - 1) // 3

    def body(joined_ref, d_out_ref, offset_ref, col_ref, logit_ref, grads, bias_grad, *scratch):
        work = Backward(
            joined_ref, d_out_ref, offset_ref, col_ref, logit_ref, grads, *scratch, head_size, scale
        )
        work.start()

        def step(pair, carry):
            work.pair(pair)
            return carry

        lax.fori_loop(0, pairs, step, 0)
        work.end(bias_grad)

    vmem = pl.BlockSpec(memory_space=pltpu.VMEM)
    return pl.pallas_call(
        body,
        in_specs=[vmem] * 5,
        out_specs=[vmem] * 2,
        out_shape=[
            jax.ShapeDtypeStruct((slots, width), jnp.bfloat16),
            jax.ShapeDtypeStruct((8, PAIR), jnp.float32),
        ],
        scratch_shapes=backward_scratch(slots),
        compiler_params=pltpu.CompilerParams(vmem_limit_bytes=56 << 20),
        cost_estimate=pl.CostEstimate(
            flops=10 * slots * slots * pairs * PAIR, bytes_accessed=14 * slots * pairs * PAIR, transcendentals=0
        ),
        name="attention_bwd",
    )(joined, d_out, offset, col, logit)


MESH = pl.DeviceIdType.MESH
VMEM_LIMIT = 62 << 20


def square(groups):
    return groups == 4


def sides():
    rank = lax.axis_index("seq")
    return rank, rank + 1 - 2 * lax.rem(rank, 2), lax.rem(rank + 2, 4), 3 - rank


def meet(*others):
    barrier = pltpu.get_barrier_semaphore()
    for other in others:
        pl.semaphore_signal(barrier, inc=1, device_id=other, device_id_type=MESH)
    pl.semaphore_wait(barrier, len(others))


def push(source, target, send, recv, device):
    copy = pltpu.make_async_remote_copy(
        src_ref=source,
        dst_ref=target,
        send_sem=send,
        recv_sem=recv,
        device_id=device,
        device_id_type=MESH,
    )
    copy.start()
    return copy


def by_rows(rows, work):
    def step(number, carry):
        work(pl.ds(pl.multiple_of(number * 16, 16), 16))
        return carry

    lax.fori_loop(0, rows // 16, step, 0)


class Streams:
    def __init__(self, sems):
        self.sems, self.made = sems, []

    def start(self, source, target):
        copy = pltpu.make_async_copy(source, target, self.sems.at[len(self.made)])
        self.made.append(copy)
        copy.start()
        return copy

    def end(self):
        for copy in self.made:
            copy.wait()


class SquareGather:
    def __init__(self, own, full, send, recv):
        self.own, self.full, self.send, self.recv = own, full, send, recv
        self.rows = own.shape[0]
        self.half = self.rows // 2

    def place(self, rank, part):
        return self.full.at[pl.ds(pl.multiple_of(rank * self.rows + part * self.half, self.half), self.half)]

    def copy(self, index):
        me, side, down, across = sides()
        mine = [self.own.at[pl.ds(part * self.half, self.half)] for part in (0, 1)]
        source, target, peer = (
            (mine[0], self.place(me, 0), side),
            (mine[1], self.place(me, 1), down),
            (mine[1], self.place(me, 1), side),
            (mine[0], self.place(me, 0), down),
            (self.place(side, 0), self.place(side, 0), down),
            (self.place(down, 1), self.place(down, 1), side),
        )[index]
        return pltpu.make_async_remote_copy(
            src_ref=source,
            dst_ref=target,
            send_sem=self.send.at[index],
            recv_sem=self.recv.at[index],
            device_id={"seq": peer},
            device_id_type=MESH,
        )

    def start(self):
        for index in range(4):
            self.copy(index).start()

    def relay(self):
        for index in (0, 1):
            self.copy(index).wait_recv()
            self.copy(4 + index).start()

    def near(self):
        self.copy(2).wait_recv()
        self.copy(3).wait_recv()

    def far(self):
        self.copy(4).wait_recv()
        self.copy(5).wait_recv()

    def finish(self):
        for index in range(6):
            self.copy(index).wait_send()


def block_product(left, right, transposed, tile, store):
    total = right.shape[0] if transposed else right.shape[1]

    def step(number, carry):
        columns = pl.ds(pl.multiple_of(number * tile, tile), tile)
        if transposed:
            store(columns, product_nt(left[...], right[columns, :]))
        else:
            store(columns, product(left[...], right[:, columns]))
        return carry

    lax.fori_loop(0, total // tile, step, 0)


def transposed_product(left, right, out):
    tall = 512 if out.shape[0] % 512 == 0 else 384
    wide = next(size for size in (512, 384, 640, 128) if out.shape[1] % size == 0)
    across = out.shape[1] // wide

    def step(number, carry):
        rows = pl.ds(pl.multiple_of((number // across) * tall, tall), tall)
        columns = pl.ds(pl.multiple_of(lax.rem(number, across) * wide, wide), wide)
        out[rows, columns] = product_tn(left[:, rows], right[:, columns]).astype(out.dtype)
        return carry

    lax.fori_loop(0, (out.shape[0] // tall) * across, step, 0)


def line():
    shards, place = lax.axis_size("wshard"), lax.axis_index("wshard")
    chips = shards // 2
    chip, core = place // 2, lax.rem(place, 2)
    forth = {"wshard": lax.rem(place + 2, shards)}
    back = {"wshard": lax.rem(place + shards - 2, shards)}
    twin = {"wshard": place + 1 - 2 * core}
    return chips, chip, core, forth, back, twin


class LineGather:
    @staticmethod
    def scratch(chips):
        dma = pltpu.SemaphoreType.DMA
        return [dma((3, chips)), dma((2 * chips,)), dma((1,))]

    def __init__(self, own, full, send, recv, local):
        self.own, self.full, self.local = own, full, local.at[0]
        self.sends = (send.at[0], send.at[1], send.at[2])
        self.recv = recv
        self.rows = own.shape[0]
        self.chips, self.chip, self.core, *self.devices = line()

    def place(self, chip, core):
        return self.full.at[pl.ds(pl.multiple_of((2 * chip + core) * self.rows, self.rows), self.rows)]

    def copy(self, way, chip, source=None):
        target = self.place(chip, self.core)
        return pltpu.make_async_remote_copy(
            src_ref=target if source is None else source,
            dst_ref=target,
            send_sem=self.sends[way].at[chip],
            recv_sem=self.recv.at[2 * chip + self.core],
            device_id=self.devices[way],
            device_id_type=MESH,
        )

    def wait_for(self, chip, core):
        target = self.place(chip, core)
        pltpu.make_async_remote_copy(
            src_ref=target,
            dst_ref=target,
            send_sem=self.sends[2].at[0],
            recv_sem=self.recv.at[2 * chip + core],
            device_id=self.devices[2],
            device_id_type=MESH,
        ).wait_recv()

    def start(self):
        @pl.when(self.chip < self.chips - 1)
        def _():
            self.copy(0, self.chip, self.own).start()

        @pl.when(self.chip > 0)
        def _():
            self.copy(1, self.chip, self.own).start()

        self.copy(2, self.chip, self.own).start()
        self.keep().start()

    def keep(self):
        return pltpu.make_async_copy(self.own, self.place(self.chip, self.core), self.local)

    def step(self, number):
        left, right = self.chip - number, self.chip + number

        @pl.when(left >= 0)
        def _():
            self.wait_for(left, self.core)

            @pl.when(self.chip < self.chips - 1)
            def _():
                self.copy(0, left).start()

            self.copy(2, left).start()

        @pl.when(right < self.chips)
        def _():
            self.wait_for(right, self.core)

            @pl.when(self.chip > 0)
            def _():
                self.copy(1, right).start()

            self.copy(2, right).start()

    def finish(self):
        for chip in range(self.chips):
            self.wait_for(chip, 1 - self.core)
            self.copy(2, chip).wait_send()

            @pl.when((chip <= self.chip) & (self.chip < self.chips - 1))
            def _():
                self.copy(0, chip).wait_send()

            @pl.when((chip >= self.chip) & (self.chip > 0))
            def _():
                self.copy(1, chip).wait_send()

        self.keep().wait()


class PartExchange:
    @staticmethod
    def scratch():
        dma = pltpu.SemaphoreType.DMA
        return [dma((4,)), dma((4,)), dma((1,))]

    def __init__(self, parts, out, send, recv, local):
        self.parts, self.out, self.send, self.recv, self.local = parts, out, send, recv, local
        self.rank = lax.axis_index("seq")
        self.core, self.twin = line()[2], line()[5]
        self.others = [{"seq": lax.rem(self.rank + k, 4)} for k in range(1, 4)]
        self.rows = out.shape[2]

    def part(self, rank):
        return self.parts.at[pl.ds(pl.multiple_of((2 * rank + self.core) * self.rows, self.rows), self.rows)]

    def copy(self, index):
        if index == 3:
            source = target = self.out.at[self.core]
        else:
            source = self.part(lax.rem(self.rank + index + 1, 4))
            target = self.out.at[self.core, self.rank]
        return pltpu.make_async_remote_copy(
            src_ref=source,
            dst_ref=target,
            send_sem=self.send.at[index],
            recv_sem=self.recv.at[index],
            device_id=self.twin if index == 3 else self.others[index],
            device_id_type=MESH,
        )

    def keep(self):
        return pltpu.make_async_copy(self.part(self.rank), self.out.at[self.core, self.rank], self.local.at[0])

    def start(self):
        for index in (1, 0, 2):
            self.copy(index).start()
        self.keep().start()

    def relay(self):
        for index in range(3):
            self.copy(index).wait()
        self.keep().wait()
        self.copy(3).start()

    def end(self):
        self.copy(3).wait()


class Regroup:
    @staticmethod
    def scratch(rows, width):
        dma = pltpu.SemaphoreType.DMA
        return [pltpu.VMEM((4, rows, width), jnp.bfloat16), dma((7,)), dma((7,))]

    def __init__(self, piece, out, fours, send, recv):
        self.piece, self.out, self.fours, self.send, self.recv = piece, out, fours, send, recv
        self.rank, self.place = lax.axis_index("seq"), lax.axis_index("wshard")
        self.number = lax.rem(self.place, 4)
        self.others = [{"seq": lax.rem(self.rank + k, 4)} for k in range(1, 4)]
        self.along = [{"wshard": lax.rem(self.place + k, 8)} for k in range(1, 8)]

    def near(self, index):
        return pltpu.make_async_remote_copy(
            src_ref=self.piece,
            dst_ref=self.fours.at[self.rank],
            send_sem=self.send.at[index],
            recv_sem=self.recv.at[index],
            device_id=self.others[index],
            device_id_type=MESH,
        )

    def owner(self, rank):
        return 2 * rank + self.place // 4

    def far(self, rank, number):
        return pltpu.make_async_remote_copy(
            src_ref=self.fours.at[rank],
            dst_ref=self.out.at[number],
            send_sem=self.send.at[3 + rank],
            recv_sem=self.recv.at[3 + number],
            device_id={"wshard": self.owner(rank)},
            device_id_type=MESH,
        )

    def start(self):
        for index in range(3):
            self.near(index).start()
        self.fours[self.rank] = self.piece[...]

    def relay(self):
        for index in range(3):
            self.near(index).wait()
        for rank in range(4):

            @pl.when(self.owner(rank) != self.place)
            def _():
                self.far(rank, self.number).start()

            @pl.when(self.owner(rank) == self.place)
            def _():
                self.out[self.number] = self.fours[rank]

    def end(self):
        for rank in range(4):

            @pl.when(self.owner(rank) != self.place)
            def _():
                self.far(rank, self.number).wait_send()

        for number in range(4):

            @pl.when(4 * lax.rem(self.place, 2) + number != self.place)
            def _():
                self.far(0, number).wait_recv()


class Everywhere:
    @staticmethod
    def scratch(shape):
        dma = pltpu.SemaphoreType.DMA
        return [
            pltpu.VMEM((4,) + shape, jnp.float32),
            pltpu.VMEM(shape, jnp.float32),
            pltpu.VMEM((8,) + shape, jnp.float32),
            dma((12,)),
            dma((12,)),
        ]

    def __init__(self, values, out, ranks, total, places, send, recv):
        self.values, self.out, self.ranks, self.total, self.places = values, out, ranks, total, places
        self.send, self.recv = send, recv
        self.groups, self.shards = ranks.shape[0], places.shape[0]
        self.rank, self.place = lax.axis_index("seq"), lax.axis_index("wshard")

    def others(self):
        return [{"seq": lax.rem(self.rank + k, self.groups)} for k in range(1, self.groups)]

    def along(self):
        return [{"wshard": lax.rem(self.place + k, self.shards)} for k in range(1, self.shards)]

    def start(self):
        self.first = [
            push(self.values, self.ranks.at[self.rank], self.send.at[k], self.recv.at[k], other)
            for k, other in enumerate(self.others())
        ]
        self.ranks[self.rank] = self.values[...]

    def relay(self):
        for copy in self.first:
            copy.wait()
        ranks, groups = self.ranks, self.groups
        self.total[...] = (ranks[0] + ranks[1]) + (ranks[2] + ranks[3])
        self.second = [
            push(self.total, self.places.at[self.place], self.send.at[groups + k], self.recv.at[groups + k], other)
            for k, other in enumerate(self.along())
        ]
        self.places[self.place] = self.total[...]

    def end(self):
        for copy in self.second:
            copy.wait()
        sums = [self.places[k] + self.places[k + 1] for k in range(0, self.shards, 2)]
        self.out[...] = (sums[0] + sums[1]) + (sums[2] + sums[3])


def join_shares(every, gate, every_gate, every_up, down, out, columns, starts, forget_at, heads, part):
    groups, rows, lanes = every.shape
    units = every_gate.shape[2]
    own = heads // groups
    steps = 4
    tall = rows // steps

    def body(every_ref, gate_ref, wide_gate, wide_up, down_in, out_in, *outs):
        firsts = len(starts)
        for group in range(groups):
            to = slice(group * columns, (group + 1) * columns)
            for start, result in zip(starts, outs):
                result[:, to] = every_ref[group, :, start : start + columns].astype(jnp.float32)
            outs[firsts][:, to] = gate_ref[group].astype(jnp.float32)
            outs[firsts + 1][:, group * own : (group + 1) * own] = every_ref[
                group, :, forget_at : forget_at + own
            ].astype(jnp.float32)
            for source, result in ((wide_gate, outs[firsts + 2]), (wide_up, outs[firsts + 3])):
                for block in range(units // part):
                    at = (block * groups + group) * part
                    result[:, at : at + part] = source[group, :, block * part : (block + 1) * part].astype(
                        jnp.float32
                    )
        outs[firsts + 4][...] = down_in[...].astype(jnp.float32)
        outs[firsts + 5][...] = out_in[...].astype(jnp.float32)

    def flat(value):
        return pl.BlockSpec((value.shape[0] // steps, value.shape[1]), lambda i: (i, 0))

    def ranks(value):
        return pl.BlockSpec((groups, tall, value.shape[2]), lambda i: (0, i, 0))

    def shape(size):
        return jax.ShapeDtypeStruct(size, jnp.float32)

    results = [shape((rows, groups * columns))] * (len(starts) + 1) + [
        shape((rows, heads)),
        shape((rows, groups * units)),
        shape((rows, groups * units)),
        shape(down.shape),
        shape(out.shape),
    ]
    return pl.pallas_call(
        body,
        grid=(steps,),
        in_specs=[ranks(v) for v in (every, gate, every_gate, every_up)] + [flat(down), flat(out)],
        out_specs=[flat(value) for value in results],
        out_shape=results,
        compiler_params=pltpu.CompilerParams(vmem_limit_bytes=56 << 20),
        name="join_shares",
    )(every, gate, every_gate, every_up, down, out)


def norm_rows(values, gain):
    scale = lax.rsqrt(jnp.mean(values * values, axis=-1, keepdims=True) + EPS)
    return scale, values * scale * gain


def whole_forward(inputs, gain, cotangent, weights, forget, bias, length, block, w_gate, w_up,
                  head_size, scale, collective_id):
    rows, depth = inputs.shape
    groups = 4
    slots = groups * rows
    chips = groups
    shards = 2 * chips
    mine = weights[0].shape[0]
    columns = depth // groups
    front = 3 * columns + PAIR
    pairs = columns // PAIR
    part = w_gate.shape[1] // (groups * shards)
    units = shards * part
    early = units + units // 2
    low = jnp.bfloat16

    def body(inputs_ref, gain_ref, cot_ref, q_ref, k_ref, v_ref, og_ref, forget_ref, bias_ref, length_ref, block_ref,
             gate_ref, up_ref,
             normed_hbm, cot_full, full_front_hbm, full_gate_hbm, full_out_hbm, full_ffn, joined_hbm, attended_hbm,
             offset, col, logit, gate_pre_hbm, gated_hbm, middle, own_up,
             own_normed, own_front, own_gate, own_ffn, own_out, parts_out, own_cot, row, picks, cot_send, cot_recv, keep,
             x_send, x_recv, normed, full_front, full_gate, full_out, joined, attended, gate_pre, gated, store_sems,
             *scratch):
        store = Streams(store_sems)
        me, side, down, across = sides()
        line_chips, chip, core, forth, back, twin = line()
        halves = (pl.ds(0, 2 * columns), pl.ds(2 * columns, front - 2 * columns))
        first_line = LineGather(own_front.at[:, halves[0]], full_front.at[:, halves[0]], *scratch[0:3])
        second_line = LineGather(own_front.at[:, halves[1]], full_front.at[:, halves[1]], *scratch[22:25])
        gate_line = LineGather(own_gate, full_gate, *scratch[3:6])
        ffn_line = LineGather(own_ffn, full_ffn, *scratch[6:9])
        out_line = LineGather(own_out, parts_out, *scratch[9:12])
        exchange = PartExchange(parts_out, full_out, *scratch[12:15])
        job = SquareScatter([gated], [full_out_rows(full_out)], False, middle, *scratch[15:22])
        taken = []
        my_columns = pl.ds(pl.multiple_of(me * columns, columns), columns)
        for index, source in enumerate((q_ref, k_ref, v_ref)):
            taken.append((source.at[:, my_columns], own_front.at[:, pl.ds(index * columns, columns)]))
        taken.append((og_ref.at[:, my_columns], own_gate))
        tall = own_out.shape[0]
        taken.append((block_ref.at[pl.ds(pl.multiple_of(me * tall, tall), tall)], own_out))
        for index, source in enumerate((gate_ref, up_ref)):
            for number in range(shards):
                column = pl.ds(pl.multiple_of((number * groups + me) * part, part), part)
                to = index * units + number * part
                target = own_ffn.at[:, pl.ds(to, part)] if to < early else own_up.at[:, pl.ds(to - early, part)]
                taken.append((source.at[:, column], target))
        taken = [pltpu.make_async_copy(a, b, picks.at[i]) for i, (a, b) in enumerate(taken)]
        for copy in taken:
            copy.start()
        values = inputs_ref[...].astype(jnp.float32)
        own_normed[...] = norm_rows(values, gain_ref[...])[1].astype(low)
        own_front[:, 3 * columns :] = forget_ref[...]
        positions = me * rows + lax.broadcasted_iota(jnp.int32, (rows, depth), 0)
        own_cot[...] = jnp.where(positions < length_ref[:, :1], cot_ref[...], jnp.zeros((), low))
        meet(*exchange.others, forth, back, twin)
        one = SquareGather(own_normed, normed, x_send, x_recv)
        two = SquareGather(own_cot, cot_full, cot_send, cot_recv)
        one.start()
        for copy in taken:
            copy.wait()
        first_line.start()
        second_line.start()
        at_me = pl.ds(pl.multiple_of(me * rows, rows), rows)
        kept = pltpu.make_async_copy(own_cot, cot_full.at[at_me], keep.at[0])
        kept.start()
        normed[at_me, :] = own_normed[...]
        one.relay()
        two.start()
        first_line.step(1)
        second_line.step(1)
        first_line.step(2)
        second_line.step(2)
        one.near()
        one.far()
        first_line.step(3)
        second_line.step(3)
        store.start(normed, normed_hbm)
        out_line.start()
        gate_line.start()
        two.relay()
        first_line.finish()

        def product_of(columns_of_front):
            view = joined.at[:, columns_of_front]

            def store_joined(at_columns, value):
                view[:, at_columns] = value.astype(low)

            block_product(normed, full_front.at[:, columns_of_front], False, 256, store_joined)

        product_of(halves[0])
        second_line.finish()
        product_of(halves[1])
        store.start(full_front, full_front_hbm)
        one.finish()
        store.start(joined, joined_hbm)
        work = Forward(joined, bias_ref, length_ref, attended, offset, col, logit, row, head_size, scale)
        offset[...] = jnp.zeros_like(offset)
        out_line.step(1)
        gate_line.step(1)
        work.start()

        def step(pair, carry):
            work.pair(pair)

            @pl.when(pair == 0)
            def _():
                out_line.step(2)
                gate_line.step(2)

            @pl.when(pair == 1)
            def _():
                out_line.step(3)
                out_line.finish()
                exchange.start()
                gate_line.step(3)
                ffn_line.start()

            return carry

        lax.fori_loop(0, pairs, step, 0)
        store.start(attended, attended_hbm)
        gate_line.finish()
        store.start(full_gate, full_gate_hbm)

        def store_gate(at_columns, value):
            gate_pre[:, at_columns] = value

        block_product(normed, full_gate, False, PAIR, store_gate)
        gated[...] = (attended[...].astype(jnp.float32) * jax.nn.sigmoid(gate_pre[...])).astype(low)
        exchange.relay()
        store.start(gate_pre, gate_pre_hbm)
        store.start(gated, gated_hbm)
        exchange.end()
        store.start(full_out, full_out_hbm)
        job.begin()
        ffn_line.step(1)
        job.relay()
        job.own()
        two.near()
        two.far()
        two.finish()
        kept.wait()
        ffn_line.step(2)
        job.end()
        middle[...] += inputs_ref[...].astype(jnp.float32)
        ffn_line.step(3)
        ffn_line.finish()
        store.end()

    def shape(size, kind=low):
        return jax.ShapeDtypeStruct(size, kind)

    vmem = pl.BlockSpec(memory_space=pltpu.VMEM)
    anywhere = pl.BlockSpec(memory_space=pl.ANY)
    dma = pltpu.SemaphoreType.DMA
    results = [
        shape((slots, depth)),
        shape((slots, depth)),
        shape((depth, front)),
        shape((depth, columns)),
        shape((2, 4, block.shape[0] // 4, depth)),
        shape((depth, early)),
        shape((slots, front)),
        *Forward.results(slots, pairs),
        shape((slots, columns), jnp.float32),
        shape((slots, columns)),
        shape((rows, depth), jnp.float32),
        shape((mine, 2 * units - early)),
    ]
    kept_here = [results[i] for i in (0, 2, 3, 4, 6, 7, 11, 12)]
    return pl.pallas_call(
        body,
        in_specs=[vmem] * 3 + [anywhere] * 4 + [vmem] * 3 + [anywhere] * 3,
        out_specs=[anywhere] * 8 + [vmem] * 3 + [anywhere] * 2 + [vmem] * 2,
        out_shape=results,
        scratch_shapes=[
            pltpu.VMEM((rows, depth), low),
            pltpu.VMEM((mine, front), low),
            pltpu.VMEM((mine, columns), low),
            pltpu.VMEM((mine, early), low),
            pltpu.VMEM((block.shape[0] // 4, depth), low),
            pltpu.VMEM((shards * block.shape[0] // 4, depth), low),
            pltpu.VMEM((rows, depth), low),
            pltpu.VMEM((Forward.some, slots), jnp.float32),
            dma((5 + 2 * shards,)),
            dma((6,)),
            dma((6,)),
            dma((1,)),
            dma((6,)),
            dma((6,)),
            *(pltpu.VMEM(value.shape, value.dtype) for value in kept_here),
            dma((len(kept_here),)),
        ]
        + 4 * LineGather.scratch(chips)
        + PartExchange.scratch()
        + SquareScatter.scratch(rows, depth)
        + LineGather.scratch(chips),
        compiler_params=pltpu.CompilerParams(
            collective_id=collective_id, has_side_effects=True, vmem_limit_bytes=VMEM_LIMIT
        ),
        name="whole_forward",
    )(inputs, gain, cotangent, *weights, forget, bias, length, block, w_gate, w_up)


class full_out_rows:
    def __init__(self, ref):
        self.ref = ref
        self.shape = (ref.shape[0] * ref.shape[1] * ref.shape[2], ref.shape[3])

    def __getitem__(self, index):
        taken = self.ref[:, :, :, index[1]]
        return taken.reshape(self.shape[0], taken.shape[3])


def feed_forward(middle, gain, weights, own_up, own_down, cotangent, collective_id):
    rows, depth = middle.shape
    slots = 4 * rows
    units = 4 * own_down.shape[0] * 2
    early = weights.shape[1]
    chips = 4
    low = jnp.bfloat16

    def body(middle_ref, gain_ref, weights_hbm, up_ref, down_ref, cot_hbm,
             normed_hbm, hidden_hbm, full_up_hbm, full_down_hbm, grads_hbm, terms_hbm,
             own_normed, both, send, recv,
             weights_ref, cot_ref, normed, hidden, full_up, full_down, grads, terms, fetch_sems, store_sems, *scratch):
        fetch, store = Streams(fetch_sems), Streams(store_sems)
        weights_in = fetch.start(weights_hbm, weights_ref)
        cot_in = fetch.start(cot_hbm, cot_ref)
        me, side, down, across = sides()
        line_chips, chip, core, forth, back, twin = line()
        up_line = LineGather(up_ref, full_up, *scratch[:3])
        down_line = LineGather(down_ref, full_down, *scratch[3:])
        own_normed[...] = norm_rows(middle_ref[...], gain_ref[...])[1].astype(low)
        meet({"seq": side}, {"seq": down}, forth, back, twin)
        job = SquareGather(own_normed, normed, send, recv)
        up_line.start()
        down_line.start()
        job.start()

        def rows_of(rank):
            return pl.ds(pl.multiple_of(rank * rows, rows), rows)

        def multiply(rank):
            at = rows_of(rank)

            def store(columns, value):
                both[at, columns] = value

            block_product(normed.at[at], weights_ref, False, 512, store)

        normed[rows_of(me), :] = own_normed[...]
        weights_in.wait()
        multiply(me)
        up_line.step(1)
        job.relay()
        down_line.step(1)
        up_line.step(2)
        job.near()
        multiply(side)
        up_line.step(3)
        multiply(down)
        job.far()
        store.start(normed, normed_hbm)
        down_line.step(2)
        multiply(across)
        job.finish()
        up_line.finish()
        store.start(full_up, full_up_hbm)

        def ahead(number, carry):
            at = rows_of(number)
            both[at, early:] = product(normed[at, :], full_up[...])
            gate, upward = both[at, :units], both[at, units:]
            hidden[at, :] = (gate * jax.nn.sigmoid(gate) * upward).astype(low)
            return carry

        lax.fori_loop(0, 4, ahead, 0)
        store.start(hidden, hidden_hbm)
        down_line.step(3)
        cot_in.wait()
        transposed_product(hidden, cot_ref, terms)
        store.start(terms, terms_hbm)
        down_line.finish()
        store.start(full_down, full_down_hbm)

        def behind(number, carry):
            at = rows_of(number)
            grad_hidden = product_nt(cot_ref[at, :], full_down[...])
            gate, upward = both[at, :units], both[at, units:]
            sigma = jax.nn.sigmoid(gate)
            grads[at, :units] = (grad_hidden * upward * sigma * (1.0 + gate * (1.0 - sigma))).astype(low)
            grads[at, units:] = (grad_hidden * gate * sigma).astype(low)
            part(number).start()
            return carry

        def part(number):
            at = rows_of(number)
            return pltpu.make_async_copy(grads.at[at], grads_hbm.at[at], store_sems.at[5 + number])

        lax.fori_loop(0, 4, behind, 0)
        for number in range(4):
            part(number).wait()
        store.end()

    def shape(size, kind=low):
        return jax.ShapeDtypeStruct(size, kind)

    vmem = pl.BlockSpec(memory_space=pltpu.VMEM)
    anywhere = pl.BlockSpec(memory_space=pl.ANY)
    dma = pltpu.SemaphoreType.DMA
    results = [
        shape((slots, depth)),
        shape((slots, units)),
        shape((depth, own_up.shape[1])),
        shape((units, depth)),
        shape((slots, 2 * units)),
        shape((units, depth)),
    ]
    return pl.pallas_call(
        body,
        in_specs=[vmem, vmem, anywhere, vmem, vmem, anywhere],
        out_specs=[anywhere] * 6,
        out_shape=results,
        scratch_shapes=[
            pltpu.VMEM((rows, depth), low),
            pltpu.VMEM((slots, 2 * units), jnp.float32),
            dma((6,)),
            dma((6,)),
            *(pltpu.VMEM(value.shape, value.dtype) for value in (weights, cotangent, *results)),
            dma((2,)),
            dma((9,)),
        ]
        + 2 * LineGather.scratch(chips),
        compiler_params=pltpu.CompilerParams(
            collective_id=collective_id, has_side_effects=True, vmem_limit_bytes=VMEM_LIMIT
        ),
        name="feed_forward",
    )(middle, gain, weights, own_up, own_down, cotangent)


def feed_backward(grads, weights, up_weights, normed, terms_down, w_out, middle, gain, cotangent, attended, gate_pre,
                  collective_id):
    rows, depth = middle.shape
    slots = 4 * rows
    units = grads.shape[1] // 2
    early = weights.shape[1]
    columns = attended.shape[1]
    shards = 2 * lax.axis_size("seq")
    chips = shards // 2
    low = jnp.bfloat16

    def body(grads_hbm, weights_hbm, up_weights_hbm, normed_hbm, down_hbm, out_hbm, middle_hbm, gain_ref, cot_hbm,
             attended_hbm, pre_hbm,
             grad_middle_hbm, grad_gain, branch_hbm, d_attended, d_pre, terms_up_hbm, share_down, share_gate,
             own_branch, summed, terms_gate, send, recv,
             grads_ref, weights_ref, up_weights_ref, normed_ref, down_ref, out_ref, middle_ref, cot_ref,
             attended_ref, pre_ref, grad_middle, branch, terms_up, fetch_sems, store_sems, *scratch):
        fetch, store = Streams(fetch_sems), Streams(store_sems)
        own_rows = pl.ds(pl.multiple_of(lax.axis_index("seq") * rows, rows), rows)
        first_in = [
            fetch.start(*both)
            for both in (
                (down_hbm, down_ref),
                (grads_hbm, grads_ref),
                (weights_hbm, weights_ref),
                (up_weights_hbm, up_weights_ref),
            )
        ]
        normed_in = fetch.start(normed_hbm, normed_ref)
        rest_in = [
            fetch.start(*both)
            for both in (
                (middle_hbm, middle_ref),
                (cot_hbm.at[own_rows], cot_ref),
                (out_hbm, out_ref),
                (attended_hbm, attended_ref),
                (pre_hbm, pre_ref),
            )
        ]
        me, side, down, across = sides()
        line_chips, chip, core, forth, back, twin = line()
        meet({"seq": side}, {"seq": down}, forth, back, twin)
        first, second = grads_ref.at[:, pl.ds(0, units)], grads_ref.at[:, pl.ds(units, units)]
        job = SquareScatter(
            [grads_ref.at[:, pl.ds(0, early)], grads_ref.at[:, pl.ds(early, 2 * units - early)]],
            [weights_ref, up_weights_ref],
            True,
            summed,
            *scratch[:7],
        )
        run_down = LineScatter(down_ref, share_down, *scratch[7:12])
        run_gate = LineScatter(terms_gate, share_gate, *scratch[12:])
        every = SquareGather(own_branch, branch, send, recv)
        first_in[0].wait()
        run_down.start()
        for copy in first_in[1:]:
            copy.wait()
        job.begin_far()
        run_down.slot(0)
        job.begin_near()
        normed_in.wait()
        transposed_product(normed_ref, first, terms_gate)
        run_gate.start()
        job.relay()
        run_down.slot(1)
        run_gate.slot(0)
        job.own()
        transposed_product(normed_ref, second, terms_up)
        store.start(terms_up, terms_up_hbm)
        run_down.slot(2)
        for copy in rest_in:
            copy.wait()
        job.end()
        values, change = middle_ref[...], summed[...]
        scale = norm_rows(values, gain_ref[...])[0]
        grad_gain[...] = jnp.sum(change * values * scale, axis=0, keepdims=True)
        change = change * gain_ref[...]
        mean = jnp.mean(change * values, axis=-1, keepdims=True)
        total = cot_ref[...].astype(jnp.float32) + scale * change - values * (scale * scale * scale * mean)
        grad_middle[...] = total
        own_branch[...] = total.astype(low)
        every.start()
        store.start(grad_middle, grad_middle_hbm)

        def rows_of(rank):
            return pl.ds(pl.multiple_of(rank * rows, rows), rows)

        def multiply(rank):
            at = rows_of(rank)
            grad_gated = product_nt(branch[at, :], out_ref[...])
            sigma = jax.nn.sigmoid(pre_ref[at, :])
            d_attended[at, :] = (grad_gated * sigma).astype(low)
            d_pre[at, :] = (
                grad_gated * attended_ref[at, :].astype(jnp.float32) * sigma * (1.0 - sigma)
            ).astype(low)

        branch[rows_of(me), :] = own_branch[...]
        multiply(me)
        run_gate.slot(1)
        every.relay()
        run_gate.slot(2)
        every.near()
        multiply(side)
        multiply(down)
        run_down.end()
        every.far()
        store.start(branch, branch_hbm)
        multiply(across)
        every.finish()
        run_gate.end()
        store.end()

    def shape(size, kind=low):
        return jax.ShapeDtypeStruct(size, kind)

    vmem = pl.BlockSpec(memory_space=pltpu.VMEM)
    anywhere = pl.BlockSpec(memory_space=pl.ANY)
    dma = pltpu.SemaphoreType.DMA
    own_shape = jax.ShapeDtypeStruct((rows, depth), low)
    fetched = (grads, weights, up_weights, normed, terms_down, w_out, middle, own_shape, attended, gate_pre)
    return pl.pallas_call(
        body,
        in_specs=[anywhere] * 7 + [vmem] + [anywhere] * 3,
        out_specs=[anywhere, vmem, anywhere, vmem, vmem, anywhere, vmem, vmem],
        out_shape=[
            shape((rows, depth), jnp.float32),
            shape((1, depth), jnp.float32),
            shape((slots, depth)),
            shape((slots, columns)),
            shape((slots, columns)),
            shape((depth, units)),
            shape((terms_down.shape[0] // shards, depth)),
            shape((depth // shards, units)),
        ],
        scratch_shapes=[
            pltpu.VMEM((rows, depth), low),
            pltpu.VMEM((rows, depth), jnp.float32),
            pltpu.VMEM((depth, units), low),
            dma((6,)),
            dma((6,)),
            *(pltpu.VMEM(value.shape, value.dtype) for value in fetched),
            pltpu.VMEM((rows, depth), jnp.float32),
            pltpu.VMEM((slots, depth), low),
            pltpu.VMEM((depth, units), low),
            dma((len(fetched),)),
            dma((3,)),
        ]
        + SquareScatter.scratch(rows, depth)
        + LineScatter.scratch(chips, terms_down.shape[0] // shards, depth)
        + LineScatter.scratch(chips, depth // shards, units),
        compiler_params=pltpu.CompilerParams(
            collective_id=collective_id, has_side_effects=True, vmem_limit_bytes=VMEM_LIMIT
        ),
        name="feed_backward",
    )(grads, weights, up_weights, normed, terms_down, w_out, middle, gain, cotangent, attended, gate_pre)


class SquareScatter:
    @staticmethod
    def scratch(rows, width):
        half = rows // 2
        low = jnp.bfloat16
        return [
            pltpu.VMEM((rows, width), low),
            pltpu.VMEM((2, half, width), low),
            pltpu.VMEM((2, half, width), jnp.float32),
            pltpu.VMEM((6, half, width), low),
            pltpu.VMEM((2, half, width), low),
            pltpu.SemaphoreType.DMA((6,)),
            pltpu.SemaphoreType.DMA((6,)),
        ]

    def __init__(self, lefts, rights, transposed, out, far, near, kept, land, carry, send, recv):
        self.lefts, self.rights, self.transposed, self.out = lefts, rights, transposed, out
        self.far, self.near, self.kept, self.land, self.carry = far, near, kept, land, carry
        self.send, self.recv = send, recv
        self.rows, self.width = out.shape
        self.half = self.rows // 2
        self.tile = self.width // 3 if self.width % 384 == 0 else self.width

    def copy(self, index):
        me, side, down, across = sides()
        source = (
            self.far.at[pl.ds(0, self.half)],
            self.far.at[pl.ds(self.half, self.half)],
            self.near.at[0],
            self.near.at[1],
            self.carry.at[0],
            self.carry.at[1],
        )[index]
        return pltpu.make_async_remote_copy(
            src_ref=source,
            dst_ref=self.land.at[index],
            send_sem=self.send.at[index],
            recv_sem=self.recv.at[index],
            device_id={"seq": down if index in (0, 3, 5) else side},
            device_id_type=MESH,
        )

    def partial(self, rank, store):
        at = pl.ds(pl.multiple_of(rank * self.rows, self.rows), self.rows)

        def step(number, carried):
            columns = pl.ds(pl.multiple_of(number * self.tile, self.tile), self.tile)
            value = None
            for a, b in zip(self.lefts, self.rights):
                if self.transposed:
                    term = product_nt(a[at, :], b[columns, :])
                else:
                    term = product(a[at, :], b[:, columns])
                value = term if value is None else value + term
            store(columns, value)
            return carried

        lax.fori_loop(0, self.width // self.tile, step, 0)

    def begin(self):
        self.begin_far()
        self.begin_near()

    def begin_far(self):
        me, side, down, across = sides()
        far = self.far

        def store_far(columns, value):
            far[:, columns] = value.astype(far.dtype)

        self.partial(across, store_far)
        self.copy(0).start()
        self.copy(1).start()

    def begin_near(self):
        me, side, down, across = sides()
        half, near, kept = self.half, self.near, self.kept

        def store_side(columns, value):
            kept[0, :, columns] = value[:half]
            near[0, :, columns] = value[half:].astype(near.dtype)

        def store_down(columns, value):
            near[1, :, columns] = value[:half].astype(near.dtype)
            kept[1, :, columns] = value[half:]

        self.partial(side, store_side)
        self.copy(2).start()
        self.partial(down, store_down)
        self.copy(3).start()

    def relay(self):
        for index in (0, 1):
            self.copy(index).wait_recv()

            def add(at, index=index):
                total = self.kept[index, at, :] + self.land[index, at, :].astype(jnp.float32)
                self.carry[index, at, :] = total.astype(self.carry.dtype)

            by_rows(self.half, add)
            self.copy(4 + index).start()

    def own(self):
        out = self.out

        def store_own(columns, value):
            out[:, columns] = value

        self.partial(lax.axis_index("seq"), store_own)

    def end(self):
        for index in (2, 3, 4, 5):
            self.copy(index).wait_recv()
        land, half, out = self.land, self.half, self.out

        def add(at):
            out[at, :] += land[3, at, :].astype(jnp.float32) + land[4, at, :].astype(jnp.float32)

        def add_second(at):
            to = pl.ds(at.start + half, at.size)
            out[to, :] += land[2, at, :].astype(jnp.float32) + land[5, at, :].astype(jnp.float32)

        by_rows(half, add)
        by_rows(half, add_second)
        for index in range(6):
            self.copy(index).wait_send()


class LineScatter:
    @staticmethod
    def scratch(chips, rows, width):
        low = jnp.bfloat16
        dma = pltpu.SemaphoreType.DMA
        return [pltpu.VMEM((chips, rows, width), low)] * 3 + [dma((2, chips)), dma((3, chips))]

    def __init__(self, terms, out, twin_in, forth_in, back_in, send, recv):
        self.terms, self.out, self.twin_in = terms, out, twin_in
        self.forth_in, self.back_in, self.send, self.recv = forth_in, back_in, send, recv
        self.chips, self.chip, self.core, *self.devices = line()
        self.rows = twin_in.shape[1]

    def term(self, chip, core):
        return self.terms.at[pl.ds(pl.multiple_of((2 * chip + core) * self.rows, self.rows), self.rows)]

    def swap(self, chip):
        return pltpu.make_async_remote_copy(
            src_ref=self.term(chip, 1 - self.core),
            dst_ref=self.twin_in.at[chip],
            send_sem=self.send.at[0, chip],
            recv_sem=self.recv.at[0, chip],
            device_id=self.devices[2],
            device_id_type=MESH,
        )

    def hop(self, way, chip):
        return pltpu.make_async_remote_copy(
            src_ref=self.twin_in.at[chip],
            dst_ref=(self.forth_in, self.back_in)[way].at[chip],
            send_sem=self.send.at[1, chip],
            recv_sem=self.recv.at[1 + way, chip],
            device_id=self.devices[way],
            device_id_type=MESH,
        )

    def start(self):
        for chip in (self.chips - 1, 0, *range(1, self.chips - 1)):
            self.swap(chip).start()

    def add(self, chip, ways, out):
        def step(at):
            start = pl.multiple_of((2 * chip + self.core) * self.rows + at.start, at.size)
            total = self.terms[pl.ds(start, at.size), :].astype(jnp.float32)
            total = total + self.twin_in[chip, at, :].astype(jnp.float32)
            for way in ways:
                total = total + (self.forth_in, self.back_in)[way][chip, at, :].astype(jnp.float32)
            out[at, :] = total.astype(out.dtype)

        by_rows(self.rows, step)

    def pass_on(self, way, chip, first):
        self.swap(chip).wait_recv()
        if not first:
            self.hop(way, chip).wait_recv()
        self.add(chip, () if first else (way,), self.twin_in.at[chip])
        self.hop(way, chip).start()

    def slot(self, number):
        last = self.chips - 1
        for chip in range(self.chips):
            forth, back = number - (last - chip), last - (number - chip)
            if 0 <= forth < chip:

                @pl.when(self.chip == forth)
                def _():
                    self.pass_on(0, chip, forth == 0)

            if chip < back <= last:

                @pl.when(self.chip == back)
                def _():
                    self.pass_on(1, chip, back == last)

    def end(self):
        for chip in range(self.chips):

            @pl.when(self.chip == chip)
            def _():
                self.swap(chip).wait_recv()
                ways = [way for way, there in enumerate((chip > 0, chip < self.chips - 1)) if there]
                for way in ways:
                    self.hop(way, chip).wait_recv()
                self.add(chip, ways, self.out)

            self.swap(chip).wait_send()

            @pl.when(self.chip != chip)
            def _():
                self.hop(0, chip).wait_send()


def middle_backward(joined, d_out, offset, col, logit, hidden, w_down, gated, grad_branch, terms_up, shares,
                    normed, d_pre, middle, head_size, scale, collective_id):
    slots, lanes = joined.shape
    width = w_down.shape[1]
    tokens = slots // 4
    columns = gated.shape[1]
    shards = 2 * lax.axis_size("seq")
    chips = shards // 2
    rows_up = terms_up.shape[0] // shards
    fetched = (terms_up, hidden, w_down, gated, grad_branch, normed, d_pre, joined, d_out, middle)

    def body(*refs):
        sources, refs = refs[:10], refs[10:]
        (offset_ref, col_ref, logit_ref, *share_refs), refs = refs[:5], refs[5:]
        (grads, bias_grad, layer_output, collected, share_up, share_pre, *every_refs), refs = refs[:8], refs[8:]
        buffers, refs = refs[:10], refs[10:]
        terms, terms_pre, lowered, send, recv, keep, fetch_sems, *scratch = refs
        up_ref, hidden_ref, down_ref, gated_ref, branch_ref, normed_ref, pre_ref, joined_ref, d_out_ref = buffers[:9]
        fetch = Streams(fetch_sems)
        comes = [fetch.start(source, buffer) for source, buffer in zip(sources, buffers)]
        me, side, down, across = sides()
        line_chips, chip, core, forth, back, twin = line()
        meet({"seq": side}, {"seq": down}, forth, back, twin)
        work = Backward(
            joined_ref, d_out_ref, offset_ref, col_ref, logit_ref, grads, *scratch[:4], head_size, scale
        )
        job = SquareScatter([hidden_ref], [down_ref], False, lowered, *scratch[4:11])
        collect = LineScatter(terms, collected, *scratch[11:16])
        run = LineScatter(up_ref, share_up, *scratch[16:21])
        run_pre = LineScatter(terms_pre, share_pre, *scratch[21:])
        every = [SquareGather(share_refs[i], every_refs[i], send.at[i], recv.at[i]) for i in range(2)]
        every[0].start()
        comes[0].wait()
        run.start()
        kept = []
        for i in range(2):
            size = share_refs[i].shape[0]
            kept.append(
                pltpu.make_async_copy(
                    share_refs[i],
                    every_refs[i].at[pl.ds(pl.multiple_of(me * size, size), size)],
                    keep.at[i],
                )
            )
            kept[i].start()
        comes[1].wait()
        comes[2].wait()
        job.begin_far()
        run.slot(0)
        job.begin_near()
        comes[3].wait()
        comes[4].wait()
        transposed_product(gated_ref, branch_ref, terms)
        collect.start()
        comes[5].wait()
        comes[6].wait()
        transposed_product(normed_ref, pre_ref, terms_pre)
        run_pre.start()
        collect.slot(0)
        for copy in comes[7:]:
            copy.wait()
        run_pre.slot(0)
        run.slot(1)
        work.start()

        def step(pair, carry):
            work.pair(pair)

            @pl.when(pair == 0)
            def _():
                job.relay()
                every[0].relay()
                every[1].start()
                collect.slot(1)
                run_pre.slot(1)
                run.slot(2)

            @pl.when(pair == 1)
            def _():
                collect.slot(2)
                run_pre.slot(2)
                every[1].relay()

            return carry

        lax.fori_loop(0, work.pairs, step, 0)
        job.own()
        work.end(bias_grad)
        job.end()
        layer_output[...] = (buffers[9][...] + lowered[...]).astype(layer_output.dtype)
        run.end()
        collect.end()
        run_pre.end()
        for gathering, copy in zip(every, kept):
            gathering.near()
            gathering.far()
            gathering.finish()
            copy.wait()

    vmem = pl.BlockSpec(memory_space=pltpu.VMEM)
    anywhere = pl.BlockSpec(memory_space=pl.ANY)
    low = jnp.bfloat16
    dma = pltpu.SemaphoreType.DMA
    return pl.pallas_call(
        body,
        in_specs=[anywhere] * 10 + [vmem] * 5,
        out_specs=[vmem] * 6 + [anywhere] * 2,
        out_shape=[
            jax.ShapeDtypeStruct((slots, lanes), low),
            jax.ShapeDtypeStruct((8, PAIR), jnp.float32),
            jax.ShapeDtypeStruct((tokens, width), low),
            jax.ShapeDtypeStruct((columns // shards, width), low),
            jax.ShapeDtypeStruct((rows_up, terms_up.shape[1]), low),
            jax.ShapeDtypeStruct((rows_up, columns), low),
            *(jax.ShapeDtypeStruct((4 * v.shape[0], v.shape[1]), low) for v in shares),
        ],
        scratch_shapes=[
            *(pltpu.VMEM(value.shape, value.dtype) for value in fetched),
            pltpu.VMEM((columns, width), low),
            pltpu.VMEM((width, columns), low),
            pltpu.VMEM((tokens, width), jnp.float32),
            dma((2, 6)),
            dma((2, 6)),
            dma((2,)),
            dma((10,)),
        ]
        + backward_scratch(slots)
        + SquareScatter.scratch(tokens, width)
        + LineScatter.scratch(chips, columns // shards, width)
        + LineScatter.scratch(chips, rows_up, terms_up.shape[1])
        + LineScatter.scratch(chips, rows_up, columns),
        compiler_params=pltpu.CompilerParams(
            collective_id=collective_id, has_side_effects=True, vmem_limit_bytes=VMEM_LIMIT
        ),
        name="middle_backward",
    )(*fetched, offset, col, logit, *shares)


def last_backward(grads, d_pre, normed, weights, gate_weights, collected, shares, inputs, gain, grad_middle,
                  small, collective_id):
    slots, depth = normed.shape
    front = grads.shape[1]
    tokens = slots // 4
    shards = 2 * lax.axis_size("seq")
    rows = depth // shards
    fetched = (normed, grads, d_pre, weights, gate_weights, inputs, grad_middle)

    def body(*refs):
        sources, refs = refs[:7], refs[7:]
        (collected_ref, gain_ref, small_ref, *share_refs), refs = refs[:5], refs[5:]
        (grad_input, small_out, regrouped, *every_refs), refs = refs[:6], refs[6:]
        buffers, refs = refs[:7], refs[7:]
        terms, summed, share, small_own, send, recv, keep, fetch_sems, *scratch = refs
        normed_ref, grads_ref, pre_ref, weights_ref, gate_weights_ref, inputs_ref, middle_ref = buffers
        fetch = Streams(fetch_sems)
        comes = [fetch.start(source, buffer) for source, buffer in zip(sources, buffers)]
        me, side, down, across = sides()
        regroup = Regroup(collected_ref, regrouped, *scratch[12:15])
        total = Everywhere(small_own, small_out, *scratch[20:])
        meet(*regroup.others, *regroup.along)
        job = SquareScatter([grads_ref, pre_ref], [weights_ref, gate_weights_ref], True, summed, *scratch[:7])
        halves = (pl.ds(0, front // 2), pl.ds(front // 2, front // 2))
        runs = [
            LineScatter(terms.at[:, half], share.at[:, half], *scratch[at : at + 5])
            for half, at in zip(halves, (7, 15))
        ]
        regroup.start()
        every = [SquareGather(share_refs[i], every_refs[i], send.at[i], recv.at[i]) for i in range(2)]
        every[0].start()
        every[1].start()
        kept = []
        for i in range(2):
            size = share_refs[i].shape[0]
            kept.append(
                pltpu.make_async_copy(
                    share_refs[i],
                    every_refs[i].at[pl.ds(pl.multiple_of(me * size, size), size)],
                    keep.at[i],
                )
            )
            kept[i].start()
        comes[0].wait()
        comes[1].wait()
        for half, run in zip(halves, runs):
            transposed_product(normed_ref, grads_ref.at[:, half], terms.at[:, half])
            run.start()
        runs[0].slot(0)
        for copy in comes[2:]:
            copy.wait()
        job.begin_far()
        runs[1].slot(0)
        regroup.relay()
        runs[0].slot(1)
        job.begin_near()
        runs[1].slot(1)
        every[0].relay()
        job.relay()
        runs[0].slot(2)
        every[1].relay()
        runs[1].slot(2)
        job.own()
        job.end()
        values, change = inputs_ref[...].astype(jnp.float32), summed[...]
        scale = norm_rows(values, gain_ref[...])[0]
        small_own[...] = small_ref[...]
        small_own[:, :depth] = jnp.sum(change * values * scale, axis=0, keepdims=True)
        total.start()
        change = change * gain_ref[...]
        mean = jnp.mean(change * values, axis=-1, keepdims=True)
        grad_input[...] = middle_ref[...] + scale * change - values * (scale * scale * scale * mean)
        for run in runs:
            run.end()
        every.append(SquareGather(share, every_refs[2], send.at[2], recv.at[2]))
        every[2].start()
        size = share.shape[0]
        kept.append(
            pltpu.make_async_copy(
                share, every_refs[2].at[pl.ds(pl.multiple_of(me * size, size), size)], keep.at[2]
            )
        )
        kept[2].start()
        total.relay()
        every[2].relay()
        regroup.end()
        total.end()
        for gathering, copy in zip(every, kept):
            gathering.near()
            gathering.far()
            gathering.finish()
            copy.wait()

    vmem = pl.BlockSpec(memory_space=pltpu.VMEM)
    anywhere = pl.BlockSpec(memory_space=pl.ANY)
    low = jnp.bfloat16
    dma = pltpu.SemaphoreType.DMA
    return pl.pallas_call(
        body,
        in_specs=[anywhere] * 7 + [vmem] * 5,
        out_specs=[vmem] * 3 + [anywhere] * 3,
        out_shape=[
            jax.ShapeDtypeStruct((tokens, depth), jnp.float32),
            jax.ShapeDtypeStruct(small.shape, jnp.float32),
            jax.ShapeDtypeStruct((4,) + collected.shape, low),
            *(jax.ShapeDtypeStruct((4 * v.shape[0], v.shape[1]), low) for v in shares),
            jax.ShapeDtypeStruct((4 * rows, front), low),
        ],
        scratch_shapes=[
            *(pltpu.VMEM(value.shape, value.dtype) for value in fetched),
            pltpu.VMEM((depth, front), low),
            pltpu.VMEM((tokens, depth), jnp.float32),
            pltpu.VMEM((rows, front), low),
            pltpu.VMEM(small.shape, jnp.float32),
            dma((3, 6)),
            dma((3, 6)),
            dma((3,)),
            dma((7,)),
        ]
        + SquareScatter.scratch(tokens, depth)
        + LineScatter.scratch(shards // 2, rows, front // 2)
        + Regroup.scratch(*collected.shape)
        + LineScatter.scratch(shards // 2, rows, front // 2)
        + Everywhere.scratch(small.shape),
        compiler_params=pltpu.CompilerParams(
            collective_id=collective_id, has_side_effects=True, vmem_limit_bytes=VMEM_LIMIT
        ),
        name="last_backward",
    )(*fetched, collected, gain, small, *shares)


def gather(value, axis_name):
    return lax.all_gather(value, axis_name, axis=0, tiled=True)


def scatter(value, axis_name):
    return lax.psum_scatter(value, axis_name, scatter_dimension=0, tiled=True)


def on_device(
    layer_input,
    lengths,
    norm_attn,
    w_query,
    w_key,
    w_value,
    w_ogate,
    w_forget,
    forget_bias,
    w_out,
    norm_ffn,
    w_gate,
    w_up,
    w_down,
    output_grad,
):
    low = jnp.bfloat16
    tokens, width = layer_input.shape[1:]
    heads = forget_bias.shape[0]
    groups = lax.axis_size("seq")
    shards = lax.axis_size("wshard")
    fast = square(groups) and shards == 2 * groups
    local_heads = heads // groups
    head_size = width // heads
    columns = width // groups
    lanes = columns + -columns % PAIR
    front = 3 * lanes + PAIR
    slots = tokens * groups
    hidden_size = w_gate.shape[1]
    part = hidden_size // (groups * shards)
    units = shards * part
    scale = head_size ** (-0.5)
    length = lengths[0]
    seq_rank = lax.axis_index("seq")
    shard_rank = lax.axis_index("wshard")
    per_block = shards // groups
    positions = seq_rank * tokens + jnp.arange(tokens, dtype=jnp.int32)
    valid_slots = (positions < length)[:, None]
    inputs = layer_input[0].astype(jnp.float32)
    cotangent_low = jnp.where(valid_slots, output_grad[0], jnp.zeros((), low))
    cotangent = cotangent_low.astype(jnp.float32)

    def own_columns(weight, size):
        taken = lax.dynamic_slice_in_dim(weight, seq_rank * columns, columns, 1)
        return jnp.pad(taken, ((0, 0), (0, size - columns))) if size > columns else taken

    def own_units(weight):
        split = weight.reshape(weight.shape[0], shards, groups, part)
        mine = lax.dynamic_index_in_dim(split, seq_rank, 2, keepdims=False)
        return mine.reshape(weight.shape[0], units)

    def own_bias_grad(bias_rows):
        return lax.dynamic_update_slice_in_dim(
            jnp.zeros((heads,), jnp.float32), bias_rows[:local_heads, 0], seq_rank * local_heads, 0
        )

    own_forget = lax.dynamic_slice_in_dim(w_forget, seq_rank * local_heads, local_heads, 1)
    own_forget = jnp.pad(own_forget, ((0, 0), (0, PAIR - local_heads)))
    own_bias = lax.dynamic_slice_in_dim(forget_bias, seq_rank * local_heads, local_heads)
    own_bias = jnp.pad(own_bias, (0, PAIR - local_heads))[None]
    length_row = jnp.broadcast_to(lengths[:, None], (1, PAIR))
    mine_down = lax.dynamic_slice_in_dim(w_down, seq_rank * part, part, 0)
    if fast:
        (
            normed_attn, cotangent_all, full_front, full_ogate, full_out, full_ffn,
            joined, attended_low, offset, col, logit, gate_pre, gated, middle, mine_up,
        ) = whole_forward(
            layer_input[0], norm_attn[None], output_grad[0], (w_query, w_key, w_value, w_ogate), own_forget,
            own_bias, length_row, w_out, w_gate, w_up, head_size, scale, 0,
        )
        full_out = full_out.reshape(columns, width)
        normed_ffn, hidden, full_up, full_down, grad_gate_up, terms_down = feed_forward(
            middle, norm_ffn[None], full_ffn, mine_up, mine_down, cotangent_all, 1
        )
        (
            grad_middle, grad_norm_ffn, grad_branch, grad_attended, grad_gate_pre, terms_up, share_down, share_gate,
        ) = feed_backward(
            grad_gate_up, full_ffn, full_up, normed_ffn, terms_down, full_out, middle, norm_ffn[None],
            cotangent_all, attended_low, gate_pre, 2,
        )
        grad_norm_ffn = grad_norm_ffn[0]
        grads, bias_rows, layer_output, collected, share_up, share_ogate, grad_down, every_gate = middle_backward(
            joined, grad_attended, offset, col, logit, hidden, full_down, gated, grad_branch, terms_up,
            (share_down, share_gate), normed_attn, grad_gate_pre, middle, head_size, scale, 3,
        )
        vector = jnp.concatenate([jnp.zeros((width,), jnp.float32), grad_norm_ffn, own_bias_grad(bias_rows)])
        vector = jnp.pad(vector, (0, -vector.shape[0] % PAIR))[None]
        grad_input, vector, grad_out, every_ogate, every_up, every_attn = last_backward(
            grads, grad_gate_pre, normed_attn, full_front, full_ogate, collected, (share_ogate, share_up),
            layer_input[0], norm_attn[None], grad_middle, vector, 4,
        )
        small = vector[0, :width], vector[0, width : 2 * width], vector[0, 2 * width : 2 * width + heads]
        grad_out = grad_out.reshape(columns // per_block, width)
    else:
        mine_front = jnp.concatenate(
            [*(own_columns(w, lanes) for w in (w_query, w_key, w_value)), own_forget], axis=1
        )
        full_front = gather(mine_front, "wshard")
        full_ogate = gather(own_columns(w_ogate, columns), "wshard")
        normed_attn = gather(rms_norm(inputs, norm_attn).astype(low), "seq")
        cotangent_all = gather(cotangent_low, "seq")
        full_out = lax.dynamic_slice_in_dim(gather(w_out, "wshard"), seq_rank * columns, columns, 0)
        full_ffn = gather(jnp.concatenate([own_units(w_gate), own_units(w_up)], axis=1), "wshard")
        joined = product(normed_attn, full_front).astype(low)
        gate_pre = product(normed_attn, full_ogate)
        attended_low, offset, col, logit = attention_fwd(joined, own_bias, length_row, head_size, scale)
        attended = attended_low[:, :columns].astype(jnp.float32)
        gated_full, pull_gate = jax.vjp(gate_product, attended, gate_pre)
        gated = gated_full.astype(low)
        middle = inputs + scatter(product(gated, full_out).astype(low), "seq").astype(jnp.float32)
        normed_ffn_own, pull_ffn_norm = jax.vjp(rms_norm, middle, norm_ffn)
        full_down = gather(mine_down, "wshard")
        normed_ffn = gather(normed_ffn_own.astype(low), "seq")
        gate_up = product(normed_ffn, full_ffn)
        hidden_full, pull_swiglu = jax.vjp(swiglu, gate_up[:, :units], gate_up[:, units:])
        hidden = hidden_full.astype(low)
        grad_hidden = product_nt(cotangent_all, full_down)
        grad_gate_full, grad_up_full = pull_swiglu(grad_hidden)
        grad_gate_up = jnp.concatenate([grad_gate_full.astype(low), grad_up_full.astype(low)], axis=1)
        share_down = scatter(product_tn(hidden, cotangent_all).astype(low), "wshard")
        share_ffn = scatter(product_tn(normed_ffn, grad_gate_up).astype(low), "wshard")
        grad_normed_ffn = scatter(product_nt(grad_gate_up, full_ffn).astype(low), "seq").astype(jnp.float32)
        grad_middle_part, grad_norm_ffn = pull_ffn_norm(grad_normed_ffn)
        grad_middle = cotangent + grad_middle_part
        grad_branch = gather(grad_middle.astype(low), "seq")
        grad_attended_full, grad_gate_pre_full = pull_gate(product_nt(grad_branch, full_out))
        grad_attended = grad_attended_full.astype(low)
        grad_gate_pre = grad_gate_pre_full.astype(low)
        if lanes > columns:
            grad_attended = jnp.pad(grad_attended, ((0, 0), (0, lanes - columns)))
        grads, bias_rows = attention_bwd(joined, grad_attended, offset, col, logit, head_size, scale)
        grad_projected = jnp.concatenate([grads, grad_gate_pre], axis=1)
        share_attn = scatter(product_tn(normed_attn, grad_projected).astype(low), "wshard")
        full_attn = jnp.concatenate([full_front, full_ogate], axis=1)
        grad_normed_attn = scatter(product_nt(grad_projected, full_attn).astype(low), "seq").astype(jnp.float32)
        lowered = scatter(product(hidden, full_down).astype(low), "seq").astype(jnp.float32)
        share_out = scatter(product_tn(gated, grad_branch).astype(low), "wshard")
        rows_out = columns // shards
        pieces_out = lax.all_gather(share_out, "seq", axis=0, tiled=False)
        takes = shards // per_block
        slots_out = jnp.where(
            (jnp.arange(per_block) == shard_rank // takes)[None, :, None, None],
            pieces_out[:, None],
            jnp.zeros((), low),
        ).reshape(shards, rows_out, width)
        moved = lax.all_to_all(slots_out, "wshard", split_axis=0, concat_axis=0, tiled=True)
        moved = moved.reshape(per_block, takes, rows_out, width)
        mine_out = lax.dynamic_index_in_dim(moved, shard_rank % per_block, 0, keepdims=False)
        grad_out = mine_out.reshape(columns // per_block, width).astype(jnp.float32)
        layer_output = (middle + lowered).astype(low)
        unused_normed, pull_attn_norm = jax.vjp(rms_norm, inputs, norm_attn)
        grad_input_part, grad_norm_attn = pull_attn_norm(grad_normed_attn)
        grad_input = grad_middle + grad_input_part
    if not fast:
        every_attn, every_ffn, grad_down = [gather(v, "seq") for v in (share_attn, share_ffn, share_down)]
        small = lax.psum((grad_norm_attn, grad_norm_ffn, own_bias_grad(bias_rows)), ("seq", "wshard"))
    rows = width // shards
    every_attn = every_attn.reshape(groups, rows, every_attn.shape[1])
    if fast:
        *weight_grads, grad_forget_w, grad_w_gate, grad_w_up, grad_down, grad_out = join_shares(
            every_attn,
            every_ogate.reshape((groups,) + share_ogate.shape),
            every_gate.reshape((groups,) + share_gate.shape),
            every_up.reshape((groups,) + share_up.shape),
            grad_down,
            grad_out,
            columns,
            (0, lanes, 2 * lanes),
            3 * lanes,
            heads,
            part,
        )
    else:

        def join(first):
            taken = every_attn[:, :, first : first + columns]
            return taken.transpose(1, 0, 2).reshape(rows, width).astype(jnp.float32)

        def join_own_units(first):
            taken = every_ffn.reshape((groups,) + share_ffn.shape)[:, :, first * units : (first + 1) * units]
            taken = taken.reshape(groups, rows, shards, part).transpose(1, 2, 0, 3)
            return taken.reshape(rows, hidden_size).astype(jnp.float32)

        weight_grads = [join(first) for first in (0, lanes, 2 * lanes, front)]
        grad_w_gate, grad_w_up = join_own_units(0), join_own_units(1)
        grad_down = grad_down.astype(jnp.float32)
        grad_forget_w = every_attn[:, :, 3 * lanes : 3 * lanes + local_heads]
        grad_forget_w = grad_forget_w.transpose(1, 0, 2).reshape(rows, heads).astype(jnp.float32)
    return (
        layer_output[None],
        grad_input[None],
        small[0],
        *weight_grads,
        grad_forget_w,
        small[2],
        grad_out,
        small[1],
        grad_w_gate,
        grad_w_up,
        grad_down,
    )


def solution(mesh):
    return jax.shard_map(
        on_device,
        mesh=mesh,
        in_specs=(
            P("wshard", "seq", None),
            P("wshard"),
            P(),
            P("wshard", None),
            P("wshard", None),
            P("wshard", None),
            P("wshard", None),
            P("wshard", None),
            P(),
            P("wshard", None),
            P(),
            P("wshard", None),
            P("wshard", None),
            P("wshard", None),
            P("wshard", "seq", None),
        ),
        out_specs=(
            P("wshard", "seq", None),
            P("wshard", "seq", None),
            P(),
            P("wshard", None),
            P("wshard", None),
            P("wshard", None),
            P("wshard", None),
            P("wshard", None),
            P(),
            P("wshard", None),
            P(),
            P("wshard", None),
            P("wshard", None),
            P("wshard", None),
        ),
        check_vma=False,
    )
```
